32 devices in a mesh: dp: 8 (over y, x, core), seq: 4 (over z).
Axes of the slice: x: 2, y: 2, z: 4, core: 2. Of those that a mesh axis runs over, the one named last changes fastest.
Arguments:
- inputs: float32 [16, 768, 512], P('dp', 'seq'), may hold values from -6 to 6
- lengths: int32 [16], P('dp'), may hold values from 192 to 768, as said below
- rel_bucket: int32 [1535], replicated, may hold values from 0 to 31
- params: float32 [6059776], P(('dp', 'seq')), may hold values from -3 to 3, as said below
- moment_one: float32 [6059776], P(('dp', 'seq')), may hold values from -12288 to 12288
- moment_two: float32 [6059776], P(('dp', 'seq')), may hold values from 0 to 12288, as said below
- cotangent: float32 [16, 768, 512], P('dp', 'seq'), may hold values from -6 to 6
Outputs:
- block_output: float32 [16, 768, 512], P('dp', 'seq')
- input_grad: float32 [16, 768, 512], P('dp', 'seq')
- param_grad: float32 [6059776], P(('dp', 'seq'))
- new_params: float32 [6059776], P(('dp', 'seq'))
- new_moment_one: float32 [6059776], P(('dp', 'seq'))
- new_moment_two: float32 [6059776], P(('dp', 'seq'))
The draws below stay inside these ranges and needn't reach their ends.
Inputs may be any that keep to these rules, and one draw needn't show every extreme that they name: `lengths`: some sequence is 768 tokens long in every draw. `params`: norm and batch-norm gains lie in 0.5 to 1.5. `moment_two`: every entry is positive.
All inputs are finite; a program needn't handle non-finite values.
Results may differ from the reference program's by a relative error of at most 0.012.
Values may be sent and summed in bfloat16 or wider, within the bound.
A program may use at most 256 MiB of HBM per device.

```python
import math
import jax
import jax.numpy as jnp
from jax import lax

D = 512
H = 8
HD = 64
FF = 2048
K = 31
NB = 32
STEP = 4
LEN = 768
SEQS = 16
PARAMS = 6059776


def segments_drawn():

    def feed_block(prefix):
        return [(prefix + '_norm_gain', (D,)), (prefix + '_norm_bias', (D,)), (prefix + '_w_in', (D, FF)), (prefix + '_b_in', (FF,)), (prefix + '_w_out', (FF, D)), (prefix + '_b_out', (D,))]
    listing = feed_block('first')
    listing = listing + [('attn_norm_gain', (D,)), ('attn_norm_bias', (D,)), ('w_query', (D, D)), ('b_query', (D,)), ('w_key', (D, D)), ('w_value', (D, D)), ('b_value', (D,)), ('w_output', (D, D)), ('b_output', (D,)), ('rel_table', (NB, H))]
    listing = listing + [('conv_norm_gain', (D,)), ('conv_norm_bias', (D,)), ('w_point_in', (D, 2 * D)), ('b_point_in', (2 * D,)), ('w_depth', (K, D)), ('batch_gain', (D,)), ('batch_bias', (D,)), ('w_point_out', (D, D)), ('b_point_out', (D,))]
    listing = listing + feed_block('second') + [('final_gain', (D,)), ('final_bias', (D,))]
    return listing


def draw_params(key, part):
    pieces = []
    listing = segments_drawn()
    for number in range(len(listing)):
        entry_name, entry_shape = listing[number]
        subkey = jax.random.fold_in(key, number)
        if entry_name[-4:] == 'gain':
            segment = 1.0 + 0.5 * jax.random.uniform(subkey, entry_shape, jnp.float32, -1.0, 1.0)
        elif entry_name == 'rel_table':
            segment = jax.random.uniform(subkey, entry_shape, jnp.float32, -2.0, 2.0)
        elif len(entry_shape) == 2:
            factor = 4.0 if entry_name == 'w_output' else 1.0
            segment = factor * jax.random.truncated_normal(subkey, -3.0, 3.0, entry_shape, jnp.float32) / math.sqrt(entry_shape[0])
        else:
            segment = 0.3 * jax.random.truncated_normal(subkey, -3.0, 3.0, entry_shape, jnp.float32)
        pieces.append(segment.reshape(-1))
    used = sum((segment.shape[0] for segment in pieces))
    pieces.append(0.02 * jax.random.truncated_normal(jax.random.fold_in(key, 999), -3.0, 3.0, (PARAMS - used,), jnp.float32))
    return jnp.concatenate(pieces)


def grad_scales():
    base_size = 0.5 * math.sqrt(SEQS * LEN)
    pieces = []
    for entry_name, entry_shape in segments_drawn():
        factor = 0.03 if entry_name == 'rel_table' else 1.0
        pieces.append(jnp.full((math.prod(entry_shape),), base_size * factor, jnp.float32))
    used = sum((segment.shape[0] for segment in pieces))
    pieces.append(jnp.full((PARAMS - used,), 0.01, jnp.float32))
    return jnp.concatenate(pieces)


def draw_moment_one(key, part):
    noise = jax.random.truncated_normal(jax.random.fold_in(key, 11), -4.0, 4.0, (PARAMS,), jnp.float32)
    return 0.2 * grad_scales() * noise


def draw_moment_two(key, part):
    spread = jnp.exp(jax.random.uniform(jax.random.fold_in(key, 12), (PARAMS,), jnp.float32, 0.0, math.log(4.0)))
    sizes = grad_scales()
    return 0.02 / 0.98 * sizes * sizes * spread


def draw_lengths(key, part):
    drawn_lengths = jax.random.randint(key, (SEQS,), LEN // 4, LEN + 1)
    chosen = jax.random.randint(jax.random.fold_in(key, 1), (), 0, SEQS)
    return drawn_lengths.at[chosen].set(LEN)


def touch_ends(values, key, low, high):
    shape = values.shape
    spot = [jax.random.randint(jax.random.fold_in(key, axis), (), 0, shape[axis]) for axis in range(len(shape))]
    values = values.at[tuple(spot)].set(low)
    longest = shape.index(max(shape))
    spot[longest] = (spot[longest] + 1) % shape[longest]
    return values.at[tuple(spot)].set(high)


def level_of(rng, shape, split, low, largest):
    def one(position, shards_of):
        heights = jax.random.uniform(jax.random.fold_in(jax.random.fold_in(rng, 6), position), (shards_of,), jnp.float32, low / len(split), largest / len(split))
        return jnp.repeat(jnp.exp(heights), shape[position] // shards_of).reshape((-1,) + (1,) * (len(shape) - position - 1))

    factor_of = one(*split[0])
    for cut in split[1:]:
        factor_of = factor_of * one(*cut)
    return factor_of


def scatter_about(own_key, shape, width, bound, shards=(), kind=jnp.bfloat16):
    entries = jax.random.normal(own_key, shape, jnp.float32) * width
    if len(shards) > 0:
        entries = level_of(own_key, shape, shards, -0.22, 0.18) * entries
    return jnp.clip(entries, min=-bound, max=bound).astype(kind)


def setup_inputs(seed: int = 0) -> dict:
    seeds = jax.random.split(jax.random.key(seed), 8)
    return {
        "inputs": scatter_about(seeds[0], (SEQS, LEN, D), 1.0, 6.0, ((0, 8), (1, 4)), jnp.float32),
        "lengths": draw_lengths(jax.random.fold_in(seeds[7], 71), 0),
        "rel_bucket": touch_ends(jax.random.randint(seeds[2], (2 * LEN - 1,), 0, NB), jax.random.fold_in(seeds[2], 1), 0, NB - 1).astype(jnp.int32),
        "params": draw_params(jax.random.fold_in(seeds[7], 71), 0),
        "moment_one": draw_moment_one(jax.random.fold_in(seeds[7], 71), 0),
        "moment_two": draw_moment_two(jax.random.fold_in(seeds[7], 71), 0),
        "cotangent": scatter_about(seeds[6], (SEQS, LEN, D), 1.0, 6.0, ((0, 8), (1, 4)), jnp.float32),
    }


NORM_EPS = 1e-05
BATCH_EPS = 1e-05
LEARN_RATE = 0.005
DECAY = 0.01
BETA_ONE = 0.9
BETA_TWO = 0.98
ADAM_EPS = 1e-08

def segments():

    def feed_block(prefix):
        return [(prefix + '_norm_gain', (D,)), (prefix + '_norm_bias', (D,)), (prefix + '_w_in', (D, FF)), (prefix + '_b_in', (FF,)), (prefix + '_w_out', (FF, D)), (prefix + '_b_out', (D,))]
    listing = feed_block('first')
    listing = listing + [('attn_norm_gain', (D,)), ('attn_norm_bias', (D,)), ('w_query', (D, D)), ('b_query', (D,)), ('w_key', (D, D)), ('w_value', (D, D)), ('b_value', (D,)), ('w_output', (D, D)), ('b_output', (D,)), ('rel_table', (NB, H))]
    listing = listing + [('conv_norm_gain', (D,)), ('conv_norm_bias', (D,)), ('w_point_in', (D, 2 * D)), ('b_point_in', (2 * D,)), ('w_depth', (K, D)), ('batch_gain', (D,)), ('batch_bias', (D,)), ('w_point_out', (D, D)), ('b_point_out', (D,))]
    listing = listing + feed_block('second') + [('final_gain', (D,)), ('final_bias', (D,))]
    return listing

def unpack(flat_vec):
    result = {}
    offset = 0
    for entry_name, entry_shape in segments():
        extent = math.prod(entry_shape)
        result[entry_name] = flat_vec[offset:offset + extent].reshape(entry_shape)
        offset = offset + extent
    return result

def pack_flat(gradients, total_len):
    pieces = [gradients[listed[0]].reshape(-1).astype(jnp.float32) for listed in segments()]
    used = sum((segment.shape[0] for segment in pieces))
    pieces.append(jnp.zeros((total_len - used,), jnp.float32))
    return jnp.concatenate(pieces)

def zero_grads():
    return {listed[0]: jnp.zeros(listed[1], jnp.float32) for listed in segments()}

def add_into(running, partial_grads):
    result = dict(running)
    for entry_name in partial_grads:
        result[entry_name] = running[entry_name] + partial_grads[entry_name]
    return result

def vector(weights, entry_name):
    return weights[entry_name].astype(jnp.float32)

def swish_act(values):
    return values * jax.nn.sigmoid(values)

def swish_grad(values):
    sig_vals = jax.nn.sigmoid(values)
    return sig_vals * (1.0 + values * (1.0 - sig_vals))

def norm_rows(values, scale_vec, shift_vec):
    centre = values - lax.optimization_barrier(jnp.mean(values, -1, keepdims=True))
    spread = lax.optimization_barrier(jnp.mean(centre * centre, -1, keepdims=True))
    return centre * lax.rsqrt(spread + NORM_EPS) * scale_vec + shift_vec

def norm_back(values, scale_vec, shift_vec, grad_out):
    _, pullback = jax.vjp(norm_rows, values, scale_vec, shift_vec)
    return pullback(grad_out)

def forward_dot(left_mat, weight):
    return jnp.dot(left_mat, weight, preferred_element_type=jnp.float32)

def cross_dot(left_mat, right_mat):
    return lax.dot_general(left_mat, right_mat, (((0,), (0,)), ((), ())), preferred_element_type=jnp.float32)

def back_dot(grad_in, weight):
    return lax.dot_general(grad_in, weight, (((1,), (1,)), ((), ())), preferred_element_type=jnp.float32)

def mixed_einsum(form, left_mat, right_mat):
    return jnp.einsum(form, left_mat.astype(jnp.float32), right_mat.astype(jnp.float32), precision=lax.Precision.HIGHEST)

def ffn_forward(stream, weights, prefix):
    normed_b = norm_rows(stream, vector(weights, prefix + '_norm_gain'), vector(weights, prefix + '_norm_bias')).astype(jnp.bfloat16)
    hidden = forward_dot(normed_b, weights[prefix + '_w_in']) + vector(weights, prefix + '_b_in')
    active = swish_act(hidden).astype(jnp.bfloat16)
    output = stream + 0.5 * (forward_dot(active, weights[prefix + '_w_out']) + vector(weights, prefix + '_b_out'))
    return (output, (normed_b, hidden, active))

def ffn_backward(stream, weights, prefix, stored, grad_out):
    normed_b, hidden, active = stored
    half_grad = 0.5 * grad_out
    half_b = half_grad.astype(jnp.bfloat16)
    gradients = {prefix + '_w_out': cross_dot(active, half_b), prefix + '_b_out': lax.optimization_barrier(jnp.sum(half_grad, 0))}
    d_hidden = back_dot(half_b, weights[prefix + '_w_out']) * swish_grad(hidden)
    d_hidden_b = d_hidden.astype(jnp.bfloat16)
    gradients[prefix + '_w_in'] = cross_dot(normed_b, d_hidden_b)
    gradients[prefix + '_b_in'] = lax.optimization_barrier(jnp.sum(d_hidden, 0))
    d_normed = back_dot(d_hidden_b, weights[prefix + '_w_in'])
    d_stream, gain_grad, shift_grad = norm_back(stream, vector(weights, prefix + '_norm_gain'), vector(weights, prefix + '_norm_bias'), d_normed)
    gradients[prefix + '_norm_gain'] = gain_grad
    gradients[prefix + '_norm_bias'] = shift_grad
    return (grad_out + d_stream, gradients)

def masked_scores(queries4, keys4, pos_bias, valid_keys):
    scores = mixed_einsum('sqhd,skhd->shqk', queries4, keys4) / math.sqrt(HD) + pos_bias[None]
    return jnp.where(valid_keys[:, None, None, :], scores, -jnp.inf)

def attend_forward(stream, weights, valid_keys, pos_bias):
    normed_b = norm_rows(stream, vector(weights, 'attn_norm_gain'), vector(weights, 'attn_norm_bias')).astype(jnp.bfloat16)
    queries = (forward_dot(normed_b, weights['w_query']) + vector(weights, 'b_query')).astype(jnp.bfloat16)
    key_rows = forward_dot(normed_b, weights['w_key']).astype(jnp.bfloat16)
    values = (forward_dot(normed_b, weights['w_value']) + vector(weights, 'b_value')).astype(jnp.bfloat16)
    shape_four = (valid_keys.shape[0], -1, H, HD)
    queries4 = queries.reshape(shape_four)
    keys4 = key_rows.reshape(shape_four)
    values4 = values.reshape(shape_four)
    scores = masked_scores(queries4, keys4, pos_bias, valid_keys)
    row_max = lax.optimization_barrier(jnp.max(scores, -1, keepdims=True))
    log_total = row_max + jnp.log(lax.optimization_barrier(jnp.sum(jnp.exp(scores - row_max), -1, keepdims=True)))
    probs_b = jnp.exp(scores - log_total).astype(jnp.bfloat16)
    context = mixed_einsum('shqk,skhd->sqhd', probs_b, values4).astype(jnp.bfloat16).reshape(stream.shape)
    output = stream + forward_dot(context, weights['w_output']) + vector(weights, 'b_output')
    return (output, (normed_b, queries4, keys4, values4, log_total, context))

def project_back(stream, weights, normed_b, d_queries, d_keys, d_values, grad_out, gradients):
    query_grad = d_queries.reshape(stream.shape)
    key_grad = d_keys.reshape(stream.shape)
    value_grad = d_values.reshape(stream.shape)
    query_b = query_grad.astype(jnp.bfloat16)
    key_b = key_grad.astype(jnp.bfloat16)
    value_b = value_grad.astype(jnp.bfloat16)
    gradients['w_query'] = cross_dot(normed_b, query_b)
    gradients['b_query'] = lax.optimization_barrier(jnp.sum(query_grad, 0))
    gradients['w_key'] = cross_dot(normed_b, key_b)
    gradients['w_value'] = cross_dot(normed_b, value_b)
    gradients['b_value'] = lax.optimization_barrier(jnp.sum(value_grad, 0))
    d_normed = back_dot(query_b, weights['w_query']) + back_dot(key_b, weights['w_key']) + back_dot(value_b, weights['w_value'])
    d_stream, gain_grad, shift_grad = norm_back(stream, vector(weights, 'attn_norm_gain'), vector(weights, 'attn_norm_bias'), d_normed)
    gradients['attn_norm_gain'] = gain_grad
    gradients['attn_norm_bias'] = shift_grad
    return (grad_out + d_stream, gradients)

def attend_backward(stream, weights, stored, grad_out, valid_keys, pos_bias, bucket_ids):
    normed_b, queries4, keys4, values4, log_total, context = stored
    grad_b = grad_out.astype(jnp.bfloat16)
    gradients = {'w_output': cross_dot(context, grad_b), 'b_output': lax.optimization_barrier(jnp.sum(grad_out, 0))}
    d_context = back_dot(grad_b, weights['w_output']).astype(jnp.bfloat16).reshape(queries4.shape)
    attn_probs = jnp.exp(masked_scores(queries4, keys4, pos_bias, valid_keys) - log_total)
    probs_b = attn_probs.astype(jnp.bfloat16)
    d_probs = mixed_einsum('sqhd,skhd->shqk', d_context, values4)
    d_values = mixed_einsum('shqk,sqhd->skhd', probs_b, d_context)
    d_scores = attn_probs * (d_probs - lax.optimization_barrier(jnp.sum(attn_probs * d_probs, -1, keepdims=True)))
    d_scores_b = d_scores.astype(jnp.bfloat16)
    d_queries = mixed_einsum('shqk,skhd->sqhd', d_scores_b, keys4) / math.sqrt(HD)
    d_keys = mixed_einsum('shqk,sqhd->skhd', d_scores_b, queries4) / math.sqrt(HD)
    summed_heads = jnp.moveaxis(lax.optimization_barrier(jnp.sum(d_scores, 0)), 0, -1).reshape(-1, H)
    gradients['rel_table'] = jax.ops.segment_sum(summed_heads, bucket_ids.reshape(-1), num_segments=NB)
    return project_back(stream, weights, normed_b, d_queries, d_keys, d_values, grad_out, gradients)

def depthwise(padded, kernel):
    length = padded.shape[1] - kernel.shape[0] + 1
    summed = jnp.zeros((padded.shape[0], length, padded.shape[2]), jnp.float32)
    for offset in range(kernel.shape[0]):
        summed = summed + kernel[offset] * padded[:, offset:offset + length]
    return summed.reshape(-1, padded.shape[2])

def depth_back(padded, d_depth3, d_padded, kernel):
    length = d_depth3.shape[1]
    taps_count = kernel.shape[0]
    kernel_grad = jnp.stack([lax.optimization_barrier(jnp.sum(padded[:, offset:offset + length] * d_depth3, (0, 1))) for offset in range(taps_count)])
    d_gated = jnp.zeros(d_depth3.shape, jnp.float32)
    for offset in range(taps_count):
        start_at = taps_count - 1 - offset
        d_gated = d_gated + kernel[offset] * d_padded[:, start_at:start_at + length]
    return (kernel_grad, d_gated.reshape(-1, d_depth3.shape[2]))

def conv_front(stream, weights, valid_rows, seq_count):
    normed_b = norm_rows(stream, vector(weights, 'conv_norm_gain'), vector(weights, 'conv_norm_bias')).astype(jnp.bfloat16)
    pre_gate = forward_dot(normed_b, weights['w_point_in']) + vector(weights, 'b_point_in')
    gated = pre_gate[:, :D] * jax.nn.sigmoid(pre_gate[:, D:]) * valid_rows[:, None]
    padded = jnp.pad(gated.reshape(seq_count, -1, D), ((0, 0), (K // 2, K // 2), (0, 0)))
    depth = depthwise(padded, vector(weights, 'w_depth'))
    return (normed_b, pre_gate, padded, depth)

def conv_tail(stream, weights, depth, batch_mean, inv_std):
    standard = (depth - batch_mean) * inv_std
    normed_bn = standard * vector(weights, 'batch_gain') + vector(weights, 'batch_bias')
    active = swish_act(normed_bn).astype(jnp.bfloat16)
    output = stream + forward_dot(active, weights['w_point_out']) + vector(weights, 'b_point_out')
    return (output, (standard, normed_bn, active))

def conv_tail_back(weights, stored, grad_out, valid_rows):
    standard, normed_bn, active = stored
    grad_b = grad_out.astype(jnp.bfloat16)
    gradients = {'w_point_out': cross_dot(active, grad_b), 'b_point_out': lax.optimization_barrier(jnp.sum(grad_out, 0))}
    d_normed = back_dot(grad_b, weights['w_point_out']) * swish_grad(normed_bn)
    gradients['batch_gain'] = lax.optimization_barrier(jnp.sum(d_normed * standard, 0))
    gradients['batch_bias'] = lax.optimization_barrier(jnp.sum(d_normed, 0))
    d_standard = d_normed * vector(weights, 'batch_gain') * valid_rows[:, None]
    return (d_standard, gradients)

def gate_back(stream, weights, normed_b, pre_gate, d_gated, valid_rows, grad_out, kernel_grad):
    linear_half = pre_gate[:, :D]
    gate_sig = jax.nn.sigmoid(pre_gate[:, D:])
    d_gated = d_gated * valid_rows[:, None]
    d_pre = jnp.concatenate([d_gated * gate_sig, d_gated * linear_half * gate_sig * (1.0 - gate_sig)], 1)
    d_pre_b = d_pre.astype(jnp.bfloat16)
    gradients = {'w_depth': kernel_grad, 'w_point_in': cross_dot(normed_b, d_pre_b), 'b_point_in': lax.optimization_barrier(jnp.sum(d_pre, 0))}
    d_normed = back_dot(d_pre_b, weights['w_point_in'])
    d_stream, gain_grad, shift_grad = norm_back(stream, vector(weights, 'conv_norm_gain'), vector(weights, 'conv_norm_bias'), d_normed)
    gradients['conv_norm_gain'] = gain_grad
    gradients['conv_norm_bias'] = shift_grad
    return (grad_out + d_stream, gradients)

def adam_update(param_vec, grad_in, first_mom, second):
    new_first = BETA_ONE * first_mom + (1.0 - BETA_ONE) * grad_in
    new_second = BETA_TWO * second + (1.0 - BETA_TWO) * grad_in * grad_in
    corr_one = 1.0 - BETA_ONE ** STEP
    corr_two = 1.0 - BETA_TWO ** STEP
    step_size = new_first / corr_one / (jnp.sqrt(new_second / corr_two) + ADAM_EPS)
    return (param_vec - LEARN_RATE * (step_size + DECAY * param_vec), new_first, new_second)

def reference(inputs, lengths, rel_bucket, params, moment_one, moment_two, cotangent):
    weights = unpack(params.astype(jnp.bfloat16))
    group_size = math.gcd(SEQS, 4)
    group_total = SEQS // group_size
    positions = jnp.arange(LEN, dtype=jnp.int32)
    valid_all = positions[None, :] < lengths[:, None]
    bucket_ids = jnp.take(rel_bucket, positions[None, :] - positions[:, None] + LEN - 1)
    pos_bias = jnp.transpose(jnp.take(vector(weights, 'rel_table'), bucket_ids, axis=0), (2, 0, 1))
    inputs_g = inputs.reshape(group_total, group_size, LEN, D)
    valid_g = valid_all.reshape(group_total, group_size, LEN)
    cot_g = cotangent.reshape(group_total, group_size, LEN, D)

    def run_front(inputs_one, valid_one):
        stream0 = inputs_one.reshape(-1, D)
        stream1, stored1 = ffn_forward(stream0, weights, 'first')
        stream2, stored2 = attend_forward(stream1, weights, valid_one, pos_bias)
        valid_rows = valid_one.reshape(-1).astype(jnp.float32)
        stored3 = conv_front(stream2, weights, valid_rows, valid_one.shape[0])
        return (stream0, stream1, stream2, stored1, stored2, stored3, valid_rows)

    def stats_step(running, group_data):
        inputs_one, valid_one = group_data
        parts_all = run_front(inputs_one, valid_one)
        depth = parts_all[5][3]
        valid_rows = parts_all[6]
        return ((running[0] + lax.optimization_barrier(jnp.sum(depth * valid_rows[:, None], 0)), running[1] + lax.optimization_barrier(jnp.sum(depth * depth * valid_rows[:, None], 0))), None)
    zero_vec = jnp.zeros((D,), jnp.float32)
    (first_sum, square_sum), _ = lax.scan(stats_step, (zero_vec, zero_vec), (inputs_g, valid_g))
    token_count = jnp.sum(lengths).astype(jnp.float32)
    batch_mean = first_sum / token_count
    inv_std = lax.rsqrt(square_sum / token_count - batch_mean * batch_mean + BATCH_EPS)

    def tail_step(running, group_data):
        inputs_one, valid_one, cot_one = group_data
        stream0, stream1, stream2, stored1, stored2, stored3, valid_rows = run_front(inputs_one, valid_one)
        stream3, stored4 = conv_tail(stream2, weights, stored3[3], batch_mean, inv_std)
        stream4, stored5 = ffn_forward(stream3, weights, 'second')
        output = norm_rows(stream4, vector(weights, 'final_gain'), vector(weights, 'final_bias'))
        grad_out = cot_one.reshape(-1, D) * valid_rows[:, None]
        d_stream4, gain_grad, shift_grad = norm_back(stream4, vector(weights, 'final_gain'), vector(weights, 'final_bias'), grad_out)
        gradients, sum_dz, sum_dzz = running
        gradients = add_into(gradients, {'final_gain': gain_grad, 'final_bias': shift_grad})
        d_stream3, partial_grads = ffn_backward(stream3, weights, 'second', stored5, d_stream4)
        gradients = add_into(gradients, partial_grads)
        d_standard, partial_grads = conv_tail_back(weights, stored4, d_stream3, valid_rows)
        gradients = add_into(gradients, partial_grads)
        standard = stored4[0]
        sum_dz = sum_dz + lax.optimization_barrier(jnp.sum(d_standard, 0))
        sum_dzz = sum_dzz + lax.optimization_barrier(jnp.sum(d_standard * standard, 0))
        return ((gradients, sum_dz, sum_dzz), (output, d_stream3, d_standard))
    (gradients, sum_dz, sum_dzz), (outputs, d_stream3_all, d_standard_all) = lax.scan(tail_step, (zero_grads(), zero_vec, zero_vec), (inputs_g, valid_g, cot_g))

    def head_step(running, group_data):
        inputs_one, valid_one, d_stream3, d_standard = group_data
        stream0, stream1, stream2, stored1, stored2, stored3, valid_rows = run_front(inputs_one, valid_one)
        normed_b, pre_gate, padded, depth = stored3
        standard = (depth - batch_mean) * inv_std
        d_depth = valid_rows[:, None] * inv_std * (d_standard - sum_dz / token_count - standard * sum_dzz / token_count)
        d_depth3 = d_depth.reshape(valid_one.shape[0], -1, D)
        d_padded = jnp.pad(d_depth3, ((0, 0), (K // 2, K // 2), (0, 0)))
        kernel_grad, d_gated = depth_back(padded, d_depth3, d_padded, vector(weights, 'w_depth'))
        d_stream2, partial_grads = gate_back(stream2, weights, normed_b, pre_gate, d_gated, valid_rows, d_stream3, kernel_grad)
        running = add_into(running, partial_grads)
        d_stream1, partial_grads = attend_backward(stream1, weights, stored2, d_stream2, valid_one, pos_bias, bucket_ids)
        running = add_into(running, partial_grads)
        d_stream0, partial_grads = ffn_backward(stream0, weights, 'first', stored1, d_stream1)
        running = add_into(running, partial_grads)
        return (running, d_stream0)
    gradients, input_grads = lax.scan(head_step, gradients, (inputs_g, valid_g, d_stream3_all, d_standard_all))
    param_grad = pack_flat(gradients, PARAMS)
    new_params, new_first, new_second = adam_update(params, param_grad, moment_one, moment_two)
    return (outputs.reshape(SEQS, LEN, D), input_grads.reshape(SEQS, LEN, D), param_grad, new_params, new_first, new_second)
```

```python
import functools
import math

import jax
import jax.numpy as jnp
from jax import lax
from jax.experimental import pallas as pl
from jax.experimental.pallas import tpu as pltpu
from jax.sharding import PartitionSpec as P

D = 512
H = 8
HD = 64
FF = 2048
K = 31
NB = 32
DP = "dp"
SEQ = "seq"
STEP = 4


NORM_EPS = 1e-05
BATCH_EPS = 1e-05
LEARN_RATE = 0.005
DECAY = 0.01
BETA_ONE = 0.9
BETA_TWO = 0.98
ADAM_EPS = 1e-08


def with_halo(shard, sides, width):
    for axis, dim in sides:
        devices, length = (lax.axis_size(axis), shard.shape[dim])
        up = [(i, (i + 1) % devices) for i in range(devices - 1)]
        down = [(j, i) for i, j in up]
        last = lax.slice_in_dim(shard, length - width, length, axis=dim)
        leading = lax.slice_in_dim(shard, 0, width, axis=dim)
        before = lax.ppermute(last, axis, up)
        after = lax.ppermute(leading, axis, down)
        shard = jnp.concatenate([before, shard, after], axis=dim)
    return shard


def segments():

    def feed_block(prefix):
        return [
            (prefix + "_ng", (D,)),
            (prefix + "_nb", (D,)),
            (prefix + "_w_in", (D, FF)),
            (prefix + "_b_in", (FF,)),
            (prefix + "_w_out", (FF, D)),
            (prefix + "_b_out", (D,)),
        ]

    listing = feed_block("first")
    listing = listing + [
        ("attn_ng", (D,)),
        ("attn_nb", (D,)),
        ("w_q", (D, D)),
        ("b_q", (D,)),
        ("w_k", (D, D)),
        ("w_v", (D, D)),
        ("b_v", (D,)),
        ("w_o", (D, D)),
        ("b_o", (D,)),
        ("rel", (NB, H)),
    ]
    listing = listing + [
        ("conv_ng", (D,)),
        ("conv_nb", (D,)),
        ("w_pi", (D, 2 * D)),
        ("b_pi", (2 * D,)),
        ("w_depth", (K, D)),
        ("bng", (D,)),
        ("bnb", (D,)),
        ("w_po", (D, D)),
        ("b_po", (D,)),
    ]
    listing = listing + feed_block("second") + [("fin_g", (D,)), ("fin_b", (D,))]
    return listing


def arrange():
    places, gaps = {}, []
    linear = inner = 0
    for entry_name, entry_shape in segments():
        extent = math.prod(entry_shape)
        tail = 2 * D if entry_name == "conv_ng" else 0
        if extent >= D * D or tail:
            pad = -(inner + tail) % TILE
            if pad:
                gaps.append((linear, pad))
                inner = inner + pad
        places[entry_name] = inner // LANES
        linear, inner = linear + extent, inner + extent
    return places, gaps, -(-inner // TILE)


def unpack(rows):
    result = {}
    places = arrange()[0]
    for entry_name, entry_shape in segments():
        extent = math.prod(entry_shape)
        first = places[entry_name]
        piece = rows[first : first + -(-extent // LANES)]
        if extent < LANES:
            piece = piece[:, :extent]
        result[entry_name] = piece.reshape(entry_shape)
    return result


def device_index():
    return lax.axis_index(DP) * lax.axis_size(SEQ) + lax.axis_index(SEQ)


def own_block(plan, params):
    index = device_index()
    shift_down = [(i + 1, i) for i in range(plan.n - 1)]
    following = lax.ppermute(params[:TILE], (DP, SEQ), shift_down)
    length = plan.hi * TILE
    room = max(length + TILE - plan.shard - TILE, 0)
    front = max(size for _, size in plan.gaps)
    extended = jnp.concatenate(
        [jnp.zeros((front,), jnp.float32), params, following, jnp.zeros((room,), jnp.float32)]
    )
    table = jnp.asarray(plan.block_table, jnp.int32)[index]
    early = lax.dynamic_slice(extended, (front + table[0],), (length,))
    late = lax.dynamic_slice(extended, (front + table[0] - table[2],), (length,))
    block = jnp.where(jnp.arange(length, dtype=jnp.int32) < table[1], early, late)
    return block.astype(jnp.bfloat16).reshape(plan.hi, 8, LANES)


def own_shard(plan, window):
    table = jnp.asarray(plan.shard_table, jnp.int32)[device_index()]
    flat = window.reshape(-1)
    early = lax.dynamic_slice(flat, (table[0],), (plan.shard,))
    late = lax.dynamic_slice(flat, (table[0] + table[2],), (plan.shard,))
    return jnp.where(jnp.arange(plan.shard, dtype=jnp.int32) < table[1], early, late)


def vector(weights, entry_name):
    return weights[entry_name].astype(jnp.float32)


def swish_act(values):
    return values * jax.nn.sigmoid(values)


def swish_grad(values):
    sig_vals = jax.nn.sigmoid(values)
    return sig_vals * (1.0 + values * (1.0 - sig_vals))


def norm_rows(values, scale_vec, shift_vec):
    centre = values - jnp.mean(values, -1, keepdims=True)
    spread = jnp.mean(centre * centre, -1, keepdims=True)
    return centre * lax.rsqrt(spread + NORM_EPS) * scale_vec + shift_vec


def norm_back(values, scale_vec, shift_vec, grad_out):
    _, pullback = jax.vjp(norm_rows, values, scale_vec, shift_vec)
    return pullback(grad_out)


def forward_dot(left_mat, weight):
    return jnp.dot(left_mat, weight, preferred_element_type=jnp.float32)


def cross_dot(left_mat, right_mat):
    return lax.dot_general(
        left_mat, right_mat, (((0,), (0,)), ((), ())), preferred_element_type=jnp.float32
    )


def back_dot(grad_in, weight):
    return lax.dot_general(
        grad_in, weight, (((1,), (1,)), ((), ())), preferred_element_type=jnp.float32
    )


def ffn_forward(stream, weights, prefix):
    normed_b = norm_rows(
        stream, vector(weights, prefix + "_ng"), vector(weights, prefix + "_nb")
    ).astype(jnp.bfloat16)
    hidden = forward_dot(normed_b, weights[prefix + "_w_in"]) + vector(weights, prefix + "_b_in")
    active = swish_act(hidden).astype(jnp.bfloat16)
    output = stream + 0.5 * (
        forward_dot(active, weights[prefix + "_w_out"]) + vector(weights, prefix + "_b_out")
    )
    return (output, (normed_b, hidden, active))


def ffn_backward(stream, weights, prefix, stored, grad_out):
    normed_b, hidden, active = stored
    half_grad = 0.5 * grad_out
    half_b = half_grad.astype(jnp.bfloat16)
    gradients = {
        prefix + "_w_out": (active, half_b),
        prefix + "_b_out": jnp.sum(half_grad, 0),
    }
    d_hidden = back_dot(half_b, weights[prefix + "_w_out"]) * swish_grad(hidden)
    d_hidden_b = d_hidden.astype(jnp.bfloat16)
    gradients[prefix + "_w_in"] = (normed_b, d_hidden_b)
    gradients[prefix + "_b_in"] = jnp.sum(d_hidden, 0)
    d_normed = back_dot(d_hidden_b, weights[prefix + "_w_in"])
    d_stream, gain_grad, shift_grad = norm_back(
        stream,
        vector(weights, prefix + "_ng"),
        vector(weights, prefix + "_nb"),
        d_normed,
    )
    gradients[prefix + "_ng"] = gain_grad
    gradients[prefix + "_nb"] = shift_grad
    return (grad_out + d_stream, gradients)


MESH = pl.DeviceIdType.MESH
LANES=512
TILE=8*LANES

class Plan:
    def __init__(self, ndp, nseq, shard):
        self.ndp, self.nseq, self.shard = ndp, nseq, shard
        self.k = ndp.bit_length() - 1
        self.phases = self.k - 1
        self.n = n = ndp * nseq
        self.places, self.gaps, self.total = arrange()
        begins = [self.inner(d * shard) for d in range(n)]
        starts = [-(-b // TILE) for b in begins] + [self.total]
        sizes = [b - a for a, b in zip(starts, starts[1:])]
        self.lo, self.hi = min(sizes), max(sizes)
        self.slots = nseq * 2**self.phases
        floors = [b // TILE for b in begins]
        ends = [self.inner((d + 1) * shard - 1) // TILE + 1 for d in range(n)]
        self.win = max(e - f for e, f in zip(ends, floors))
        self.win += self.win % 2
        self.padded = max(self.total, max(floors) + self.win)
        self.block_table, self.shard_table = [], []
        for d in range(n):
            near = [g for g in self.gaps if d * shard < g[0] < (d + 1) * shard + TILE]
            assert len(near) <= 1
            cut, size = near[0] if near else (2**30, 0)
            lead = starts[d] * TILE - begins[d]
            self.block_table.append((lead, cut - d * shard - lead, size))
            self.shard_table.append((begins[d] - floors[d] * TILE, cut - d * shard, size))

    def inner(self, position):
        if isinstance(position, int):
            return position + sum(size for at, size in self.gaps if at <= position)
        result = position
        for at, size in self.gaps:
            result = result + jnp.where(position >= at, size, 0)
        return result

    def order(self):
        ev=[]
        for s in range(self.nseq):
            for sign in ((0,) if s==0 else (-1,1)):
                for t in range(2**self.phases):
                    ev.append((s+0.5*bin(t).count("1")+0.01*t, s, sign, t))
        ev.sort()
        return [e[1:] for e in ev]

def flip(di, mask_bits, bits, t, phases):
    out=di
    for p in range(phases):
        if (t>>p)&1:
            out = out + mask_bits[p]*(1-2*bits[p])
    return out

def phase_masks(di, c, phases):
    masks, bits=[],[]
    for p in range(phases):
        a, b = 1<<(p+1), 1<<(phases-p)
        masks.append(a+c*(b-a))
        ba, bb = (di//a)%2, (di//b)%2
        bits.append(ba+c*(bb-ba))
    return masks, bits

def block_of(plan, dpi, z):
    d = dpi*plan.nseq+z
    a = (plan.inner(d*plan.shard)+TILE-1)//TILE
    b = (plan.inner((d+1)*plan.shard)+TILE-1)//TILE
    b = jnp.where(d == plan.n-1, plan.total, b)
    return a, b-a

def floor_of(plan, dpi, z):
    return plan.inner((dpi*plan.nseq+z)*plan.shard)//TILE

def gather_kernel(plan, src, out, send_a, send_b, recv_a, recv_b, loc_sem):
    di, z = lax.axis_index(DP), lax.axis_index(SEQ)
    ns, ph = plan.nseq, plan.phases
    c = di%2
    masks, bits = phase_masks(di, c, ph)
    other = di+1-2*c
    omasks, obits = phase_masks(other, 1-c, ph)
    up, down = lax.rem(z+1,ns), lax.rem(z+ns-1,ns)
    partners=[(di,up),(di,down),(other,z)]+[(flip(di,masks,bits,1<<p,ph),z) for p in range(ph)]
    barrier=pltpu.get_barrier_semaphore()
    for a,b in partners:
        pl.semaphore_signal(barrier,inc=1,device_id=(a,b),device_id_type=MESH)
    pl.semaphore_wait(barrier,len(partners))
    lo, more = plan.lo, plan.hi-plan.lo
    start_own, size_own = block_of(plan, di, z)

    def pair(ref, base, dst_start, size, sidx, ridx, dev):
        copies=[pltpu.make_async_remote_copy(src_ref=ref.at[pl.ds(base,lo)],dst_ref=out.at[pl.ds(dst_start,lo)],
            send_sem=send_a.at[sidx],recv_sem=recv_a.at[ridx],device_id=dev,device_id_type=MESH)]
        for x in range(more):
            copies.append(pltpu.make_async_remote_copy(src_ref=ref.at[pl.ds(base+lo+x,1)],dst_ref=out.at[pl.ds(dst_start+lo+x,1)],
                send_sem=send_b.at[sidx*more+x],recv_sem=recv_b.at[ridx*more+x],device_id=dev,device_id_type=MESH))
        return copies, size
    def each(p, act):
        for x,copy in enumerate(p[0]):
            if x==0: act(copy)
            else:
                @pl.when(p[1]>=lo+x)
                def _(): act(copy)
    def start(p): each(p, lambda c: c.start())
    def wait_send(p): each(p, lambda c: c.wait_send())
    def wait_recv(p): each(p, lambda c: c.wait_recv())

    own=[pltpu.make_async_copy(src.at[pl.ds(0,lo)],out.at[pl.ds(start_own,lo)],loc_sem.at[0])]
    for x in range(more):
        own.append(pltpu.make_async_copy(src.at[pl.ds(lo+x,1)],out.at[pl.ds(start_own+lo+x,1)],loc_sem.at[1+x]))
    own=(own,size_own)
    start(own)
    nslot=plan.slots
    sends=[]
    sidx=[0]
    def forward(conds, ref, base, st, size, ridx, dev):
        i=sidx[0]; sidx[0]+=1
        p=pair(ref,base,st,size,i,ridx,dev)
        sends.append((conds,p))
        guard(conds, lambda: start(p))
    def guard(conds, fn):
        if not conds: fn(); return
        cond=conds[0]
        for x in conds[1:]: cond=jnp.logical_and(cond,x)
        @pl.when(cond)
        def _(): fn()

    for s, sign, t in plan.order():
        zz = z+sign*s
        conds=[] if s==0 else ([zz>=0] if sign<0 else [zz<ns])
        dpi=flip(di,masks,bits,t,ph)
        st,size=block_of(plan,dpi,zz)
        mine = s==0 and t==0
        ref, base = (src, 0) if mine else (out, st)
        slot = t*ns+zz
        if not mine:
            p=pair(out,st,st,size,0,slot,(di,z))
            guard(conds, lambda: wait_recv(p))
        if t==0:
            if sign<=0 : forward(conds+[z<ns-1],ref,base,st,size,slot,(di,z+1))
            if sign>=0 : forward(conds+[z>0],ref,base,st,size,slot,(di,z-1))
        hi_bit=t.bit_length()
        for pp in range(hi_bit,ph):
            forward(conds,ref,base,st,size,slot+(1<<pp)*ns,(flip(di,masks,bits,1<<pp,ph),z))
        forward(conds,ref,base,st,size,nslot+slot,(other,z))
    for s, sign, t in plan.order():
        zz=z+sign*s
        conds=[] if s==0 else ([zz>=0] if sign<0 else [zz<ns])
        dpi=flip(other,omasks,obits,t,ph)
        st,size=block_of(plan,dpi,zz)
        p=pair(out,st,st,size,0,nslot+t*ns+zz,(di,z))
        guard(conds,lambda: wait_recv(p))
    for conds,p in sends:
        guard(conds,lambda: wait_send(p))
    each(own, lambda c: c.wait())

def count_sends(plan):
    n=0
    for s,sign,t in plan.order():
        if t==0: n+= (2 if sign==0 else 1)
        n+=plan.phases-t.bit_length()+1
    return n

def gather(plan, block):
    ns=count_sends(plan)
    more=max(plan.hi-plan.lo,1)
    return pl.pallas_call(
        functools.partial(gather_kernel,plan),
        out_shape=jax.ShapeDtypeStruct((plan.total,8,LANES),block.dtype),
        in_specs=[pl.BlockSpec(memory_space=pl.ANY)],
        out_specs=pl.BlockSpec(memory_space=pl.ANY),
        scratch_shapes=[pltpu.SemaphoreType.DMA((ns,)),pltpu.SemaphoreType.DMA((ns*more,)),
            pltpu.SemaphoreType.DMA((2*plan.slots,)),pltpu.SemaphoreType.DMA((2*plan.slots*more,)),pltpu.SemaphoreType.DMA((1+more,))],
        compiler_params=pltpu.CompilerParams(collective_id=0,has_side_effects=True),
        name="gather_params",
    )(block)

def scatter_kernel(plan, g, out, acc, rc, rp, rz, load_sem, send_sem, core_send, core_recv, ph_recv, z_recv):
    di, z = lax.axis_index(DP), lax.axis_index(SEQ)
    ns, ph, win, nslot = plan.nseq, plan.phases, plan.win, plan.slots
    c = di%2
    masks, bits = phase_masks(di, c, ph)
    other = di+1-2*c
    omasks, obits = phase_masks(other, 1-c, ph)
    up, down = lax.rem(z+1,ns), lax.rem(z+ns-1,ns)
    partners=[(di,up),(di,down),(other,z)]+[(flip(di,masks,bits,1<<p,ph),z) for p in range(ph)]
    barrier=pltpu.get_barrier_semaphore()
    for a,b in partners:
        pl.semaphore_signal(barrier,inc=1,device_id=(a,b),device_id_type=MESH)
    order=list(reversed(plan.order()))
    def cond_of(s,sign):
        zz=z+sign*s
        return zz,([] if s==0 else ([zz>=0] if sign<0 else [zz<ns]))
    def guard(conds, fn):
        if not conds: fn(); return
        cond=conds[0]
        for x in conds[1:]: cond=jnp.logical_and(cond,x)
        @pl.when(cond)
        def _(): fn()
    def load(s,sign,t):
        zz,conds=cond_of(s,sign)
        slot=t*ns+zz
        st=floor_of(plan,flip(di,masks,bits,t,ph),zz)
        return conds,pltpu.make_async_copy(g.at[pl.ds(st,win)],acc.at[slot],load_sem.at[slot])
    def core(s,sign,t):
        zz,conds=cond_of(s,sign)
        slot=t*ns+zz
        st=floor_of(plan,flip(other,omasks,obits,t,ph),zz)
        return conds,pltpu.make_async_remote_copy(src_ref=g.at[pl.ds(st,win)],dst_ref=rc.at[slot],
            send_sem=core_send.at[slot],recv_sem=core_recv.at[slot],device_id=(other,z),device_id_type=MESH)
    for e in order:
        conds,cp=load(*e)
        guard(conds,lambda: cp.start())
    pl.semaphore_wait(barrier,len(partners))
    for e in order:
        conds,cp=core(*e)
        guard(conds,lambda: cp.start())
    sends=[]
    def send(conds,slot,dst,rsem,dev):
        i=len(sends)
        cp=pltpu.make_async_remote_copy(src_ref=acc.at[slot],dst_ref=dst,send_sem=send_sem.at[i],recv_sem=rsem,
            device_id=dev,device_id_type=MESH)
        sends.append((conds,cp))
        guard(conds,lambda: cp.start())
    def waiting(conds,dst,rsem):
        cp=pltpu.make_async_remote_copy(src_ref=dst,dst_ref=dst,send_sem=send_sem.at[0],recv_sem=rsem,
            device_id=(di,z),device_id_type=MESH)
        guard(conds,lambda: cp.wait_recv())
    step=2
    def add(dst, slot, parts, final=False):
        @pl.loop(0,win//step)
        def _(i):
            r=pl.ds(i*step,step)
            v=acc[slot,r].astype(jnp.float32)
            for p in parts:
                v=v+p(r).astype(jnp.float32)
            if final: out[r]=v
            else: acc[slot,r]=v.astype(acc.dtype)
    for s,sign,t in order:
        zz,conds=cond_of(s,sign)
        slot=t*ns+zz
        hi_bit=t.bit_length()
        def fn():
            load(s,sign,t)[1].wait()
            waiting([],rc.at[slot],core_recv.at[slot])
            parts=[lambda r: rc[slot,r]]
            for pp in range(hi_bit,ph):
                idx=((1<<pp)-1)*ns+slot
                waiting([],rp.at[idx],ph_recv.at[idx])
                parts.append(lambda r,idx=idx: rp[idx,r])
            add(None,slot,parts,final=False) if not (t==0 and s==0) else add(None,slot,parts,final=True)
        guard(conds,fn)
        if t:
            pp=hi_bit-1
            idx=((1<<pp)-1)*ns+slot-(1<<pp)*ns
            send(conds,slot,rp.at[idx],ph_recv.at[idx],(flip(di,masks,bits,1<<pp,ph),z))
        else:
            def zadd(stream, extra):
                zi=stream*ns+zz
                def fz():
                    waiting([],rz.at[zi],z_recv.at[zi])
                    @pl.loop(0,win//step)
                    def _(i):
                        r=pl.ds(i*step,step)
                        if s==0:
                            out[r]=out[r]+rz[zi,r].astype(jnp.float32)
                        else:
                            acc[slot,r]=(acc[slot,r].astype(jnp.float32)+rz[zi,r].astype(jnp.float32)).astype(acc.dtype)
                guard(conds+extra,fz)
            if sign>=0: zadd(0,[z>0])
            if sign<=0: zadd(1,[z<ns-1])
            if sign>0: send(conds,slot,rz.at[zz],z_recv.at[zz],(di,z+1))
            if sign<0: send(conds,slot,rz.at[ns+zz],z_recv.at[ns+zz],(di,z-1))
    for e in order:
        conds,cp=core(*e)
        guard(conds,lambda: cp.wait_send())
    for conds,cp in sends:
        guard(conds,lambda: cp.wait_send())

def scatter(plan, g):
    win,ns,ph,nslot=plan.win,plan.nseq,plan.phases,plan.slots
    nsend=len(plan.order())
    return pl.pallas_call(
        functools.partial(scatter_kernel,plan),
        out_shape=jax.ShapeDtypeStruct((win,8,LANES),jnp.float32),
        in_specs=[pl.BlockSpec(memory_space=pl.ANY)],
        out_specs=pl.BlockSpec(memory_space=pltpu.VMEM),
        scratch_shapes=[pltpu.VMEM((nslot,win,8,LANES),g.dtype),pltpu.VMEM((nslot,win,8,LANES),g.dtype),
            pltpu.VMEM(((2**ph-1)*ns,win,8,LANES),g.dtype),pltpu.VMEM((2*ns,win,8,LANES),g.dtype),
            pltpu.SemaphoreType.DMA((nslot,)),pltpu.SemaphoreType.DMA((nsend,)),
            pltpu.SemaphoreType.DMA((nslot,)),pltpu.SemaphoreType.DMA((nslot,)),
            pltpu.SemaphoreType.DMA(((2**ph-1)*ns,)),pltpu.SemaphoreType.DMA((2*ns,))],
        compiler_params=pltpu.CompilerParams(collective_id=1,has_side_effects=True,vmem_limit_bytes=48*1024*1024),
        name="scatter_grads",
    )(g)


def weight_kernel(plan, names, *refs):
    inputs = dict(zip(names, refs))
    out, mix = refs[len(names) :]
    rows = (((0,), (0,)), ((), ()))
    for name, shape in segments():
        first = plan.places[name]
        if math.prod(shape) < D * D:
            values = inputs[name + "0"]
            for r in range(-(-math.prod(shape) // LANES)):
                if name == "w_depth":
                    line = inputs[name + str(r)][...]
                else:
                    line = values[:, r * LANES : (r + 1) * LANES]
                tile, row = divmod(first + r, 8)
                out[tile, row : row + 1, : line.shape[1]] = line.astype(out.dtype)
            continue
        left, right = inputs[name + "0"], inputs[name + "1"]
        fold = shape[1] // LANES
        step = 256 if fold == 1 else 128

        @pl.loop(0, shape[0] // step)
        def _(i):
            part = left[:, pl.ds(pl.multiple_of(i * step, step), step)]
            value = lax.dot_general(part, right[...], rows, preferred_element_type=jnp.float32)
            if fold > 1:
                for j in range(fold):
                    for lane in range(LANES // 128):
                        at = j * LANES + lane * 128
                        mix[lane, pl.ds(j, step, stride=fold), :] = value[:, at : at + 128]
                value = jnp.concatenate([mix[lane, : step * fold] for lane in range(LANES // 128)], 1)
            tiles = step * fold // 8
            out[pl.ds(first // 8 + i * tiles, tiles)] = value.astype(out.dtype).reshape(tiles, 8, LANES)


def weight_grads(plan, gradients):
    names, operands = [], []
    for name, shape in segments():
        extent = math.prod(shape)
        if extent >= D * D:
            parts = gradients[name]
        elif name == "w_depth":
            parts = [value.reshape(1, D) for value in gradients[name]]
        else:
            parts = [gradients[name].reshape(1, extent)]
        for number, value in enumerate(parts):
            names.append(name + str(number))
            operands.append(value)
    vmem = pl.BlockSpec(memory_space=pltpu.VMEM)
    return pl.pallas_call(
        functools.partial(weight_kernel, plan, names),
        out_shape=jax.ShapeDtypeStruct((plan.padded, 8, LANES), jnp.bfloat16),
        in_specs=[vmem] * len(operands),
        out_specs=vmem,
        scratch_shapes=[pltpu.VMEM((LANES // 128, 512, 128), jnp.float32)],
        compiler_params=pltpu.CompilerParams(vmem_limit_bytes=60 * 1024 * 1024),
        name="weight_grads",
    )(*operands)


def sum_kernel(ndp, nseq, left, right, valid, out, part, line, cross, seq_send, seq_recv, dp_send, dp_recv):
    di, z = lax.axis_index(DP), lax.axis_index(SEQ)
    barrier = pltpu.get_barrier_semaphore()
    peers = [(di, lax.rem(z + i, nseq)) for i in range(1, nseq)]
    peers = peers + [(lax.rem(di + i, ndp), z) for i in range(1, ndp)]
    for peer in peers:
        pl.semaphore_signal(barrier, inc=1, device_id=peer, device_id_type=MESH)
    value, mask = left[...], valid[...]
    value = value * mask
    rows = [
        jnp.sum(value, 0, keepdims=True),
        jnp.sum(value * right[...], 0, keepdims=True),
        jnp.broadcast_to(jnp.sum(mask, 0, keepdims=True), (1, LANES)),
        jnp.zeros((5, LANES), jnp.float32),
    ]
    part[...] = jnp.concatenate(rows, 0)
    pl.semaphore_wait(barrier, len(peers))

    def exchange(count, me, target, slots, send, recv):
        copies = []
        for i in range(1, count):
            copy = pltpu.make_async_remote_copy(
                src_ref=part, dst_ref=slots.at[me], send_sem=send.at[i], recv_sem=recv.at[me],
                device_id=target(lax.rem(me + i, count)), device_id_type=MESH,
            )
            copy.start()
            copies.append(copy)
        slots[me] = part[...]
        for i in range(1, count):
            source = lax.rem(me + count - i, count)
            pltpu.make_async_remote_copy(
                src_ref=part, dst_ref=slots.at[source], send_sem=send.at[i], recv_sem=recv.at[source],
                device_id=(di, z), device_id_type=MESH,
            ).wait_recv()
        for copy in copies:
            copy.wait_send()
        total = slots[0]
        for i in range(1, count):
            total = total + slots[i]
        return total

    part[...] = exchange(nseq, z, lambda i: (di, i), line, seq_send, seq_recv)
    out[...] = exchange(ndp, di, lambda i: (i, z), cross, dp_send, dp_recv)


def batch_sums(left, right, valid, number):
    ndp, nseq = lax.axis_size(DP), lax.axis_size(SEQ)
    vmem = pl.BlockSpec(memory_space=pltpu.VMEM)
    return pl.pallas_call(
        functools.partial(sum_kernel, ndp, nseq),
        out_shape=jax.ShapeDtypeStruct((8, LANES), jnp.float32),
        in_specs=[vmem] * 3,
        out_specs=vmem,
        scratch_shapes=[
            pltpu.VMEM((8, LANES), jnp.float32),
            pltpu.VMEM((nseq, 8, LANES), jnp.float32),
            pltpu.VMEM((ndp, 8, LANES), jnp.float32),
            pltpu.SemaphoreType.DMA((nseq,)),
            pltpu.SemaphoreType.DMA((nseq,)),
            pltpu.SemaphoreType.DMA((ndp,)),
            pltpu.SemaphoreType.DMA((ndp,)),
        ],
        compiler_params=pltpu.CompilerParams(collective_id=number, has_side_effects=True),
        name="batch_sums" + str(number),
    )(left, right, valid)


def bucket_window(rel_bucket, block_len, full_len):
    first_pos = lax.axis_index(SEQ) * block_len
    width = -(-(block_len + full_len - 1) // 128) * 128
    padded = jnp.concatenate([rel_bucket, jnp.full((width,), -1, jnp.int32)])
    window = lax.dynamic_slice(padded, (full_len - block_len - first_pos,), (width,))
    return (window[:, None] == jnp.arange(NB, dtype=jnp.int32)[None, :]).astype(jnp.float32)


def head_scores(q, k, table, valid, head):
    block, width = q.shape[0], table.shape[1]
    full = k.shape[0]
    scores = lax.dot_general(q, k, (((1,), (1,)), ((), ())), preferred_element_type=jnp.float32)
    spread = jnp.broadcast_to(table[head : head + 1], (block, width))
    bias = pltpu.roll(spread, width - block + 1, 1, stride=1, stride_axis=0)[:, :full]
    return jnp.where(valid, scores * (1.0 / math.sqrt(HD)) + bias, -jnp.inf)


def attend_kernel(len_ref, q_ref, k_ref, v_ref, t_ref, ctx_ref, lse_ref):
    full = k_ref.shape[1]
    block = q_ref.shape[1]
    valid = lax.broadcasted_iota(jnp.int32, (1, full), 1) < len_ref[pl.program_id(0)]
    lane = lax.broadcasted_iota(jnp.int32, (block, 128), 1)
    lse = jnp.zeros((block, 128), jnp.float32)
    for h in range(H):
        cols = slice(h * HD, (h + 1) * HD)
        scores = head_scores(q_ref[0, :, cols], k_ref[0, :, cols], t_ref[...], valid, h)
        top = jnp.max(scores, -1, keepdims=True)
        weights = jnp.exp(scores - top)
        total = jnp.sum(weights, -1, keepdims=True)
        probs = (weights * (1.0 / total)).astype(jnp.bfloat16)
        ctx = jnp.dot(probs, v_ref[0, :, cols], preferred_element_type=jnp.float32)
        ctx_ref[0, :, cols] = ctx.astype(jnp.bfloat16)
        lse = jnp.where(lane == h, top + jnp.log(total), lse)
    lse_ref[0] = lse


def attend_back_kernel(len_ref, q_ref, k_ref, v_ref, t_ref, lse_ref, dctx_ref,
                       dq_ref, dk_ref, dv_ref, dt_ref, sums_ref):
    full = k_ref.shape[1]
    block = q_ref.shape[1]
    width = t_ref.shape[1]
    seq_id = pl.program_id(0)

    @pl.when(seq_id == 0)
    def _():
        dt_ref[...] = jnp.zeros_like(dt_ref)
        sums_ref[...] = jnp.zeros_like(sums_ref)

    valid = lax.broadcasted_iota(jnp.int32, (1, full), 1) < len_ref[seq_id]
    rows = (((0,), (0,)), ((), ()))
    for h in range(H):
        cols = slice(h * HD, (h + 1) * HD)
        q, k, v = q_ref[0, :, cols], k_ref[0, :, cols], v_ref[0, :, cols]
        dctx = dctx_ref[0, :, cols]
        scores = head_scores(q, k, t_ref[...], valid, h)
        probs = jnp.exp(scores - lse_ref[0, :, h : h + 1])
        d_probs = lax.dot_general(dctx, v, (((1,), (1,)), ((), ())), preferred_element_type=jnp.float32)
        delta = jnp.sum(probs * d_probs, -1, keepdims=True)
        d_scores = probs * (d_probs - delta)
        d_scores_b = d_scores.astype(jnp.bfloat16)
        dq = jnp.dot(d_scores_b, k, preferred_element_type=jnp.float32) * (1.0 / math.sqrt(HD))
        dk = lax.dot_general(d_scores_b, q, rows, preferred_element_type=jnp.float32)
        dv = lax.dot_general(probs.astype(jnp.bfloat16), dctx, rows, preferred_element_type=jnp.float32)
        dq_ref[0, :, cols] = dq.astype(jnp.bfloat16)
        dk_ref[0, :, cols] = (dk * (1.0 / math.sqrt(HD))).astype(jnp.bfloat16)
        dv_ref[0, :, cols] = dv.astype(jnp.bfloat16)
        sums_ref[0:1, cols] += jnp.sum(dq, 0, keepdims=True)
        sums_ref[1:2, cols] += jnp.sum(dv, 0, keepdims=True)
        wide = jnp.concatenate([d_scores, jnp.zeros((block, width - full), jnp.float32)], 1)
        folded = wide[0:8]
        folded = pltpu.roll(folded, block - 1, 1)
        for g in range(1, block // 8):
            folded = folded + pltpu.roll(wide[8 * g : 8 * g + 8], block - 1 - 8 * g, 1)
        line = folded[0:1]
        for r in range(1, 8):
            line = line + pltpu.roll(folded[r : r + 1], width - r, 1)
        dt_ref[h : h + 1, :] += line


def attend(lengths, queries, keys, values, table):
    seqs, block, width = queries.shape
    full = keys.shape[1]
    return pl.pallas_call(
        attend_kernel,
        grid_spec=pltpu.PrefetchScalarGridSpec(
            num_scalar_prefetch=1,
            grid=(seqs,),
            in_specs=[
                pl.BlockSpec((1, block, width), lambda s, n: (s, 0, 0)),
                pl.BlockSpec((1, full, width), lambda s, n: (s, 0, 0)),
                pl.BlockSpec((1, full, width), lambda s, n: (s, 0, 0)),
                pl.BlockSpec(table.shape, lambda s, n: (0, 0)),
            ],
            out_specs=[
                pl.BlockSpec((1, block, width), lambda s, n: (s, 0, 0)),
                pl.BlockSpec((1, block, 128), lambda s, n: (s, 0, 0)),
            ],
        ),
        out_shape=[
            jax.ShapeDtypeStruct((seqs, block, width), jnp.bfloat16),
            jax.ShapeDtypeStruct((seqs, block, 128), jnp.float32),
        ],
        name="attend",
    )(lengths, queries, keys, values, table)


def attend_back(lengths, queries, keys, values, table, lse, d_context):
    seqs, block, width = queries.shape
    full = keys.shape[1]
    return pl.pallas_call(
        attend_back_kernel,
        grid_spec=pltpu.PrefetchScalarGridSpec(
            num_scalar_prefetch=1,
            grid=(seqs,),
            in_specs=[
                pl.BlockSpec((1, block, width), lambda s, n: (s, 0, 0)),
                pl.BlockSpec((1, full, width), lambda s, n: (s, 0, 0)),
                pl.BlockSpec((1, full, width), lambda s, n: (s, 0, 0)),
                pl.BlockSpec(table.shape, lambda s, n: (0, 0)),
                pl.BlockSpec((1, block, 128), lambda s, n: (s, 0, 0)),
                pl.BlockSpec((1, block, width), lambda s, n: (s, 0, 0)),
            ],
            out_specs=[
                pl.BlockSpec((1, block, width), lambda s, n: (s, 0, 0)),
                pl.BlockSpec((1, full, width), lambda s, n: (s, 0, 0)),
                pl.BlockSpec((1, full, width), lambda s, n: (s, 0, 0)),
                pl.BlockSpec(table.shape, lambda s, n: (0, 0)),
                pl.BlockSpec((8, width), lambda s, n: (0, 0)),
            ],
        ),
        out_shape=[
            jax.ShapeDtypeStruct((seqs, block, width), jnp.bfloat16),
            jax.ShapeDtypeStruct((seqs, full, width), jnp.bfloat16),
            jax.ShapeDtypeStruct((seqs, full, width), jnp.bfloat16),
            jax.ShapeDtypeStruct(table.shape, jnp.float32),
            jax.ShapeDtypeStruct((8, width), jnp.float32),
        ],
        name="attend_back",
    )(lengths, queries, keys, values, table, lse, d_context)


def seq_gather(rows, seq_count):
    return lax.all_gather(rows.reshape(seq_count, -1, D), SEQ, axis=1, tiled=True)


def seq_scatter(rows):
    return lax.psum_scatter(rows, SEQ, scatter_dimension=1, tiled=True)


def attend_forward(stream, weights, lengths, onehot, seq_count):
    normed_b = norm_rows(
        stream, vector(weights, "attn_ng"), vector(weights, "attn_nb")
    ).astype(jnp.bfloat16)
    normed_all = seq_gather(normed_b, seq_count)
    queries = (forward_dot(normed_b, weights["w_q"]) + vector(weights, "b_q")).astype(
        jnp.bfloat16
    )
    flat_all = normed_all.reshape(-1, D)
    keys = forward_dot(flat_all, weights["w_k"]).astype(jnp.bfloat16)
    values = (forward_dot(flat_all, weights["w_v"]) + vector(weights, "b_v")).astype(
        jnp.bfloat16
    )
    table = lax.dot_general(
        weights["rel"], onehot.astype(jnp.bfloat16), (((0,), (1,)), ((), ())),
        preferred_element_type=jnp.float32,
    )
    queries3 = queries.reshape(seq_count, -1, D)
    keys3 = keys.reshape(seq_count, -1, D)
    values3 = values.reshape(seq_count, -1, D)
    context, lse = attend(lengths, queries3, keys3, values3, table)
    context = context.reshape(-1, D)
    output = stream + forward_dot(context, weights["w_o"]) + vector(weights, "b_o")
    return (output, (normed_b, flat_all, queries3, keys3, values3, table, lse, context))


def attend_backward(stream, weights, stored, grad_out, lengths, onehot):
    normed_b, flat_all, queries3, keys3, values3, table, lse, context = stored
    grad_b = grad_out.astype(jnp.bfloat16)
    gradients = {"w_o": (context, grad_b), "b_o": jnp.sum(grad_out, 0)}
    d_context = back_dot(grad_b, weights["w_o"]).astype(jnp.bfloat16).reshape(queries3.shape)
    dq, dk, dv, dt, sums = attend_back(lengths, queries3, keys3, values3, table, lse, d_context)
    gradients["rel"] = lax.dot_general(
        onehot, dt, (((0,), (1,)), ((), ())), precision=lax.Precision.HIGHEST
    )
    query_b, key_b, value_b = dq.reshape(-1, D), dk.reshape(-1, D), dv.reshape(-1, D)
    remote = back_dot(key_b, weights["w_k"]) + back_dot(value_b, weights["w_v"])
    remote = seq_scatter(remote.astype(jnp.bfloat16).reshape(keys3.shape)).reshape(stream.shape)
    gradients["w_q"] = (normed_b, query_b)
    gradients["b_q"] = sums[0]
    gradients["w_k"] = (flat_all, key_b)
    gradients["w_v"] = (flat_all, value_b)
    gradients["b_v"] = sums[1]
    d_normed = back_dot(query_b, weights["w_q"]) + remote.astype(jnp.float32)
    d_stream, gain_grad, shift_grad = norm_back(
        stream, vector(weights, "attn_ng"), vector(weights, "attn_nb"), d_normed
    )
    gradients["attn_ng"] = gain_grad
    gradients["attn_nb"] = shift_grad
    return (grad_out + d_stream, gradients)


def depthwise(padded, kernel):
    length = padded.shape[1] - kernel.shape[0] + 1
    summed = jnp.zeros((padded.shape[0], length, padded.shape[2]), jnp.float32)
    for offset in range(kernel.shape[0]):
        summed = summed + kernel[offset] * padded[:, offset : offset + length]
    return summed.reshape(-1, padded.shape[2])


def depth_back(padded, d_depth3, d_padded, kernel):
    length = d_depth3.shape[1]
    taps_count = kernel.shape[0]
    kernel_grad = [
        jnp.sum(padded[:, offset : offset + length] * d_depth3, (0, 1))
        for offset in range(taps_count)
    ]
    d_gated = jnp.zeros(d_depth3.shape, jnp.float32)
    for offset in range(taps_count):
        start_at = taps_count - 1 - offset
        d_gated = d_gated + kernel[offset] * d_padded[:, start_at : start_at + length]
    return (kernel_grad, d_gated.reshape(-1, d_depth3.shape[2]))


def conv_front(stream, weights, valid_rows, seq_count):
    normed_b = norm_rows(
        stream, vector(weights, "conv_ng"), vector(weights, "conv_nb")
    ).astype(jnp.bfloat16)
    pre_gate = forward_dot(normed_b, weights["w_pi"]) + vector(weights, "b_pi")
    gated = pre_gate[:, :D] * jax.nn.sigmoid(pre_gate[:, D:]) * valid_rows[:, None]
    padded = with_halo(gated.reshape(seq_count, -1, D), ((SEQ, 1),), K // 2)
    depth = depthwise(padded, vector(weights, "w_depth"))
    return (normed_b, pre_gate, padded, depth)


def conv_tail(stream, weights, depth, batch_mean, inv_std):
    standard = (depth - batch_mean) * inv_std
    normed_bn = standard * vector(weights, "bng") + vector(weights, "bnb")
    active = swish_act(normed_bn).astype(jnp.bfloat16)
    output = stream + forward_dot(active, weights["w_po"]) + vector(weights, "b_po")
    return (output, (standard, normed_bn, active))


def conv_tail_back(weights, stored, grad_out, valid_rows):
    standard, normed_bn, active = stored
    grad_b = grad_out.astype(jnp.bfloat16)
    gradients = {"w_po": (active, grad_b), "b_po": jnp.sum(grad_out, 0)}
    d_normed = back_dot(grad_b, weights["w_po"]) * swish_grad(normed_bn)
    gradients["bng"] = jnp.sum(d_normed * standard, 0)
    gradients["bnb"] = jnp.sum(d_normed, 0)
    d_standard = d_normed * vector(weights, "bng") * valid_rows[:, None]
    return (d_standard, gradients)


def gate_back(stream, weights, normed_b, pre_gate, d_gated, valid_rows, grad_out, kernel_grad):
    linear_half = pre_gate[:, :D]
    gate_sig = jax.nn.sigmoid(pre_gate[:, D:])
    d_gated = d_gated * valid_rows[:, None]
    d_pre = jnp.concatenate(
        [d_gated * gate_sig, d_gated * linear_half * gate_sig * (1.0 - gate_sig)], 1
    )
    d_pre_b = d_pre.astype(jnp.bfloat16)
    gradients = {
        "w_depth": kernel_grad,
        "w_pi": (normed_b, d_pre_b),
        "b_pi": jnp.sum(d_pre, 0),
    }
    d_normed = back_dot(d_pre_b, weights["w_pi"])
    d_stream, gain_grad, shift_grad = norm_back(
        stream, vector(weights, "conv_ng"), vector(weights, "conv_nb"), d_normed
    )
    gradients["conv_ng"] = gain_grad
    gradients["conv_nb"] = shift_grad
    return (grad_out + d_stream, gradients)


def conv_front_back(stream, weights, stored, d_depth, valid_rows, grad_out, seq_count):
    normed_b, pre_gate, padded, depth = stored
    d_depth3 = d_depth.reshape(seq_count, -1, D)
    d_padded = with_halo(d_depth3, ((SEQ, 1),), K // 2)
    kernel_grad, d_gated = depth_back(padded, d_depth3, d_padded, vector(weights, "w_depth"))
    return gate_back(
        stream, weights, normed_b, pre_gate, d_gated, valid_rows, grad_out, kernel_grad
    )


def adam_update(param_vec, grad_in, first_mom, second):
    new_first = BETA_ONE * first_mom + (1.0 - BETA_ONE) * grad_in
    new_second = BETA_TWO * second + (1.0 - BETA_TWO) * grad_in * grad_in
    corr_one = 1.0 - BETA_ONE**STEP
    corr_two = 1.0 - BETA_TWO**STEP
    step_size = new_first / corr_one / (jnp.sqrt(new_second / corr_two) + ADAM_EPS)
    return (param_vec - LEARN_RATE * (step_size + DECAY * param_vec), new_first, new_second)


def per_device(inputs, lengths, rel_bucket, params, moment_one, moment_two, cotangent):
    seq_count, block_len, model_width = inputs.shape
    full_len = block_len * lax.axis_size(SEQ)
    first_pos = lax.axis_index(SEQ) * block_len
    positions = first_pos + jnp.arange(block_len, dtype=jnp.int32)
    valid_own = positions[None, :] < lengths[:, None]
    valid_rows = valid_own.astype(jnp.float32).reshape(-1)
    onehot = bucket_window(rel_bucket, block_len, full_len)
    plan = Plan(lax.axis_size(DP), lax.axis_size(SEQ), params.shape[0])
    gathered = gather(plan, own_block(plan, params))
    weights = unpack(gathered.reshape(-1, LANES))
    stream0 = inputs.reshape(-1, model_width)
    stream1, stored1 = ffn_forward(stream0, weights, "first")
    stream2, stored2 = attend_forward(stream1, weights, lengths, onehot, seq_count)
    stored3 = conv_front(stream2, weights, valid_rows, seq_count)
    depth = stored3[3]
    valid_column = valid_rows[:, None]
    sums = batch_sums(depth, depth, valid_column, 2)
    first_sum, square_sum, token_count = sums[0], sums[1], sums[2, 0]
    batch_mean = first_sum / token_count
    inv_std = lax.rsqrt(square_sum / token_count - batch_mean * batch_mean + BATCH_EPS)
    stream3, stored4 = conv_tail(stream2, weights, depth, batch_mean, inv_std)
    stream4, stored5 = ffn_forward(stream3, weights, "second")
    output = norm_rows(stream4, vector(weights, "fin_g"), vector(weights, "fin_b"))
    grad_out = cotangent.reshape(-1, model_width) * valid_rows[:, None]
    d_stream4, gain_grad, shift_grad = norm_back(
        stream4, vector(weights, "fin_g"), vector(weights, "fin_b"), grad_out
    )
    gradients = {"fin_g": gain_grad, "fin_b": shift_grad}
    d_stream3, partial_grads = ffn_backward(stream3, weights, "second", stored5, d_stream4)
    gradients.update(partial_grads)
    d_standard, partial_grads = conv_tail_back(weights, stored4, d_stream3, valid_rows)
    gradients.update(partial_grads)
    standard = stored4[0]
    sums = batch_sums(d_standard, standard, valid_column, 3)
    sum_dz, sum_dzz = sums[0], sums[1]
    d_depth = (
        valid_rows[:, None]
        * inv_std
        * (d_standard - sum_dz / token_count - standard * sum_dzz / token_count)
    )
    d_stream2, partial_grads = conv_front_back(
        stream2, weights, stored3, d_depth, valid_rows, d_stream3, seq_count
    )
    gradients.update(partial_grads)
    d_stream1, partial_grads = attend_backward(
        stream1, weights, stored2, d_stream2, lengths, onehot
    )
    gradients.update(partial_grads)
    d_stream0, partial_grads = ffn_backward(stream0, weights, "first", stored1, d_stream1)
    gradients.update(partial_grads)
    window = scatter(plan, weight_grads(plan, gradients))
    grad_shard = own_shard(plan, window)
    new_params, new_first, new_second = adam_update(params, grad_shard, moment_one, moment_two)
    return (
        output.reshape(inputs.shape),
        d_stream0.reshape(inputs.shape),
        grad_shard,
        new_params,
        new_first,
        new_second,
    )


def solution(mesh):
    return jax.shard_map(
        per_device,
        mesh=mesh,
        in_specs=(
            P(DP, SEQ, None),
            P(DP),
            P(),
            P((DP, SEQ)),
            P((DP, SEQ)),
            P((DP, SEQ)),
            P(DP, SEQ, None),
        ),
        out_specs=(
            P(DP, SEQ, None),
            P(DP, SEQ, None),
            P((DP, SEQ)),
            P((DP, SEQ)),
            P((DP, SEQ)),
            P((DP, SEQ)),
        ),
        check_vma=False,
    )
```

```python
import functools
import math

import jax
import jax.numpy as jnp
from jax import lax
from jax.experimental import pallas as pl
from jax.experimental.pallas import tpu as pltpu
from jax.sharding import PartitionSpec as P

D = 512
H = 8
HD = 64
FF = 2048
K = 31
NB = 32
DP = "dp"
SEQ = "seq"
STEP = 4


NORM_EPS = 1e-05
BATCH_EPS = 1e-05
LEARN_RATE = 0.005
DECAY = 0.01
BETA_ONE = 0.9
BETA_TWO = 0.98
ADAM_EPS = 1e-08


def segments():

    def feed_block(prefix):
        return [
            (prefix + "_ng", (D,)),
            (prefix + "_nb", (D,)),
            (prefix + "_w_in", (D, FF)),
            (prefix + "_b_in", (FF,)),
            (prefix + "_w_out", (FF, D)),
            (prefix + "_b_out", (D,)),
        ]

    listing = feed_block("first")
    listing = listing + [
        ("attn_ng", (D,)),
        ("attn_nb", (D,)),
        ("w_q", (D, D)),
        ("b_q", (D,)),
        ("w_k", (D, D)),
        ("w_v", (D, D)),
        ("b_v", (D,)),
        ("w_o", (D, D)),
        ("b_o", (D,)),
        ("rel", (NB, H)),
    ]
    listing = listing + [
        ("conv_ng", (D,)),
        ("conv_nb", (D,)),
        ("w_pi", (D, 2 * D)),
        ("b_pi", (2 * D,)),
        ("w_depth", (K, D)),
        ("bng", (D,)),
        ("bnb", (D,)),
        ("w_po", (D, D)),
        ("b_po", (D,)),
    ]
    listing = listing + feed_block("second") + [("fin_g", (D,)), ("fin_b", (D,))]
    return listing


def arrange():
    places, gaps = {}, []
    linear = inner = 0
    for entry_name, entry_shape in segments():
        extent = math.prod(entry_shape)
        tail = 2 * D if entry_name == "conv_ng" else 0
        if extent >= D * D or tail:
            pad = -(inner + tail) % TILE
            if pad:
                gaps.append((linear, pad))
                inner = inner + pad
        places[entry_name] = inner // LANES
        linear, inner = linear + extent, inner + extent
    return places, gaps, -(-inner // TILE)


def unpack(rows):
    result = {}
    places = arrange()[0]
    for entry_name, entry_shape in segments():
        extent = math.prod(entry_shape)
        first = places[entry_name]
        piece = rows[first : first + -(-extent // LANES)]
        if extent < LANES:
            piece = piece[:, :extent]
        result[entry_name] = piece.reshape(entry_shape)
    return result


def device_index():
    return lax.axis_index(DP) * lax.axis_size(SEQ) + lax.axis_index(SEQ)


def own_block(plan, params):
    index = device_index()
    shift_down = [(i + 1, i) for i in range(plan.n - 1)]
    following = lax.ppermute(params[:TILE], (DP, SEQ), shift_down)
    length = plan.hi * TILE
    room = max(length + TILE - plan.shard - TILE, 0)
    front = max(size for _, size in plan.gaps)
    extended = jnp.concatenate(
        [jnp.zeros((front,), jnp.float32), params, following, jnp.zeros((room,), jnp.float32)]
    )
    table = jnp.asarray(plan.block_table, jnp.int32)[index]
    early = lax.dynamic_slice(extended, (front + table[0],), (length,))
    late = lax.dynamic_slice(extended, (front + table[0] - table[2],), (length,))
    block = jnp.where(jnp.arange(length, dtype=jnp.int32) < table[1], early, late)
    return block.astype(jnp.bfloat16).reshape(plan.hi, 8, LANES)


def own_shard(plan, window):
    table = jnp.asarray(plan.shard_table, jnp.int32)[device_index()]
    flat = window.reshape(-1)
    early = lax.dynamic_slice(flat, (table[0],), (plan.shard,))
    late = lax.dynamic_slice(flat, (table[0] + table[2],), (plan.shard,))
    return jnp.where(jnp.arange(plan.shard, dtype=jnp.int32) < table[1], early, late)


def vector(weights, entry_name):
    return weights[entry_name].astype(jnp.float32)


def swish_act(values):
    return values * jax.nn.sigmoid(values)


def swish_grad(values):
    sig_vals = jax.nn.sigmoid(values)
    return sig_vals * (1.0 + values * (1.0 - sig_vals))


def forward_dot(left_mat, weight):
    return jnp.dot(left_mat, weight, preferred_element_type=jnp.float32)


def back_dot(grad_in, weight):
    return lax.dot_general(
        grad_in, weight, (((1,), (1,)), ((), ())), preferred_element_type=jnp.float32
    )


MESH = pl.DeviceIdType.MESH
LANES=512
TILE=8*LANES

class Plan:
    def __init__(self, ndp, nseq, shard):
        self.ndp, self.nseq, self.shard = ndp, nseq, shard
        self.k = ndp.bit_length() - 1
        self.phases = self.k - 1
        self.n = n = ndp * nseq
        self.places, self.gaps, self.total = arrange()
        begins = [self.inner(d * shard) for d in range(n)]
        starts = [-(-b // TILE) for b in begins] + [self.total]
        sizes = [b - a for a, b in zip(starts, starts[1:])]
        self.lo, self.hi = min(sizes), max(sizes)
        self.slots = nseq * 2**self.phases
        floors = [b // TILE for b in begins]
        ends = [self.inner((d + 1) * shard - 1) // TILE + 1 for d in range(n)]
        self.win = max(e - f for e, f in zip(ends, floors))
        self.win += self.win % 2
        self.padded = max(self.total, max(floors) + self.win)
        self.block_table, self.shard_table = [], []
        for d in range(n):
            near = [g for g in self.gaps if d * shard < g[0] < (d + 1) * shard + TILE]
            assert len(near) <= 1
            cut, size = near[0] if near else (2**30, 0)
            lead = starts[d] * TILE - begins[d]
            self.block_table.append((lead, cut - d * shard - lead, size))
            self.shard_table.append((begins[d] - floors[d] * TILE, cut - d * shard, size))

    def inner(self, position):
        if isinstance(position, int):
            return position + sum(size for at, size in self.gaps if at <= position)
        result = position
        for at, size in self.gaps:
            result = result + jnp.where(position >= at, size, 0)
        return result

    def order(self):
        ev=[]
        for s in range(self.nseq):
            for sign in ((0,) if s==0 else (-1,1)):
                for t in range(2**self.phases):
                    ev.append((s+0.5*bin(t).count("1")+0.01*t, s, sign, t))
        ev.sort()
        return [e[1:] for e in ev]

def flip(di, mask_bits, bits, t, phases):
    out=di
    for p in range(phases):
        if (t>>p)&1:
            out = out + mask_bits[p]*(1-2*bits[p])
    return out

def phase_masks(di, c, phases):
    masks, bits=[],[]
    for p in range(phases):
        a, b = 1<<(p+1), 1<<(phases-p)
        masks.append(a+c*(b-a))
        ba, bb = (di//a)%2, (di//b)%2
        bits.append(ba+c*(bb-ba))
    return masks, bits

def block_of(plan, dpi, z):
    d = dpi*plan.nseq+z
    a = (plan.inner(d*plan.shard)+TILE-1)//TILE
    b = (plan.inner((d+1)*plan.shard)+TILE-1)//TILE
    b = jnp.where(d == plan.n-1, plan.total, b)
    return a, b-a

def floor_of(plan, dpi, z):
    return plan.inner((dpi*plan.nseq+z)*plan.shard)//TILE

def gather_kernel(plan, src, out, send_a, send_b, recv_a, recv_b, loc_sem):
    di, z = lax.axis_index(DP), lax.axis_index(SEQ)
    ns, ph = plan.nseq, plan.phases
    c = di%2
    masks, bits = phase_masks(di, c, ph)
    other = di+1-2*c
    omasks, obits = phase_masks(other, 1-c, ph)
    up, down = lax.rem(z+1,ns), lax.rem(z+ns-1,ns)
    partners=[(di,up),(di,down),(other,z)]+[(flip(di,masks,bits,1<<p,ph),z) for p in range(ph)]
    barrier=pltpu.get_barrier_semaphore()
    for a,b in partners:
        pl.semaphore_signal(barrier,inc=1,device_id=(a,b),device_id_type=MESH)
    pl.semaphore_wait(barrier,len(partners))
    lo, more = plan.lo, plan.hi-plan.lo
    start_own, size_own = block_of(plan, di, z)

    def pair(ref, base, dst_start, size, sidx, ridx, dev):
        copies=[pltpu.make_async_remote_copy(src_ref=ref.at[pl.ds(base,lo)],dst_ref=out.at[pl.ds(dst_start,lo)],
            send_sem=send_a.at[sidx],recv_sem=recv_a.at[ridx],device_id=dev,device_id_type=MESH)]
        for x in range(more):
            copies.append(pltpu.make_async_remote_copy(src_ref=ref.at[pl.ds(base+lo+x,1)],dst_ref=out.at[pl.ds(dst_start+lo+x,1)],
                send_sem=send_b.at[sidx*more+x],recv_sem=recv_b.at[ridx*more+x],device_id=dev,device_id_type=MESH))
        return copies, size
    def each(p, act):
        for x,copy in enumerate(p[0]):
            if x==0: act(copy)
            else:
                @pl.when(p[1]>=lo+x)
                def _(): act(copy)
    def start(p): each(p, lambda c: c.start())
    def wait_send(p): each(p, lambda c: c.wait_send())
    def wait_recv(p): each(p, lambda c: c.wait_recv())

    own=[pltpu.make_async_copy(src.at[pl.ds(0,lo)],out.at[pl.ds(start_own,lo)],loc_sem.at[0])]
    for x in range(more):
        own.append(pltpu.make_async_copy(src.at[pl.ds(lo+x,1)],out.at[pl.ds(start_own+lo+x,1)],loc_sem.at[1+x]))
    own=(own,size_own)
    start(own)
    nslot=plan.slots
    sends=[]
    sidx=[0]
    def forward(conds, ref, base, st, size, ridx, dev):
        i=sidx[0]; sidx[0]+=1
        p=pair(ref,base,st,size,i,ridx,dev)
        sends.append((conds,p))
        guard(conds, lambda: start(p))
    def guard(conds, fn):
        if not conds: fn(); return
        cond=conds[0]
        for x in conds[1:]: cond=jnp.logical_and(cond,x)
        @pl.when(cond)
        def _(): fn()

    for s, sign, t in plan.order():
        zz = z+sign*s
        conds=[] if s==0 else ([zz>=0] if sign<0 else [zz<ns])
        dpi=flip(di,masks,bits,t,ph)
        st,size=block_of(plan,dpi,zz)
        mine = s==0 and t==0
        ref, base = (src, 0) if mine else (out, st)
        slot = t*ns+zz
        if not mine:
            p=pair(out,st,st,size,0,slot,(di,z))
            guard(conds, lambda: wait_recv(p))
        if t==0:
            if sign<=0 : forward(conds+[z<ns-1],ref,base,st,size,slot,(di,z+1))
            if sign>=0 : forward(conds+[z>0],ref,base,st,size,slot,(di,z-1))
        hi_bit=t.bit_length()
        for pp in range(hi_bit,ph):
            forward(conds,ref,base,st,size,slot+(1<<pp)*ns,(flip(di,masks,bits,1<<pp,ph),z))
        forward(conds,ref,base,st,size,nslot+slot,(other,z))
    for s, sign, t in plan.order():
        zz=z+sign*s
        conds=[] if s==0 else ([zz>=0] if sign<0 else [zz<ns])
        dpi=flip(other,omasks,obits,t,ph)
        st,size=block_of(plan,dpi,zz)
        p=pair(out,st,st,size,0,nslot+t*ns+zz,(di,z))
        guard(conds,lambda: wait_recv(p))
    for conds,p in sends:
        guard(conds,lambda: wait_send(p))
    each(own, lambda c: c.wait())

def count_sends(plan):
    n=0
    for s,sign,t in plan.order():
        if t==0: n+= (2 if sign==0 else 1)
        n+=plan.phases-t.bit_length()+1
    return n

def gather(plan, block):
    ns=count_sends(plan)
    more=max(plan.hi-plan.lo,1)
    return pl.pallas_call(
        functools.partial(gather_kernel,plan),
        out_shape=jax.ShapeDtypeStruct((plan.total,8,LANES),block.dtype),
        in_specs=[pl.BlockSpec(memory_space=pl.ANY)],
        out_specs=pl.BlockSpec(memory_space=pl.ANY),
        scratch_shapes=[pltpu.SemaphoreType.DMA((ns,)),pltpu.SemaphoreType.DMA((ns*more,)),
            pltpu.SemaphoreType.DMA((2*plan.slots,)),pltpu.SemaphoreType.DMA((2*plan.slots*more,)),pltpu.SemaphoreType.DMA((1+more,))],
        compiler_params=pltpu.CompilerParams(collective_id=0,has_side_effects=True),
        name="gather_params",
    )(block)

def scatter_kernel(plan, g, out, acc, rc, rp, rz, load_sem, send_sem, core_send, core_recv, ph_recv, z_recv):
    di, z = lax.axis_index(DP), lax.axis_index(SEQ)
    ns, ph, win, nslot = plan.nseq, plan.phases, plan.win, plan.slots
    c = di%2
    masks, bits = phase_masks(di, c, ph)
    other = di+1-2*c
    omasks, obits = phase_masks(other, 1-c, ph)
    up, down = lax.rem(z+1,ns), lax.rem(z+ns-1,ns)
    partners=[(di,up),(di,down),(other,z)]+[(flip(di,masks,bits,1<<p,ph),z) for p in range(ph)]
    barrier=pltpu.get_barrier_semaphore()
    for a,b in partners:
        pl.semaphore_signal(barrier,inc=1,device_id=(a,b),device_id_type=MESH)
    order=list(reversed(plan.order()))
    def cond_of(s,sign):
        zz=z+sign*s
        return zz,([] if s==0 else ([zz>=0] if sign<0 else [zz<ns]))
    def guard(conds, fn):
        if not conds: fn(); return
        cond=conds[0]
        for x in conds[1:]: cond=jnp.logical_and(cond,x)
        @pl.when(cond)
        def _(): fn()
    def load(s,sign,t):
        zz,conds=cond_of(s,sign)
        slot=t*ns+zz
        st=floor_of(plan,flip(di,masks,bits,t,ph),zz)
        return conds,pltpu.make_async_copy(g.at[pl.ds(st,win)],acc.at[slot],load_sem.at[slot])
    def core(s,sign,t):
        zz,conds=cond_of(s,sign)
        slot=t*ns+zz
        st=floor_of(plan,flip(other,omasks,obits,t,ph),zz)
        return conds,pltpu.make_async_remote_copy(src_ref=g.at[pl.ds(st,win)],dst_ref=rc.at[slot],
            send_sem=core_send.at[slot],recv_sem=core_recv.at[slot],device_id=(other,z),device_id_type=MESH)
    for e in order:
        conds,cp=load(*e)
        guard(conds,lambda: cp.start())
    pl.semaphore_wait(barrier,len(partners))
    for e in order:
        conds,cp=core(*e)
        guard(conds,lambda: cp.start())
    sends=[]
    def send(conds,slot,dst,rsem,dev):
        i=len(sends)
        cp=pltpu.make_async_remote_copy(src_ref=acc.at[slot],dst_ref=dst,send_sem=send_sem.at[i],recv_sem=rsem,
            device_id=dev,device_id_type=MESH)
        sends.append((conds,cp))
        guard(conds,lambda: cp.start())
    def waiting(conds,dst,rsem):
        cp=pltpu.make_async_remote_copy(src_ref=dst,dst_ref=dst,send_sem=send_sem.at[0],recv_sem=rsem,
            device_id=(di,z),device_id_type=MESH)
        guard(conds,lambda: cp.wait_recv())
    step=2
    def add(dst, slot, parts, final=False):
        @pl.loop(0,win//step)
        def _(i):
            r=pl.ds(i*step,step)
            v=acc[slot,r].astype(jnp.float32)
            for p in parts:
                v=v+p(r).astype(jnp.float32)
            if final: out[r]=v
            else: acc[slot,r]=v.astype(acc.dtype)
    for s,sign,t in order:
        zz,conds=cond_of(s,sign)
        slot=t*ns+zz
        hi_bit=t.bit_length()
        def fn():
            load(s,sign,t)[1].wait()
            waiting([],rc.at[slot],core_recv.at[slot])
            parts=[lambda r: rc[slot,r]]
            for pp in range(hi_bit,ph):
                idx=((1<<pp)-1)*ns+slot
                waiting([],rp.at[idx],ph_recv.at[idx])
                parts.append(lambda r,idx=idx: rp[idx,r])
            add(None,slot,parts,final=False) if not (t==0 and s==0) else add(None,slot,parts,final=True)
        guard(conds,fn)
        if t:
            pp=hi_bit-1
            idx=((1<<pp)-1)*ns+slot-(1<<pp)*ns
            send(conds,slot,rp.at[idx],ph_recv.at[idx],(flip(di,masks,bits,1<<pp,ph),z))
        else:
            def zadd(stream, extra):
                zi=stream*ns+zz
                def fz():
                    waiting([],rz.at[zi],z_recv.at[zi])
                    @pl.loop(0,win//step)
                    def _(i):
                        r=pl.ds(i*step,step)
                        if s==0:
                            out[r]=out[r]+rz[zi,r].astype(jnp.float32)
                        else:
                            acc[slot,r]=(acc[slot,r].astype(jnp.float32)+rz[zi,r].astype(jnp.float32)).astype(acc.dtype)
                guard(conds+extra,fz)
            if sign>=0: zadd(0,[z>0])
            if sign<=0: zadd(1,[z<ns-1])
            if sign>0: send(conds,slot,rz.at[zz],z_recv.at[zz],(di,z+1))
            if sign<0: send(conds,slot,rz.at[ns+zz],z_recv.at[ns+zz],(di,z-1))
    for e in order:
        conds,cp=core(*e)
        guard(conds,lambda: cp.wait_send())
    for conds,cp in sends:
        guard(conds,lambda: cp.wait_send())

def scatter(plan, g):
    win,ns,ph,nslot=plan.win,plan.nseq,plan.phases,plan.slots
    nsend=len(plan.order())
    return pl.pallas_call(
        functools.partial(scatter_kernel,plan),
        out_shape=jax.ShapeDtypeStruct((win,8,LANES),jnp.float32),
        in_specs=[pl.BlockSpec(memory_space=pl.ANY)],
        out_specs=pl.BlockSpec(memory_space=pltpu.VMEM),
        scratch_shapes=[pltpu.VMEM((nslot,win,8,LANES),g.dtype),pltpu.VMEM((nslot,win,8,LANES),g.dtype),
            pltpu.VMEM(((2**ph-1)*ns,win,8,LANES),g.dtype),pltpu.VMEM((2*ns,win,8,LANES),g.dtype),
            pltpu.SemaphoreType.DMA((nslot,)),pltpu.SemaphoreType.DMA((nsend,)),
            pltpu.SemaphoreType.DMA((nslot,)),pltpu.SemaphoreType.DMA((nslot,)),
            pltpu.SemaphoreType.DMA(((2**ph-1)*ns,)),pltpu.SemaphoreType.DMA((2*ns,))],
        compiler_params=pltpu.CompilerParams(collective_id=1,has_side_effects=True,vmem_limit_bytes=48*1024*1024),
        name="scatter_grads",
    )(g)


def weight_kernel(plan, names, places, *refs):
    pairs = {name: refs[2 * i : 2 * i + 2] for i, name in enumerate(names)}
    vectors = refs[2 * len(names) : -2]
    out, mix = refs[-2:]
    rows = (((0,), (0,)), ((), ()))
    for name, shape in segments():
        first = plan.places[name]
        if math.prod(shape) < D * D:
            array, begin = places[name]
            for r in range(-(-math.prod(shape) // LANES)):
                line = vectors[array][begin + r : begin + r + 1, :]
                tile, row = divmod(first + r, 8)
                out[tile, row : row + 1, : line.shape[1]] = line.astype(out.dtype)
            continue
        left, right = pairs[name]
        fold = shape[1] // LANES
        step = 256 if fold == 1 else 128

        @pl.loop(0, shape[0] // step)
        def _(i):
            part = left[:, pl.ds(pl.multiple_of(i * step, step), step)]
            value = lax.dot_general(part, right[...], rows, preferred_element_type=jnp.float32)
            if fold > 1:
                for j in range(fold):
                    for lane in range(LANES // 128):
                        at = j * LANES + lane * 128
                        mix[lane, pl.ds(j, step, stride=fold), :] = value[:, at : at + 128]
                value = jnp.concatenate([mix[lane, : step * fold] for lane in range(LANES // 128)], 1)
            tiles = step * fold // 8
            out[pl.ds(first // 8 + i * tiles, tiles)] = value.astype(out.dtype).reshape(tiles, 8, LANES)


def weight_grads(plan, gradients, vectors, places):
    names = list(gradients)
    operands = [value for name in names for value in gradients[name]] + vectors
    return pl.pallas_call(
        functools.partial(weight_kernel, plan, names, places),
        out_shape=jax.ShapeDtypeStruct((plan.padded, 8, LANES), jnp.bfloat16),
        in_specs=[VMEM_SPEC] * len(operands),
        out_specs=VMEM_SPEC,
        scratch_shapes=[pltpu.VMEM((LANES // 128, 512, 128), jnp.float32)],
        compiler_params=pltpu.CompilerParams(vmem_limit_bytes=60 * 1024 * 1024),
        name="weight_grads",
    )(*operands)


def bucket_window(rel_bucket, block_len, full_len):
    first_pos = lax.axis_index(SEQ) * block_len
    width = -(-(block_len + full_len - 1) // 128) * 128
    padded = jnp.concatenate([rel_bucket, jnp.full((width,), -1, jnp.int32)])
    window = lax.dynamic_slice(padded, (full_len - block_len - first_pos,), (width,))
    return (window[:, None] == jnp.arange(NB, dtype=jnp.int32)[None, :]).astype(jnp.float32)


def head_scores(q, k, table, valid, head):
    block, width = q.shape[0], table.shape[1]
    full = k.shape[0]
    scores = lax.dot_general(q, k, (((1,), (1,)), ((), ())), preferred_element_type=jnp.float32)
    spread = jnp.broadcast_to(table[head : head + 1], (block, width))
    bias = pltpu.roll(spread, width - block + 1, 1, stride=1, stride_axis=0)[:, :full]
    return jnp.where(valid, scores * (1.0 / math.sqrt(HD)) + bias, -jnp.inf)


def attend_kernel(len_ref, q_ref, k_ref, v_ref, t_ref, ctx_ref, lse_ref):
    full = k_ref.shape[1]
    block = q_ref.shape[1]
    valid = lax.broadcasted_iota(jnp.int32, (1, full), 1) < len_ref[pl.program_id(0)]
    lane = lax.broadcasted_iota(jnp.int32, (block, 128), 1)
    lse = jnp.zeros((block, 128), jnp.float32)
    for h in range(H):
        cols = slice(h * HD, (h + 1) * HD)
        scores = head_scores(q_ref[0, :, cols], k_ref[0, :, cols], t_ref[...], valid, h)
        top = jnp.max(scores, -1, keepdims=True)
        weights = jnp.exp(scores - top)
        total = jnp.sum(weights, -1, keepdims=True)
        probs = (weights * (1.0 / total)).astype(jnp.bfloat16)
        ctx = jnp.dot(probs, v_ref[0, :, cols], preferred_element_type=jnp.float32)
        ctx_ref[0, :, cols] = ctx.astype(jnp.bfloat16)
        lse = jnp.where(lane == h, top + jnp.log(total), lse)
    lse_ref[0] = lse


def attend_back_kernel(len_ref, q_ref, k_ref, v_ref, t_ref, lse_ref, dctx_ref,
                       dq_ref, dk_ref, dv_ref, dt_ref, sums_ref):
    full = k_ref.shape[1]
    block = q_ref.shape[1]
    width = t_ref.shape[1]
    seq_id = pl.program_id(0)

    @pl.when(seq_id == 0)
    def _():
        dt_ref[...] = jnp.zeros_like(dt_ref)
        sums_ref[...] = jnp.zeros_like(sums_ref)

    valid = lax.broadcasted_iota(jnp.int32, (1, full), 1) < len_ref[seq_id]
    rows = (((0,), (0,)), ((), ()))
    for h in range(H):
        cols = slice(h * HD, (h + 1) * HD)
        q, k, v = q_ref[0, :, cols], k_ref[0, :, cols], v_ref[0, :, cols]
        dctx = dctx_ref[0, :, cols]
        scores = head_scores(q, k, t_ref[...], valid, h)
        probs = jnp.exp(scores - lse_ref[0, :, h : h + 1])
        d_probs = lax.dot_general(dctx, v, (((1,), (1,)), ((), ())), preferred_element_type=jnp.float32)
        delta = jnp.sum(probs * d_probs, -1, keepdims=True)
        d_scores = probs * (d_probs - delta)
        d_scores_b = d_scores.astype(jnp.bfloat16)
        dq = jnp.dot(d_scores_b, k, preferred_element_type=jnp.float32) * (1.0 / math.sqrt(HD))
        dk = lax.dot_general(d_scores_b, q, rows, preferred_element_type=jnp.float32)
        dv = lax.dot_general(probs.astype(jnp.bfloat16), dctx, rows, preferred_element_type=jnp.float32)
        dq_ref[0, :, cols] = dq.astype(jnp.bfloat16)
        dk_ref[0, :, cols] = (dk * (1.0 / math.sqrt(HD))).astype(jnp.bfloat16)
        dv_ref[0, :, cols] = dv.astype(jnp.bfloat16)
        sums_ref[0:1, cols] += jnp.sum(dq, 0, keepdims=True)
        sums_ref[1:2, cols] += jnp.sum(dv, 0, keepdims=True)
        wide = jnp.concatenate([d_scores, jnp.zeros((block, width - full), jnp.float32)], 1)
        folded = wide[0:8]
        folded = pltpu.roll(folded, block - 1, 1)
        for g in range(1, block // 8):
            folded = folded + pltpu.roll(wide[8 * g : 8 * g + 8], block - 1 - 8 * g, 1)
        line = folded[0:1]
        for r in range(1, 8):
            line = line + pltpu.roll(folded[r : r + 1], width - r, 1)
        dt_ref[h : h + 1, :] += line


def attend(lengths, queries, keys, values, table):
    seqs, block, width = queries.shape
    full = keys.shape[1]
    return pl.pallas_call(
        attend_kernel,
        grid_spec=pltpu.PrefetchScalarGridSpec(
            num_scalar_prefetch=1,
            grid=(seqs,),
            in_specs=[
                pl.BlockSpec((1, block, width), lambda s, n: (s, 0, 0)),
                pl.BlockSpec((1, full, width), lambda s, n: (s, 0, 0)),
                pl.BlockSpec((1, full, width), lambda s, n: (s, 0, 0)),
                pl.BlockSpec(table.shape, lambda s, n: (0, 0)),
            ],
            out_specs=[
                pl.BlockSpec((1, block, width), lambda s, n: (s, 0, 0)),
                pl.BlockSpec((1, block, 128), lambda s, n: (s, 0, 0)),
            ],
        ),
        out_shape=[
            jax.ShapeDtypeStruct((seqs, block, width), jnp.bfloat16),
            jax.ShapeDtypeStruct((seqs, block, 128), jnp.float32),
        ],
        name="attend",
    )(lengths, queries, keys, values, table)


def attend_back(lengths, queries, keys, values, table, lse, d_context):
    seqs, block, width = queries.shape
    full = keys.shape[1]
    return pl.pallas_call(
        attend_back_kernel,
        grid_spec=pltpu.PrefetchScalarGridSpec(
            num_scalar_prefetch=1,
            grid=(seqs,),
            in_specs=[
                pl.BlockSpec((1, block, width), lambda s, n: (s, 0, 0)),
                pl.BlockSpec((1, full, width), lambda s, n: (s, 0, 0)),
                pl.BlockSpec((1, full, width), lambda s, n: (s, 0, 0)),
                pl.BlockSpec(table.shape, lambda s, n: (0, 0)),
                pl.BlockSpec((1, block, 128), lambda s, n: (s, 0, 0)),
                pl.BlockSpec((1, block, width), lambda s, n: (s, 0, 0)),
            ],
            out_specs=[
                pl.BlockSpec((1, block, width), lambda s, n: (s, 0, 0)),
                pl.BlockSpec((1, full, width), lambda s, n: (s, 0, 0)),
                pl.BlockSpec((1, full, width), lambda s, n: (s, 0, 0)),
                pl.BlockSpec(table.shape, lambda s, n: (0, 0)),
                pl.BlockSpec((8, width), lambda s, n: (0, 0)),
            ],
        ),
        out_shape=[
            jax.ShapeDtypeStruct((seqs, block, width), jnp.bfloat16),
            jax.ShapeDtypeStruct((seqs, full, width), jnp.bfloat16),
            jax.ShapeDtypeStruct((seqs, full, width), jnp.bfloat16),
            jax.ShapeDtypeStruct(table.shape, jnp.float32),
            jax.ShapeDtypeStruct((8, width), jnp.float32),
        ],
        name="attend_back",
    )(lengths, queries, keys, values, table, lse, d_context)


def seq_gather(rows, seq_count):
    return lax.all_gather(rows.reshape(seq_count, -1, D), SEQ, axis=1, tiled=True)


def seq_scatter(rows):
    return lax.psum_scatter(rows, SEQ, scatter_dimension=1, tiled=True)


def attend_forward(normed_b, queries, weights, lengths, onehot, seq_count):
    normed_all = seq_gather(normed_b, seq_count)
    flat_all = normed_all.reshape(-1, D)
    keys = forward_dot(flat_all, weights["w_k"]).astype(jnp.bfloat16)
    values = (forward_dot(flat_all, weights["w_v"]) + vector(weights, "b_v")).astype(jnp.bfloat16)
    table = lax.dot_general(
        weights["rel"], onehot.astype(jnp.bfloat16), (((0,), (1,)), ((), ())),
        preferred_element_type=jnp.float32,
    )
    queries3 = queries.reshape(seq_count, -1, D)
    keys3 = keys.reshape(seq_count, -1, D)
    values3 = values.reshape(seq_count, -1, D)
    context, lse = attend(lengths, queries3, keys3, values3, table)
    return context.reshape(-1, D), (flat_all, queries3, keys3, values3, table, lse)


def attend_backward(weights, stored, d_context, lengths, onehot):
    flat_all, queries3, keys3, values3, table, lse = stored
    d_context = d_context.reshape(queries3.shape)
    dq, dk, dv, dt, sums = attend_back(lengths, queries3, keys3, values3, table, lse, d_context)
    rel_grad = lax.dot_general(onehot, dt, (((0,), (1,)), ((), ())), precision=lax.Precision.HIGHEST)
    query_b, key_b, value_b = dq.reshape(-1, D), dk.reshape(-1, D), dv.reshape(-1, D)
    remote = back_dot(key_b, weights["w_k"]) + back_dot(value_b, weights["w_v"])
    remote = seq_scatter(remote.astype(jnp.bfloat16).reshape(keys3.shape)).reshape(query_b.shape)
    gradients = {"w_k": (flat_all, key_b), "w_v": (flat_all, value_b)}
    return query_b, remote, rel_grad.reshape(1, -1), sums, gradients


def adam_update(param_vec, grad_in, first_mom, second):
    new_first = BETA_ONE * first_mom + (1.0 - BETA_ONE) * grad_in
    new_second = BETA_TWO * second + (1.0 - BETA_TWO) * grad_in * grad_in
    corr_one = 1.0 - BETA_ONE**STEP
    corr_two = 1.0 - BETA_TWO**STEP
    step_size = new_first / corr_one / (jnp.sqrt(new_second / corr_two) + ADAM_EPS)
    return (param_vec - LEARN_RATE * (step_size + DECAY * param_vec), new_first, new_second)


def unit_rows(values):
    centre = values - jnp.mean(values, -1, keepdims=True)
    scale = lax.rsqrt(jnp.mean(centre * centre, -1, keepdims=True) + NORM_EPS)
    return centre * scale, scale


def unit_back(unit, scale, gain, grad):
    shifted = grad * gain
    first = jnp.mean(shifted, -1, keepdims=True)
    second = jnp.mean(shifted * unit, -1, keepdims=True)
    return scale * (shifted - first - unit * second), total_rows(grad * unit), total_rows(grad)


def total_rows(values):
    return jnp.sum(values, 0, keepdims=True)


def split_rows(source, mix, target, fold):
    block = mix.shape[1]
    lanes = LANES // 128

    @pl.loop(0, source.shape[0] // block)
    def _(i):
        part = source[pl.ds(pl.multiple_of(i * block, block), block), :].astype(jnp.float32)
        for lane in range(lanes):
            mix[lane] = part[:, lane * 128 : (lane + 1) * 128]
        for j in range(fold):
            rows = [mix[lane, pl.ds(j, block // fold, stride=fold), :] for lane in range(lanes)]
            at = pl.multiple_of(i * (block // fold), block // fold)
            target[j, pl.ds(at, block // fold), :] = jnp.concatenate(rows, 1).astype(target.dtype)


class Fetch:
    def __init__(self, plan, packed, sem):
        self.plan, self.packed, self.sem, self.count = plan, packed, sem, 0

    def __call__(self, name, target):
        row = self.plan.places[name] // 8 * 8
        copy = pltpu.make_async_copy(
            self.packed.at[pl.ds(row, target.shape[0])], target, self.sem.at[self.count]
        )
        self.count += 1
        copy.start()
        return copy


def wait_all(*copies):
    for copy in copies:
        copy.wait()


def ffn_first_kernel(plan, x, packed, x_out, n_out, q_out, w_out, w_in, w_second, w_q, v0, v1, v2, v3, mix, sem):
    fetch = Fetch(plan, packed, sem)
    early = [fetch("first_ng", v0), fetch("first_b_in", v1), fetch("first_b_out", v2), fetch("b_q", v3)]
    in_copy = fetch("first_w_in", w_in)
    late = [fetch("first_w_out", w_second), fetch("w_q", w_q)]
    wait_all(*early)
    gains, bias_in, tail = v0[...].astype(jnp.float32), v1[...].astype(jnp.float32), v2[...].astype(jnp.float32)
    stream = x[...]
    unit, _ = unit_rows(stream)
    normed = (unit * gains[0:1] + gains[1:2]).astype(jnp.bfloat16)
    in_copy.wait()
    split_rows(w_in, mix, w_out, FF // LANES)
    wait_all(*late)
    total = jnp.zeros(stream.shape, jnp.float32)
    for j in range(FF // LANES):
        hidden = forward_dot(normed, w_out[j]) + bias_in[j : j + 1]
        active = swish_act(hidden).astype(jnp.bfloat16)
        total = total + forward_dot(active, w_second[j * LANES : (j + 1) * LANES, :])
    stream = stream + 0.5 * (total + tail[0:1])
    x_out[...] = stream
    unit, _ = unit_rows(stream)
    normed = (unit * tail[1:2] + tail[2:3]).astype(jnp.bfloat16)
    n_out[...] = normed
    q_out[...] = (forward_dot(normed, w_q[...]) + v3[...].astype(jnp.float32)[0:1]).astype(jnp.bfloat16)


def ffn_first_back_kernel(plan, x, x_one, d_two, d_query, remote, w_in, packed,
                          d_out, a_out, r_out, n_out, h_out, vec_out, w_second, w_q, v0, v1, v2, sem):
    fetch = Fetch(plan, packed, sem)
    early = [fetch("first_ng", v0), fetch("first_b_in", v1), fetch("first_b_out", v2), fetch("w_q", w_q)]
    late = fetch("first_w_out", w_second)
    wait_all(*early)
    gains, bias_in, tail = v0[...].astype(jnp.float32), v1[...].astype(jnp.float32), v2[...].astype(jnp.float32)
    unit, scale = unit_rows(x_one[...])
    d_normed = back_dot(d_query[...], w_q[...]) + remote[...].astype(jnp.float32)
    d_norm, gain_grad, shift_grad = unit_back(unit, scale, tail[1:2], d_normed)
    vec_out[0:1] = gain_grad
    vec_out[1:2] = shift_grad
    grad = d_two[...] + d_norm
    half = 0.5 * grad
    vec_out[2:3] = total_rows(half)
    half_b = half.astype(jnp.bfloat16)
    r_out[...] = half_b
    unit, scale = unit_rows(x[...])
    normed = (unit * gains[0:1] + gains[1:2]).astype(jnp.bfloat16)
    n_out[...] = normed
    late.wait()
    d_normed = jnp.zeros(grad.shape, jnp.float32)
    for j in range(FF // LANES):
        cols = slice(j * LANES, (j + 1) * LANES)
        hidden = forward_dot(normed, w_in[j]) + bias_in[j : j + 1]
        a_out[:, cols] = swish_act(hidden).astype(jnp.bfloat16)
        d_hidden = back_dot(half_b, w_second[cols, :]) * swish_grad(hidden)
        vec_out[5 + j : 6 + j] = total_rows(d_hidden)
        d_hidden = d_hidden.astype(jnp.bfloat16)
        h_out[:, cols] = d_hidden
        d_normed = d_normed + back_dot(d_hidden, w_in[j])
    d_norm, gain_grad, shift_grad = unit_back(unit, scale, gains[0:1], d_normed)
    vec_out[3:4] = gain_grad
    vec_out[4:5] = shift_grad
    d_out[...] = grad + d_norm


def gate_kernel(plan, ctx, x, valid, packed, x_out, n_out, g_out, u_out, w_out, w_o, w_pi, v0, v1, mix, sem):
    fetch = Fetch(plan, packed, sem)
    early = [fetch("w_o", w_o), fetch("b_o", v0), fetch("b_pi", v1)]
    late = fetch("w_pi", w_pi)
    wait_all(*early)
    rows, bias_in = v0[...].astype(jnp.float32), v1[...].astype(jnp.float32)
    stream = x[...] + forward_dot(ctx[...], w_o[...]) + rows[0:1]
    x_out[...] = stream
    unit, _ = unit_rows(stream)
    normed = (unit * rows[6:7] + rows[7:8]).astype(jnp.bfloat16)
    n_out[...] = normed
    late.wait()
    split_rows(w_pi, mix, w_out, 2)
    linear = forward_dot(normed, w_out[0]) + bias_in[0:1]
    gate = forward_dot(normed, w_out[1]) + bias_in[1:2]
    g_out[:, :D] = linear
    g_out[:, D:] = gate
    u_out[...] = linear * jax.nn.sigmoid(gate) * valid[...]


def gate_back_kernel(plan, du, pre_gate, x, d_three, valid, w_pi, packed,
                     g_out, d_out, o_out, c_out, vec_out, w_o, v0, sem):
    fetch = Fetch(plan, packed, sem)
    copies = [fetch("b_o", v0), fetch("w_o", w_o)]
    d_gated = du[...] * valid[...]
    gate_sig = jax.nn.sigmoid(pre_gate[:, D:])
    d_linear = d_gated * gate_sig
    d_gate = d_gated * pre_gate[:, :D] * gate_sig * (1.0 - gate_sig)
    vec_out[0:1] = total_rows(d_linear)
    vec_out[1:2] = total_rows(d_gate)
    d_linear, d_gate = d_linear.astype(jnp.bfloat16), d_gate.astype(jnp.bfloat16)
    g_out[:, :D] = d_linear
    g_out[:, D:] = d_gate
    d_normed = back_dot(d_linear, w_pi[0]) + back_dot(d_gate, w_pi[1])
    unit, scale = unit_rows(x[...])
    wait_all(*copies)
    d_norm, gain_grad, shift_grad = unit_back(unit, scale, v0[...].astype(jnp.float32)[6:7], d_normed)
    vec_out[2:3] = gain_grad
    vec_out[3:4] = shift_grad
    grad = d_three[...] + d_norm
    d_out[...] = grad
    vec_out[4:5] = total_rows(grad)
    grad_b = grad.astype(jnp.bfloat16)
    o_out[...] = grad_b
    c_out[...] = back_dot(grad_b, w_o[...]).astype(jnp.bfloat16)


def middle_kernel(plan, x, depth, sums, cot, valid, packed,
                  y_out, d_out, z_out, part_out, stat_out, e_out, rb_out, a_out, r_out, n_out, h_out, vec_out,
                  w_po, w_in, w_second, w_mix, held, v_bn, v0, v1, v2, mix, sem):
    fetch = Fetch(plan, packed, sem)
    early = [fetch("b_pi", v_bn), fetch("w_po", w_po), fetch("b_po", v0), fetch("second_b_in", v1)]
    early.append(fetch("second_b_out", v2))
    in_copy = fetch("second_w_in", w_in)
    late = fetch("second_w_out", w_second)
    wait_all(*early)
    base = plan.places["bng"] - plan.places["b_pi"]
    batch, head = v_bn[...].astype(jnp.float32), v0[...].astype(jnp.float32)
    bias_in, tail = v1[...].astype(jnp.float32), v2[...].astype(jnp.float32)
    gain, shift = batch[base : base + 1], batch[base + 1 : base + 2]
    count = sums[2:3]
    mean = sums[0:1] / count
    inv_std = lax.rsqrt(sums[1:2] / count - mean * mean + BATCH_EPS)
    stat_out[0:1] = mean
    stat_out[1:2] = inv_std
    stat_out[2:3] = count
    stat_out[3:8] = jnp.zeros((5, D), jnp.float32)
    standard = (depth[...] - mean) * inv_std
    e_out[...] = swish_act(standard * gain + shift).astype(jnp.bfloat16)
    three = x[...] + forward_dot(e_out[...], w_po[...]) + head[0:1]
    unit, scale = unit_rows(three)
    n_out[...] = (unit * head[1:2] + head[2:3]).astype(jnp.bfloat16)
    in_copy.wait()
    split_rows(w_in, mix, w_mix, FF // LANES)
    late.wait()
    total = jnp.zeros(three.shape, jnp.float32)
    for j in range(FF // LANES):
        cols = slice(j * LANES, (j + 1) * LANES)
        hidden = forward_dot(n_out[...], w_mix[j]) + bias_in[j : j + 1]
        held[j] = hidden
        active = swish_act(hidden).astype(jnp.bfloat16)
        a_out[:, cols] = active
        total = total + forward_dot(active, w_second[cols, :])
    four = three + 0.5 * (total + tail[0:1])
    last, last_scale = unit_rows(four)
    y_out[...] = last * tail[1:2] + tail[2:3]
    grad = cot[...] * valid[...]
    grad, gain_grad, shift_grad = unit_back(last, last_scale, tail[1:2], grad)
    vec_out[0:1] = gain_grad
    vec_out[1:2] = shift_grad
    half = 0.5 * grad
    vec_out[2:3] = total_rows(half)
    r_out[...] = half.astype(jnp.bfloat16)
    d_normed = jnp.zeros(three.shape, jnp.float32)
    for j in range(FF // LANES):
        cols = slice(j * LANES, (j + 1) * LANES)
        d_hidden = back_dot(r_out[...], w_second[cols, :]) * swish_grad(held[j])
        vec_out[8 + j : 9 + j] = total_rows(d_hidden)
        d_hidden = d_hidden.astype(jnp.bfloat16)
        h_out[:, cols] = d_hidden
        d_normed = d_normed + back_dot(d_hidden, w_mix[j])
    d_norm, gain_grad, shift_grad = unit_back(unit, scale, head[1:2], d_normed)
    vec_out[3:4] = gain_grad
    vec_out[4:5] = shift_grad
    grad = grad + d_norm
    d_out[...] = grad
    vec_out[5:6] = total_rows(grad)
    rb_out[...] = grad.astype(jnp.bfloat16)
    standard = (depth[...] - mean) * inv_std
    d_active = back_dot(rb_out[...], w_po[...]) * swish_grad(standard * gain + shift)
    d_gain, d_shift = total_rows(d_active * standard), total_rows(d_active)
    vec_out[6:7] = d_gain
    vec_out[7:8] = d_shift
    vec_out[12:16] = jnp.zeros((4, D), jnp.float32)
    d_standard = d_active * gain * valid[...]
    z_out[...] = d_standard
    part_out[0:1] = total_rows(d_standard)
    part_out[1:2] = total_rows(d_standard * standard)
    part_out[2:8] = jnp.zeros((6, D), jnp.float32)


def group_barrier(ndp, nseq):
    di, z = lax.axis_index(DP), lax.axis_index(SEQ)
    peers = [(di, lax.rem(z + i, nseq)) for i in range(1, nseq)]
    peers = peers + [(lax.rem(di + i, ndp), z) for i in range(1, ndp)]
    barrier = pltpu.get_barrier_semaphore()
    for peer in peers:
        pl.semaphore_signal(barrier, inc=1, device_id=peer, device_id_type=MESH)
    return lambda: pl.semaphore_wait(barrier, len(peers))


def exchange_sum(ndp, nseq, part, line, cross, sems):
    di, z = lax.axis_index(DP), lax.axis_index(SEQ)

    def phase(count, me, target, slots, send, recv):
        copies = []
        for i in range(1, count):
            copy = pltpu.make_async_remote_copy(
                src_ref=part, dst_ref=slots.at[me], send_sem=send.at[i], recv_sem=recv.at[me],
                device_id=target(lax.rem(me + i, count)), device_id_type=MESH,
            )
            copy.start()
            copies.append(copy)
        slots[me] = part[...]
        for i in range(1, count):
            source = lax.rem(me + count - i, count)
            pltpu.make_async_remote_copy(
                src_ref=part, dst_ref=slots.at[source], send_sem=send.at[i], recv_sem=recv.at[source],
                device_id=(di, z), device_id_type=MESH,
            ).wait_recv()
        for copy in copies:
            copy.wait_send()
        total = slots[0]
        for i in range(1, count):
            total = total + slots[i]
        return total

    part[...] = phase(nseq, z, lambda i: (di, i), line, sems[0], sems[1])
    return phase(ndp, di, lambda i: (i, z), cross, sems[2], sems[3])


HALO = 16


class Halo:
    def __init__(self, nseq, buffer, sem):
        di, z = lax.axis_index(DP), lax.axis_index(SEQ)
        rows = buffer.shape[1]
        self.has = (z > 0, z < nseq - 1)

        def copy(source, target, number, to):
            return pltpu.make_async_remote_copy(
                src_ref=buffer.at[:, pl.ds(source, HALO)], dst_ref=buffer.at[:, pl.ds(target, HALO)],
                send_sem=sem.at[number], recv_sem=sem.at[2 + number], device_id=(di, to), device_id_type=MESH,
            )

        self.up = copy(rows - 2 * HALO, 0, 0, lax.rem(z + 1, nseq))
        self.down = copy(HALO, rows - HALO, 1, lax.rem(z + nseq - 1, nseq))
        self.buffer, self.rows = buffer, rows

    def start(self):
        @pl.when(self.has[1])
        def _():
            self.up.start()

        @pl.when(self.has[0])
        def _():
            self.down.start()

    def finish(self):
        empty = jnp.zeros((self.buffer.shape[0], HALO, self.buffer.shape[2]), jnp.float32)

        @pl.when(self.has[0])
        def _():
            self.up.wait_recv()
            self.down.wait_send()

        @pl.when(jnp.logical_not(self.has[0]))
        def _():
            self.buffer[:, :HALO] = empty

        @pl.when(self.has[1])
        def _():
            self.down.wait_recv()
            self.up.wait_send()

        @pl.when(jnp.logical_not(self.has[1]))
        def _():
            self.buffer[:, self.rows - HALO :] = empty


def slide(padded, taps, index, out, length):
    lanes = LANES // 128

    @pl.loop(0, padded.shape[0] * lanes)
    def _(i):
        s, lane = i // lanes, pl.ds(pl.multiple_of(i % lanes * 128, 128), 128)
        total = jnp.zeros((length, 128), jnp.float32)
        for b in range(8):
            part = None
            for a in range(4):
                if 0 < 8 * a + b < K + 1:
                    row = index(8 * a + b)
                    term = taps[row : row + 1, lane] * padded[s, 8 * a : 8 * a + length + 8, lane]
                    part = term if part is None else part + term
            total = total + part[b : b + length]
        out[pl.ds(pl.multiple_of(s * length, length), length), lane] = total


def depth_kernel(plan, u, valid, packed, c_out, sum_out, padded, taps, taps_b, part, line, cross, sem,
                 halo_sem, *sems):
    ndp, nseq = plan.ndp, plan.nseq
    arrived = group_barrier(ndp, nseq)
    length = padded.shape[1] - 2 * HALO
    copy = Fetch(plan, packed, sem)("b_pi", taps_b)
    padded[:, HALO : HALO + length] = u[...].reshape(-1, length, D)
    arrived()
    halo = Halo(nseq, padded, halo_sem)
    halo.start()
    copy.wait()
    taps[...] = taps_b[...].astype(jnp.float32)
    halo.finish()
    base = plan.places["w_depth"] - plan.places["b_pi"]
    slide(padded, taps, lambda i: base + i - 1, c_out, length)
    depth, mask = c_out[...], valid[...]
    value = depth * mask
    part[0:1] = total_rows(value)
    part[1:2] = total_rows(value * depth)
    part[2:3] = jnp.broadcast_to(total_rows(mask), (1, LANES))
    part[3:8] = jnp.zeros((5, LANES), jnp.float32)
    sum_out[...] = exchange_sum(ndp, nseq, part, line, cross, sems)


def depth_back_kernel(plan, dz, depth, stats, local, valid, u_pad, packed, u_out, tap_out,
                      padded, own, taps, taps_b, part, line, cross, sem, halo_sem, *sems):
    ndp, nseq = plan.ndp, plan.nseq
    arrived = group_barrier(ndp, nseq)
    seqs, length = padded.shape[0], padded.shape[1] - 2 * HALO
    copy = Fetch(plan, packed, sem)("b_pi", taps_b)
    part[...] = local[...]
    arrived()
    sums = exchange_sum(ndp, nseq, part, line, cross, sems)
    mean, inv_std, count = stats[0:1], stats[1:2], stats[2:3]
    standard = (depth[...] - mean) * inv_std
    d_depth = valid[...] * inv_std * (dz[...] - sums[0:1] / count - standard * (sums[1:2] / count))
    d_depth = d_depth.reshape(seqs, length, D)
    padded[:, HALO : HALO + length] = d_depth
    halo = Halo(nseq, padded, halo_sem)
    halo.start()
    own[:, :8] = jnp.zeros((seqs, 8, D), jnp.float32)
    own[:, 8 : 8 + length] = d_depth
    own[:, 8 + length :] = jnp.zeros((seqs, 8, D), jnp.float32)
    copy.wait()
    taps[...] = taps_b[...].astype(jnp.float32)
    base = plan.places["w_depth"] - plan.places["b_pi"]

    @pl.loop(0, LANES // 128)
    def _(i):
        lane = pl.ds(pl.multiple_of(i * 128, 128), 128)
        for b in range(8):
            sums_b = [None] * 4
            for s in range(seqs):
                moved = own[s, 8 - b : 8 - b + length + 8, lane]
                for a in range(4):
                    if 0 < 8 * a + b < K + 1:
                        term = total_rows(u_pad[s, 8 * a : 8 * a + length + 8, lane] * moved)
                        sums_b[a] = term if sums_b[a] is None else sums_b[a] + term
            for a in range(4):
                if sums_b[a] is not None:
                    tap_out[8 * a + b - 1 : 8 * a + b, lane] = sums_b[a]
        tap_out[K : K + 1, lane] = jnp.zeros((1, 128), jnp.float32)

    halo.finish()
    slide(padded, taps, lambda i: base + K - i, u_out, length)


VMEM_SPEC = pl.BlockSpec(memory_space=pltpu.VMEM)
ANY_SPEC = pl.BlockSpec(memory_space=pl.ANY)


def stage(kernel, plan, operands, packed, outs, scratch, name, number=None):
    params = {}
    if number is not None:
        params = {"collective_id": number, "has_side_effects": True}
    specs = [VMEM_SPEC] * len(operands) + [ANY_SPEC]
    return pl.pallas_call(
        functools.partial(kernel, plan),
        out_shape=[jax.ShapeDtypeStruct(shape, dtype) for shape, dtype in outs],
        in_specs=specs,
        out_specs=[VMEM_SPEC] * len(outs),
        scratch_shapes=scratch,
        compiler_params=pltpu.CompilerParams(vmem_limit_bytes=56 * 1024 * 1024, **params),
        name=name,
    )(*operands, packed)


F32, BF16 = jnp.float32, jnp.bfloat16
DMA = pltpu.SemaphoreType.DMA


def vm(shape, dtype=jnp.bfloat16):
    return pltpu.VMEM(shape, dtype)


def exchange_scratch(plan):
    return [vm((8, D), F32), vm((plan.nseq, 8, D), F32), vm((plan.ndp, 8, D), F32), DMA((1,)), DMA((4,)),
            DMA((plan.nseq,)), DMA((plan.nseq,)), DMA((plan.ndp,)), DMA((plan.ndp,))]


def per_device(inputs, lengths, rel_bucket, params, moment_one, moment_two, cotangent):
    seq_count, block_len, model_width = inputs.shape
    rows = seq_count * block_len
    full_len = block_len * lax.axis_size(SEQ)
    first_pos = lax.axis_index(SEQ) * block_len
    positions = first_pos + jnp.arange(block_len, dtype=jnp.int32)
    valid_own = positions[None, :] < lengths[:, None]
    valid = valid_own.astype(jnp.float32).reshape(-1, 1)
    onehot = bucket_window(rel_bucket, block_len, full_len)
    plan = Plan(lax.axis_size(DP), lax.axis_size(SEQ), params.shape[0])
    packed = gather(plan, own_block(plan, params)).reshape(-1, LANES)
    full, wide = (rows, D), (rows, FF)
    square, tall, group = vm((D, D)), vm((FF, D)), vm((8, D))
    mix = vm((LANES // 128, 256, 128), F32)
    stream0 = inputs.reshape(full)
    stream1, normed2, queries, w_first = stage(
        ffn_first_kernel, plan, [stream0], packed,
        [(full, F32), (full, BF16), (full, BF16), ((FF // D, D, D), BF16)],
        [tall, tall, square, group, group, group, group, mix, DMA((7,))], "ffn_first",
    )
    weights = unpack(packed)
    context, stored2 = attend_forward(normed2, queries, weights, lengths, onehot, seq_count)
    stream2, normed3, pre_gate, gated, w_gate = stage(
        gate_kernel, plan, [context, stream1, valid], packed,
        [(full, F32), (full, BF16), ((rows, 2 * D), F32), (full, F32), ((2, D, D), BF16)],
        [square, vm((2 * D, D)), group, group, mix, DMA((4,))], "gate",
    )
    padded_shape = (seq_count, block_len + 2 * HALO, D)
    depth, sums, padded = stage(
        depth_kernel, plan, [gated, valid], packed,
        [(full, F32), ((8, D), F32), (padded_shape, F32)],
        [vm((40, D), F32), vm((40, D))] + exchange_scratch(plan), "depth", 2,
    )
    (output, d_stream3, d_standard, local, stats, active3, grad3_b, active4, half4, normed4, d_hidden4,
     vec_mid) = stage(
        middle_kernel, plan, [stream2, depth, sums, cotangent.reshape(full), valid], packed,
        [(full, F32), (full, F32), (full, F32), ((8, D), F32), ((8, D), F32), (full, BF16), (full, BF16),
         (wide, BF16), (full, BF16), (full, BF16), (wide, BF16), ((16, D), F32)],
        [square, tall, tall, vm((FF // D, D, D)), vm((FF // D, rows, D), F32), vm((40, D)), group, group, group,
         mix, DMA((7,))], "middle",
    )
    d_gated, tap_grads = stage(
        depth_back_kernel, plan, [d_standard, depth, stats, local, valid, padded], packed,
        [(full, F32), ((32, D), F32)],
        [vm(padded_shape, F32), vm((seq_count, block_len + 16, D), F32), vm((40, D), F32), vm((40, D))]
        + exchange_scratch(plan), "depth_back", 3,
    )
    d_gate, d_stream2, grad2_b, d_context, vec_gate = stage(
        gate_back_kernel, plan, [d_gated, pre_gate, stream2, d_stream3, valid, w_gate], packed,
        [((rows, 2 * D), BF16), (full, F32), (full, BF16), (full, BF16), ((8, D), F32)],
        [square, group, DMA((2,))], "gate_back",
    )
    d_query, remote, rel_grad, vec_attend, gradients = attend_backward(weights, stored2, d_context, lengths, onehot)
    d_stream0, active1, half1, normed1, d_hidden1, vec_first = stage(
        ffn_first_back_kernel, plan, [stream0, stream1, d_stream2, d_query, remote, w_first], packed,
        [(full, F32), (wide, BF16), (full, BF16), (full, BF16), (wide, BF16), ((16, D), F32)],
        [tall, square, group, group, group, DMA((5,))], "ffn_first_back",
    )
    gradients.update({
        "first_w_in": (normed1, d_hidden1), "first_w_out": (active1, half1), "w_q": (normed2, d_query),
        "w_o": (context, grad2_b), "w_pi": (normed3, d_gate), "w_po": (active3, grad3_b),
        "second_w_in": (normed4, d_hidden4), "second_w_out": (active4, half4),
    })
    places = {
        "attn_ng": (0, 0), "attn_nb": (0, 1), "first_b_out": (0, 2), "first_ng": (0, 3), "first_nb": (0, 4),
        "first_b_in": (0, 5), "b_pi": (1, 0), "conv_ng": (1, 2), "conv_nb": (1, 3), "b_o": (1, 4),
        "fin_g": (2, 0), "fin_b": (2, 1), "second_b_out": (2, 2), "second_ng": (2, 3), "second_nb": (2, 4),
        "b_po": (2, 5), "bng": (2, 6), "bnb": (2, 7), "second_b_in": (2, 8), "w_depth": (3, 0),
        "b_q": (4, 0), "b_v": (4, 1), "rel": (5, 0),
    }
    vectors = [vec_first, vec_gate, vec_mid, tap_grads, vec_attend, rel_grad]
    window = scatter(plan, weight_grads(plan, gradients, vectors, places))
    grad_shard = own_shard(plan, window)
    new_params, new_first, new_second = adam_update(params, grad_shard, moment_one, moment_two)
    return (
        output.reshape(inputs.shape),
        d_stream0.reshape(inputs.shape),
        grad_shard,
        new_params,
        new_first,
        new_second,
    )


def solution(mesh):
    return jax.shard_map(
        per_device,
        mesh=mesh,
        in_specs=(
            P(DP, SEQ, None),
            P(DP),
            P(),
            P((DP, SEQ)),
            P((DP, SEQ)),
            P((DP, SEQ)),
            P(DP, SEQ, None),
        ),
        out_specs=(
            P(DP, SEQ, None),
            P(DP, SEQ, None),
            P((DP, SEQ)),
            P((DP, SEQ)),
            P((DP, SEQ)),
            P((DP, SEQ)),
        ),
        check_vma=False,
    )
```

```python
import functools
import math

import jax
import jax.numpy as jnp
from jax import lax
from jax.experimental import pallas as pl
from jax.experimental.pallas import tpu as pltpu
from jax.sharding import PartitionSpec as P

D = 512
H = 8
HD = 64
FF = 2048
K = 31
NB = 32
DP = "dp"
SEQ = "seq"
STEP = 4


NORM_EPS = 1e-05
BATCH_EPS = 1e-05
LEARN_RATE = 0.005
DECAY = 0.01
BETA_ONE = 0.9
BETA_TWO = 0.98
ADAM_EPS = 1e-08


def segments():

    def feed_block(prefix):
        return [
            (prefix + "_ng", (D,)),
            (prefix + "_nb", (D,)),
            (prefix + "_w_in", (D, FF)),
            (prefix + "_b_in", (FF,)),
            (prefix + "_w_out", (FF, D)),
            (prefix + "_b_out", (D,)),
        ]

    listing = feed_block("first")
    listing = listing + [
        ("attn_ng", (D,)),
        ("attn_nb", (D,)),
        ("w_q", (D, D)),
        ("b_q", (D,)),
        ("w_k", (D, D)),
        ("w_v", (D, D)),
        ("b_v", (D,)),
        ("w_o", (D, D)),
        ("b_o", (D,)),
        ("rel", (NB, H)),
    ]
    listing = listing + [
        ("conv_ng", (D,)),
        ("conv_nb", (D,)),
        ("w_pi", (D, 2 * D)),
        ("b_pi", (2 * D,)),
        ("w_depth", (K, D)),
        ("bng", (D,)),
        ("bnb", (D,)),
        ("w_po", (D, D)),
        ("b_po", (D,)),
    ]
    listing = listing + feed_block("second") + [("fin_g", (D,)), ("fin_b", (D,))]
    return listing


def arrange():
    places, gaps = {}, []
    linear = inner = 0
    for entry_name, entry_shape in segments():
        extent = math.prod(entry_shape)
        tail = 2 * D if entry_name == "conv_ng" else 0
        if extent >= D * D or tail:
            pad = -(inner + tail) % TILE
            if pad:
                gaps.append((linear, pad))
                inner = inner + pad
        places[entry_name] = inner // LANES
        linear, inner = linear + extent, inner + extent
    return places, gaps, -(-inner // TILE)


def device_index():
    return lax.axis_index(DP) * lax.axis_size(SEQ) + lax.axis_index(SEQ)


def own_block(plan, params):
    index = device_index()
    shift_down = [(i + 1, i) for i in range(plan.n - 1)]
    following = lax.ppermute(params[:TILE], (DP, SEQ), shift_down)
    length = plan.hi * TILE
    room = max(length + TILE - plan.shard - TILE, 0)
    front = max(size for _, size in plan.gaps)
    extended = jnp.concatenate(
        [jnp.zeros((front,), jnp.float32), params, following, jnp.zeros((room,), jnp.float32)]
    )
    table = jnp.asarray(plan.block_table, jnp.int32)[index]
    early = lax.dynamic_slice(extended, (front + table[0],), (length,))
    late = lax.dynamic_slice(extended, (front + table[0] - table[2],), (length,))
    block = jnp.where(jnp.arange(length, dtype=jnp.int32) < table[1], early, late)
    return block.astype(jnp.bfloat16).reshape(plan.hi, 8, LANES)


def own_shard(plan, window):
    table = jnp.asarray(plan.shard_table, jnp.int32)[device_index()]
    flat = window.reshape(-1)
    early = lax.dynamic_slice(flat, (table[0],), (plan.shard,))
    late = lax.dynamic_slice(flat, (table[0] + table[2],), (plan.shard,))
    return jnp.where(jnp.arange(plan.shard, dtype=jnp.int32) < table[1], early, late)


def swish_act(values):
    return values * jax.nn.sigmoid(values)


def swish_grad(values):
    sig_vals = jax.nn.sigmoid(values)
    return sig_vals * (1.0 + values * (1.0 - sig_vals))


def forward_dot(left_mat, weight):
    return jnp.dot(left_mat, weight, preferred_element_type=jnp.float32)


def back_dot(grad_in, weight):
    return lax.dot_general(
        grad_in, weight, (((1,), (1,)), ((), ())), preferred_element_type=jnp.float32
    )


MESH = pl.DeviceIdType.MESH
LANES=512
TILE=8*LANES

class Plan:
    def __init__(self, ndp, nseq, shard):
        self.ndp, self.nseq, self.shard = ndp, nseq, shard
        self.k = ndp.bit_length() - 1
        self.phases = self.k - 1
        self.n = n = ndp * nseq
        self.places, self.gaps, self.total = arrange()
        begins = [self.inner(d * shard) for d in range(n)]
        starts = [-(-b // TILE) for b in begins] + [self.total]
        sizes = [b - a for a, b in zip(starts, starts[1:])]
        self.lo, self.hi = min(sizes), max(sizes)
        self.slots = nseq * 2**self.phases
        floors = [b // TILE for b in begins]
        ends = [self.inner((d + 1) * shard - 1) // TILE + 1 for d in range(n)]
        self.win = max(e - f for e, f in zip(ends, floors))
        self.win += self.win % 2
        self.padded = max(self.total, max(floors) + self.win)
        self.block_table, self.shard_table = [], []
        for d in range(n):
            near = [g for g in self.gaps if d * shard < g[0] < (d + 1) * shard + TILE]
            assert len(near) <= 1
            cut, size = near[0] if near else (2**30, 0)
            lead = starts[d] * TILE - begins[d]
            self.block_table.append((lead, cut - d * shard - lead, size))
            self.shard_table.append((begins[d] - floors[d] * TILE, cut - d * shard, size))

    def inner(self, position):
        if isinstance(position, int):
            return position + sum(size for at, size in self.gaps if at <= position)
        result = position
        for at, size in self.gaps:
            result = result + jnp.where(position >= at, size, 0)
        return result

    def order(self):
        ev=[]
        for s in range(self.nseq):
            for sign in ((0,) if s==0 else (-1,1)):
                for t in range(2**self.phases):
                    ev.append((s+0.5*bin(t).count("1")+0.01*t, s, sign, t))
        ev.sort()
        return [e[1:] for e in ev]

def flip(di, mask_bits, bits, t, phases):
    out=di
    for p in range(phases):
        if (t>>p)&1:
            out = out + mask_bits[p]*(1-2*bits[p])
    return out

def phase_masks(di, c, phases):
    masks, bits=[],[]
    for p in range(phases):
        a, b = 1<<(p+1), 1<<(phases-p)
        masks.append(a+c*(b-a))
        ba, bb = (di//a)%2, (di//b)%2
        bits.append(ba+c*(bb-ba))
    return masks, bits

def block_of(plan, dpi, z):
    d = dpi*plan.nseq+z
    a = (plan.inner(d*plan.shard)+TILE-1)//TILE
    b = (plan.inner((d+1)*plan.shard)+TILE-1)//TILE
    b = jnp.where(d == plan.n-1, plan.total, b)
    return a, b-a

def floor_of(plan, dpi, z):
    return plan.inner((dpi*plan.nseq+z)*plan.shard)//TILE

def gather_kernel(plan, src, out, send_a, send_b, recv_a, recv_b, loc_sem):
    di, z = lax.axis_index(DP), lax.axis_index(SEQ)
    ns, ph = plan.nseq, plan.phases
    c = di%2
    masks, bits = phase_masks(di, c, ph)
    other = di+1-2*c
    omasks, obits = phase_masks(other, 1-c, ph)
    up, down = lax.rem(z+1,ns), lax.rem(z+ns-1,ns)
    partners=[(di,up),(di,down),(other,z)]+[(flip(di,masks,bits,1<<p,ph),z) for p in range(ph)]
    barrier=pltpu.get_barrier_semaphore()
    for a,b in partners:
        pl.semaphore_signal(barrier,inc=1,device_id=(a,b),device_id_type=MESH)
    pl.semaphore_wait(barrier,len(partners))
    lo, more = plan.lo, plan.hi-plan.lo
    start_own, size_own = block_of(plan, di, z)

    def pair(ref, base, dst_start, size, sidx, ridx, dev):
        copies=[pltpu.make_async_remote_copy(src_ref=ref.at[pl.ds(base,lo)],dst_ref=out.at[pl.ds(dst_start,lo)],
            send_sem=send_a.at[sidx],recv_sem=recv_a.at[ridx],device_id=dev,device_id_type=MESH)]
        for x in range(more):
            copies.append(pltpu.make_async_remote_copy(src_ref=ref.at[pl.ds(base+lo+x,1)],dst_ref=out.at[pl.ds(dst_start+lo+x,1)],
                send_sem=send_b.at[sidx*more+x],recv_sem=recv_b.at[ridx*more+x],device_id=dev,device_id_type=MESH))
        return copies, size
    def each(p, act):
        for x,copy in enumerate(p[0]):
            if x==0: act(copy)
            else:
                @pl.when(p[1]>=lo+x)
                def _(): act(copy)
    def start(p): each(p, lambda c: c.start())
    def wait_send(p): each(p, lambda c: c.wait_send())
    def wait_recv(p): each(p, lambda c: c.wait_recv())

    own=[pltpu.make_async_copy(src.at[pl.ds(0,lo)],out.at[pl.ds(start_own,lo)],loc_sem.at[0])]
    for x in range(more):
        own.append(pltpu.make_async_copy(src.at[pl.ds(lo+x,1)],out.at[pl.ds(start_own+lo+x,1)],loc_sem.at[1+x]))
    own=(own,size_own)
    start(own)
    nslot=plan.slots
    sends=[]
    sidx=[0]
    def forward(conds, ref, base, st, size, ridx, dev):
        i=sidx[0]; sidx[0]+=1
        p=pair(ref,base,st,size,i,ridx,dev)
        sends.append((conds,p))
        guard(conds, lambda: start(p))
    def guard(conds, fn):
        if not conds: fn(); return
        cond=conds[0]
        for x in conds[1:]: cond=jnp.logical_and(cond,x)
        @pl.when(cond)
        def _(): fn()

    for s, sign, t in plan.order():
        zz = z+sign*s
        conds=[] if s==0 else ([zz>=0] if sign<0 else [zz<ns])
        dpi=flip(di,masks,bits,t,ph)
        st,size=block_of(plan,dpi,zz)
        mine = s==0 and t==0
        ref, base = (src, 0) if mine else (out, st)
        slot = t*ns+zz
        if not mine:
            p=pair(out,st,st,size,0,slot,(di,z))
            guard(conds, lambda: wait_recv(p))
        if t==0:
            if sign<=0 : forward(conds+[z<ns-1],ref,base,st,size,slot,(di,z+1))
            if sign>=0 : forward(conds+[z>0],ref,base,st,size,slot,(di,z-1))
        hi_bit=t.bit_length()
        for pp in range(hi_bit,ph):
            forward(conds,ref,base,st,size,slot+(1<<pp)*ns,(flip(di,masks,bits,1<<pp,ph),z))
        forward(conds,ref,base,st,size,nslot+slot,(other,z))
    for s, sign, t in plan.order():
        zz=z+sign*s
        conds=[] if s==0 else ([zz>=0] if sign<0 else [zz<ns])
        dpi=flip(other,omasks,obits,t,ph)
        st,size=block_of(plan,dpi,zz)
        p=pair(out,st,st,size,0,nslot+t*ns+zz,(di,z))
        guard(conds,lambda: wait_recv(p))
    for conds,p in sends:
        guard(conds,lambda: wait_send(p))
    each(own, lambda c: c.wait())

def count_sends(plan):
    n=0
    for s,sign,t in plan.order():
        if t==0: n+= (2 if sign==0 else 1)
        n+=plan.phases-t.bit_length()+1
    return n

def gather(plan, block):
    ns=count_sends(plan)
    more=max(plan.hi-plan.lo,1)
    return pl.pallas_call(
        functools.partial(gather_kernel,plan),
        out_shape=jax.ShapeDtypeStruct((plan.total,8,LANES),block.dtype),
        in_specs=[pl.BlockSpec(memory_space=pl.ANY)],
        out_specs=pl.BlockSpec(memory_space=pl.ANY),
        scratch_shapes=[pltpu.SemaphoreType.DMA((ns,)),pltpu.SemaphoreType.DMA((ns*more,)),
            pltpu.SemaphoreType.DMA((2*plan.slots,)),pltpu.SemaphoreType.DMA((2*plan.slots*more,)),pltpu.SemaphoreType.DMA((1+more,))],
        compiler_params=pltpu.CompilerParams(collective_id=0,has_side_effects=True),
        name="gather_params",
    )(block)

def scatter_kernel(plan, g, out, acc, rc, rp, rz, load_sem, send_sem, core_send, core_recv, ph_recv, z_recv):
    di, z = lax.axis_index(DP), lax.axis_index(SEQ)
    ns, ph, win, nslot = plan.nseq, plan.phases, plan.win, plan.slots
    c = di%2
    masks, bits = phase_masks(di, c, ph)
    other = di+1-2*c
    omasks, obits = phase_masks(other, 1-c, ph)
    up, down = lax.rem(z+1,ns), lax.rem(z+ns-1,ns)
    partners=[(di,up),(di,down),(other,z)]+[(flip(di,masks,bits,1<<p,ph),z) for p in range(ph)]
    barrier=pltpu.get_barrier_semaphore()
    for a,b in partners:
        pl.semaphore_signal(barrier,inc=1,device_id=(a,b),device_id_type=MESH)
    order=list(reversed(plan.order()))
    def cond_of(s,sign):
        zz=z+sign*s
        return zz,([] if s==0 else ([zz>=0] if sign<0 else [zz<ns]))
    def guard(conds, fn):
        if not conds: fn(); return
        cond=conds[0]
        for x in conds[1:]: cond=jnp.logical_and(cond,x)
        @pl.when(cond)
        def _(): fn()
    def load(s,sign,t):
        zz,conds=cond_of(s,sign)
        slot=t*ns+zz
        st=floor_of(plan,flip(di,masks,bits,t,ph),zz)
        return conds,pltpu.make_async_copy(g.at[pl.ds(st,win)],acc.at[slot],load_sem.at[slot])
    def core(s,sign,t):
        zz,conds=cond_of(s,sign)
        slot=t*ns+zz
        st=floor_of(plan,flip(other,omasks,obits,t,ph),zz)
        return conds,pltpu.make_async_remote_copy(src_ref=g.at[pl.ds(st,win)],dst_ref=rc.at[slot],
            send_sem=core_send.at[slot],recv_sem=core_recv.at[slot],device_id=(other,z),device_id_type=MESH)
    for e in order:
        conds,cp=load(*e)
        guard(conds,lambda: cp.start())
    pl.semaphore_wait(barrier,len(partners))
    for e in order:
        conds,cp=core(*e)
        guard(conds,lambda: cp.start())
    sends=[]
    def send(conds,slot,dst,rsem,dev):
        i=len(sends)
        cp=pltpu.make_async_remote_copy(src_ref=acc.at[slot],dst_ref=dst,send_sem=send_sem.at[i],recv_sem=rsem,
            device_id=dev,device_id_type=MESH)
        sends.append((conds,cp))
        guard(conds,lambda: cp.start())
    def waiting(conds,dst,rsem):
        cp=pltpu.make_async_remote_copy(src_ref=dst,dst_ref=dst,send_sem=send_sem.at[0],recv_sem=rsem,
            device_id=(di,z),device_id_type=MESH)
        guard(conds,lambda: cp.wait_recv())
    step=2
    def add(dst, slot, parts, final=False):
        @pl.loop(0,win//step)
        def _(i):
            r=pl.ds(i*step,step)
            v=acc[slot,r].astype(jnp.float32)
            for p in parts:
                v=v+p(r).astype(jnp.float32)
            if final: out[r]=v
            else: acc[slot,r]=v.astype(acc.dtype)
    for s,sign,t in order:
        zz,conds=cond_of(s,sign)
        slot=t*ns+zz
        hi_bit=t.bit_length()
        def fn():
            load(s,sign,t)[1].wait()
            waiting([],rc.at[slot],core_recv.at[slot])
            parts=[lambda r: rc[slot,r]]
            for pp in range(hi_bit,ph):
                idx=((1<<pp)-1)*ns+slot
                waiting([],rp.at[idx],ph_recv.at[idx])
                parts.append(lambda r,idx=idx: rp[idx,r])
            add(None,slot,parts,final=False) if not (t==0 and s==0) else add(None,slot,parts,final=True)
        guard(conds,fn)
        if t:
            pp=hi_bit-1
            idx=((1<<pp)-1)*ns+slot-(1<<pp)*ns
            send(conds,slot,rp.at[idx],ph_recv.at[idx],(flip(di,masks,bits,1<<pp,ph),z))
        else:
            def zadd(stream, extra):
                zi=stream*ns+zz
                def fz():
                    waiting([],rz.at[zi],z_recv.at[zi])
                    @pl.loop(0,win//step)
                    def _(i):
                        r=pl.ds(i*step,step)
                        if s==0:
                            out[r]=out[r]+rz[zi,r].astype(jnp.float32)
                        else:
                            acc[slot,r]=(acc[slot,r].astype(jnp.float32)+rz[zi,r].astype(jnp.float32)).astype(acc.dtype)
                guard(conds+extra,fz)
            if sign>=0: zadd(0,[z>0])
            if sign<=0: zadd(1,[z<ns-1])
            if sign>0: send(conds,slot,rz.at[zz],z_recv.at[zz],(di,z+1))
            if sign<0: send(conds,slot,rz.at[ns+zz],z_recv.at[ns+zz],(di,z-1))
    for e in order:
        conds,cp=core(*e)
        guard(conds,lambda: cp.wait_send())
    for conds,cp in sends:
        guard(conds,lambda: cp.wait_send())

def scatter(plan, g):
    win,ns,ph,nslot=plan.win,plan.nseq,plan.phases,plan.slots
    nsend=len(plan.order())
    return pl.pallas_call(
        functools.partial(scatter_kernel,plan),
        out_shape=jax.ShapeDtypeStruct((win,8,LANES),jnp.float32),
        in_specs=[pl.BlockSpec(memory_space=pl.ANY)],
        out_specs=pl.BlockSpec(memory_space=pltpu.VMEM),
        scratch_shapes=[pltpu.VMEM((nslot,win,8,LANES),g.dtype),pltpu.VMEM((nslot,win,8,LANES),g.dtype),
            pltpu.VMEM(((2**ph-1)*ns,win,8,LANES),g.dtype),pltpu.VMEM((2*ns,win,8,LANES),g.dtype),
            pltpu.SemaphoreType.DMA((nslot,)),pltpu.SemaphoreType.DMA((nsend,)),
            pltpu.SemaphoreType.DMA((nslot,)),pltpu.SemaphoreType.DMA((nslot,)),
            pltpu.SemaphoreType.DMA(((2**ph-1)*ns,)),pltpu.SemaphoreType.DMA((2*ns,))],
        compiler_params=pltpu.CompilerParams(collective_id=1,has_side_effects=True,vmem_limit_bytes=48*1024*1024),
        name="scatter_grads",
    )(g)


def weight_kernel(plan, names, places, *refs):
    pairs = {name: refs[2 * i : 2 * i + 2] for i, name in enumerate(names)}
    vectors = refs[2 * len(names) : -2]
    out, mix = refs[-2:]
    rows = (((0,), (0,)), ((), ()))
    for name, shape in segments():
        first = plan.places[name]
        if math.prod(shape) < D * D:
            array, begin = places[name]
            for r in range(-(-math.prod(shape) // LANES)):
                line = vectors[array][begin + r : begin + r + 1, :]
                tile, row = divmod(first + r, 8)
                out[tile, row : row + 1, : line.shape[1]] = line.astype(out.dtype)
            continue
        left, right = pairs[name]
        fold = shape[1] // LANES
        step = 256 if fold == 1 else 128

        @pl.loop(0, shape[0] // step)
        def _(i):
            part = left[:, pl.ds(pl.multiple_of(i * step, step), step)]
            value = lax.dot_general(part, right[...], rows, preferred_element_type=jnp.float32)
            if fold > 1:
                for j in range(fold):
                    for lane in range(LANES // 128):
                        at = j * LANES + lane * 128
                        mix[lane, pl.ds(j, step, stride=fold), :] = value[:, at : at + 128]
                value = jnp.concatenate([mix[lane, : step * fold] for lane in range(LANES // 128)], 1)
            tiles = step * fold // 8
            out[pl.ds(first // 8 + i * tiles, tiles)] = value.astype(out.dtype).reshape(tiles, 8, LANES)


def weight_grads(plan, gradients, vectors, places):
    names = list(gradients)
    operands = [value for name in names for value in gradients[name]] + vectors
    return pl.pallas_call(
        functools.partial(weight_kernel, plan, names, places),
        out_shape=jax.ShapeDtypeStruct((plan.padded, 8, LANES), jnp.bfloat16),
        in_specs=[VMEM_SPEC] * len(operands),
        out_specs=VMEM_SPEC,
        scratch_shapes=[pltpu.VMEM((LANES // 128, 512, 128), jnp.float32)],
        compiler_params=pltpu.CompilerParams(vmem_limit_bytes=60 * 1024 * 1024),
        name="weight_grads",
    )(*operands)


def bucket_windows(rel_bucket, block_len, count):
    width = -(-(block_len * (count + 1) - 1) // 128) * 128
    padded = jnp.concatenate([rel_bucket, jnp.full((width,), -1, jnp.int32)])
    windows = [padded[(count - 1 - b) * block_len :][:width] for b in range(count)]
    return (jnp.stack(windows)[:, None, :] == jnp.arange(NB, dtype=jnp.int32)[None, :, None]).astype(jnp.float32)


def adam_update(param_vec, grad_in, first_mom, second):
    new_first = BETA_ONE * first_mom + (1.0 - BETA_ONE) * grad_in
    new_second = BETA_TWO * second + (1.0 - BETA_TWO) * grad_in * grad_in
    corr_one = 1.0 - BETA_ONE**STEP
    corr_two = 1.0 - BETA_TWO**STEP
    step_size = new_first / corr_one / (jnp.sqrt(new_second / corr_two) + ADAM_EPS)
    return (param_vec - LEARN_RATE * (step_size + DECAY * param_vec), new_first, new_second)


def unit_rows(values):
    centre = values - jnp.mean(values, -1, keepdims=True)
    scale = lax.rsqrt(jnp.mean(centre * centre, -1, keepdims=True) + NORM_EPS)
    return centre * scale, scale


def unit_back(unit, scale, gain, grad):
    shifted = grad * gain
    first = jnp.mean(shifted, -1, keepdims=True)
    second = jnp.mean(shifted * unit, -1, keepdims=True)
    return scale * (shifted - first - unit * second), total_rows(grad * unit), total_rows(grad)


def total_rows(values):
    return jnp.sum(values, 0, keepdims=True)


def split_rows(source, mix, target, fold):
    block = mix.shape[1]
    lanes = LANES // 128

    @pl.loop(0, source.shape[0] // block)
    def _(i):
        part = source[pl.ds(pl.multiple_of(i * block, block), block), :].astype(jnp.float32)
        for lane in range(lanes):
            mix[lane] = part[:, lane * 128 : (lane + 1) * 128]
        for j in range(fold):
            rows = [mix[lane, pl.ds(j, block // fold, stride=fold), :] for lane in range(lanes)]
            at = pl.multiple_of(i * (block // fold), block // fold)
            target[j, pl.ds(at, block // fold), :] = jnp.concatenate(rows, 1).astype(target.dtype)


class Fetch:
    def __init__(self, plan, packed, sem):
        self.plan, self.packed, self.sem, self.count = plan, packed, sem, 0

    def __call__(self, name, target):
        row = self.plan.places[name] // 8 * 8
        copy = pltpu.make_async_copy(
            self.packed.at[pl.ds(row, target.shape[0])], target, self.sem.at[self.count]
        )
        self.count += 1
        copy.start()
        return copy


def wait_all(*copies):
    for copy in copies:
        copy.wait()


def ffn_first_kernel(plan, x, packed, x_out, n_out, w_out, w_in, w_second, v0, v1, v2, mix, sem):
    fetch = Fetch(plan, packed, sem)
    early = [fetch("first_ng", v0), fetch("first_b_in", v1), fetch("first_b_out", v2)]
    in_copy = fetch("first_w_in", w_in)
    late = [fetch("first_w_out", w_second)]
    wait_all(*early)
    gains, bias_in, tail = v0[...].astype(jnp.float32), v1[...].astype(jnp.float32), v2[...].astype(jnp.float32)
    stream = x[...]
    unit, _ = unit_rows(stream)
    normed = (unit * gains[0:1] + gains[1:2]).astype(jnp.bfloat16)
    in_copy.wait()
    split_rows(w_in, mix, w_out, FF // LANES)
    wait_all(*late)
    total = jnp.zeros(stream.shape, jnp.float32)
    for j in range(FF // LANES):
        hidden = forward_dot(normed, w_out[j]) + bias_in[j : j + 1]
        active = swish_act(hidden).astype(jnp.bfloat16)
        total = total + forward_dot(active, w_second[j * LANES : (j + 1) * LANES, :])
    stream = stream + 0.5 * (total + tail[0:1])
    x_out[...] = stream
    unit, _ = unit_rows(stream)
    normed = (unit * tail[1:2] + tail[2:3]).astype(jnp.bfloat16)
    n_out[...] = normed


def ffn_first_back_kernel(plan, x, x_one, d_two, d_norm_in, w_in, packed,
                          d_out, a_out, r_out, n_out, h_out, vec_out, w_second, v0, v1, v2, sem):
    fetch = Fetch(plan, packed, sem)
    early = [fetch("first_ng", v0), fetch("first_b_in", v1), fetch("first_b_out", v2)]
    late = fetch("first_w_out", w_second)
    wait_all(*early)
    gains, bias_in, tail = v0[...].astype(jnp.float32), v1[...].astype(jnp.float32), v2[...].astype(jnp.float32)
    unit, scale = unit_rows(x_one[...])
    d_normed = d_norm_in[...].astype(jnp.float32)
    d_norm, gain_grad, shift_grad = unit_back(unit, scale, tail[1:2], d_normed)
    vec_out[0:1] = gain_grad
    vec_out[1:2] = shift_grad
    grad = d_two[...] + d_norm
    half = 0.5 * grad
    vec_out[2:3] = total_rows(half)
    half_b = half.astype(jnp.bfloat16)
    r_out[...] = half_b
    unit, scale = unit_rows(x[...])
    normed = (unit * gains[0:1] + gains[1:2]).astype(jnp.bfloat16)
    n_out[...] = normed
    late.wait()
    d_normed = jnp.zeros(grad.shape, jnp.float32)
    for j in range(FF // LANES):
        cols = slice(j * LANES, (j + 1) * LANES)
        hidden = forward_dot(normed, w_in[j]) + bias_in[j : j + 1]
        a_out[:, cols] = swish_act(hidden).astype(jnp.bfloat16)
        d_hidden = back_dot(half_b, w_second[cols, :]) * swish_grad(hidden)
        vec_out[5 + j : 6 + j] = total_rows(d_hidden)
        d_hidden = d_hidden.astype(jnp.bfloat16)
        h_out[:, cols] = d_hidden
        d_normed = d_normed + back_dot(d_hidden, w_in[j])
    d_norm, gain_grad, shift_grad = unit_back(unit, scale, gains[0:1], d_normed)
    vec_out[3:4] = gain_grad
    vec_out[4:5] = shift_grad
    d_out[...] = grad + d_norm


def gate_kernel(plan, ctx, x, valid, packed, x_out, n_out, g_out, u_out, w_out, w_o, w_pi, v0, v1, mix, sem):
    fetch = Fetch(plan, packed, sem)
    early = [fetch("w_o", w_o), fetch("b_o", v0), fetch("b_pi", v1)]
    late = fetch("w_pi", w_pi)
    wait_all(*early)
    rows, bias_in = v0[...].astype(jnp.float32), v1[...].astype(jnp.float32)
    stream = x[...] + forward_dot(ctx[...], w_o[...]) + rows[0:1]
    x_out[...] = stream
    unit, _ = unit_rows(stream)
    normed = (unit * rows[6:7] + rows[7:8]).astype(jnp.bfloat16)
    n_out[...] = normed
    late.wait()
    split_rows(w_pi, mix, w_out, 2)
    linear = forward_dot(normed, w_out[0]) + bias_in[0:1]
    gate = forward_dot(normed, w_out[1]) + bias_in[1:2]
    g_out[:, :D] = linear
    g_out[:, D:] = gate
    u_out[...] = linear * jax.nn.sigmoid(gate) * valid[...]


def gate_back_kernel(plan, du, pre_gate, x, d_three, valid, w_pi, packed,
                     g_out, d_out, o_out, c_out, vec_out, w_o, v0, sem):
    fetch = Fetch(plan, packed, sem)
    copies = [fetch("b_o", v0), fetch("w_o", w_o)]
    d_gated = du[...] * valid[...]
    gate_sig = jax.nn.sigmoid(pre_gate[:, D:])
    d_linear = d_gated * gate_sig
    d_gate = d_gated * pre_gate[:, :D] * gate_sig * (1.0 - gate_sig)
    vec_out[0:1] = total_rows(d_linear)
    vec_out[1:2] = total_rows(d_gate)
    d_linear, d_gate = d_linear.astype(jnp.bfloat16), d_gate.astype(jnp.bfloat16)
    g_out[:, :D] = d_linear
    g_out[:, D:] = d_gate
    d_normed = back_dot(d_linear, w_pi[0]) + back_dot(d_gate, w_pi[1])
    unit, scale = unit_rows(x[...])
    wait_all(*copies)
    d_norm, gain_grad, shift_grad = unit_back(unit, scale, v0[...].astype(jnp.float32)[6:7], d_normed)
    vec_out[2:3] = gain_grad
    vec_out[3:4] = shift_grad
    grad = d_three[...] + d_norm
    d_out[...] = grad
    vec_out[4:5] = total_rows(grad)
    grad_b = grad.astype(jnp.bfloat16)
    o_out[...] = grad_b
    c_out[...] = back_dot(grad_b, w_o[...]).astype(jnp.bfloat16)


def middle_kernel(plan, x, depth, sums, cot, valid, packed,
                  y_out, d_out, z_out, part_out, stat_out, e_out, rb_out, a_out, r_out, n_out, h_out, vec_out,
                  w_po, w_in, w_second, w_mix, held, v_bn, v0, v1, v2, mix, sem):
    fetch = Fetch(plan, packed, sem)
    early = [fetch("b_pi", v_bn), fetch("w_po", w_po), fetch("b_po", v0), fetch("second_b_in", v1)]
    early.append(fetch("second_b_out", v2))
    in_copy = fetch("second_w_in", w_in)
    late = fetch("second_w_out", w_second)
    wait_all(*early)
    base = plan.places["bng"] - plan.places["b_pi"]
    batch, head = v_bn[...].astype(jnp.float32), v0[...].astype(jnp.float32)
    bias_in, tail = v1[...].astype(jnp.float32), v2[...].astype(jnp.float32)
    gain, shift = batch[base : base + 1], batch[base + 1 : base + 2]
    count = sums[2:3]
    mean = sums[0:1] / count
    inv_std = lax.rsqrt(sums[1:2] / count - mean * mean + BATCH_EPS)
    stat_out[0:1] = mean
    stat_out[1:2] = inv_std
    stat_out[2:3] = count
    stat_out[3:8] = jnp.zeros((5, D), jnp.float32)
    standard = (depth[...] - mean) * inv_std
    e_out[...] = swish_act(standard * gain + shift).astype(jnp.bfloat16)
    three = x[...] + forward_dot(e_out[...], w_po[...]) + head[0:1]
    unit, scale = unit_rows(three)
    n_out[...] = (unit * head[1:2] + head[2:3]).astype(jnp.bfloat16)
    in_copy.wait()
    split_rows(w_in, mix, w_mix, FF // LANES)
    late.wait()
    total = jnp.zeros(three.shape, jnp.float32)
    for j in range(FF // LANES):
        cols = slice(j * LANES, (j + 1) * LANES)
        hidden = forward_dot(n_out[...], w_mix[j]) + bias_in[j : j + 1]
        held[j] = hidden
        active = swish_act(hidden).astype(jnp.bfloat16)
        a_out[:, cols] = active
        total = total + forward_dot(active, w_second[cols, :])
    four = three + 0.5 * (total + tail[0:1])
    last, last_scale = unit_rows(four)
    y_out[...] = last * tail[1:2] + tail[2:3]
    grad = cot[...] * valid[...]
    grad, gain_grad, shift_grad = unit_back(last, last_scale, tail[1:2], grad)
    vec_out[0:1] = gain_grad
    vec_out[1:2] = shift_grad
    half = 0.5 * grad
    vec_out[2:3] = total_rows(half)
    r_out[...] = half.astype(jnp.bfloat16)
    d_normed = jnp.zeros(three.shape, jnp.float32)
    for j in range(FF // LANES):
        cols = slice(j * LANES, (j + 1) * LANES)
        d_hidden = back_dot(r_out[...], w_second[cols, :]) * swish_grad(held[j])
        vec_out[8 + j : 9 + j] = total_rows(d_hidden)
        d_hidden = d_hidden.astype(jnp.bfloat16)
        h_out[:, cols] = d_hidden
        d_normed = d_normed + back_dot(d_hidden, w_mix[j])
    d_norm, gain_grad, shift_grad = unit_back(unit, scale, head[1:2], d_normed)
    vec_out[3:4] = gain_grad
    vec_out[4:5] = shift_grad
    grad = grad + d_norm
    d_out[...] = grad
    vec_out[5:6] = total_rows(grad)
    rb_out[...] = grad.astype(jnp.bfloat16)
    standard = (depth[...] - mean) * inv_std
    d_active = back_dot(rb_out[...], w_po[...]) * swish_grad(standard * gain + shift)
    d_gain, d_shift = total_rows(d_active * standard), total_rows(d_active)
    vec_out[6:7] = d_gain
    vec_out[7:8] = d_shift
    vec_out[12:16] = jnp.zeros((4, D), jnp.float32)
    d_standard = d_active * gain * valid[...]
    z_out[...] = d_standard
    part_out[0:1] = total_rows(d_standard)
    part_out[1:2] = total_rows(d_standard * standard)
    part_out[2:8] = jnp.zeros((6, D), jnp.float32)


def group_barrier(ndp, nseq):
    di, z = lax.axis_index(DP), lax.axis_index(SEQ)
    peers = [(di, lax.rem(z + i, nseq)) for i in range(1, nseq)]
    peers = peers + [(lax.rem(di + i, ndp), z) for i in range(1, ndp)]
    barrier = pltpu.get_barrier_semaphore()
    for peer in peers:
        pl.semaphore_signal(barrier, inc=1, device_id=peer, device_id_type=MESH)
    return lambda: pl.semaphore_wait(barrier, len(peers))


def exchange_sum(ndp, nseq, part, line, cross, sems):
    di, z = lax.axis_index(DP), lax.axis_index(SEQ)

    def phase(count, me, target, slots, send, recv):
        copies = []
        for i in range(1, count):
            copy = pltpu.make_async_remote_copy(
                src_ref=part, dst_ref=slots.at[me], send_sem=send.at[i], recv_sem=recv.at[me],
                device_id=target(lax.rem(me + i, count)), device_id_type=MESH,
            )
            copy.start()
            copies.append(copy)
        slots[me] = part[...]
        for i in range(1, count):
            source = lax.rem(me + count - i, count)
            pltpu.make_async_remote_copy(
                src_ref=part, dst_ref=slots.at[source], send_sem=send.at[i], recv_sem=recv.at[source],
                device_id=(di, z), device_id_type=MESH,
            ).wait_recv()
        for copy in copies:
            copy.wait_send()
        total = slots[0]
        for i in range(1, count):
            total = total + slots[i]
        return total

    part[...] = phase(nseq, z, lambda i: (di, i), line, sems[0], sems[1])
    return phase(ndp, di, lambda i: (i, z), cross, sems[2], sems[3])


HALO = 16


class Halo:
    def __init__(self, nseq, buffer, sem):
        di, z = lax.axis_index(DP), lax.axis_index(SEQ)
        rows = buffer.shape[1]
        self.has = (z > 0, z < nseq - 1)

        def copy(source, target, number, to):
            return pltpu.make_async_remote_copy(
                src_ref=buffer.at[:, pl.ds(source, HALO)], dst_ref=buffer.at[:, pl.ds(target, HALO)],
                send_sem=sem.at[number], recv_sem=sem.at[2 + number], device_id=(di, to), device_id_type=MESH,
            )

        self.up = copy(rows - 2 * HALO, 0, 0, lax.rem(z + 1, nseq))
        self.down = copy(HALO, rows - HALO, 1, lax.rem(z + nseq - 1, nseq))
        self.buffer, self.rows = buffer, rows

    def start(self):
        @pl.when(self.has[1])
        def _():
            self.up.start()

        @pl.when(self.has[0])
        def _():
            self.down.start()

    def finish(self):
        empty = jnp.zeros((self.buffer.shape[0], HALO, self.buffer.shape[2]), jnp.float32)

        @pl.when(self.has[0])
        def _():
            self.up.wait_recv()
            self.down.wait_send()

        @pl.when(jnp.logical_not(self.has[0]))
        def _():
            self.buffer[:, :HALO] = empty

        @pl.when(self.has[1])
        def _():
            self.down.wait_recv()
            self.up.wait_send()

        @pl.when(jnp.logical_not(self.has[1]))
        def _():
            self.buffer[:, self.rows - HALO :] = empty


def slide(padded, taps, index, out, length):
    lanes = LANES // 128

    @pl.loop(0, padded.shape[0] * lanes)
    def _(i):
        s, lane = i // lanes, pl.ds(pl.multiple_of(i % lanes * 128, 128), 128)
        total = jnp.zeros((length, 128), jnp.float32)
        for b in range(8):
            part = None
            for a in range(4):
                if 0 < 8 * a + b < K + 1:
                    row = index(8 * a + b)
                    term = taps[row : row + 1, lane] * padded[s, 8 * a : 8 * a + length + 8, lane]
                    part = term if part is None else part + term
            total = total + part[b : b + length]
        out[pl.ds(pl.multiple_of(s * length, length), length), lane] = total


def depth_kernel(plan, u, valid, packed, c_out, sum_out, padded, taps, taps_b, part, line, cross, sem,
                 halo_sem, *sems):
    ndp, nseq = plan.ndp, plan.nseq
    arrived = group_barrier(ndp, nseq)
    length = padded.shape[1] - 2 * HALO
    copy = Fetch(plan, packed, sem)("b_pi", taps_b)
    padded[:, HALO : HALO + length] = u[...].reshape(-1, length, D)
    arrived()
    halo = Halo(nseq, padded, halo_sem)
    halo.start()
    copy.wait()
    taps[...] = taps_b[...].astype(jnp.float32)
    halo.finish()
    base = plan.places["w_depth"] - plan.places["b_pi"]
    slide(padded, taps, lambda i: base + i - 1, c_out, length)
    depth, mask = c_out[...], valid[...]
    value = depth * mask
    part[0:1] = total_rows(value)
    part[1:2] = total_rows(value * depth)
    part[2:3] = jnp.broadcast_to(total_rows(mask), (1, LANES))
    part[3:8] = jnp.zeros((5, LANES), jnp.float32)
    sum_out[...] = exchange_sum(ndp, nseq, part, line, cross, sems)


def depth_back_kernel(plan, dz, depth, stats, local, valid, u_pad, packed, u_out, tap_out,
                      padded, own, taps, taps_b, part, line, cross, sem, halo_sem, *sems):
    ndp, nseq = plan.ndp, plan.nseq
    arrived = group_barrier(ndp, nseq)
    seqs, length = padded.shape[0], padded.shape[1] - 2 * HALO
    copy = Fetch(plan, packed, sem)("b_pi", taps_b)
    part[...] = local[...]
    arrived()
    sums = exchange_sum(ndp, nseq, part, line, cross, sems)
    mean, inv_std, count = stats[0:1], stats[1:2], stats[2:3]
    standard = (depth[...] - mean) * inv_std
    d_depth = valid[...] * inv_std * (dz[...] - sums[0:1] / count - standard * (sums[1:2] / count))
    d_depth = d_depth.reshape(seqs, length, D)
    padded[:, HALO : HALO + length] = d_depth
    halo = Halo(nseq, padded, halo_sem)
    halo.start()
    own[:, :8] = jnp.zeros((seqs, 8, D), jnp.float32)
    own[:, 8 : 8 + length] = d_depth
    own[:, 8 + length :] = jnp.zeros((seqs, 8, D), jnp.float32)
    copy.wait()
    taps[...] = taps_b[...].astype(jnp.float32)
    base = plan.places["w_depth"] - plan.places["b_pi"]

    @pl.loop(0, LANES // 128)
    def _(i):
        lane = pl.ds(pl.multiple_of(i * 128, 128), 128)
        for b in range(8):
            sums_b = [None] * 4
            for s in range(seqs):
                moved = own[s, 8 - b : 8 - b + length + 8, lane]
                for a in range(4):
                    if 0 < 8 * a + b < K + 1:
                        term = total_rows(u_pad[s, 8 * a : 8 * a + length + 8, lane] * moved)
                        sums_b[a] = term if sums_b[a] is None else sums_b[a] + term
            for a in range(4):
                if sums_b[a] is not None:
                    tap_out[8 * a + b - 1 : 8 * a + b, lane] = sums_b[a]
        tap_out[K : K + 1, lane] = jnp.zeros((1, 128), jnp.float32)

    halo.finish()
    slide(padded, taps, lambda i: base + K - i, u_out, length)


def head_scores(q, k, line, valid):
    block, full, width = q.shape[0], k.shape[0], line.shape[1]
    scores = lax.dot_general(q, k, (((1,), (1,)), ((), ())), preferred_element_type=jnp.float32)
    spread = jnp.broadcast_to(line, (block, width))
    bias = pltpu.roll(spread, width - block + 1, 1, stride=1, stride_axis=0)[:, :full]
    return jnp.where(valid, scores * (1.0 / math.sqrt(HD)) + bias, -jnp.inf)


def remote(source, target, send, recv, device):
    return pltpu.make_async_remote_copy(
        src_ref=source, dst_ref=target, send_sem=send, recv_sem=recv, device_id=device, device_id_type=MESH
    )


class Team:
    def __init__(self, plan, seqs):
        self.di, self.z = lax.axis_index(DP), lax.axis_index(SEQ)
        self.count, self.seqs = plan.nseq, seqs
        self.c = self.di % 2
        self.base = self.di - self.c
        self.other = self.base + 1 - self.c
        self.owner = self.base + self.z // seqs
        self.main = self.z // seqs == self.c
        self.slot = self.z % seqs
        self.half = pl.ds(pl.multiple_of(self.c * (D // 2), D // 2), D // 2)

    def enter(self):
        barrier = pltpu.get_barrier_semaphore()
        peers = [(self.other, self.z)]
        for i in range(1, self.count):
            to = lax.rem(self.z + i, self.count)
            peers += [(self.di, to), (self.other, to)]
        for peer in peers:
            pl.semaphore_signal(barrier, inc=1, device_id=peer, device_id_type=MESH)
        return lambda: pl.semaphore_wait(barrier, len(peers))

    def turn(self, i):
        return lax.rem(self.z + i, self.count)


def half_copy(packed, plan, name, team, target, sem):
    copy = pltpu.make_async_copy(packed.at[pl.ds(plan.places[name], D), team.half], target, sem)
    copy.start()
    return copy


def attend_kernel(plan, normed, length, tables, packed, ctx_out, all_out, q_out, k_out, v_out, lse_out,
                  w_q, w_k, w_v, b_q, b_v, held, mine, sem, in_send, relay_send, in_recv, ctx_send, ctx_recv):
    seqs, block, _ = normed.shape
    count = plan.nseq
    team = Team(plan, seqs)
    arrived = team.enter()
    fetch = Fetch(plan, packed, sem)
    copies = [fetch("b_q", b_q), fetch("b_v", b_v)]
    for i, (name, target) in enumerate((("w_q", w_q), ("w_k", w_k), ("w_v", w_v))):
        copies.append(half_copy(packed, plan, name, team, target, sem.at[2 + i]))
    arrived()
    c, z = team.c, team.z
    sends = []
    for s in range(seqs):
        to = c * seqs + s
        copy = remote(normed.at[s], all_out.at[z], in_send.at[s], in_recv.at[z], (team.di, to))
        sends.append((to != z, copy))
        pl.when(to != z)(copy.start)
    relays = []
    for i in range(count):
        b = team.turn(i)
        source = normed.at[team.slot] if i == 0 else all_out.at[b]
        relays.append(remote(source, all_out.at[b], relay_send.at[b], in_recv.at[b], (team.other, z)))
    pl.when(team.main)(relays[0].start)

    @pl.when(team.main)
    def _():
        all_out[z] = normed[team.slot]

    wait_all(*copies)
    mine[0] = b_q[...].astype(jnp.float32)
    mine[1] = b_v[...].astype(jnp.float32)
    bias_q, bias_v = mine[0, 0:1, team.half], mine[1, 0:1, team.half]
    for i in range(count):
        b = team.turn(i)
        if i == 0:
            pl.when(jnp.logical_not(team.main))(relays[0].wait_recv)
        else:
            relays[i].wait_recv()
            pl.when(team.main)(relays[i].start)
        part = all_out[b]
        at = pl.ds(pl.multiple_of(b * block, block), block)
        q_out[at, :] = (forward_dot(part, w_q[...]) + bias_q).astype(jnp.bfloat16)
        k_out[at, :] = forward_dot(part, w_k[...]).astype(jnp.bfloat16)
        v_out[at, :] = (forward_dot(part, w_v[...]) + bias_v).astype(jnp.bfloat16)
    full = count * block
    valid = lax.broadcasted_iota(jnp.int32, (1, full), 1) < length[0:1, 0:1]
    lane = lax.broadcasted_iota(jnp.int32, (block, 128), 1)

    def back(b):
        return remote(held.at[b], ctx_out.at[team.slot, :, team.half], ctx_send.at[b],
                      ctx_recv.at[team.slot * 2 + c], (team.owner, b))

    @pl.loop(0, count)
    def _(i):
        b = lax.rem(z + 1 + i, count)
        at = pl.ds(pl.multiple_of(b * block, block), block)
        lse = jnp.zeros((block, 128), jnp.float32)
        for h in range(H // 2):
            cols = slice(h * HD, (h + 1) * HD)
            line = tables[b, pl.ds(c * (H // 2) + h, 1), :]
            scores = head_scores(q_out[at, cols], k_out[:, cols], line, valid)
            top = jnp.max(scores, -1, keepdims=True)
            weights = jnp.exp(scores - top)
            total = jnp.sum(weights, -1, keepdims=True)
            probs = (weights * (1.0 / total)).astype(jnp.bfloat16)
            ctx = jnp.dot(probs, v_out[:, cols], preferred_element_type=jnp.float32)
            held[b, :, cols] = ctx.astype(jnp.bfloat16)
            lse = jnp.where(lane == h, top + jnp.log(total), lse)
        lse_out[at, :] = lse
        own = jnp.logical_and(b == z, team.main)

        @pl.when(own)
        def _():
            ctx_out[team.slot, :, team.half] = held[b]

        @pl.when(jnp.logical_not(own))
        def _():
            back(b).start()

    for s in range(seqs):
        for h in range(2):
            own = jnp.logical_and(c * seqs + s == z, c == h)
            here = ctx_out.at[s, :, pl.ds(h * (D // 2), D // 2)]
            copy = remote(held.at[0], here, ctx_send.at[0], ctx_recv.at[s * 2 + h], (team.di, z))
            pl.when(jnp.logical_not(own))(copy.wait_recv)
    for flag, copy in sends:
        pl.when(flag)(copy.wait_send)
    for i in range(count):
        pl.when(team.main)(relays[i].wait_send)
        b = team.turn(i)
        own = jnp.logical_and(b == z, team.main)
        pl.when(jnp.logical_not(own))(back(b).wait_send)


def attend_back_kernel(plan, d_ctx, q_all, k_all, v_all, lse_all, length, tables, packed,
                       dn_out, dq_out, dk_out, dv_out, dt_out, vec_out,
                       w_q, w_k, w_v, d_in, dq_part, dk_sum, dv_sum, give, take, final, sem,
                       in_send, in_recv, swap_send, swap_recv, dn_send, dn_recv):
    seqs, block, _ = d_ctx.shape
    count = plan.nseq
    full = count * block
    team = Team(plan, seqs)
    arrived = team.enter()
    copies = []
    for i, (name, target) in enumerate((("w_q", w_q), ("w_k", w_k), ("w_v", w_v))):
        copies.append(half_copy(packed, plan, name, team, target, sem.at[i]))
    arrived()
    c, z = team.c, team.z
    sends = []
    for s in range(seqs):
        for h in range(2):
            to = c * seqs + s
            own = jnp.logical_and(to == z, c == h)
            source = d_ctx.at[s, :, pl.ds(h * (D // 2), D // 2)]
            copy = remote(source, d_in.at[z], in_send.at[2 * s + h], in_recv.at[z], (team.base + h, to))
            sends.append((jnp.logical_not(own), copy))
            pl.when(jnp.logical_not(own))(copy.start)

    @pl.when(team.main)
    def _():
        d_in[z] = d_ctx[team.slot, :, team.half]

    dk_sum[...] = jnp.zeros(dk_sum.shape, jnp.float32)
    dv_sum[...] = jnp.zeros(dv_sum.shape, jnp.float32)
    dt_out[...] = jnp.zeros(dt_out.shape, jnp.float32)
    vec_out[...] = jnp.zeros(vec_out.shape, jnp.float32)
    away = pl.ds(pl.multiple_of((1 - c) * (D // 2), D // 2), D // 2)
    for out in (dq_out, dk_out, dv_out):
        out[:, away] = jnp.zeros((full, D // 2), jnp.bfloat16)
    valid = lax.broadcasted_iota(jnp.int32, (1, full), 1) < length[0:1, 0:1]
    rows = (((0,), (0,)), ((), ()))
    inv = 1.0 / math.sqrt(HD)

    @pl.loop(0, count)
    def _(i):
        b = lax.rem(z + i, count)
        own = jnp.logical_and(b == z, team.main)
        copy = remote(d_in.at[b], d_in.at[b], in_send.at[0], in_recv.at[b], (team.di, z))
        pl.when(jnp.logical_not(own))(copy.wait_recv)
        at = pl.ds(pl.multiple_of(b * block, block), block)
        totals = []
        for h in range(H // 2):
            cols = slice(h * HD, (h + 1) * HD)
            q, k, v = q_all[at, cols], k_all[:, cols], v_all[:, cols]
            dctx = d_in[b, :, cols]
            line = tables[b, pl.ds(c * (H // 2) + h, 1), :]
            width = line.shape[1]
            scores = head_scores(q, k, line, valid)
            probs = jnp.exp(scores - lse_all[at, h : h + 1])
            d_probs = lax.dot_general(dctx, v, (((1,), (1,)), ((), ())), preferred_element_type=jnp.float32)
            delta = jnp.sum(probs * d_probs, -1, keepdims=True)
            d_scores = probs * (d_probs - delta)
            d_scores_b = d_scores.astype(jnp.bfloat16)
            dq = jnp.dot(d_scores_b, k, preferred_element_type=jnp.float32) * inv
            totals.append(total_rows(dq))
            dk_sum[:, cols] += lax.dot_general(d_scores_b, q, rows, preferred_element_type=jnp.float32)
            dv_sum[:, cols] += lax.dot_general(
                probs.astype(jnp.bfloat16), dctx, rows, preferred_element_type=jnp.float32
            )
            dq_part[at, cols] = dq.astype(jnp.bfloat16)
            wide = jnp.concatenate([d_scores, jnp.zeros((block, width - full), jnp.float32)], 1)
            folded = pltpu.roll(wide[0:8], block - 1, 1)
            for g in range(1, block // 8):
                folded = folded + pltpu.roll(wide[8 * g : 8 * g + 8], block - 1 - 8 * g, 1)
            line = folded[0:1]
            for r in range(1, 8):
                line = line + pltpu.roll(folded[r : r + 1], width - r, 1)
            dt_out[b, pl.ds(c * (H // 2) + h, 1), :] = line
        vec_out[0:1, team.half] += jnp.concatenate(totals, 1)

    vec_out[1:2, team.half] = total_rows(dv_sum[...])
    dk_part = (dk_sum[...] * inv).astype(jnp.bfloat16)
    dk_out[:, team.half] = dk_part
    dv_part = dv_sum[...].astype(jnp.bfloat16)
    dv_out[:, team.half] = dv_part
    dq_out[:, team.half] = dq_part[...]
    wait_all(*copies)

    def partial(b):
        at = pl.ds(pl.multiple_of(b * block, block), block)
        dk_rows, dv_rows = dk_out[at, team.half], dv_out[at, team.half]
        return back_dot(dq_part[at, :], w_q[...]) + back_dot(dk_rows, w_k[...]) + back_dot(dv_rows, w_v[...])

    share = count // 2
    swaps, ends = [], []
    for i in range(share):
        give[i] = partial((1 - c) * share + i).astype(jnp.bfloat16)
        copy = remote(give.at[i], take.at[i], swap_send.at[i], swap_recv.at[i], (team.other, z))
        copy.start()
        swaps.append(copy)
    for i in range(share):
        b = c * share + i
        value = partial(b)
        swaps[i].wait_recv()
        value = (value + take[i].astype(jnp.float32)).astype(jnp.bfloat16)
        final[i] = value
        own = jnp.logical_and(b == z, team.main)
        copy = remote(final.at[i], dn_out.at[team.slot], dn_send.at[i], dn_recv.at[team.slot], (team.owner, b))
        ends.append((jnp.logical_not(own), copy))
        pl.when(jnp.logical_not(own))(copy.start)

        @pl.when(own)
        def _():
            dn_out[team.slot] = final[i]

    for s in range(seqs):
        own = jnp.logical_and(c * seqs + s == z, z // share == c)
        copy = remote(final.at[0], dn_out.at[s], dn_send.at[0], dn_recv.at[s], (team.di, z))
        pl.when(jnp.logical_not(own))(copy.wait_recv)
    for copy in swaps:
        copy.wait_send()
    for flag, copy in sends + ends:
        pl.when(flag)(copy.wait_send)


VMEM_SPEC = pl.BlockSpec(memory_space=pltpu.VMEM)
ANY_SPEC = pl.BlockSpec(memory_space=pl.ANY)


def stage(kernel, plan, operands, packed, outs, scratch, name, number=None):
    params = {}
    if number is not None:
        params = {"collective_id": number, "has_side_effects": True}
    specs = [VMEM_SPEC] * len(operands) + [ANY_SPEC]
    return pl.pallas_call(
        functools.partial(kernel, plan),
        out_shape=[jax.ShapeDtypeStruct(shape, dtype) for shape, dtype in outs],
        in_specs=specs,
        out_specs=[VMEM_SPEC] * len(outs),
        scratch_shapes=scratch,
        compiler_params=pltpu.CompilerParams(vmem_limit_bytes=56 * 1024 * 1024, **params),
        name=name,
    )(*operands, packed)


F32, BF16 = jnp.float32, jnp.bfloat16
DMA = pltpu.SemaphoreType.DMA


def vm(shape, dtype=jnp.bfloat16):
    return pltpu.VMEM(shape, dtype)


def exchange_scratch(plan):
    return [vm((8, D), F32), vm((plan.nseq, 8, D), F32), vm((plan.ndp, 8, D), F32), DMA((1,)), DMA((4,)),
            DMA((plan.nseq,)), DMA((plan.nseq,)), DMA((plan.ndp,)), DMA((plan.ndp,))]


def per_device(inputs, lengths, rel_bucket, params, moment_one, moment_two, cotangent):
    seq_count, block_len, model_width = inputs.shape
    rows = seq_count * block_len
    first_pos = lax.axis_index(SEQ) * block_len
    positions = first_pos + jnp.arange(block_len, dtype=jnp.int32)
    valid_own = positions[None, :] < lengths[:, None]
    valid = valid_own.astype(jnp.float32).reshape(-1, 1)
    onehot = bucket_windows(rel_bucket, block_len, lax.axis_size(SEQ))
    core = lax.axis_index(DP) % 2
    paired = lax.ppermute(lengths, DP, [(i, i + 1 - 2 * (i % 2)) for i in range(lax.axis_size(DP))])
    group_lengths = jnp.concatenate(
        [jnp.where(core == 0, lengths, paired), jnp.where(core == 0, paired, lengths)]
    )
    assert group_lengths.shape[0] == lax.axis_size(SEQ)
    length = jnp.broadcast_to(lax.dynamic_slice(group_lengths, (lax.axis_index(SEQ),), (1,))[:, None], (1, 128))
    plan = Plan(lax.axis_size(DP), lax.axis_size(SEQ), params.shape[0])
    packed = gather(plan, own_block(plan, params)).reshape(-1, LANES)
    full, wide = (rows, D), (rows, FF)
    square, tall, group = vm((D, D)), vm((FF, D)), vm((8, D))
    mix = vm((LANES // 128, 256, 128), F32)
    stream0 = inputs.reshape(full)
    stream1, normed2, w_first = stage(
        ffn_first_kernel, plan, [stream0], packed,
        [(full, F32), (full, BF16), ((FF // D, D, D), BF16)],
        [tall, tall, group, group, group, mix, DMA((5,))], "ffn_first",
    )
    table_row = plan.places["rel"]
    rel = packed[table_row : table_row + 1, : NB * H].reshape(NB, H)
    tables = jnp.einsum("nh,bnw->bhw", rel, onehot.astype(BF16), preferred_element_type=F32)
    tall_half, split = (plan.nseq * block_len, D // 2), (plan.nseq, block_len, D // 2)
    local3, all3 = (seq_count, block_len, D), (plan.nseq, block_len, D)
    half, nseq = vm((D, D // 2)), plan.nseq
    context, owned, queries, keys, values, lse = stage(
        attend_kernel, plan, [normed2.reshape(local3), length, tables], packed,
        [(local3, BF16), (all3, BF16), (tall_half, BF16), (tall_half, BF16), (tall_half, BF16),
         ((tall_half[0], 128), F32)],
        [half, half, half, group, group, vm(split), vm((2, 8, D), F32), DMA((5,)), DMA((seq_count,)), DMA((nseq,)),
         DMA((nseq,)), DMA((nseq,)), DMA((2 * seq_count,))], "attend", 4,
    )
    context = context.reshape(full)
    stream2, normed3, pre_gate, gated, w_gate = stage(
        gate_kernel, plan, [context, stream1, valid], packed,
        [(full, F32), (full, BF16), ((rows, 2 * D), F32), (full, F32), ((2, D, D), BF16)],
        [square, vm((2 * D, D)), group, group, mix, DMA((4,))], "gate",
    )
    padded_shape = (seq_count, block_len + 2 * HALO, D)
    depth, sums, padded = stage(
        depth_kernel, plan, [gated, valid], packed,
        [(full, F32), ((8, D), F32), (padded_shape, F32)],
        [vm((40, D), F32), vm((40, D))] + exchange_scratch(plan), "depth", 2,
    )
    (output, d_stream3, d_standard, local, stats, active3, grad3_b, active4, half4, normed4, d_hidden4,
     vec_mid) = stage(
        middle_kernel, plan, [stream2, depth, sums, cotangent.reshape(full), valid], packed,
        [(full, F32), (full, F32), (full, F32), ((8, D), F32), ((8, D), F32), (full, BF16), (full, BF16),
         (wide, BF16), (full, BF16), (full, BF16), (wide, BF16), ((16, D), F32)],
        [square, tall, tall, vm((FF // D, D, D)), vm((FF // D, rows, D), F32), vm((40, D)), group, group, group,
         mix, DMA((7,))], "middle",
    )
    d_gated, tap_grads = stage(
        depth_back_kernel, plan, [d_standard, depth, stats, local, valid, padded], packed,
        [(full, F32), ((32, D), F32)],
        [vm(padded_shape, F32), vm((seq_count, block_len + 16, D), F32), vm((40, D), F32), vm((40, D))]
        + exchange_scratch(plan), "depth_back", 3,
    )
    d_gate, d_stream2, grad2_b, d_context, vec_gate = stage(
        gate_back_kernel, plan, [d_gated, pre_gate, stream2, d_stream3, valid, w_gate], packed,
        [((rows, 2 * D), BF16), (full, F32), (full, BF16), (full, BF16), ((8, D), F32)],
        [square, group, DMA((2,))], "gate_back",
    )
    whole = (tall_half[0], D)
    d_norm2, d_query, d_key, d_value, d_tables, vec_attend = stage(
        attend_back_kernel, plan, [d_context.reshape(local3), queries, keys, values, lse, length, tables], packed,
        [(local3, BF16), (whole, BF16), (whole, BF16), (whole, BF16), (tables.shape, F32), ((8, D), F32)],
        [half, half, half, vm(split), vm(tall_half), vm(tall_half, F32), vm(tall_half, F32),
         vm((nseq // 2, block_len, D)), vm((nseq // 2, block_len, D)), vm((nseq // 2, block_len, D)), DMA((3,)),
         DMA((2 * seq_count,)), DMA((nseq,)), DMA((nseq // 2,)), DMA((nseq // 2,)), DMA((nseq // 2,)),
         DMA((seq_count,))], "attend_back", 5,
    )
    rel_grad = jnp.einsum("bnw,bhw->nh", onehot, d_tables, precision=lax.Precision.HIGHEST).reshape(1, -1)
    owned = owned.reshape(whole)
    d_stream0, active1, half1, normed1, d_hidden1, vec_first = stage(
        ffn_first_back_kernel, plan, [stream0, stream1, d_stream2, d_norm2.reshape(full), w_first], packed,
        [(full, F32), (wide, BF16), (full, BF16), (full, BF16), (wide, BF16), ((16, D), F32)],
        [tall, group, group, group, DMA((4,))], "ffn_first_back",
    )
    gradients = {
        "w_k": (owned, d_key), "w_v": (owned, d_value),
        "first_w_in": (normed1, d_hidden1), "first_w_out": (active1, half1), "w_q": (owned, d_query),
        "w_o": (context, grad2_b), "w_pi": (normed3, d_gate), "w_po": (active3, grad3_b),
        "second_w_in": (normed4, d_hidden4), "second_w_out": (active4, half4),
    }
    places = {
        "attn_ng": (0, 0), "attn_nb": (0, 1), "first_b_out": (0, 2), "first_ng": (0, 3), "first_nb": (0, 4),
        "first_b_in": (0, 5), "b_pi": (1, 0), "conv_ng": (1, 2), "conv_nb": (1, 3), "b_o": (1, 4),
        "fin_g": (2, 0), "fin_b": (2, 1), "second_b_out": (2, 2), "second_ng": (2, 3), "second_nb": (2, 4),
        "b_po": (2, 5), "bng": (2, 6), "bnb": (2, 7), "second_b_in": (2, 8), "w_depth": (3, 0),
        "b_q": (4, 0), "b_v": (4, 1), "rel": (5, 0),
    }
    vectors = [vec_first, vec_gate, vec_mid, tap_grads, vec_attend, rel_grad]
    window = scatter(plan, weight_grads(plan, gradients, vectors, places))
    grad_shard = own_shard(plan, window)
    new_params, new_first, new_second = adam_update(params, grad_shard, moment_one, moment_two)
    return (
        output.reshape(inputs.shape),
        d_stream0.reshape(inputs.shape),
        grad_shard,
        new_params,
        new_first,
        new_second,
    )


def solution(mesh):
    return jax.shard_map(
        per_device,
        mesh=mesh,
        in_specs=(
            P(DP, SEQ, None),
            P(DP),
            P(),
            P((DP, SEQ)),
            P((DP, SEQ)),
            P((DP, SEQ)),
            P(DP, SEQ, None),
        ),
        out_specs=(
            P(DP, SEQ, None),
            P(DP, SEQ, None),
            P((DP, SEQ)),
            P((DP, SEQ)),
            P((DP, SEQ)),
            P((DP, SEQ)),
        ),
        check_vma=False,
    )
```

```python
import functools
import math

import jax
import jax.numpy as jnp
from jax import lax
from jax.experimental import pallas as pl
from jax.experimental.pallas import tpu as pltpu
from jax.sharding import PartitionSpec as P

D = 512
H = 8
HD = 64
FF = 2048
K = 31
NB = 32
DP = "dp"
SEQ = "seq"
STEP = 4


NORM_EPS = 1e-05
BATCH_EPS = 1e-05
LEARN_RATE = 0.005
DECAY = 0.01
BETA_ONE = 0.9
BETA_TWO = 0.98
ADAM_EPS = 1e-08


def segments():

    def feed_block(prefix):
        return [
            (prefix + "_ng", (D,)),
            (prefix + "_nb", (D,)),
            (prefix + "_w_in", (D, FF)),
            (prefix + "_b_in", (FF,)),
            (prefix + "_w_out", (FF, D)),
            (prefix + "_b_out", (D,)),
        ]

    listing = feed_block("first")
    listing = listing + [
        ("attn_ng", (D,)),
        ("attn_nb", (D,)),
        ("w_q", (D, D)),
        ("b_q", (D,)),
        ("w_k", (D, D)),
        ("w_v", (D, D)),
        ("b_v", (D,)),
        ("w_o", (D, D)),
        ("b_o", (D,)),
        ("rel", (NB, H)),
    ]
    listing = listing + [
        ("conv_ng", (D,)),
        ("conv_nb", (D,)),
        ("w_pi", (D, 2 * D)),
        ("b_pi", (2 * D,)),
        ("w_depth", (K, D)),
        ("bng", (D,)),
        ("bnb", (D,)),
        ("w_po", (D, D)),
        ("b_po", (D,)),
    ]
    listing = listing + feed_block("second") + [("fin_g", (D,)), ("fin_b", (D,))]
    return listing


def arrange():
    places, gaps = {}, []
    linear = inner = 0
    for entry_name, entry_shape in segments():
        extent = math.prod(entry_shape)
        tail = 2 * D if entry_name == "conv_ng" else 0
        if extent >= D * D or tail:
            pad = -(inner + tail) % TILE
            if pad:
                gaps.append((linear, pad))
                inner = inner + pad
        places[entry_name] = inner // LANES
        linear, inner = linear + extent, inner + extent
    return places, gaps, -(-inner // TILE)


def device_index():
    return lax.axis_index(DP) * lax.axis_size(SEQ) + lax.axis_index(SEQ)


def own_shard(plan, window):
    table = jnp.asarray(plan.shard_table, jnp.int32)[device_index()]
    flat = window.reshape(-1)
    early = lax.dynamic_slice(flat, (table[0],), (plan.shard,))
    late = lax.dynamic_slice(flat, (table[0] + table[2],), (plan.shard,))
    return jnp.where(jnp.arange(plan.shard, dtype=jnp.int32) < table[1], early, late)


def swish_act(values):
    return values * jax.nn.sigmoid(values)


def swish_grad(values):
    sig_vals = jax.nn.sigmoid(values)
    return sig_vals * (1.0 + values * (1.0 - sig_vals))


def forward_dot(left_mat, weight):
    return jnp.dot(left_mat, weight, preferred_element_type=jnp.float32)


def back_dot(grad_in, weight):
    return lax.dot_general(
        grad_in, weight, (((1,), (1,)), ((), ())), preferred_element_type=jnp.float32
    )


MESH = pl.DeviceIdType.MESH
LANES=512
TILE=8*LANES

class Plan:
    def __init__(self, ndp, nseq, shard):
        self.ndp, self.nseq, self.shard = ndp, nseq, shard
        self.k = ndp.bit_length() - 1
        self.phases = self.k - 1
        self.n = n = ndp * nseq
        self.places, self.gaps, self.total = arrange()
        begins = [self.inner(d * shard) for d in range(n)]
        starts = [-(-b // TILE) for b in begins] + [self.total]
        sizes = [b - a for a, b in zip(starts, starts[1:])]
        self.lo, self.hi = min(sizes), max(sizes)
        self.slots = nseq * 2**self.phases
        floors = [b // TILE for b in begins]
        ends = [self.inner((d + 1) * shard - 1) // TILE + 1 for d in range(n)]
        self.win = max(e - f for e, f in zip(ends, floors))
        self.win += self.win % 2
        self.padded = max(self.total, max(floors) + self.win)
        self.block_table, self.shard_table = [], []
        for d in range(n):
            near = [g for g in self.gaps if d * shard < g[0] < (d + 1) * shard + TILE]
            assert len(near) <= 1
            cut, size = near[0] if near else (2**30, 0)
            lead = starts[d] * TILE - begins[d]
            self.block_table.append((lead, cut - d * shard - lead, size))
            self.shard_table.append((begins[d] - floors[d] * TILE, cut - d * shard, size))

    def inner(self, position):
        if isinstance(position, int):
            return position + sum(size for at, size in self.gaps if at <= position)
        result = position
        for at, size in self.gaps:
            result = result + jnp.where(position >= at, size, 0)
        return result

    def order(self):
        ev=[]
        for s in range(self.nseq):
            for sign in ((0,) if s==0 else (-1,1)):
                for t in range(2**self.phases):
                    ev.append((s+0.5*bin(t).count("1")+0.01*t, s, sign, t))
        ev.sort()
        return [e[1:] for e in ev]

def flip(di, mask_bits, bits, t, phases):
    out=di
    for p in range(phases):
        if (t>>p)&1:
            out = out + mask_bits[p]*(1-2*bits[p])
    return out

def phase_masks(di, c, phases):
    masks, bits=[],[]
    for p in range(phases):
        a, b = 1<<(p+1), 1<<(phases-p)
        masks.append(a+c*(b-a))
        ba, bb = (di//a)%2, (di//b)%2
        bits.append(ba+c*(bb-ba))
    return masks, bits

def block_of(plan, dpi, z):
    d = dpi*plan.nseq+z
    a = (plan.inner(d*plan.shard)+TILE-1)//TILE
    b = (plan.inner((d+1)*plan.shard)+TILE-1)//TILE
    b = jnp.where(d == plan.n-1, plan.total, b)
    return a, b-a

def floor_of(plan, dpi, z):
    return plan.inner((dpi*plan.nseq+z)*plan.shard)//TILE

FRONT, NEAR, BACK = 32, 40, 64


def shard_rows(plan):
    return -(-plan.shard // 1024) * 8


def place_rows(plan, rolled, block, first, rows, lead, cut, skip):
    shift, begin = lead % 128, FRONT + lead // 128
    lane = lax.broadcasted_iota(jnp.int32, (rows, 128), 1)
    at = (lax.broadcasted_iota(jnp.int32, (rows, 128), 0) + first) * LANES + lane
    for j in range(LANES // 128):

        def read(start):
            here = rolled[pl.ds(start, rows, stride=4), :]
            after = rolled[pl.ds(start + 1, rows, stride=4), :]
            return jnp.where(lane < 128 - shift, here, after)

        start = begin + j + 4 * first
        value = jnp.where(at + 128 * j < cut, read(start), read(start - skip)).astype(block.dtype)
        part = slice(first // 8, (first + rows) // 8)
        block[part, :, j * 128 : (j + 1) * 128] = value.reshape(rows // 8, 8, 128)


def gather_kernel(plan, x, out, src, line, rolled, give, take, near_sem, send_a, send_b, recv_a, recv_b, loc_sem):
    di, z = lax.axis_index(DP), lax.axis_index(SEQ)
    ns, ph = plan.nseq, plan.phases
    c = di%2
    masks, bits = phase_masks(di, c, ph)
    other = di+1-2*c
    omasks, obits = phase_masks(other, 1-c, ph)
    up, down = lax.rem(z+1,ns), lax.rem(z+ns-1,ns)
    partners=[(di,up),(di,down),(other,z)]+[(flip(di,masks,bits,1<<p,ph),z) for p in range(ph)]
    barrier=pltpu.get_barrier_semaphore()
    for a,b in partners:
        pl.semaphore_signal(barrier,inc=1,device_id=(a,b),device_id_type=MESH)
    index = di * ns + z
    following, before = lax.rem(index + 1, plan.n), lax.rem(index + plan.n - 1, plan.n)
    pl.semaphore_signal(barrier, inc=1, device_id=(following // ns, lax.rem(following, ns)), device_id_type=MESH)
    lo, more = plan.lo-1, plan.hi-plan.lo+1
    start_own, size_own = block_of(plan, di, z)
    rows = x.shape[0]
    joint, shift = divmod(plan.shard, 128)
    lane = lax.broadcasted_iota(jnp.int32, (NEAR, 128), 1)
    moved = pltpu.roll(x[:NEAR], shift, 1)
    earlier = jnp.concatenate([jnp.zeros((1, 128), jnp.float32), moved[: NEAR - 1]], 0)
    give[...] = jnp.where(lane >= shift, moved, earlier)
    line[:FRONT] = jnp.zeros((FRONT, 128), jnp.float32)
    line[FRONT : FRONT + rows] = x[...]
    line[FRONT + rows :] = jnp.zeros((line.shape[0] - FRONT - rows, 128), jnp.float32)
    begin = index * plan.shard
    inner = plan.inner(begin)
    lead = (inner + TILE - 1) // TILE * TILE - inner
    cut, skip = 2**30, 0
    for position, size in plan.gaps:
        hit = jnp.logical_and(position > begin, position < begin + plan.shard + TILE)
        cut = jnp.where(hit, position - begin - lead, cut)
        skip = jnp.where(hit, size // 128, skip)
    turn = lax.rem(128 - lead % 128, 128)
    rolled[...] = pltpu.roll(line[...], turn, 1)
    place_rows(plan, rolled, src, 0, 8 * lo, lead, cut, skip)
    pl.semaphore_wait(barrier,len(partners)+1)
    near = pltpu.make_async_remote_copy(src_ref=give,dst_ref=take,send_sem=near_sem.at[0],recv_sem=near_sem.at[1],
        device_id=(before // ns, lax.rem(before, ns)),device_id_type=MESH)
    near.start()

    def pair(ref, base, dst_start, size, sidx, ridx, dev):
        copies=[pltpu.make_async_remote_copy(src_ref=ref.at[pl.ds(base,lo)],dst_ref=out.at[pl.ds(dst_start,lo)],
            send_sem=send_a.at[sidx],recv_sem=recv_a.at[ridx],device_id=dev,device_id_type=MESH)]
        for x in range(more):
            copies.append(pltpu.make_async_remote_copy(src_ref=ref.at[pl.ds(base+lo+x,1)],dst_ref=out.at[pl.ds(dst_start+lo+x,1)],
                send_sem=send_b.at[sidx*more+x],recv_sem=recv_b.at[ridx*more+x],device_id=dev,device_id_type=MESH))
        return copies, size
    def each(p, act, part=None):
        for x,copy in enumerate(p[0]):
            if part is not None and (x==0) != (part==0): continue
            if x<2: act(copy)
            else:
                @pl.when(p[1]>=lo+x)
                def _(): act(copy)
    def start(p,part): each(p, lambda c: c.start(), part)
    def wait_send(p): each(p, lambda c: c.wait_send())
    def wait_recv(p,part=None): each(p, lambda c: c.wait_recv(), part)

    own=[pltpu.make_async_copy(src.at[pl.ds(0,lo)],out.at[pl.ds(start_own,lo)],loc_sem.at[0])]
    for x in range(more):
        own.append(pltpu.make_async_copy(src.at[pl.ds(lo+x,1)],out.at[pl.ds(start_own+lo+x,1)],loc_sem.at[1+x]))
    own=(own,size_own)
    own[0][0].start()
    def finish_block():
        near.wait_recv()
        at = FRONT + joint
        line[at:at+1] = line[at:at+1] + take[0:1]
        line[at+1:at+NEAR] = take[1:]
        low = at // 8 * 8
        rolled[low:] = pltpu.roll(line[low:], turn, 1)
        place_rows(plan, rolled, src, 8*lo, 8*more, lead, cut, skip)
        for x,copy in enumerate(own[0][1:]):
            if x==0: copy.start()
            else:
                @pl.when(size_own>lo+x)
                def _(): copy.start()
    nslot=plan.slots
    sends=[]
    def guard(conds, fn):
        if not conds: fn(); return
        cond=conds[0]
        for x in conds[1:]: cond=jnp.logical_and(cond,x)
        @pl.when(cond)
        def _(): fn()

    tasks=[]
    for s, sign, t in plan.order():
        zz = z+sign*s
        conds=[] if s==0 else ([zz>=0] if sign<0 else [zz<ns])
        dpi=flip(di,masks,bits,t,ph)
        st,size=block_of(plan,dpi,zz)
        mine = s==0 and t==0
        ref, base = (src, 0) if mine else (out, st)
        slot = t*ns+zz
        got = None if mine else pair(out,st,st,size,0,slot,(di,z))
        copies=[]
        def forward(conds, ridx, dev):
            p=pair(ref,base,st,size,len(sends),ridx,dev)
            sends.append((conds,p))
            copies.append((conds,p))
        if t==0:
            if sign<=0 : forward(conds+[z<ns-1],slot,(di,z+1))
            if sign>=0 : forward(conds+[z>0],slot,(di,z-1))
        for pp in range(t.bit_length(),ph):
            forward(conds,slot+(1<<pp)*ns,(flip(di,masks,bits,1<<pp,ph),z))
        forward(conds,nslot+slot,(other,z))
        tasks.append((conds,got,copies))
    def run(task,part):
        conds,got,copies=task
        if got is None:
            if part==1: finish_block()
        else:
            guard(conds, lambda: wait_recv(got,part))
        for also,p in copies:
            guard(also, lambda: start(p,part))
    lag=4
    for i in range(len(tasks)+lag):
        if i<len(tasks): run(tasks[i],0)
        if i>=lag: run(tasks[i-lag],1)
    for s, sign, t in plan.order():
        zz=z+sign*s
        conds=[] if s==0 else ([zz>=0] if sign<0 else [zz<ns])
        dpi=flip(other,omasks,obits,t,ph)
        st,size=block_of(plan,dpi,zz)
        p=pair(out,st,st,size,0,nslot+t*ns+zz,(di,z))
        guard(conds,lambda: wait_recv(p))
    for conds,p in sends:
        guard(conds,lambda: wait_send(p))
    each(own, lambda c: c.wait())
    near.wait_send()

def count_sends(plan):
    n=0
    for s,sign,t in plan.order():
        if t==0: n+= (2 if sign==0 else 1)
        n+=plan.phases-t.bit_length()+1
    return n

def gather(plan, params):
    ns, more = count_sends(plan), plan.hi - plan.lo + 1
    rows = shard_rows(plan)
    lines = FRONT + rows + NEAR + BACK
    lines += -lines % 8
    values = jnp.pad(params, (0, rows * 128 - plan.shard)).reshape(rows, 128)
    return pl.pallas_call(
        functools.partial(gather_kernel, plan),
        out_shape=jax.ShapeDtypeStruct((plan.total, 8, LANES), jnp.bfloat16),
        in_specs=[pl.BlockSpec(memory_space=pltpu.VMEM)],
        out_specs=pl.BlockSpec(memory_space=pl.ANY),
        scratch_shapes=[
            pltpu.VMEM((plan.hi, 8, LANES), jnp.bfloat16), pltpu.VMEM((lines, 128), jnp.float32),
            pltpu.VMEM((lines, 128), jnp.float32), pltpu.VMEM((NEAR, 128), jnp.float32),
            pltpu.VMEM((NEAR, 128), jnp.float32), pltpu.SemaphoreType.DMA((2,)),
            pltpu.SemaphoreType.DMA((ns,)), pltpu.SemaphoreType.DMA((ns * more,)),
            pltpu.SemaphoreType.DMA((2 * plan.slots,)), pltpu.SemaphoreType.DMA((2 * plan.slots * more,)),
            pltpu.SemaphoreType.DMA((1 + more,)),
        ],
        compiler_params=pltpu.CompilerParams(collective_id=0, has_side_effects=True),
        name="gather_params",
    )(values)


def scatter_kernel(plan, g, out, acc, rc, rp, rz, load_sem, send_sem, core_send, core_recv, ph_recv, z_recv):
    di, z = lax.axis_index(DP), lax.axis_index(SEQ)
    ns, ph, win, nslot = plan.nseq, plan.phases, plan.win, plan.slots
    c = di%2
    masks, bits = phase_masks(di, c, ph)
    other = di+1-2*c
    omasks, obits = phase_masks(other, 1-c, ph)
    up, down = lax.rem(z+1,ns), lax.rem(z+ns-1,ns)
    partners=[(di,up),(di,down),(other,z)]+[(flip(di,masks,bits,1<<p,ph),z) for p in range(ph)]
    barrier=pltpu.get_barrier_semaphore()
    for a,b in partners:
        pl.semaphore_signal(barrier,inc=1,device_id=(a,b),device_id_type=MESH)
    order=list(reversed(plan.order()))
    def cond_of(s,sign):
        zz=z+sign*s
        return zz,([] if s==0 else ([zz>=0] if sign<0 else [zz<ns]))
    def guard(conds, fn):
        if not conds: fn(); return
        cond=conds[0]
        for x in conds[1:]: cond=jnp.logical_and(cond,x)
        @pl.when(cond)
        def _(): fn()
    def load(s,sign,t):
        zz,conds=cond_of(s,sign)
        slot=t*ns+zz
        st=floor_of(plan,flip(di,masks,bits,t,ph),zz)
        return conds,pltpu.make_async_copy(g.at[pl.ds(st,win)],acc.at[slot],load_sem.at[slot])
    def core(s,sign,t):
        zz,conds=cond_of(s,sign)
        slot=t*ns+zz
        st=floor_of(plan,flip(other,omasks,obits,t,ph),zz)
        return conds,pltpu.make_async_remote_copy(src_ref=g.at[pl.ds(st,win)],dst_ref=rc.at[slot],
            send_sem=core_send.at[slot],recv_sem=core_recv.at[slot],device_id=(other,z),device_id_type=MESH)
    for e in order:
        conds,cp=load(*e)
        guard(conds,lambda: cp.start())
    pl.semaphore_wait(barrier,len(partners))
    for e in order:
        conds,cp=core(*e)
        guard(conds,lambda: cp.start())
    sends=[]
    def send(conds,slot,dst,rsem,dev):
        i=len(sends)
        cp=pltpu.make_async_remote_copy(src_ref=acc.at[slot],dst_ref=dst,send_sem=send_sem.at[i],recv_sem=rsem,
            device_id=dev,device_id_type=MESH)
        sends.append((conds,cp))
        guard(conds,lambda: cp.start())
    def waiting(conds,dst,rsem):
        cp=pltpu.make_async_remote_copy(src_ref=dst,dst_ref=dst,send_sem=send_sem.at[0],recv_sem=rsem,
            device_id=(di,z),device_id_type=MESH)
        guard(conds,lambda: cp.wait_recv())
    step=2
    def add(dst, slot, parts, final=False):
        @pl.loop(0,win//step)
        def _(i):
            r=pl.ds(i*step,step)
            v=acc[slot,r].astype(jnp.float32)
            for p in parts:
                v=v+p(r).astype(jnp.float32)
            if final: out[r]=v
            else: acc[slot,r]=v.astype(acc.dtype)
    for s,sign,t in order:
        zz,conds=cond_of(s,sign)
        slot=t*ns+zz
        hi_bit=t.bit_length()
        def fn():
            load(s,sign,t)[1].wait()
            waiting([],rc.at[slot],core_recv.at[slot])
            parts=[lambda r: rc[slot,r]]
            for pp in range(hi_bit,ph):
                idx=((1<<pp)-1)*ns+slot
                waiting([],rp.at[idx],ph_recv.at[idx])
                parts.append(lambda r,idx=idx: rp[idx,r])
            add(None,slot,parts,final=False) if not (t==0 and s==0) else add(None,slot,parts,final=True)
        guard(conds,fn)
        if t:
            pp=hi_bit-1
            idx=((1<<pp)-1)*ns+slot-(1<<pp)*ns
            send(conds,slot,rp.at[idx],ph_recv.at[idx],(flip(di,masks,bits,1<<pp,ph),z))
        else:
            def zadd(stream, extra):
                zi=stream*ns+zz
                def fz():
                    waiting([],rz.at[zi],z_recv.at[zi])
                    @pl.loop(0,win//step)
                    def _(i):
                        r=pl.ds(i*step,step)
                        if s==0:
                            out[r]=out[r]+rz[zi,r].astype(jnp.float32)
                        else:
                            acc[slot,r]=(acc[slot,r].astype(jnp.float32)+rz[zi,r].astype(jnp.float32)).astype(acc.dtype)
                guard(conds+extra,fz)
            if sign>=0: zadd(0,[z>0])
            if sign<=0: zadd(1,[z<ns-1])
            if sign>0: send(conds,slot,rz.at[zz],z_recv.at[zz],(di,z+1))
            if sign<0: send(conds,slot,rz.at[ns+zz],z_recv.at[ns+zz],(di,z-1))
    for e in order:
        conds,cp=core(*e)
        guard(conds,lambda: cp.wait_send())
    for conds,cp in sends:
        guard(conds,lambda: cp.wait_send())

def scatter(plan, g):
    win,ns,ph,nslot=plan.win,plan.nseq,plan.phases,plan.slots
    nsend=len(plan.order())
    return pl.pallas_call(
        functools.partial(scatter_kernel,plan),
        out_shape=jax.ShapeDtypeStruct((win,8,LANES),jnp.float32),
        in_specs=[pl.BlockSpec(memory_space=pl.ANY)],
        out_specs=pl.BlockSpec(memory_space=pltpu.VMEM),
        scratch_shapes=[pltpu.VMEM((nslot,win,8,LANES),g.dtype),pltpu.VMEM((nslot,win,8,LANES),g.dtype),
            pltpu.VMEM(((2**ph-1)*ns,win,8,LANES),g.dtype),pltpu.VMEM((2*ns,win,8,LANES),g.dtype),
            pltpu.SemaphoreType.DMA((nslot,)),pltpu.SemaphoreType.DMA((nsend,)),
            pltpu.SemaphoreType.DMA((nslot,)),pltpu.SemaphoreType.DMA((nslot,)),
            pltpu.SemaphoreType.DMA(((2**ph-1)*ns,)),pltpu.SemaphoreType.DMA((2*ns,))],
        compiler_params=pltpu.CompilerParams(collective_id=1,has_side_effects=True,vmem_limit_bytes=48*1024*1024),
        name="scatter_grads",
    )(g)


def weight_kernel(plan, names, places, *refs):
    count = 2 * len(names)
    sources, refs = refs[:count], refs[count:]
    vectors, refs = refs[: len(refs) - count - 4], refs[len(refs) - count - 4 :]
    target, stores, (out, mix, sem) = refs[0], refs[1 : count + 1], refs[count + 1 :]
    loads = []
    for i in range(count):
        loads.append(pltpu.make_async_copy(sources[i], stores[i], sem.at[i]))
        loads[i].start()
    rows = (((0,), (0,)), ((), ()))
    sent = []

    def send(first, tiles):
        if tiles:
            part = pl.ds(first, tiles)
            copy = pltpu.make_async_copy(out.at[part], target.at[part], sem.at[count + len(sent)])
            copy.start()
            sent.append(copy)

    edge = 0
    for name, shape in segments():
        if math.prod(shape) < D * D:
            first = plan.places[name]
            array, begin = places[name]
            for r in range(-(-math.prod(shape) // LANES)):
                line = vectors[array][begin + r : begin + r + 1, :]
                tile, row = divmod(first + r, 8)
                out[tile, row : row + 1, : line.shape[1]] = line.astype(out.dtype)
    for name, shape in segments():
        if math.prod(shape) >= D * D:
            first = plan.places[name] // 8
            send(edge, first - edge)
            edge = first + math.prod(shape) // TILE
    send(edge, plan.total - edge)
    shapes = dict(segments())
    for number, name in enumerate(names):
        shape, first = shapes[name], plan.places[name]
        left, right = stores[2 * number], stores[2 * number + 1]
        wait_all(*loads[2 * number : 2 * number + 2])
        fold = shape[1] // LANES
        step = 256 if fold == 1 else 128

        @pl.loop(0, shape[0] // step)
        def _(i):
            part = left[:, pl.ds(pl.multiple_of(i * step, step), step)]
            value = lax.dot_general(part, right[...], rows, preferred_element_type=jnp.float32)
            if fold > 1:
                for j in range(fold):
                    for lane in range(LANES // 128):
                        at = j * LANES + lane * 128
                        mix[lane, pl.ds(j, step, stride=fold), :] = value[:, at : at + 128]
                value = jnp.concatenate([mix[lane, : step * fold] for lane in range(LANES // 128)], 1)
            tiles = step * fold // 8
            out[pl.ds(first // 8 + i * tiles, tiles)] = value.astype(out.dtype).reshape(tiles, 8, LANES)

        send(first // 8, math.prod(shape) // TILE)
    wait_all(*sent)


def weight_grads(plan, gradients, vectors, places):
    names = list(gradients)
    operands = [value for name in names for value in gradients[name]]
    return pl.pallas_call(
        functools.partial(weight_kernel, plan, names, places),
        out_shape=jax.ShapeDtypeStruct((plan.padded, 8, LANES), jnp.bfloat16),
        in_specs=[ANY_SPEC] * len(operands) + [VMEM_SPEC] * len(vectors),
        out_specs=ANY_SPEC,
        scratch_shapes=[vm(value.shape) for value in operands] + [
            vm((plan.padded, 8, LANES)), vm((LANES // 128, 512, 128), F32),
            DMA((len(operands) + len(segments()),)),
        ],
        compiler_params=pltpu.CompilerParams(vmem_limit_bytes=60 * 1024 * 1024),
        name="weight_grads",
    )(*operands, *vectors)


def bucket_windows(rel_bucket, block_len, count):
    width = -(-(block_len * (count + 1) - 1) // 128) * 128
    padded = jnp.concatenate([rel_bucket, jnp.full((width,), -1, jnp.int32)])
    windows = [padded[(count - 1 - b) * block_len :][:width] for b in range(count)]
    return (jnp.stack(windows)[:, None, :] == jnp.arange(NB, dtype=jnp.int32)[None, :, None]).astype(jnp.float32)


def adam_update(param_vec, grad_in, first_mom, second):
    new_first = BETA_ONE * first_mom + (1.0 - BETA_ONE) * grad_in
    new_second = BETA_TWO * second + (1.0 - BETA_TWO) * grad_in * grad_in
    corr_one = 1.0 - BETA_ONE**STEP
    corr_two = 1.0 - BETA_TWO**STEP
    step_size = new_first / corr_one / (jnp.sqrt(new_second / corr_two) + ADAM_EPS)
    return (param_vec - LEARN_RATE * (step_size + DECAY * param_vec), new_first, new_second)


def unit_rows(values):
    centre = values - jnp.mean(values, -1, keepdims=True)
    scale = lax.rsqrt(jnp.mean(centre * centre, -1, keepdims=True) + NORM_EPS)
    return centre * scale, scale


def unit_back(unit, scale, gain, grad):
    shifted = grad * gain
    first = jnp.mean(shifted, -1, keepdims=True)
    second = jnp.mean(shifted * unit, -1, keepdims=True)
    return scale * (shifted - first - unit * second), total_rows(grad * unit), total_rows(grad)


def total_rows(values):
    return jnp.sum(values, 0, keepdims=True)


def split_rows(source, mix, target, fold):
    block = mix.shape[1]
    lanes = LANES // 128

    @pl.loop(0, source.shape[0] // block)
    def _(i):
        part = source[pl.ds(pl.multiple_of(i * block, block), block), :].astype(jnp.float32)
        for lane in range(lanes):
            mix[lane] = part[:, lane * 128 : (lane + 1) * 128]
        for j in range(fold):
            rows = [mix[lane, pl.ds(j, block // fold, stride=fold), :] for lane in range(lanes)]
            at = pl.multiple_of(i * (block // fold), block // fold)
            target[j, pl.ds(at, block // fold), :] = jnp.concatenate(rows, 1).astype(target.dtype)


class Fetch:
    def __init__(self, plan, packed, sem):
        self.plan, self.packed, self.sem, self.count = plan, packed, sem, 0

    def __call__(self, name, target):
        row = self.plan.places[name] // 8 * 8
        copy = pltpu.make_async_copy(
            self.packed.at[pl.ds(row, target.shape[0])], target, self.sem.at[self.count]
        )
        self.count += 1
        copy.start()
        return copy


def column(j):
    return pl.ds(pl.multiple_of(j * LANES, LANES), LANES)


def wait_all(*copies):
    for copy in copies:
        copy.wait()


def ffn_first_kernel(plan, x, packed, x_out, n_out, w_out, w_in, w_second, v0, v1, v2, bias, acc, mix, sem):
    fetch = Fetch(plan, packed, sem)
    early = [fetch("first_ng", v0), fetch("first_b_in", v1), fetch("first_b_out", v2)]
    in_copy = fetch("first_w_in", w_in)
    late = [fetch("first_w_out", w_second)]
    wait_all(*early)
    gains, bias_in, tail = v0[...].astype(jnp.float32), v1[...].astype(jnp.float32), v2[...].astype(jnp.float32)
    stream = x[...]
    unit, _ = unit_rows(stream)
    normed = (unit * gains[0:1] + gains[1:2]).astype(jnp.bfloat16)
    in_copy.wait()
    split_rows(w_in, mix, w_out, FF // LANES)
    wait_all(*late)
    n_out[...] = normed
    bias[...] = bias_in
    acc[...] = jnp.zeros(acc.shape, jnp.float32)

    @pl.loop(0, FF // LANES)
    def _(j):
        hidden = forward_dot(n_out[...], w_out[j]) + bias[pl.ds(j, 1), :]
        active = swish_act(hidden).astype(jnp.bfloat16)
        acc[...] += forward_dot(active, w_second[column(j), :])

    stream = x[...] + 0.5 * (acc[...] + tail[0:1])
    x_out[...] = stream
    unit, _ = unit_rows(stream)
    normed = (unit * tail[1:2] + tail[2:3]).astype(jnp.bfloat16)
    n_out[...] = normed


def ffn_first_back_kernel(plan, x, x_one, d_two, d_norm_in, w_in, packed,
                          d_out, a_out, r_out, n_out, h_out, vec_out, w_second, v0, v1, v2, bias, acc, sem):
    fetch = Fetch(plan, packed, sem)
    early = [fetch("first_ng", v0), fetch("first_b_in", v1), fetch("first_b_out", v2)]
    late = fetch("first_w_out", w_second)
    wait_all(*early)
    gains, bias_in, tail = v0[...].astype(jnp.float32), v1[...].astype(jnp.float32), v2[...].astype(jnp.float32)
    unit, scale = unit_rows(x_one[...])
    d_normed = d_norm_in[...].astype(jnp.float32)
    d_norm, gain_grad, shift_grad = unit_back(unit, scale, tail[1:2], d_normed)
    vec_out[0:1] = gain_grad
    vec_out[1:2] = shift_grad
    grad = d_two[...] + d_norm
    half = 0.5 * grad
    vec_out[2:3] = total_rows(half)
    half_b = half.astype(jnp.bfloat16)
    r_out[...] = half_b
    unit, scale = unit_rows(x[...])
    normed = (unit * gains[0:1] + gains[1:2]).astype(jnp.bfloat16)
    n_out[...] = normed
    late.wait()
    bias[...] = bias_in
    acc[...] = jnp.zeros(acc.shape, jnp.float32)
    d_out[...] = grad

    @pl.loop(0, FF // LANES)
    def _(j):
        cols = column(j)
        hidden = forward_dot(n_out[...], w_in[j]) + bias[pl.ds(j, 1), :]
        a_out[:, cols] = swish_act(hidden).astype(jnp.bfloat16)
        d_hidden = back_dot(r_out[...], w_second[cols, :]) * swish_grad(hidden)
        vec_out[pl.ds(5 + j, 1), :] = total_rows(d_hidden)
        d_hidden = d_hidden.astype(jnp.bfloat16)
        h_out[:, cols] = d_hidden
        acc[...] += back_dot(d_hidden, w_in[j])

    unit, scale = unit_rows(x[...])
    d_norm, gain_grad, shift_grad = unit_back(unit, scale, gains[0:1], acc[...])
    vec_out[3:4] = gain_grad
    vec_out[4:5] = shift_grad
    d_out[...] += d_norm


def gate_kernel(plan, ctx, x, valid, packed, x_out, n_out, g_out, u_out, w_out, w_o, w_pi, v0, v1, mix, sem):
    fetch = Fetch(plan, packed, sem)
    early = [fetch("w_o", w_o), fetch("b_o", v0), fetch("b_pi", v1)]
    late = fetch("w_pi", w_pi)
    wait_all(*early)
    rows, bias_in = v0[...].astype(jnp.float32), v1[...].astype(jnp.float32)
    stream = x[...] + forward_dot(ctx[...], w_o[...]) + rows[0:1]
    x_out[...] = stream
    unit, _ = unit_rows(stream)
    normed = (unit * rows[6:7] + rows[7:8]).astype(jnp.bfloat16)
    n_out[...] = normed
    late.wait()
    split_rows(w_pi, mix, w_out, 2)
    linear = forward_dot(normed, w_out[0]) + bias_in[0:1]
    gate = forward_dot(normed, w_out[1]) + bias_in[1:2]
    g_out[:, :D] = linear
    g_out[:, D:] = gate
    u_out[...] = linear * jax.nn.sigmoid(gate) * valid[...]


def gate_back_kernel(plan, du, pre_gate, x, d_three, valid, w_pi, packed,
                     g_out, d_out, o_out, c_out, vec_out, w_o, v0, sem):
    fetch = Fetch(plan, packed, sem)
    copies = [fetch("b_o", v0), fetch("w_o", w_o)]
    d_gated = du[...] * valid[...]
    gate_sig = jax.nn.sigmoid(pre_gate[:, D:])
    d_linear = d_gated * gate_sig
    d_gate = d_gated * pre_gate[:, :D] * gate_sig * (1.0 - gate_sig)
    vec_out[0:1] = total_rows(d_linear)
    vec_out[1:2] = total_rows(d_gate)
    d_linear, d_gate = d_linear.astype(jnp.bfloat16), d_gate.astype(jnp.bfloat16)
    g_out[:, :D] = d_linear
    g_out[:, D:] = d_gate
    d_normed = back_dot(d_linear, w_pi[0]) + back_dot(d_gate, w_pi[1])
    unit, scale = unit_rows(x[...])
    wait_all(*copies)
    d_norm, gain_grad, shift_grad = unit_back(unit, scale, v0[...].astype(jnp.float32)[6:7], d_normed)
    vec_out[2:3] = gain_grad
    vec_out[3:4] = shift_grad
    grad = d_three[...] + d_norm
    d_out[...] = grad
    vec_out[4:5] = total_rows(grad)
    grad_b = grad.astype(jnp.bfloat16)
    o_out[...] = grad_b
    c_out[...] = back_dot(grad_b, w_o[...]).astype(jnp.bfloat16)


def middle_kernel(plan, x, depth, sums, cot, valid, packed,
                  y_out, d_out, z_out, part_out, stat_out, e_out, rb_out, a_out, r_out, n_out, h_out, vec_out,
                  w_po, w_in, w_second, w_mix, held, v_bn, v0, v1, v2, bias, acc, mix, sem):
    fetch = Fetch(plan, packed, sem)
    early = [fetch("b_pi", v_bn), fetch("w_po", w_po), fetch("b_po", v0), fetch("second_b_in", v1)]
    early.append(fetch("second_b_out", v2))
    in_copy = fetch("second_w_in", w_in)
    late = fetch("second_w_out", w_second)
    wait_all(*early)
    base = plan.places["bng"] - plan.places["b_pi"]
    batch, head = v_bn[...].astype(jnp.float32), v0[...].astype(jnp.float32)
    bias_in, tail = v1[...].astype(jnp.float32), v2[...].astype(jnp.float32)
    gain, shift = batch[base : base + 1], batch[base + 1 : base + 2]
    count = sums[2:3]
    mean = sums[0:1] / count
    inv_std = lax.rsqrt(sums[1:2] / count - mean * mean + BATCH_EPS)
    stat_out[0:1] = mean
    stat_out[1:2] = inv_std
    stat_out[2:3] = count
    stat_out[3:8] = jnp.zeros((5, D), jnp.float32)
    standard = (depth[...] - mean) * inv_std
    e_out[...] = swish_act(standard * gain + shift).astype(jnp.bfloat16)
    three = x[...] + forward_dot(e_out[...], w_po[...]) + head[0:1]
    unit, scale = unit_rows(three)
    n_out[...] = (unit * head[1:2] + head[2:3]).astype(jnp.bfloat16)
    in_copy.wait()
    split_rows(w_in, mix, w_mix, FF // LANES)
    late.wait()
    bias[...] = bias_in
    acc[...] = jnp.zeros(acc.shape, jnp.float32)
    d_out[...] = three

    @pl.loop(0, FF // LANES)
    def _(j):
        cols = column(j)
        hidden = forward_dot(n_out[...], w_mix[j]) + bias[pl.ds(j, 1), :]
        held[j] = hidden
        active = swish_act(hidden).astype(jnp.bfloat16)
        a_out[:, cols] = active
        acc[...] += forward_dot(active, w_second[cols, :])

    three = d_out[...]
    four = three + 0.5 * (acc[...] + tail[0:1])
    last, last_scale = unit_rows(four)
    y_out[...] = last * tail[1:2] + tail[2:3]
    grad = cot[...] * valid[...]
    grad, gain_grad, shift_grad = unit_back(last, last_scale, tail[1:2], grad)
    vec_out[0:1] = gain_grad
    vec_out[1:2] = shift_grad
    half = 0.5 * grad
    vec_out[2:3] = total_rows(half)
    r_out[...] = half.astype(jnp.bfloat16)
    acc[...] = jnp.zeros(acc.shape, jnp.float32)
    z_out[...] = grad

    @pl.loop(0, FF // LANES)
    def _(j):
        cols = column(j)
        d_hidden = back_dot(r_out[...], w_second[cols, :]) * swish_grad(held[j])
        vec_out[pl.ds(8 + j, 1), :] = total_rows(d_hidden)
        d_hidden = d_hidden.astype(jnp.bfloat16)
        h_out[:, cols] = d_hidden
        acc[...] += back_dot(d_hidden, w_mix[j])

    unit, scale = unit_rows(d_out[...])
    d_norm, gain_grad, shift_grad = unit_back(unit, scale, head[1:2], acc[...])
    vec_out[3:4] = gain_grad
    vec_out[4:5] = shift_grad
    grad = z_out[...] + d_norm
    d_out[...] = grad
    vec_out[5:6] = total_rows(grad)
    rb_out[...] = grad.astype(jnp.bfloat16)
    standard = (depth[...] - mean) * inv_std
    d_active = back_dot(rb_out[...], w_po[...]) * swish_grad(standard * gain + shift)
    d_gain, d_shift = total_rows(d_active * standard), total_rows(d_active)
    vec_out[6:7] = d_gain
    vec_out[7:8] = d_shift
    vec_out[12:16] = jnp.zeros((4, D), jnp.float32)
    d_standard = d_active * gain * valid[...]
    z_out[...] = d_standard
    part_out[0:1] = total_rows(d_standard)
    part_out[1:2] = total_rows(d_standard * standard)
    part_out[2:8] = jnp.zeros((6, D), jnp.float32)


def group_barrier(ndp, nseq):
    di, z = lax.axis_index(DP), lax.axis_index(SEQ)
    peers = [(di, lax.rem(z + i, nseq)) for i in range(1, nseq)]
    peers = peers + [(lax.rem(di + i, ndp), z) for i in range(1, ndp)]
    barrier = pltpu.get_barrier_semaphore()
    for peer in peers:
        pl.semaphore_signal(barrier, inc=1, device_id=peer, device_id_type=MESH)
    return lambda: pl.semaphore_wait(barrier, len(peers))


def exchange_sum(ndp, nseq, part, line, cross, sems):
    di, z = lax.axis_index(DP), lax.axis_index(SEQ)

    def phase(count, me, target, slots, send, recv):
        copies = []
        for i in range(1, count):
            copy = pltpu.make_async_remote_copy(
                src_ref=part, dst_ref=slots.at[me], send_sem=send.at[i], recv_sem=recv.at[me],
                device_id=target(lax.rem(me + i, count)), device_id_type=MESH,
            )
            copy.start()
            copies.append(copy)
        slots[me] = part[...]
        for i in range(1, count):
            source = lax.rem(me + count - i, count)
            pltpu.make_async_remote_copy(
                src_ref=part, dst_ref=slots.at[source], send_sem=send.at[i], recv_sem=recv.at[source],
                device_id=(di, z), device_id_type=MESH,
            ).wait_recv()
        for copy in copies:
            copy.wait_send()
        total = slots[0]
        for i in range(1, count):
            total = total + slots[i]
        return total

    part[...] = phase(nseq, z, lambda i: (di, i), line, sems[0], sems[1])
    return phase(ndp, di, lambda i: (i, z), cross, sems[2], sems[3])


HALO = 16


class Halo:
    def __init__(self, nseq, buffer, sem):
        di, z = lax.axis_index(DP), lax.axis_index(SEQ)
        rows = buffer.shape[1]
        self.has = (z > 0, z < nseq - 1)

        def copy(source, target, number, to):
            return pltpu.make_async_remote_copy(
                src_ref=buffer.at[:, pl.ds(source, HALO)], dst_ref=buffer.at[:, pl.ds(target, HALO)],
                send_sem=sem.at[number], recv_sem=sem.at[2 + number], device_id=(di, to), device_id_type=MESH,
            )

        self.up = copy(rows - 2 * HALO, 0, 0, lax.rem(z + 1, nseq))
        self.down = copy(HALO, rows - HALO, 1, lax.rem(z + nseq - 1, nseq))
        self.buffer, self.rows = buffer, rows

    def start(self):
        @pl.when(self.has[1])
        def _():
            self.up.start()

        @pl.when(self.has[0])
        def _():
            self.down.start()

    def finish(self):
        empty = jnp.zeros((self.buffer.shape[0], HALO, self.buffer.shape[2]), jnp.float32)

        @pl.when(self.has[0])
        def _():
            self.up.wait_recv()
            self.down.wait_send()

        @pl.when(jnp.logical_not(self.has[0]))
        def _():
            self.buffer[:, :HALO] = empty

        @pl.when(self.has[1])
        def _():
            self.down.wait_recv()
            self.up.wait_send()

        @pl.when(jnp.logical_not(self.has[1]))
        def _():
            self.buffer[:, self.rows - HALO :] = empty


def slide(padded, taps, index, out, length):
    lanes = LANES // 128

    @pl.loop(0, padded.shape[0] * lanes)
    def _(i):
        s, lane = i // lanes, pl.ds(pl.multiple_of(i % lanes * 128, 128), 128)
        total = jnp.zeros((length, 128), jnp.float32)
        for b in range(8):
            part = None
            for a in range(4):
                if 0 < 8 * a + b < K + 1:
                    row = index(8 * a + b)
                    term = taps[row : row + 1, lane] * padded[s, 8 * a : 8 * a + length + 8, lane]
                    part = term if part is None else part + term
            total = total + part[b : b + length]
        out[pl.ds(pl.multiple_of(s * length, length), length), lane] = total


def depth_kernel(plan, u, valid, packed, c_out, sum_out, padded, taps, taps_b, part, line, cross, sem,
                 halo_sem, *sems):
    ndp, nseq = plan.ndp, plan.nseq
    arrived = group_barrier(ndp, nseq)
    length = padded.shape[1] - 2 * HALO
    copy = Fetch(plan, packed, sem)("b_pi", taps_b)
    padded[:, HALO : HALO + length] = u[...].reshape(-1, length, D)
    arrived()
    halo = Halo(nseq, padded, halo_sem)
    halo.start()
    copy.wait()
    taps[...] = taps_b[...].astype(jnp.float32)
    halo.finish()
    base = plan.places["w_depth"] - plan.places["b_pi"]
    slide(padded, taps, lambda i: base + i - 1, c_out, length)
    depth, mask = c_out[...], valid[...]
    value = depth * mask
    part[0:1] = total_rows(value)
    part[1:2] = total_rows(value * depth)
    part[2:3] = jnp.broadcast_to(total_rows(mask), (1, LANES))
    part[3:8] = jnp.zeros((5, LANES), jnp.float32)
    sum_out[...] = exchange_sum(ndp, nseq, part, line, cross, sems)


def depth_back_kernel(plan, dz, depth, stats, local, valid, u_pad, packed, u_out, tap_out,
                      padded, own, taps, taps_b, part, line, cross, sem, halo_sem, *sems):
    ndp, nseq = plan.ndp, plan.nseq
    arrived = group_barrier(ndp, nseq)
    seqs, length = padded.shape[0], padded.shape[1] - 2 * HALO
    copy = Fetch(plan, packed, sem)("b_pi", taps_b)
    part[...] = local[...]
    arrived()
    sums = exchange_sum(ndp, nseq, part, line, cross, sems)
    mean, inv_std, count = stats[0:1], stats[1:2], stats[2:3]
    standard = (depth[...] - mean) * inv_std
    d_depth = valid[...] * inv_std * (dz[...] - sums[0:1] / count - standard * (sums[1:2] / count))
    d_depth = d_depth.reshape(seqs, length, D)
    padded[:, HALO : HALO + length] = d_depth
    halo = Halo(nseq, padded, halo_sem)
    halo.start()
    own[:, :8] = jnp.zeros((seqs, 8, D), jnp.float32)
    own[:, 8 : 8 + length] = d_depth
    own[:, 8 + length :] = jnp.zeros((seqs, 8, D), jnp.float32)
    copy.wait()
    taps[...] = taps_b[...].astype(jnp.float32)
    base = plan.places["w_depth"] - plan.places["b_pi"]

    @pl.loop(0, LANES // 128)
    def _(i):
        lane = pl.ds(pl.multiple_of(i * 128, 128), 128)
        for b in range(8):
            sums_b = [None] * 4
            for s in range(seqs):
                moved = own[s, 8 - b : 8 - b + length + 8, lane]
                for a in range(4):
                    if 0 < 8 * a + b < K + 1:
                        term = total_rows(u_pad[s, 8 * a : 8 * a + length + 8, lane] * moved)
                        sums_b[a] = term if sums_b[a] is None else sums_b[a] + term
            for a in range(4):
                if sums_b[a] is not None:
                    tap_out[8 * a + b - 1 : 8 * a + b, lane] = sums_b[a]
        tap_out[K : K + 1, lane] = jnp.zeros((1, 128), jnp.float32)

    halo.finish()
    slide(padded, taps, lambda i: base + K - i, u_out, length)


def head_scores(q, k, line, valid):
    block, full, width = q.shape[0], k.shape[0], line.shape[1]
    scores = lax.dot_general(q, k, (((1,), (1,)), ((), ())), preferred_element_type=jnp.float32)
    spread = jnp.broadcast_to(line, (block, width))
    bias = pltpu.roll(spread, width - block + 1, 1, stride=1, stride_axis=0)[:, :full]
    return jnp.where(valid, scores * (1.0 / math.sqrt(HD)) + bias, -jnp.inf)


def remote(source, target, send, recv, device):
    return pltpu.make_async_remote_copy(
        src_ref=source, dst_ref=target, send_sem=send, recv_sem=recv, device_id=device, device_id_type=MESH
    )


class Team:
    def __init__(self, plan, seqs):
        self.di, self.z = lax.axis_index(DP), lax.axis_index(SEQ)
        self.count, self.seqs = plan.nseq, seqs
        self.c = self.di % 2
        self.base = self.di - self.c
        self.other = self.base + 1 - self.c
        self.owner = self.base + self.z // seqs
        self.main = self.z // seqs == self.c
        self.slot = self.z % seqs
        self.half = pl.ds(pl.multiple_of(self.c * (D // 2), D // 2), D // 2)

    def enter(self):
        barrier = pltpu.get_barrier_semaphore()
        peers = [(self.other, self.z)]
        for i in range(1, self.count):
            to = lax.rem(self.z + i, self.count)
            peers += [(self.di, to), (self.other, to)]
        for peer in peers:
            pl.semaphore_signal(barrier, inc=1, device_id=peer, device_id_type=MESH)
        return lambda: pl.semaphore_wait(barrier, len(peers))

    def turn(self, i):
        return lax.rem(self.z + i, self.count)


def half_copy(packed, plan, name, team, target, sem):
    copy = pltpu.make_async_copy(packed.at[pl.ds(plan.places[name], D), team.half], target, sem)
    copy.start()
    return copy


def attend_kernel(plan, normed, lengths, tables, packed, ctx_out, all_out, q_out, k_out, v_out, lse_out, len_out,
                  w_q, w_k, w_v, b_q, b_v, held, mine, sem, in_send, relay_send, in_recv, ctx_send, ctx_recv, len_sem):
    seqs, block, _ = normed.shape
    count = plan.nseq
    team = Team(plan, seqs)
    arrived = team.enter()
    fetch = Fetch(plan, packed, sem)
    copies = [fetch("b_q", b_q), fetch("b_v", b_v)]
    for i, (name, target) in enumerate((("w_q", w_q), ("w_k", w_k), ("w_v", w_v))):
        copies.append(half_copy(packed, plan, name, team, target, sem.at[2 + i]))
    arrived()
    c, z = team.c, team.z
    sends = []
    for s in range(seqs):
        to = c * seqs + s
        copy = remote(normed.at[s], all_out.at[z], in_send.at[s], in_recv.at[z], (team.di, to))
        sends.append((to != z, copy))
        pl.when(to != z)(copy.start)
    relays = []
    for i in range(count):
        b = team.turn(i)
        source = normed.at[team.slot] if i == 0 else all_out.at[b]
        relays.append(remote(source, all_out.at[b], relay_send.at[b], in_recv.at[b], (team.other, z)))
    pl.when(team.main)(relays[0].start)
    note = remote(lengths, len_out, len_sem.at[0], len_sem.at[1], (team.other, z))
    pl.when(team.main)(note.start)

    @pl.when(team.main)
    def _():
        all_out[z] = normed[team.slot]
        len_out[...] = lengths[...]

    wait_all(*copies)
    mine[0] = b_q[...].astype(jnp.float32)
    mine[1] = b_v[...].astype(jnp.float32)
    bias_q, bias_v = mine[0, 0:1, team.half], mine[1, 0:1, team.half]
    for i in range(count):
        b = team.turn(i)
        if i == 0:
            pl.when(jnp.logical_not(team.main))(relays[0].wait_recv)
        else:
            relays[i].wait_recv()
            pl.when(team.main)(relays[i].start)
        part = all_out[b]
        at = pl.ds(pl.multiple_of(b * block, block), block)
        q_out[at, :] = (forward_dot(part, w_q[...]) + bias_q).astype(jnp.bfloat16)
        k_out[at, :] = forward_dot(part, w_k[...]).astype(jnp.bfloat16)
        v_out[at, :] = (forward_dot(part, w_v[...]) + bias_v).astype(jnp.bfloat16)
    full = count * block
    pl.when(jnp.logical_not(team.main))(note.wait_recv)
    valid = lax.broadcasted_iota(jnp.int32, (1, full), 1) < len_out[pl.ds(team.slot, 1), :][:, 0:1]
    lane = lax.broadcasted_iota(jnp.int32, (block, 128), 1)

    def back(b):
        return remote(held.at[b], ctx_out.at[team.slot, :, team.half], ctx_send.at[b],
                      ctx_recv.at[team.slot * 2 + c], (team.owner, b))

    @pl.loop(0, count)
    def _(i):
        b = lax.rem(z + 1 + i, count)
        at = pl.ds(pl.multiple_of(b * block, block), block)
        lse = jnp.zeros((block, 128), jnp.float32)
        for h in range(H // 2):
            cols = slice(h * HD, (h + 1) * HD)
            line = tables[b, pl.ds(c * (H // 2) + h, 1), :]
            scores = head_scores(q_out[at, cols], k_out[:, cols], line, valid)
            top = jnp.max(scores, -1, keepdims=True)
            weights = jnp.exp(scores - top)
            total = jnp.sum(weights, -1, keepdims=True)
            probs = (weights * (1.0 / total)).astype(jnp.bfloat16)
            ctx = jnp.dot(probs, v_out[:, cols], preferred_element_type=jnp.float32)
            held[b, :, cols] = ctx.astype(jnp.bfloat16)
            lse = jnp.where(lane == h, top + jnp.log(total), lse)
        lse_out[at, :] = lse
        own = jnp.logical_and(b == z, team.main)

        @pl.when(own)
        def _():
            ctx_out[team.slot, :, team.half] = held[b]

        @pl.when(jnp.logical_not(own))
        def _():
            back(b).start()

    for s in range(seqs):
        for h in range(2):
            own = jnp.logical_and(c * seqs + s == z, c == h)
            here = ctx_out.at[s, :, pl.ds(h * (D // 2), D // 2)]
            copy = remote(held.at[0], here, ctx_send.at[0], ctx_recv.at[s * 2 + h], (team.di, z))
            pl.when(jnp.logical_not(own))(copy.wait_recv)
    pl.when(team.main)(note.wait_send)
    for flag, copy in sends:
        pl.when(flag)(copy.wait_send)
    for i in range(count):
        pl.when(team.main)(relays[i].wait_send)
        b = team.turn(i)
        own = jnp.logical_and(b == z, team.main)
        pl.when(jnp.logical_not(own))(back(b).wait_send)


def attend_back_kernel(plan, d_ctx, q_all, k_all, v_all, lse_all, length, tables, packed,
                       dn_out, dq_out, dk_out, dv_out, dt_out, vec_out,
                       w_q, w_k, w_v, d_in, dq_part, dk_sum, dv_sum, give, take, final, sem,
                       in_send, in_recv, swap_send, swap_recv, dn_send, dn_recv):
    seqs, block, _ = d_ctx.shape
    count = plan.nseq
    full = count * block
    team = Team(plan, seqs)
    arrived = team.enter()
    copies = []
    for i, (name, target) in enumerate((("w_q", w_q), ("w_k", w_k), ("w_v", w_v))):
        copies.append(half_copy(packed, plan, name, team, target, sem.at[i]))
    arrived()
    c, z = team.c, team.z
    sends = []
    for s in range(seqs):
        for h in range(2):
            to = c * seqs + s
            own = jnp.logical_and(to == z, c == h)
            source = d_ctx.at[s, :, pl.ds(h * (D // 2), D // 2)]
            copy = remote(source, d_in.at[z], in_send.at[2 * s + h], in_recv.at[z], (team.base + h, to))
            sends.append((jnp.logical_not(own), copy))
            pl.when(jnp.logical_not(own))(copy.start)

    @pl.when(team.main)
    def _():
        d_in[z] = d_ctx[team.slot, :, team.half]

    dk_sum[...] = jnp.zeros(dk_sum.shape, jnp.float32)
    dv_sum[...] = jnp.zeros(dv_sum.shape, jnp.float32)
    dt_out[...] = jnp.zeros(dt_out.shape, jnp.float32)
    vec_out[...] = jnp.zeros(vec_out.shape, jnp.float32)
    away = pl.ds(pl.multiple_of((1 - c) * (D // 2), D // 2), D // 2)
    for out in (dq_out, dk_out, dv_out):
        out[:, away] = jnp.zeros((full, D // 2), jnp.bfloat16)
    valid = lax.broadcasted_iota(jnp.int32, (1, full), 1) < length[pl.ds(team.slot, 1), :][:, 0:1]
    rows = (((0,), (0,)), ((), ()))
    inv = 1.0 / math.sqrt(HD)

    @pl.loop(0, count)
    def _(i):
        b = lax.rem(z + i, count)
        own = jnp.logical_and(b == z, team.main)
        copy = remote(d_in.at[b], d_in.at[b], in_send.at[0], in_recv.at[b], (team.di, z))
        pl.when(jnp.logical_not(own))(copy.wait_recv)
        at = pl.ds(pl.multiple_of(b * block, block), block)
        totals = []
        for h in range(H // 2):
            cols = slice(h * HD, (h + 1) * HD)
            q, k, v = q_all[at, cols], k_all[:, cols], v_all[:, cols]
            dctx = d_in[b, :, cols]
            line = tables[b, pl.ds(c * (H // 2) + h, 1), :]
            width = line.shape[1]
            scores = head_scores(q, k, line, valid)
            probs = jnp.exp(scores - lse_all[at, h : h + 1])
            d_probs = lax.dot_general(dctx, v, (((1,), (1,)), ((), ())), preferred_element_type=jnp.float32)
            delta = jnp.sum(probs * d_probs, -1, keepdims=True)
            d_scores = probs * (d_probs - delta)
            d_scores_b = d_scores.astype(jnp.bfloat16)
            dq = jnp.dot(d_scores_b, k, preferred_element_type=jnp.float32) * inv
            totals.append(total_rows(dq))
            dk_sum[:, cols] += lax.dot_general(d_scores_b, q, rows, preferred_element_type=jnp.float32)
            dv_sum[:, cols] += lax.dot_general(
                probs.astype(jnp.bfloat16), dctx, rows, preferred_element_type=jnp.float32
            )
            dq_part[at, cols] = dq.astype(jnp.bfloat16)
            wide = jnp.concatenate([d_scores, jnp.zeros((block, width - full), jnp.float32)], 1)
            folded = pltpu.roll(wide[0:8], block - 1, 1)
            for g in range(1, block // 8):
                folded = folded + pltpu.roll(wide[8 * g : 8 * g + 8], block - 1 - 8 * g, 1)
            line = folded[0:1]
            for r in range(1, 8):
                line = line + pltpu.roll(folded[r : r + 1], width - r, 1)
            dt_out[b, pl.ds(c * (H // 2) + h, 1), :] = line
        vec_out[0:1, team.half] += jnp.concatenate(totals, 1)

    vec_out[1:2, team.half] = total_rows(dv_sum[...])
    dk_part = (dk_sum[...] * inv).astype(jnp.bfloat16)
    dk_out[:, team.half] = dk_part
    dv_part = dv_sum[...].astype(jnp.bfloat16)
    dv_out[:, team.half] = dv_part
    dq_out[:, team.half] = dq_part[...]
    wait_all(*copies)

    def partial(b):
        at = pl.ds(pl.multiple_of(b * block, block), block)
        dk_rows, dv_rows = dk_out[at, team.half], dv_out[at, team.half]
        return back_dot(dq_part[at, :], w_q[...]) + back_dot(dk_rows, w_k[...]) + back_dot(dv_rows, w_v[...])

    share = count // 2
    swaps, ends = [], []
    for i in range(share):
        give[i] = partial((1 - c) * share + i).astype(jnp.bfloat16)
        copy = remote(give.at[i], take.at[i], swap_send.at[i], swap_recv.at[i], (team.other, z))
        copy.start()
        swaps.append(copy)
    for i in range(share):
        b = c * share + i
        value = partial(b)
        swaps[i].wait_recv()
        value = (value + take[i].astype(jnp.float32)).astype(jnp.bfloat16)
        final[i] = value
        own = jnp.logical_and(b == z, team.main)
        copy = remote(final.at[i], dn_out.at[team.slot], dn_send.at[i], dn_recv.at[team.slot], (team.owner, b))
        ends.append((jnp.logical_not(own), copy))
        pl.when(jnp.logical_not(own))(copy.start)

        @pl.when(own)
        def _():
            dn_out[team.slot] = final[i]

    for s in range(seqs):
        own = jnp.logical_and(c * seqs + s == z, z // share == c)
        copy = remote(final.at[0], dn_out.at[s], dn_send.at[0], dn_recv.at[s], (team.di, z))
        pl.when(jnp.logical_not(own))(copy.wait_recv)
    for copy in swaps:
        copy.wait_send()
    for flag, copy in sends + ends:
        pl.when(flag)(copy.wait_send)


VMEM_SPEC = pl.BlockSpec(memory_space=pltpu.VMEM)
ANY_SPEC = pl.BlockSpec(memory_space=pl.ANY)


def stage(kernel, plan, operands, packed, outs, scratch, name, number=None):
    params = {}
    if number is not None:
        params = {"collective_id": number, "has_side_effects": True}
    specs = [VMEM_SPEC] * len(operands) + [ANY_SPEC]
    return pl.pallas_call(
        functools.partial(kernel, plan),
        out_shape=[jax.ShapeDtypeStruct(shape, dtype) for shape, dtype in outs],
        in_specs=specs,
        out_specs=[VMEM_SPEC] * len(outs),
        scratch_shapes=scratch,
        compiler_params=pltpu.CompilerParams(vmem_limit_bytes=56 * 1024 * 1024, **params),
        name=name,
    )(*operands, packed)


F32, BF16 = jnp.float32, jnp.bfloat16
DMA = pltpu.SemaphoreType.DMA


def vm(shape, dtype=jnp.bfloat16):
    return pltpu.VMEM(shape, dtype)


def exchange_scratch(plan):
    return [vm((8, D), F32), vm((plan.nseq, 8, D), F32), vm((plan.ndp, 8, D), F32), DMA((1,)), DMA((4,)),
            DMA((plan.nseq,)), DMA((plan.nseq,)), DMA((plan.ndp,)), DMA((plan.ndp,))]


def per_device(inputs, lengths, rel_bucket, params, moment_one, moment_two, cotangent):
    seq_count, block_len, model_width = inputs.shape
    rows = seq_count * block_len
    first_pos = lax.axis_index(SEQ) * block_len
    positions = first_pos + jnp.arange(block_len, dtype=jnp.int32)
    valid_own = positions[None, :] < lengths[:, None]
    valid = valid_own.astype(jnp.float32).reshape(-1, 1)
    onehot = bucket_windows(rel_bucket, block_len, lax.axis_size(SEQ))
    assert 2 * seq_count == lax.axis_size(SEQ)
    length = jnp.broadcast_to(jnp.pad(lengths, (0, 8 - seq_count))[:, None], (8, 128))
    plan = Plan(lax.axis_size(DP), lax.axis_size(SEQ), params.shape[0])
    packed = gather(plan, params).reshape(-1, LANES)
    full, wide = (rows, D), (rows, FF)
    square, tall, group = vm((D, D)), vm((FF, D)), vm((8, D))
    mix = vm((LANES // 128, 256, 128), F32)
    stream0 = inputs.reshape(full)
    stream1, normed2, w_first = stage(
        ffn_first_kernel, plan, [stream0], packed,
        [(full, F32), (full, BF16), ((FF // D, D, D), BF16)],
        [tall, tall, group, group, group, vm((8, D), F32), vm(full, F32), mix, DMA((5,))], "ffn_first",
    )
    table_row = plan.places["rel"]
    rel = packed[table_row : table_row + 1, : NB * H].reshape(NB, H)
    tables = jnp.einsum("nh,bnw->bhw", rel, onehot.astype(BF16), preferred_element_type=F32)
    tall_half, split = (plan.nseq * block_len, D // 2), (plan.nseq, block_len, D // 2)
    local3, all3 = (seq_count, block_len, D), (plan.nseq, block_len, D)
    half, nseq = vm((D, D // 2)), plan.nseq
    context, owned, queries, keys, values, lse, length = stage(
        attend_kernel, plan, [normed2.reshape(local3), length, tables], packed,
        [(local3, BF16), (all3, BF16), (tall_half, BF16), (tall_half, BF16), (tall_half, BF16),
         ((tall_half[0], 128), F32), ((8, 128), jnp.int32)],
        [half, half, half, group, group, vm(split), vm((2, 8, D), F32), DMA((5,)), DMA((seq_count,)), DMA((nseq,)),
         DMA((nseq,)), DMA((nseq,)), DMA((2 * seq_count,)), DMA((2,))], "attend", 4,
    )
    context = context.reshape(full)
    stream2, normed3, pre_gate, gated, w_gate = stage(
        gate_kernel, plan, [context, stream1, valid], packed,
        [(full, F32), (full, BF16), ((rows, 2 * D), F32), (full, F32), ((2, D, D), BF16)],
        [square, vm((2 * D, D)), group, group, mix, DMA((4,))], "gate",
    )
    padded_shape = (seq_count, block_len + 2 * HALO, D)
    depth, sums, padded = stage(
        depth_kernel, plan, [gated, valid], packed,
        [(full, F32), ((8, D), F32), (padded_shape, F32)],
        [vm((40, D), F32), vm((40, D))] + exchange_scratch(plan), "depth", 2,
    )
    (output, d_stream3, d_standard, local, stats, active3, grad3_b, active4, half4, normed4, d_hidden4,
     vec_mid) = stage(
        middle_kernel, plan, [stream2, depth, sums, cotangent.reshape(full), valid], packed,
        [(full, F32), (full, F32), (full, F32), ((8, D), F32), ((8, D), F32), (full, BF16), (full, BF16),
         (wide, BF16), (full, BF16), (full, BF16), (wide, BF16), ((16, D), F32)],
        [square, tall, tall, vm((FF // D, D, D)), vm((FF // D, rows, D), F32), vm((40, D)), group, group, group,
         vm((8, D), F32), vm(full, F32), mix, DMA((7,))], "middle",
    )
    d_gated, tap_grads = stage(
        depth_back_kernel, plan, [d_standard, depth, stats, local, valid, padded], packed,
        [(full, F32), ((32, D), F32)],
        [vm(padded_shape, F32), vm((seq_count, block_len + 16, D), F32), vm((40, D), F32), vm((40, D))]
        + exchange_scratch(plan), "depth_back", 3,
    )
    d_gate, d_stream2, grad2_b, d_context, vec_gate = stage(
        gate_back_kernel, plan, [d_gated, pre_gate, stream2, d_stream3, valid, w_gate], packed,
        [((rows, 2 * D), BF16), (full, F32), (full, BF16), (full, BF16), ((8, D), F32)],
        [square, group, DMA((2,))], "gate_back",
    )
    whole = (tall_half[0], D)
    d_norm2, d_query, d_key, d_value, d_tables, vec_attend = stage(
        attend_back_kernel, plan, [d_context.reshape(local3), queries, keys, values, lse, length, tables], packed,
        [(local3, BF16), (whole, BF16), (whole, BF16), (whole, BF16), (tables.shape, F32), ((8, D), F32)],
        [half, half, half, vm(split), vm(tall_half), vm(tall_half, F32), vm(tall_half, F32),
         vm((nseq // 2, block_len, D)), vm((nseq // 2, block_len, D)), vm((nseq // 2, block_len, D)), DMA((3,)),
         DMA((2 * seq_count,)), DMA((nseq,)), DMA((nseq // 2,)), DMA((nseq // 2,)), DMA((nseq // 2,)),
         DMA((seq_count,))], "attend_back", 5,
    )
    rel_grad = jnp.einsum("bnw,bhw->nh", onehot, d_tables, precision=lax.Precision.HIGHEST).reshape(1, -1)
    owned = owned.reshape(whole)
    d_stream0, active1, half1, normed1, d_hidden1, vec_first = stage(
        ffn_first_back_kernel, plan, [stream0, stream1, d_stream2, d_norm2.reshape(full), w_first], packed,
        [(full, F32), (wide, BF16), (full, BF16), (full, BF16), (wide, BF16), ((16, D), F32)],
        [tall, group, group, group, vm((8, D), F32), vm(full, F32), DMA((4,))], "ffn_first_back",
    )
    gradients = {
        "w_k": (owned, d_key), "w_v": (owned, d_value),
        "first_w_in": (normed1, d_hidden1), "first_w_out": (active1, half1), "w_q": (owned, d_query),
        "w_o": (context, grad2_b), "w_pi": (normed3, d_gate), "w_po": (active3, grad3_b),
        "second_w_in": (normed4, d_hidden4), "second_w_out": (active4, half4),
    }
    places = {
        "attn_ng": (0, 0), "attn_nb": (0, 1), "first_b_out": (0, 2), "first_ng": (0, 3), "first_nb": (0, 4),
        "first_b_in": (0, 5), "b_pi": (1, 0), "conv_ng": (1, 2), "conv_nb": (1, 3), "b_o": (1, 4),
        "fin_g": (2, 0), "fin_b": (2, 1), "second_b_out": (2, 2), "second_ng": (2, 3), "second_nb": (2, 4),
        "b_po": (2, 5), "bng": (2, 6), "bnb": (2, 7), "second_b_in": (2, 8), "w_depth": (3, 0),
        "b_q": (4, 0), "b_v": (4, 1), "rel": (5, 0),
    }
    vectors = [vec_first, vec_gate, vec_mid, tap_grads, vec_attend, rel_grad]
    window = scatter(plan, weight_grads(plan, gradients, vectors, places))
    grad_shard = own_shard(plan, window)
    new_params, new_first, new_second = adam_update(params, grad_shard, moment_one, moment_two)
    return (
        output.reshape(inputs.shape),
        d_stream0.reshape(inputs.shape),
        grad_shard,
        new_params,
        new_first,
        new_second,
    )


def solution(mesh):
    return jax.shard_map(
        per_device,
        mesh=mesh,
        in_specs=(
            P(DP, SEQ, None),
            P(DP),
            P(),
            P((DP, SEQ)),
            P((DP, SEQ)),
            P((DP, SEQ)),
            P(DP, SEQ, None),
        ),
        out_specs=(
            P(DP, SEQ, None),
            P(DP, SEQ, None),
            P((DP, SEQ)),
            P((DP, SEQ)),
            P((DP, SEQ)),
            P((DP, SEQ)),
        ),
        check_vma=False,
    )
```

```python
import functools
import math
import types

import jax
import jax.numpy as jnp
from jax import lax
from jax.experimental import pallas as pl
from jax.experimental.pallas import tpu as pltpu
from jax.sharding import PartitionSpec as P

D = 512
H = 8
HD = 64
FF = 2048
K = 31
NB = 32
DP = "dp"
SEQ = "seq"
STEP = 4


NORM_EPS = 1e-05
BATCH_EPS = 1e-05
LEARN_RATE = 0.005
DECAY = 0.01
BETA_ONE = 0.9
BETA_TWO = 0.98
ADAM_EPS = 1e-08


def segments():

    def feed_block(prefix):
        return [
            (prefix + "_ng", (D,)),
            (prefix + "_nb", (D,)),
            (prefix + "_w_in", (D, FF)),
            (prefix + "_b_in", (FF,)),
            (prefix + "_w_out", (FF, D)),
            (prefix + "_b_out", (D,)),
        ]

    listing = feed_block("first")
    listing = listing + [
        ("attn_ng", (D,)),
        ("attn_nb", (D,)),
        ("w_q", (D, D)),
        ("b_q", (D,)),
        ("w_k", (D, D)),
        ("w_v", (D, D)),
        ("b_v", (D,)),
        ("w_o", (D, D)),
        ("b_o", (D,)),
        ("rel", (NB, H)),
    ]
    listing = listing + [
        ("conv_ng", (D,)),
        ("conv_nb", (D,)),
        ("w_pi", (D, 2 * D)),
        ("b_pi", (2 * D,)),
        ("w_depth", (K, D)),
        ("bng", (D,)),
        ("bnb", (D,)),
        ("w_po", (D, D)),
        ("b_po", (D,)),
    ]
    listing = listing + feed_block("second") + [("fin_g", (D,)), ("fin_b", (D,))]
    return listing


def arrange():
    places, gaps = {}, []
    linear = inner = 0
    for entry_name, entry_shape in segments():
        extent = math.prod(entry_shape)
        tail = 2 * D if entry_name == "conv_ng" else 0
        if extent >= D * D or tail:
            pad = -(inner + tail) % TILE
            if pad:
                gaps.append((linear, pad))
                inner = inner + pad
        places[entry_name] = inner // LANES
        linear, inner = linear + extent, inner + extent
    return places, gaps, -(-inner // TILE)


def device_index():
    return lax.axis_index(DP) * lax.axis_size(SEQ) + lax.axis_index(SEQ)


def own_shard(plan, window):
    table = jnp.asarray(plan.shard_table, jnp.int32)[device_index()]
    flat = window.reshape(-1)
    early = lax.dynamic_slice(flat, (table[0],), (plan.shard,))
    late = lax.dynamic_slice(flat, (table[0] + table[2],), (plan.shard,))
    return jnp.where(jnp.arange(plan.shard, dtype=jnp.int32) < table[1], early, late)


def swish_act(values):
    return values * jax.nn.sigmoid(values)


def swish_grad(values):
    sig_vals = jax.nn.sigmoid(values)
    return sig_vals * (1.0 + values * (1.0 - sig_vals))


def forward_dot(left_mat, weight):
    return jnp.dot(left_mat, weight, preferred_element_type=jnp.float32)


def back_dot(grad_in, weight):
    return lax.dot_general(
        grad_in, weight, (((1,), (1,)), ((), ())), preferred_element_type=jnp.float32
    )


MESH = pl.DeviceIdType.MESH
LANES=512
TILE=8*LANES

class Plan:
    def __init__(self, ndp, nseq, shard):
        self.ndp, self.nseq, self.shard = ndp, nseq, shard
        self.k = ndp.bit_length() - 1
        self.phases = self.k - 1
        self.n = n = ndp * nseq
        self.places, self.gaps, self.total = arrange()
        begins = [self.inner(d * shard) for d in range(n)]
        starts = [-(-b // TILE) for b in begins] + [self.total]
        sizes = [b - a for a, b in zip(starts, starts[1:])]
        self.lo, self.hi = min(sizes), max(sizes)
        self.slots = nseq * 2**self.phases
        floors = [b // TILE for b in begins]
        ends = [self.inner((d + 1) * shard - 1) // TILE + 1 for d in range(n)]
        self.win = max(e - f for e, f in zip(ends, floors))
        self.win += self.win % 2
        self.padded = max(self.total, max(floors) + self.win)
        self.block_table, self.shard_table = [], []
        for d in range(n):
            near = [g for g in self.gaps if d * shard < g[0] < (d + 1) * shard + TILE]
            assert len(near) <= 1
            cut, size = near[0] if near else (2**30, 0)
            lead = starts[d] * TILE - begins[d]
            self.block_table.append((lead, cut - d * shard - lead, size))
            self.shard_table.append((begins[d] - floors[d] * TILE, cut - d * shard, size))

    def inner(self, position):
        if isinstance(position, int):
            return position + sum(size for at, size in self.gaps if at <= position)
        result = position
        for at, size in self.gaps:
            result = result + jnp.where(position >= at, size, 0)
        return result

    def order(self):
        ev=[]
        for s in range(self.nseq):
            for sign in ((0,) if s==0 else (-1,1)):
                for t in range(2**self.phases):
                    ev.append((s+0.5*bin(t).count("1")+0.01*t, s, sign, t))
        ev.sort()
        return [e[1:] for e in ev]

def flip(di, mask_bits, bits, t, phases):
    out=di
    for p in range(phases):
        if (t>>p)&1:
            out = out + mask_bits[p]*(1-2*bits[p])
    return out

def phase_masks(di, c, phases):
    masks, bits=[],[]
    for p in range(phases):
        a, b = 1<<(p+1), 1<<(phases-p)
        masks.append(a+c*(b-a))
        ba, bb = (di//a)%2, (di//b)%2
        bits.append(ba+c*(bb-ba))
    return masks, bits

def block_of(plan, dpi, z):
    d = dpi*plan.nseq+z
    a = (plan.inner(d*plan.shard)+TILE-1)//TILE
    b = (plan.inner((d+1)*plan.shard)+TILE-1)//TILE
    b = jnp.where(d == plan.n-1, plan.total, b)
    return a, b-a

def floor_of(plan, dpi, z):
    return plan.inner((dpi*plan.nseq+z)*plan.shard)//TILE

FRONT, NEAR, BACK = 32, 40, 64


def shard_rows(plan):
    return -(-plan.shard // 1024) * 8


def place_rows(plan, rolled, block, first, rows, lead, cut, skip):
    shift, begin = lead % 128, FRONT + lead // 128
    lane = lax.broadcasted_iota(jnp.int32, (rows, 128), 1)
    at = (lax.broadcasted_iota(jnp.int32, (rows, 128), 0) + first) * LANES + lane
    for j in range(LANES // 128):

        def read(start):
            here = rolled[pl.ds(start, rows, stride=4), :]
            after = rolled[pl.ds(start + 1, rows, stride=4), :]
            return jnp.where(lane < 128 - shift, here, after)

        start = begin + j + 4 * first
        value = jnp.where(at + 128 * j < cut, read(start), read(start - skip)).astype(block.dtype)
        part = slice(first // 8, (first + rows) // 8)
        block[part, :, j * 128 : (j + 1) * 128] = value.reshape(rows // 8, 8, 128)


def gather_kernel(plan, x, out, src, line, rolled, give, take, near_sem, send_a, send_b, recv_a, recv_b, loc_sem):
    di, z = lax.axis_index(DP), lax.axis_index(SEQ)
    ns, ph = plan.nseq, plan.phases
    c = di%2
    masks, bits = phase_masks(di, c, ph)
    other = di+1-2*c
    omasks, obits = phase_masks(other, 1-c, ph)
    up, down = lax.rem(z+1,ns), lax.rem(z+ns-1,ns)
    partners=[(di,up),(di,down),(other,z)]+[(flip(di,masks,bits,1<<p,ph),z) for p in range(ph)]
    barrier=pltpu.get_barrier_semaphore()
    for a,b in partners:
        pl.semaphore_signal(barrier,inc=1,device_id=(a,b),device_id_type=MESH)
    index = di * ns + z
    following, before = lax.rem(index + 1, plan.n), lax.rem(index + plan.n - 1, plan.n)
    pl.semaphore_signal(barrier, inc=1, device_id=(following // ns, lax.rem(following, ns)), device_id_type=MESH)
    lo, more = plan.lo-1, plan.hi-plan.lo+1
    start_own, size_own = block_of(plan, di, z)
    rows = x.shape[0]
    joint, shift = divmod(plan.shard, 128)
    lane = lax.broadcasted_iota(jnp.int32, (NEAR, 128), 1)
    moved = pltpu.roll(x[:NEAR], shift, 1)
    earlier = jnp.concatenate([jnp.zeros((1, 128), jnp.float32), moved[: NEAR - 1]], 0)
    give[...] = jnp.where(lane >= shift, moved, earlier)
    line[:FRONT] = jnp.zeros((FRONT, 128), jnp.float32)
    line[FRONT : FRONT + rows] = x[...]
    line[FRONT + rows :] = jnp.zeros((line.shape[0] - FRONT - rows, 128), jnp.float32)
    begin = index * plan.shard
    inner = plan.inner(begin)
    lead = (inner + TILE - 1) // TILE * TILE - inner
    cut, skip = 2**30, 0
    for position, size in plan.gaps:
        hit = jnp.logical_and(position > begin, position < begin + plan.shard + TILE)
        cut = jnp.where(hit, position - begin - lead, cut)
        skip = jnp.where(hit, size // 128, skip)
    turn = lax.rem(128 - lead % 128, 128)
    rolled[...] = pltpu.roll(line[...], turn, 1)
    place_rows(plan, rolled, src, 0, 8 * lo, lead, cut, skip)
    pl.semaphore_wait(barrier,len(partners)+1)
    near = pltpu.make_async_remote_copy(src_ref=give,dst_ref=take,send_sem=near_sem.at[0],recv_sem=near_sem.at[1],
        device_id=(before // ns, lax.rem(before, ns)),device_id_type=MESH)
    near.start()

    def pair(ref, base, dst_start, size, sidx, ridx, dev):
        copies=[pltpu.make_async_remote_copy(src_ref=ref.at[pl.ds(base,lo)],dst_ref=out.at[pl.ds(dst_start,lo)],
            send_sem=send_a.at[sidx],recv_sem=recv_a.at[ridx],device_id=dev,device_id_type=MESH)]
        for x in range(more):
            copies.append(pltpu.make_async_remote_copy(src_ref=ref.at[pl.ds(base+lo+x,1)],dst_ref=out.at[pl.ds(dst_start+lo+x,1)],
                send_sem=send_b.at[sidx*more+x],recv_sem=recv_b.at[ridx*more+x],device_id=dev,device_id_type=MESH))
        return copies, size
    def each(p, act, part=None):
        for x,copy in enumerate(p[0]):
            if part is not None and (x==0) != (part==0): continue
            if x<2: act(copy)
            else:
                @pl.when(p[1]>=lo+x)
                def _(): act(copy)
    def start(p,part): each(p, lambda c: c.start(), part)
    def wait_send(p): each(p, lambda c: c.wait_send())
    def wait_recv(p,part=None): each(p, lambda c: c.wait_recv(), part)

    own=[pltpu.make_async_copy(src.at[pl.ds(0,lo)],out.at[pl.ds(start_own,lo)],loc_sem.at[0])]
    for x in range(more):
        own.append(pltpu.make_async_copy(src.at[pl.ds(lo+x,1)],out.at[pl.ds(start_own+lo+x,1)],loc_sem.at[1+x]))
    own=(own,size_own)
    own[0][0].start()
    def finish_block():
        near.wait_recv()
        at = FRONT + joint
        line[at:at+1] = line[at:at+1] + take[0:1]
        line[at+1:at+NEAR] = take[1:]
        low = at // 8 * 8
        rolled[low:] = pltpu.roll(line[low:], turn, 1)
        place_rows(plan, rolled, src, 8*lo, 8*more, lead, cut, skip)
        for x,copy in enumerate(own[0][1:]):
            if x==0: copy.start()
            else:
                @pl.when(size_own>lo+x)
                def _(): copy.start()
    nslot=plan.slots
    sends=[]
    def guard(conds, fn):
        if not conds: fn(); return
        cond=conds[0]
        for x in conds[1:]: cond=jnp.logical_and(cond,x)
        @pl.when(cond)
        def _(): fn()

    tasks=[]
    for s, sign, t in plan.order():
        zz = z+sign*s
        conds=[] if s==0 else ([zz>=0] if sign<0 else [zz<ns])
        dpi=flip(di,masks,bits,t,ph)
        st,size=block_of(plan,dpi,zz)
        mine = s==0 and t==0
        ref, base = (src, 0) if mine else (out, st)
        slot = t*ns+zz
        got = None if mine else pair(out,st,st,size,0,slot,(di,z))
        copies=[]
        def forward(conds, ridx, dev):
            p=pair(ref,base,st,size,len(sends),ridx,dev)
            sends.append((conds,p))
            copies.append((conds,p))
        if t==0:
            if sign<=0 : forward(conds+[z<ns-1],slot,(di,z+1))
            if sign>=0 : forward(conds+[z>0],slot,(di,z-1))
        for pp in range(t.bit_length(),ph):
            forward(conds,slot+(1<<pp)*ns,(flip(di,masks,bits,1<<pp,ph),z))
        forward(conds,nslot+slot,(other,z))
        tasks.append((conds,got,copies))
    def run(task,part):
        conds,got,copies=task
        if got is None:
            if part==1: finish_block()
        else:
            guard(conds, lambda: wait_recv(got,part))
        for also,p in copies:
            guard(also, lambda: start(p,part))
    lag=4
    for i in range(len(tasks)+lag):
        if i<len(tasks): run(tasks[i],0)
        if i>=lag: run(tasks[i-lag],1)
    for s, sign, t in plan.order():
        zz=z+sign*s
        conds=[] if s==0 else ([zz>=0] if sign<0 else [zz<ns])
        dpi=flip(other,omasks,obits,t,ph)
        st,size=block_of(plan,dpi,zz)
        p=pair(out,st,st,size,0,nslot+t*ns+zz,(di,z))
        guard(conds,lambda: wait_recv(p))
    for conds,p in sends:
        guard(conds,lambda: wait_send(p))
    each(own, lambda c: c.wait())
    near.wait_send()

def count_sends(plan):
    n=0
    for s,sign,t in plan.order():
        if t==0: n+= (2 if sign==0 else 1)
        n+=plan.phases-t.bit_length()+1
    return n

def gather(plan, params):
    ns, more = count_sends(plan), plan.hi - plan.lo + 1
    rows = shard_rows(plan)
    lines = FRONT + rows + NEAR + BACK
    lines += -lines % 8
    values = jnp.pad(params, (0, rows * 128 - plan.shard)).reshape(rows, 128)
    return pl.pallas_call(
        functools.partial(gather_kernel, plan),
        out_shape=jax.ShapeDtypeStruct((plan.total, 8, LANES), jnp.bfloat16),
        in_specs=[pl.BlockSpec(memory_space=pltpu.VMEM)],
        out_specs=pl.BlockSpec(memory_space=pl.ANY),
        scratch_shapes=[
            pltpu.VMEM((plan.hi, 8, LANES), jnp.bfloat16), pltpu.VMEM((lines, 128), jnp.float32),
            pltpu.VMEM((lines, 128), jnp.float32), pltpu.VMEM((NEAR, 128), jnp.float32),
            pltpu.VMEM((NEAR, 128), jnp.float32), pltpu.SemaphoreType.DMA((2,)),
            pltpu.SemaphoreType.DMA((ns,)), pltpu.SemaphoreType.DMA((ns * more,)),
            pltpu.SemaphoreType.DMA((2 * plan.slots,)), pltpu.SemaphoreType.DMA((2 * plan.slots * more,)),
            pltpu.SemaphoreType.DMA((1 + more,)),
        ],
        compiler_params=pltpu.CompilerParams(collective_id=0, has_side_effects=True),
        name="gather_params",
    )(values)


def scatter_kernel(plan, g, out, acc, rc, rp, rz, load_sem, send_sem, core_send, core_recv, ph_recv, z_recv):
    di, z = lax.axis_index(DP), lax.axis_index(SEQ)
    ns, ph, win, nslot = plan.nseq, plan.phases, plan.win, plan.slots
    c = di%2
    masks, bits = phase_masks(di, c, ph)
    other = di+1-2*c
    omasks, obits = phase_masks(other, 1-c, ph)
    up, down = lax.rem(z+1,ns), lax.rem(z+ns-1,ns)
    partners=[(di,up),(di,down),(other,z)]+[(flip(di,masks,bits,1<<p,ph),z) for p in range(ph)]
    barrier=pltpu.get_barrier_semaphore()
    for a,b in partners:
        pl.semaphore_signal(barrier,inc=1,device_id=(a,b),device_id_type=MESH)
    order=list(reversed(plan.order()))
    def cond_of(s,sign):
        zz=z+sign*s
        return zz,([] if s==0 else ([zz>=0] if sign<0 else [zz<ns]))
    def guard(conds, fn):
        if not conds: fn(); return
        cond=conds[0]
        for x in conds[1:]: cond=jnp.logical_and(cond,x)
        @pl.when(cond)
        def _(): fn()
    def load(s,sign,t):
        zz,conds=cond_of(s,sign)
        slot=t*ns+zz
        st=floor_of(plan,flip(di,masks,bits,t,ph),zz)
        return conds,pltpu.make_async_copy(g.at[pl.ds(st,win)],acc.at[slot],load_sem.at[slot])
    def core(s,sign,t):
        zz,conds=cond_of(s,sign)
        slot=t*ns+zz
        st=floor_of(plan,flip(other,omasks,obits,t,ph),zz)
        return conds,pltpu.make_async_remote_copy(src_ref=g.at[pl.ds(st,win)],dst_ref=rc.at[slot],
            send_sem=core_send.at[slot],recv_sem=core_recv.at[slot],device_id=(other,z),device_id_type=MESH)
    for e in order:
        conds,cp=load(*e)
        guard(conds,lambda: cp.start())
    pl.semaphore_wait(barrier,len(partners))
    for e in order:
        conds,cp=core(*e)
        guard(conds,lambda: cp.start())
    sends=[]
    def send(conds,slot,dst,rsem,dev):
        i=len(sends)
        cp=pltpu.make_async_remote_copy(src_ref=acc.at[slot],dst_ref=dst,send_sem=send_sem.at[i],recv_sem=rsem,
            device_id=dev,device_id_type=MESH)
        sends.append((conds,cp))
        guard(conds,lambda: cp.start())
    def waiting(conds,dst,rsem):
        cp=pltpu.make_async_remote_copy(src_ref=dst,dst_ref=dst,send_sem=send_sem.at[0],recv_sem=rsem,
            device_id=(di,z),device_id_type=MESH)
        guard(conds,lambda: cp.wait_recv())
    step=2
    def add(dst, slot, parts, final=False):
        @pl.loop(0,win//step)
        def _(i):
            r=pl.ds(i*step,step)
            v=acc[slot,r].astype(jnp.float32)
            for p in parts:
                v=v+p(r).astype(jnp.float32)
            if final: out[r]=v
            else: acc[slot,r]=v.astype(acc.dtype)
    for s,sign,t in order:
        zz,conds=cond_of(s,sign)
        slot=t*ns+zz
        hi_bit=t.bit_length()
        def fn():
            load(s,sign,t)[1].wait()
            waiting([],rc.at[slot],core_recv.at[slot])
            parts=[lambda r: rc[slot,r]]
            for pp in range(hi_bit,ph):
                idx=((1<<pp)-1)*ns+slot
                waiting([],rp.at[idx],ph_recv.at[idx])
                parts.append(lambda r,idx=idx: rp[idx,r])
            add(None,slot,parts,final=False) if not (t==0 and s==0) else add(None,slot,parts,final=True)
        guard(conds,fn)
        if t:
            pp=hi_bit-1
            idx=((1<<pp)-1)*ns+slot-(1<<pp)*ns
            send(conds,slot,rp.at[idx],ph_recv.at[idx],(flip(di,masks,bits,1<<pp,ph),z))
        else:
            def zadd(stream, extra):
                zi=stream*ns+zz
                def fz():
                    waiting([],rz.at[zi],z_recv.at[zi])
                    @pl.loop(0,win//step)
                    def _(i):
                        r=pl.ds(i*step,step)
                        if s==0:
                            out[r]=out[r]+rz[zi,r].astype(jnp.float32)
                        else:
                            acc[slot,r]=(acc[slot,r].astype(jnp.float32)+rz[zi,r].astype(jnp.float32)).astype(acc.dtype)
                guard(conds+extra,fz)
            if sign>=0: zadd(0,[z>0])
            if sign<=0: zadd(1,[z<ns-1])
            if sign>0: send(conds,slot,rz.at[zz],z_recv.at[zz],(di,z+1))
            if sign<0: send(conds,slot,rz.at[ns+zz],z_recv.at[ns+zz],(di,z-1))
    for e in order:
        conds,cp=core(*e)
        guard(conds,lambda: cp.wait_send())
    for conds,cp in sends:
        guard(conds,lambda: cp.wait_send())

def scatter(plan, g):
    win,ns,ph,nslot=plan.win,plan.nseq,plan.phases,plan.slots
    nsend=len(plan.order())
    return pl.pallas_call(
        functools.partial(scatter_kernel,plan),
        out_shape=jax.ShapeDtypeStruct((win,8,LANES),jnp.float32),
        in_specs=[pl.BlockSpec(memory_space=pl.ANY)],
        out_specs=pl.BlockSpec(memory_space=pltpu.VMEM),
        scratch_shapes=[pltpu.VMEM((nslot,win,8,LANES),g.dtype),pltpu.VMEM((nslot,win,8,LANES),g.dtype),
            pltpu.VMEM(((2**ph-1)*ns,win,8,LANES),g.dtype),pltpu.VMEM((2*ns,win,8,LANES),g.dtype),
            pltpu.SemaphoreType.DMA((nslot,)),pltpu.SemaphoreType.DMA((nsend,)),
            pltpu.SemaphoreType.DMA((nslot,)),pltpu.SemaphoreType.DMA((nslot,)),
            pltpu.SemaphoreType.DMA(((2**ph-1)*ns,)),pltpu.SemaphoreType.DMA((2*ns,))],
        compiler_params=pltpu.CompilerParams(collective_id=1,has_side_effects=True,vmem_limit_bytes=48*1024*1024),
        name="scatter_grads",
    )(g)


def weight_kernel(plan, names, places, *refs):
    count = 2 * len(names)
    sources, refs = refs[:count], refs[count:]
    vectors, refs = refs[: len(refs) - count - 4], refs[len(refs) - count - 4 :]
    target, stores, (out, mix, sem) = refs[0], refs[1 : count + 1], refs[count + 1 :]
    loads = []
    for i in range(count):
        loads.append(pltpu.make_async_copy(sources[i], stores[i], sem.at[i]))
        loads[i].start()
    rows = (((0,), (0,)), ((), ()))
    sent = []

    def send(first, tiles):
        if tiles:
            part = pl.ds(first, tiles)
            copy = pltpu.make_async_copy(out.at[part], target.at[part], sem.at[count + len(sent)])
            copy.start()
            sent.append(copy)

    edge = 0
    for name, shape in segments():
        if math.prod(shape) < D * D:
            first = plan.places[name]
            array, begin = places[name]
            for r in range(-(-math.prod(shape) // LANES)):
                line = vectors[array][begin + r : begin + r + 1, :]
                tile, row = divmod(first + r, 8)
                out[tile, row : row + 1, : line.shape[1]] = line.astype(out.dtype)
    for name, shape in segments():
        if math.prod(shape) >= D * D:
            first = plan.places[name] // 8
            send(edge, first - edge)
            edge = first + math.prod(shape) // TILE
    send(edge, plan.total - edge)
    shapes = dict(segments())
    for number, name in enumerate(names):
        shape, first = shapes[name], plan.places[name]
        left, right = stores[2 * number], stores[2 * number + 1]
        wait_all(*loads[2 * number : 2 * number + 2])
        fold = shape[1] // LANES
        step = 256 if fold == 1 else 128

        @pl.loop(0, shape[0] // step)
        def _(i):
            part = left[:, pl.ds(pl.multiple_of(i * step, step), step)]
            value = lax.dot_general(part, right[...], rows, preferred_element_type=jnp.float32)
            if fold > 1:
                for j in range(fold):
                    for lane in range(LANES // 128):
                        at = j * LANES + lane * 128
                        mix[lane, pl.ds(j, step, stride=fold), :] = value[:, at : at + 128]
                value = jnp.concatenate([mix[lane, : step * fold] for lane in range(LANES // 128)], 1)
            tiles = step * fold // 8
            out[pl.ds(first // 8 + i * tiles, tiles)] = value.astype(out.dtype).reshape(tiles, 8, LANES)

        send(first // 8, math.prod(shape) // TILE)
    wait_all(*sent)


def weight_grads(plan, gradients, vectors, places):
    names = list(gradients)
    operands = [value for name in names for value in gradients[name]]
    return pl.pallas_call(
        functools.partial(weight_kernel, plan, names, places),
        out_shape=jax.ShapeDtypeStruct((plan.padded, 8, LANES), jnp.bfloat16),
        in_specs=[ANY_SPEC] * len(operands) + [VMEM_SPEC] * len(vectors),
        out_specs=ANY_SPEC,
        scratch_shapes=[vm(value.shape) for value in operands] + [
            vm((plan.padded, 8, LANES)), vm((LANES // 128, 512, 128), F32),
            DMA((len(operands) + len(segments()),)),
        ],
        compiler_params=pltpu.CompilerParams(vmem_limit_bytes=60 * 1024 * 1024),
        name="weight_grads",
    )(*operands, *vectors)


def bucket_windows(rel_bucket, block_len, count):
    width = -(-(block_len * (count + 1) - 1) // 128) * 128
    padded = jnp.concatenate([rel_bucket, jnp.full((width,), -1, jnp.int32)])
    windows = [padded[(count - 1 - b) * block_len :][:width] for b in range(count)]
    return (jnp.stack(windows)[:, None, :] == jnp.arange(NB, dtype=jnp.int32)[None, :, None]).astype(jnp.float32)


def adam_update(param_vec, grad_in, first_mom, second):
    new_first = BETA_ONE * first_mom + (1.0 - BETA_ONE) * grad_in
    new_second = BETA_TWO * second + (1.0 - BETA_TWO) * grad_in * grad_in
    corr_one = 1.0 - BETA_ONE**STEP
    corr_two = 1.0 - BETA_TWO**STEP
    step_size = new_first / corr_one / (jnp.sqrt(new_second / corr_two) + ADAM_EPS)
    return (param_vec - LEARN_RATE * (step_size + DECAY * param_vec), new_first, new_second)


def unit_rows(values):
    centre = values - jnp.mean(values, -1, keepdims=True)
    scale = lax.rsqrt(jnp.mean(centre * centre, -1, keepdims=True) + NORM_EPS)
    return centre * scale, scale


def unit_back(unit, scale, gain, grad):
    shifted = grad * gain
    first = jnp.mean(shifted, -1, keepdims=True)
    second = jnp.mean(shifted * unit, -1, keepdims=True)
    return scale * (shifted - first - unit * second), total_rows(grad * unit), total_rows(grad)


def total_rows(values):
    return jnp.sum(values, 0, keepdims=True)


def split_rows(source, mix, target, fold):
    block = mix.shape[1]
    lanes = LANES // 128

    @pl.loop(0, source.shape[0] // block)
    def _(i):
        part = source[pl.ds(pl.multiple_of(i * block, block), block), :].astype(jnp.float32)
        for lane in range(lanes):
            mix[lane] = part[:, lane * 128 : (lane + 1) * 128]
        for j in range(fold):
            rows = [mix[lane, pl.ds(j, block // fold, stride=fold), :] for lane in range(lanes)]
            at = pl.multiple_of(i * (block // fold), block // fold)
            target[j, pl.ds(at, block // fold), :] = jnp.concatenate(rows, 1).astype(target.dtype)


class Fetch:
    def __init__(self, plan, packed, sem):
        self.plan, self.packed, self.sem, self.count = plan, packed, sem, 0

    def __call__(self, name, target):
        row = self.plan.places[name] // 8 * 8
        copy = pltpu.make_async_copy(
            self.packed.at[pl.ds(row, target.shape[0])], target, self.sem.at[self.count]
        )
        self.count += 1
        copy.start()
        return copy


def column(j):
    return pl.ds(pl.multiple_of(j * LANES, LANES), LANES)


def wait_all(*copies):
    for copy in copies:
        copy.wait()


def ffn_first_kernel(plan, x, packed, x_out, n_out, w_out, w_in, w_second, v0, v1, v2, bias, acc, one, mix, sem):
    fetch = Fetch(plan, packed, sem)
    early = [fetch("first_ng", v0), fetch("first_b_in", v1), fetch("first_b_out", v2)]
    in_copy = fetch("first_w_in", w_in)
    late = [fetch("first_w_out", w_second)]
    yield
    wait_all(*early)
    gains, bias_in, tail = v0[...].astype(jnp.float32), v1[...].astype(jnp.float32), v2[...].astype(jnp.float32)
    stream = x[...]
    unit, _ = unit_rows(stream)
    normed = (unit * gains[0:1] + gains[1:2]).astype(jnp.bfloat16)
    in_copy.wait()
    split_rows(w_in, mix, w_out, FF // LANES)
    wait_all(*late)
    one[...] = normed
    bias[...] = bias_in
    acc[...] = jnp.zeros(acc.shape, jnp.float32)

    @pl.loop(0, FF // LANES)
    def _(j):
        hidden = forward_dot(one[...], w_out[j]) + bias[pl.ds(j, 1), :]
        active = swish_act(hidden).astype(jnp.bfloat16)
        acc[...] += forward_dot(active, w_second[column(j), :])

    stream = x[...] + 0.5 * (acc[...] + tail[0:1])
    x_out[...] = stream
    unit, _ = unit_rows(stream)
    normed = (unit * tail[1:2] + tail[2:3]).astype(jnp.bfloat16)
    n_out[...] = normed.reshape(n_out.shape)


def ffn_first_back_kernel(plan, x, x_one, d_two, d_norm_in, w_in, packed,
                          d_out, a_out, r_out, n_out, h_out, vec_out, w_second, v0, v1, v2, bias, acc, sem):
    fetch = Fetch(plan, packed, sem)
    early = [fetch("first_ng", v0), fetch("first_b_in", v1), fetch("first_b_out", v2)]
    late = fetch("first_w_out", w_second)
    yield
    wait_all(*early)
    gains, bias_in, tail = v0[...].astype(jnp.float32), v1[...].astype(jnp.float32), v2[...].astype(jnp.float32)
    unit, scale = unit_rows(x_one[...])
    d_normed = d_norm_in[...].astype(jnp.float32).reshape(-1, D)
    d_norm, gain_grad, shift_grad = unit_back(unit, scale, tail[1:2], d_normed)
    vec_out[0:1] = gain_grad
    vec_out[1:2] = shift_grad
    grad = d_two[...] + d_norm
    half = 0.5 * grad
    vec_out[2:3] = total_rows(half)
    half_b = half.astype(jnp.bfloat16)
    r_out[...] = half_b
    unit, scale = unit_rows(x[...])
    normed = (unit * gains[0:1] + gains[1:2]).astype(jnp.bfloat16)
    n_out[...] = normed
    late.wait()
    bias[...] = bias_in
    acc[...] = jnp.zeros(acc.shape, jnp.float32)
    d_out[...] = grad

    @pl.loop(0, FF // LANES)
    def _(j):
        cols = column(j)
        hidden = forward_dot(n_out[...], w_in[j]) + bias[pl.ds(j, 1), :]
        a_out[:, cols] = swish_act(hidden).astype(jnp.bfloat16)
        d_hidden = back_dot(r_out[...], w_second[cols, :]) * swish_grad(hidden)
        vec_out[pl.ds(5 + j, 1), :] = total_rows(d_hidden)
        d_hidden = d_hidden.astype(jnp.bfloat16)
        h_out[:, cols] = d_hidden
        acc[...] += back_dot(d_hidden, w_in[j])

    unit, scale = unit_rows(x[...])
    d_norm, gain_grad, shift_grad = unit_back(unit, scale, gains[0:1], acc[...])
    vec_out[3:4] = gain_grad
    vec_out[4:5] = shift_grad
    d_out[...] += d_norm


def gate_kernel(plan, ctx, x, valid, packed, x_out, n_out, g_out, u_out, w_out, w_o, w_pi, v0, v1, mix, sem):
    fetch = Fetch(plan, packed, sem)
    early = [fetch("w_o", w_o), fetch("b_o", v0), fetch("b_pi", v1)]
    late = fetch("w_pi", w_pi)
    yield
    wait_all(*early)
    rows, bias_in = v0[...].astype(jnp.float32), v1[...].astype(jnp.float32)
    stream = x[...] + forward_dot(ctx[...].reshape(-1, D), w_o[...]) + rows[0:1]
    x_out[...] = stream
    unit, _ = unit_rows(stream)
    normed = (unit * rows[6:7] + rows[7:8]).astype(jnp.bfloat16)
    n_out[...] = normed
    late.wait()
    split_rows(w_pi, mix, w_out, 2)
    linear = forward_dot(normed, w_out[0]) + bias_in[0:1]
    gate = forward_dot(normed, w_out[1]) + bias_in[1:2]
    g_out[:, :D] = linear
    g_out[:, D:] = gate
    u_out[...] = linear * jax.nn.sigmoid(gate) * valid[...]


def gate_back_kernel(plan, du, pre_gate, x, d_three, valid, w_pi, packed,
                     g_out, d_out, o_out, c_out, vec_out, w_o, v0, sem):
    fetch = Fetch(plan, packed, sem)
    copies = [fetch("b_o", v0), fetch("w_o", w_o)]
    yield
    d_gated = du[...] * valid[...]
    gate_sig = jax.nn.sigmoid(pre_gate[:, D:])
    d_linear = d_gated * gate_sig
    d_gate = d_gated * pre_gate[:, :D] * gate_sig * (1.0 - gate_sig)
    vec_out[0:1] = total_rows(d_linear)
    vec_out[1:2] = total_rows(d_gate)
    d_linear, d_gate = d_linear.astype(jnp.bfloat16), d_gate.astype(jnp.bfloat16)
    g_out[:, :D] = d_linear
    g_out[:, D:] = d_gate
    d_normed = back_dot(d_linear, w_pi[0]) + back_dot(d_gate, w_pi[1])
    unit, scale = unit_rows(x[...])
    wait_all(*copies)
    d_norm, gain_grad, shift_grad = unit_back(unit, scale, v0[...].astype(jnp.float32)[6:7], d_normed)
    vec_out[2:3] = gain_grad
    vec_out[3:4] = shift_grad
    grad = d_three[...] + d_norm
    d_out[...] = grad
    vec_out[4:5] = total_rows(grad)
    grad_b = grad.astype(jnp.bfloat16)
    o_out[...] = grad_b
    c_out[...] = back_dot(grad_b, w_o[...]).astype(jnp.bfloat16).reshape(c_out.shape)


def middle_kernel(plan, x, depth, sums, cot, valid, packed,
                  y_out, d_out, z_out, part_out, stat_out, e_out, rb_out, a_out, r_out, n_out, h_out, vec_out,
                  w_po, w_in, w_second, w_mix, held, v_bn, v0, v1, v2, bias, acc, mix, sem):
    fetch = Fetch(plan, packed, sem)
    early = [fetch("b_pi", v_bn), fetch("w_po", w_po), fetch("b_po", v0), fetch("second_b_in", v1)]
    early.append(fetch("second_b_out", v2))
    in_copy = fetch("second_w_in", w_in)
    late = fetch("second_w_out", w_second)
    yield
    wait_all(*early)
    base = plan.places["bng"] - plan.places["b_pi"]
    batch, head = v_bn[...].astype(jnp.float32), v0[...].astype(jnp.float32)
    bias_in, tail = v1[...].astype(jnp.float32), v2[...].astype(jnp.float32)
    gain, shift = batch[base : base + 1], batch[base + 1 : base + 2]
    count = sums[2:3]
    mean = sums[0:1] / count
    inv_std = lax.rsqrt(sums[1:2] / count - mean * mean + BATCH_EPS)
    stat_out[0:1] = mean
    stat_out[1:2] = inv_std
    stat_out[2:3] = count
    stat_out[3:4] = jnp.zeros((1, D), jnp.float32)
    standard = (depth[...] - mean) * inv_std
    e_out[...] = swish_act(standard * gain + shift).astype(jnp.bfloat16)
    three = x[...] + forward_dot(e_out[...], w_po[...]) + head[0:1]
    unit, scale = unit_rows(three)
    n_out[...] = (unit * head[1:2] + head[2:3]).astype(jnp.bfloat16)
    in_copy.wait()
    split_rows(w_in, mix, w_mix, FF // LANES)
    late.wait()
    bias[...] = bias_in
    acc[...] = jnp.zeros(acc.shape, jnp.float32)
    d_out[...] = three

    @pl.loop(0, FF // LANES)
    def _(j):
        cols = column(j)
        hidden = forward_dot(n_out[...], w_mix[j]) + bias[pl.ds(j, 1), :]
        held[j] = hidden
        active = swish_act(hidden).astype(jnp.bfloat16)
        a_out[:, cols] = active
        acc[...] += forward_dot(active, w_second[cols, :])

    three = d_out[...]
    four = three + 0.5 * (acc[...] + tail[0:1])
    last, last_scale = unit_rows(four)
    y_out[...] = last * tail[1:2] + tail[2:3]
    grad = cot[...] * valid[...]
    grad, gain_grad, shift_grad = unit_back(last, last_scale, tail[1:2], grad)
    vec_out[0:1] = gain_grad
    vec_out[1:2] = shift_grad
    half = 0.5 * grad
    vec_out[2:3] = total_rows(half)
    r_out[...] = half.astype(jnp.bfloat16)
    acc[...] = jnp.zeros(acc.shape, jnp.float32)
    z_out[...] = grad

    @pl.loop(0, FF // LANES)
    def _(j):
        cols = column(j)
        d_hidden = back_dot(r_out[...], w_second[cols, :]) * swish_grad(held[j])
        vec_out[pl.ds(8 + j, 1), :] = total_rows(d_hidden)
        d_hidden = d_hidden.astype(jnp.bfloat16)
        h_out[:, cols] = d_hidden
        acc[...] += back_dot(d_hidden, w_mix[j])

    unit, scale = unit_rows(d_out[...])
    d_norm, gain_grad, shift_grad = unit_back(unit, scale, head[1:2], acc[...])
    vec_out[3:4] = gain_grad
    vec_out[4:5] = shift_grad
    grad = z_out[...] + d_norm
    d_out[...] = grad
    vec_out[5:6] = total_rows(grad)
    rb_out[...] = grad.astype(jnp.bfloat16)
    standard = (depth[...] - mean) * inv_std
    d_active = back_dot(rb_out[...], w_po[...]) * swish_grad(standard * gain + shift)
    d_gain, d_shift = total_rows(d_active * standard), total_rows(d_active)
    vec_out[6:7] = d_gain
    vec_out[7:8] = d_shift
    vec_out[12:16] = jnp.zeros((4, D), jnp.float32)
    d_standard = d_active * gain * valid[...]
    z_out[...] = d_standard
    part_out[0:1] = total_rows(d_standard)
    part_out[1:2] = total_rows(d_standard * standard)
    part_out[2:4] = jnp.zeros((2, D), jnp.float32)


def everyone(plan):
    di, z = lax.axis_index(DP), lax.axis_index(SEQ)
    other = di + 1 - 2 * (di % 2)
    peers = [(lax.rem(di + i, plan.ndp), z) for i in range(1, plan.ndp)]
    for i in range(1, plan.nseq):
        to = lax.rem(z + i, plan.nseq)
        peers += [(di, to), (other, to)]
    barrier = pltpu.get_barrier_semaphore()
    for peer in peers:
        pl.semaphore_signal(barrier, inc=1, device_id=peer, device_id_type=MESH)
    return lambda: pl.semaphore_wait(barrier, len(peers))


def exchange_sum(ndp, nseq, part, line, cross, sems):
    di, z = lax.axis_index(DP), lax.axis_index(SEQ)

    def phase(count, me, target, slots, send, recv):
        copies = []
        for i in range(1, count):
            copy = pltpu.make_async_remote_copy(
                src_ref=part, dst_ref=slots.at[me], send_sem=send.at[i], recv_sem=recv.at[me],
                device_id=target(lax.rem(me + i, count)), device_id_type=MESH,
            )
            copy.start()
            copies.append(copy)
        slots[me] = part[...]
        for i in range(1, count):
            source = lax.rem(me + count - i, count)
            pltpu.make_async_remote_copy(
                src_ref=part, dst_ref=slots.at[source], send_sem=send.at[i], recv_sem=recv.at[source],
                device_id=(di, z), device_id_type=MESH,
            ).wait_recv()
        for copy in copies:
            copy.wait_send()
        total = slots[0]
        for i in range(1, count):
            total = total + slots[i]
        return total

    part[...] = phase(nseq, z, lambda i: (di, i), line, sems[0], sems[1])
    return phase(ndp, di, lambda i: (i, z), cross, sems[2], sems[3])


HALO = 16


class Halo:
    def __init__(self, nseq, buffer, sem):
        di, z = lax.axis_index(DP), lax.axis_index(SEQ)
        rows = buffer.shape[1]
        self.has = (z > 0, z < nseq - 1)

        def copy(source, target, number, to):
            return pltpu.make_async_remote_copy(
                src_ref=buffer.at[:, pl.ds(source, HALO)], dst_ref=buffer.at[:, pl.ds(target, HALO)],
                send_sem=sem.at[number], recv_sem=sem.at[2 + number], device_id=(di, to), device_id_type=MESH,
            )

        self.up = copy(rows - 2 * HALO, 0, 0, lax.rem(z + 1, nseq))
        self.down = copy(HALO, rows - HALO, 1, lax.rem(z + nseq - 1, nseq))
        self.buffer, self.rows = buffer, rows

    def start(self):
        @pl.when(self.has[1])
        def _():
            self.up.start()

        @pl.when(self.has[0])
        def _():
            self.down.start()

    def finish(self):
        empty = jnp.zeros((self.buffer.shape[0], HALO, self.buffer.shape[2]), jnp.float32)

        @pl.when(self.has[0])
        def _():
            self.up.wait_recv()
            self.down.wait_send()

        @pl.when(jnp.logical_not(self.has[0]))
        def _():
            self.buffer[:, :HALO] = empty

        @pl.when(self.has[1])
        def _():
            self.down.wait_recv()
            self.up.wait_send()

        @pl.when(jnp.logical_not(self.has[1]))
        def _():
            self.buffer[:, self.rows - HALO :] = empty


def slide(padded, taps, index, out, length):
    lanes = LANES // 128

    @pl.loop(0, padded.shape[0] * lanes)
    def _(i):
        s, lane = i // lanes, pl.ds(pl.multiple_of(i % lanes * 128, 128), 128)
        total = jnp.zeros((length, 128), jnp.float32)
        for b in range(8):
            part = None
            for a in range(4):
                if 0 < 8 * a + b < K + 1:
                    row = index(8 * a + b)
                    term = taps[row : row + 1, lane] * padded[s, 8 * a : 8 * a + length + 8, lane]
                    part = term if part is None else part + term
            total = total + part[b : b + length]
        out[pl.ds(pl.multiple_of(s * length, length), length), lane] = total


def depth_kernel(plan, u, valid, packed, c_out, sum_out, padded, taps, taps_b, part, line, cross, sem,
                 halo_sem, *sems):
    ndp, nseq = plan.ndp, plan.nseq
    length = padded.shape[1] - 2 * HALO
    copy = Fetch(plan, packed, sem)("b_pi", taps_b)
    yield
    padded[:, HALO : HALO + length] = u[...].reshape(-1, length, D)
    halo = Halo(nseq, padded, halo_sem)
    halo.start()
    copy.wait()
    taps[...] = taps_b[...].astype(jnp.float32)
    halo.finish()
    base = plan.places["w_depth"] - plan.places["b_pi"]
    slide(padded, taps, lambda i: base + i - 1, c_out, length)
    depth, mask = c_out[...], valid[...]
    value = depth * mask
    part[0:1] = total_rows(value)
    part[1:2] = total_rows(value * depth)
    part[2:3] = jnp.broadcast_to(total_rows(mask), (1, LANES))
    part[3:4] = jnp.zeros((1, LANES), jnp.float32)
    sum_out[...] = exchange_sum(ndp, nseq, part, line, cross, sems)


def depth_back_kernel(plan, dz, depth, stats, local, valid, u_pad, packed, u_out, tap_out,
                      padded, own, taps, taps_b, part, line, cross, sem, halo_sem, *sems):
    ndp, nseq = plan.ndp, plan.nseq
    seqs, length = padded.shape[0], padded.shape[1] - 2 * HALO
    copy = Fetch(plan, packed, sem)("b_pi", taps_b)
    yield
    part[...] = local[...]
    sums = exchange_sum(ndp, nseq, part, line, cross, sems)
    mean, inv_std, count = stats[0:1], stats[1:2], stats[2:3]
    standard = (depth[...] - mean) * inv_std
    d_depth = valid[...] * inv_std * (dz[...] - sums[0:1] / count - standard * (sums[1:2] / count))
    d_depth = d_depth.reshape(seqs, length, D)
    padded[:, HALO : HALO + length] = d_depth
    halo = Halo(nseq, padded, halo_sem)
    halo.start()
    own[:, :8] = jnp.zeros((seqs, 8, D), jnp.float32)
    own[:, 8 : 8 + length] = d_depth
    own[:, 8 + length :] = jnp.zeros((seqs, 8, D), jnp.float32)
    copy.wait()
    taps[...] = taps_b[...].astype(jnp.float32)
    base = plan.places["w_depth"] - plan.places["b_pi"]

    @pl.loop(0, LANES // 128)
    def _(i):
        lane = pl.ds(pl.multiple_of(i * 128, 128), 128)
        for b in range(8):
            sums_b = [None] * 4
            for s in range(seqs):
                moved = own[s, 8 - b : 8 - b + length + 8, lane]
                for a in range(4):
                    if 0 < 8 * a + b < K + 1:
                        term = total_rows(u_pad[s, 8 * a : 8 * a + length + 8, lane] * moved)
                        sums_b[a] = term if sums_b[a] is None else sums_b[a] + term
            for a in range(4):
                if sums_b[a] is not None:
                    tap_out[8 * a + b - 1 : 8 * a + b, lane] = sums_b[a]
        tap_out[K : K + 1, lane] = jnp.zeros((1, 128), jnp.float32)

    halo.finish()
    slide(padded, taps, lambda i: base + K - i, u_out, length)


def head_scores(q, k, line, valid):
    block, full, width = q.shape[0], k.shape[0], line.shape[1]
    scores = lax.dot_general(q, k, (((1,), (1,)), ((), ())), preferred_element_type=jnp.float32)
    spread = jnp.broadcast_to(line, (block, width))
    bias = pltpu.roll(spread, width - block + 1, 1, stride=1, stride_axis=0)[:, :full]
    return jnp.where(valid, scores * (1.0 / math.sqrt(HD)) + bias, -jnp.inf)


def remote(source, target, send, recv, device):
    return pltpu.make_async_remote_copy(
        src_ref=source, dst_ref=target, send_sem=send, recv_sem=recv, device_id=device, device_id_type=MESH
    )


class Team:
    def __init__(self, plan, seqs):
        self.di, self.z = lax.axis_index(DP), lax.axis_index(SEQ)
        self.count, self.seqs = plan.nseq, seqs
        self.c = self.di % 2
        self.base = self.di - self.c
        self.other = self.base + 1 - self.c
        self.owner = self.base + self.z // seqs
        self.main = self.z // seqs == self.c
        self.slot = self.z % seqs
        self.half = pl.ds(pl.multiple_of(self.c * (D // 2), D // 2), D // 2)

    def turn(self, i):
        return lax.rem(self.z + i, self.count)


def half_copy(packed, plan, name, team, target, sem):
    copy = pltpu.make_async_copy(packed.at[pl.ds(plan.places[name], D), team.half], target, sem)
    copy.start()
    return copy


def attend_kernel(plan, normed, lengths, tables, packed, ctx_out, all_out, q_out, k_out, v_out, lse_out, len_out,
                  w_q, w_k, w_v, b_q, b_v, held, mine, sem, in_send, relay_send, in_recv, ctx_send, ctx_recv, len_sem):
    seqs, block, _ = normed.shape
    count = plan.nseq
    team = Team(plan, seqs)
    fetch = Fetch(plan, packed, sem)
    copies = [fetch("b_q", b_q), fetch("b_v", b_v)]
    for i, (name, target) in enumerate((("w_q", w_q), ("w_k", w_k), ("w_v", w_v))):
        copies.append(half_copy(packed, plan, name, team, target, sem.at[2 + i]))
    yield
    c, z = team.c, team.z
    sends = []
    for s in range(seqs):
        to = c * seqs + s
        copy = remote(normed.at[s], all_out.at[z], in_send.at[s], in_recv.at[z], (team.di, to))
        sends.append((to != z, copy))
        pl.when(to != z)(copy.start)
    relays = []
    for i in range(count):
        b = team.turn(i)
        source = normed.at[team.slot] if i == 0 else all_out.at[b]
        relays.append(remote(source, all_out.at[b], relay_send.at[b], in_recv.at[b], (team.other, z)))
    pl.when(team.main)(relays[0].start)
    note = remote(lengths, len_out, len_sem.at[0], len_sem.at[1], (team.other, z))
    pl.when(team.main)(note.start)

    @pl.when(team.main)
    def _():
        all_out[z] = normed[team.slot]
        len_out[...] = lengths[...]

    wait_all(*copies)
    mine[0] = b_q[...].astype(jnp.float32)
    mine[1] = b_v[...].astype(jnp.float32)
    bias_q, bias_v = mine[0, 0:1, team.half], mine[1, 0:1, team.half]
    for i in range(count):
        b = team.turn(i)
        if i == 0:
            pl.when(jnp.logical_not(team.main))(relays[0].wait_recv)
        else:
            relays[i].wait_recv()
            pl.when(team.main)(relays[i].start)
        part = all_out[b]
        at = pl.ds(pl.multiple_of(b * block, block), block)
        q_out[at, :] = (forward_dot(part, w_q[...]) + bias_q).astype(jnp.bfloat16)
        k_out[at, :] = forward_dot(part, w_k[...]).astype(jnp.bfloat16)
        v_out[at, :] = (forward_dot(part, w_v[...]) + bias_v).astype(jnp.bfloat16)
    full = count * block
    pl.when(jnp.logical_not(team.main))(note.wait_recv)
    valid = lax.broadcasted_iota(jnp.int32, (1, full), 1) < len_out[pl.ds(team.slot, 1), :][:, 0:1]
    lane = lax.broadcasted_iota(jnp.int32, (block, 128), 1)

    def back(b):
        return remote(held.at[b], ctx_out.at[team.slot, :, team.half], ctx_send.at[b],
                      ctx_recv.at[team.slot * 2 + c], (team.owner, b))

    @pl.loop(0, count)
    def _(i):
        b = lax.rem(z + 1 + i, count)
        at = pl.ds(pl.multiple_of(b * block, block), block)
        lse = jnp.zeros((block, 128), jnp.float32)
        for h in range(H // 2):
            cols = slice(h * HD, (h + 1) * HD)
            line = tables[b, pl.ds(c * (H // 2) + h, 1), :]
            scores = head_scores(q_out[at, cols], k_out[:, cols], line, valid)
            top = jnp.max(scores, -1, keepdims=True)
            weights = jnp.exp(scores - top)
            total = jnp.sum(weights, -1, keepdims=True)
            probs = (weights * (1.0 / total)).astype(jnp.bfloat16)
            ctx = jnp.dot(probs, v_out[:, cols], preferred_element_type=jnp.float32)
            held[b, :, cols] = ctx.astype(jnp.bfloat16)
            lse = jnp.where(lane == h, top + jnp.log(total), lse)
        lse_out[at, :] = lse
        own = jnp.logical_and(b == z, team.main)

        @pl.when(own)
        def _():
            ctx_out[team.slot, :, team.half] = held[b]

        @pl.when(jnp.logical_not(own))
        def _():
            back(b).start()

    for s in range(seqs):
        for h in range(2):
            own = jnp.logical_and(c * seqs + s == z, c == h)
            here = ctx_out.at[s, :, pl.ds(h * (D // 2), D // 2)]
            copy = remote(held.at[0], here, ctx_send.at[0], ctx_recv.at[s * 2 + h], (team.di, z))
            pl.when(jnp.logical_not(own))(copy.wait_recv)
    pl.when(team.main)(note.wait_send)
    for flag, copy in sends:
        pl.when(flag)(copy.wait_send)
    for i in range(count):
        pl.when(team.main)(relays[i].wait_send)
        b = team.turn(i)
        own = jnp.logical_and(b == z, team.main)
        pl.when(jnp.logical_not(own))(back(b).wait_send)


def attend_back_kernel(plan, d_ctx, q_all, k_all, v_all, lse_all, length, tables, packed,
                       dn_out, dq_out, dk_out, dv_out, dt_out, vec_out,
                       w_q, w_k, w_v, d_in, dq_part, dk_sum, dv_sum, give, take, final, sem,
                       in_send, in_recv, swap_send, swap_recv, dn_send, dn_recv):
    seqs, block, _ = d_ctx.shape
    count = plan.nseq
    full = count * block
    team = Team(plan, seqs)
    copies = []
    for i, (name, target) in enumerate((("w_q", w_q), ("w_k", w_k), ("w_v", w_v))):
        copies.append(half_copy(packed, plan, name, team, target, sem.at[i]))
    yield
    c, z = team.c, team.z
    sends = []
    for s in range(seqs):
        for h in range(2):
            to = c * seqs + s
            own = jnp.logical_and(to == z, c == h)
            source = d_ctx.at[s, :, pl.ds(h * (D // 2), D // 2)]
            copy = remote(source, d_in.at[z], in_send.at[2 * s + h], in_recv.at[z], (team.base + h, to))
            sends.append((jnp.logical_not(own), copy))
            pl.when(jnp.logical_not(own))(copy.start)

    @pl.when(team.main)
    def _():
        d_in[z] = d_ctx[team.slot, :, team.half]

    dk_sum[...] = jnp.zeros(dk_sum.shape, jnp.float32)
    dv_sum[...] = jnp.zeros(dv_sum.shape, jnp.float32)
    dt_out[...] = jnp.zeros(dt_out.shape, jnp.float32)
    vec_out[...] = jnp.zeros(vec_out.shape, jnp.float32)
    away = pl.ds(pl.multiple_of((1 - c) * (D // 2), D // 2), D // 2)
    for out in (dq_out, dk_out, dv_out):
        out[:, away] = jnp.zeros((full, D // 2), jnp.bfloat16)
    valid = lax.broadcasted_iota(jnp.int32, (1, full), 1) < length[pl.ds(team.slot, 1), :][:, 0:1]
    rows = (((0,), (0,)), ((), ()))
    inv = 1.0 / math.sqrt(HD)

    @pl.loop(0, count)
    def _(i):
        b = lax.rem(z + i, count)
        own = jnp.logical_and(b == z, team.main)
        copy = remote(d_in.at[b], d_in.at[b], in_send.at[0], in_recv.at[b], (team.di, z))
        pl.when(jnp.logical_not(own))(copy.wait_recv)
        at = pl.ds(pl.multiple_of(b * block, block), block)
        totals = []
        for h in range(H // 2):
            cols = slice(h * HD, (h + 1) * HD)
            q, k, v = q_all[at, cols], k_all[:, cols], v_all[:, cols]
            dctx = d_in[b, :, cols]
            line = tables[b, pl.ds(c * (H // 2) + h, 1), :]
            width = line.shape[1]
            scores = head_scores(q, k, line, valid)
            probs = jnp.exp(scores - lse_all[at, h : h + 1])
            d_probs = lax.dot_general(dctx, v, (((1,), (1,)), ((), ())), preferred_element_type=jnp.float32)
            delta = jnp.sum(probs * d_probs, -1, keepdims=True)
            d_scores = probs * (d_probs - delta)
            d_scores_b = d_scores.astype(jnp.bfloat16)
            dq = jnp.dot(d_scores_b, k, preferred_element_type=jnp.float32) * inv
            totals.append(total_rows(dq))
            dk_sum[:, cols] += lax.dot_general(d_scores_b, q, rows, preferred_element_type=jnp.float32)
            dv_sum[:, cols] += lax.dot_general(
                probs.astype(jnp.bfloat16), dctx, rows, preferred_element_type=jnp.float32
            )
            dq_part[at, cols] = dq.astype(jnp.bfloat16)
            wide = jnp.concatenate([d_scores, jnp.zeros((block, width - full), jnp.float32)], 1)
            folded = pltpu.roll(wide[0:8], block - 1, 1)
            for g in range(1, block // 8):
                folded = folded + pltpu.roll(wide[8 * g : 8 * g + 8], block - 1 - 8 * g, 1)
            line = folded[0:1]
            for r in range(1, 8):
                line = line + pltpu.roll(folded[r : r + 1], width - r, 1)
            dt_out[b, pl.ds(c * (H // 2) + h, 1), :] = line
        vec_out[0:1, team.half] += jnp.concatenate(totals, 1)

    vec_out[1:2, team.half] = total_rows(dv_sum[...])
    dk_part = (dk_sum[...] * inv).astype(jnp.bfloat16)
    dk_out[:, team.half] = dk_part
    dv_part = dv_sum[...].astype(jnp.bfloat16)
    dv_out[:, team.half] = dv_part
    dq_out[:, team.half] = dq_part[...]
    wait_all(*copies)

    def partial(b):
        at = pl.ds(pl.multiple_of(b * block, block), block)
        dk_rows, dv_rows = dk_out[at, team.half], dv_out[at, team.half]
        return back_dot(dq_part[at, :], w_q[...]) + back_dot(dk_rows, w_k[...]) + back_dot(dv_rows, w_v[...])

    share = count // 2
    swaps, ends = [], []
    for i in range(share):
        give[i] = partial((1 - c) * share + i).astype(jnp.bfloat16)
        copy = remote(give.at[i], take.at[i], swap_send.at[i], swap_recv.at[i], (team.other, z))
        copy.start()
        swaps.append(copy)
    for i in range(share):
        b = c * share + i
        value = partial(b)
        swaps[i].wait_recv()
        value = (value + take[i].astype(jnp.float32)).astype(jnp.bfloat16)
        final[i] = value
        own = jnp.logical_and(b == z, team.main)
        copy = remote(final.at[i], dn_out.at[team.slot], dn_send.at[i], dn_recv.at[team.slot], (team.owner, b))
        ends.append((jnp.logical_not(own), copy))
        pl.when(jnp.logical_not(own))(copy.start)

        @pl.when(own)
        def _():
            dn_out[team.slot] = final[i]

    for s in range(seqs):
        own = jnp.logical_and(c * seqs + s == z, z // share == c)
        copy = remote(final.at[0], dn_out.at[s], dn_send.at[0], dn_recv.at[s], (team.di, z))
        pl.when(jnp.logical_not(own))(copy.wait_recv)
    for copy in swaps:
        copy.wait_send()
    for flag, copy in sends + ends:
        pl.when(flag)(copy.wait_send)


VMEM_SPEC = pl.BlockSpec(memory_space=pltpu.VMEM)
ANY_SPEC = pl.BlockSpec(memory_space=pl.ANY)


def run_all(ready, runs, first):
    for run in runs:
        next(run)
    for number, run in enumerate(runs):
        if number == first:
            ready()
        for _ in run:
            pass


def forward_kernel(plan, r):
    ready = everyone(plan)
    runs = [
        ffn_first_kernel(plan, r.x, r.packed, r.x1, r.n2, r.w_first, r.w_in, r.w_second, r.g0, r.g1, r.g2, r.bias,
                         r.acc, r.one, r.mix, r.sem0),
        attend_kernel(plan, r.n2, r.lengths, r.tables, r.packed, r.ctx, r.owned, r.q, r.k, r.v, r.lse, r.length,
                      r.w_q, r.w_k, r.w_v, r.g3, r.g4, r.held, r.mine, r.sem1, r.sem2, r.sem3, r.sem4, r.sem5, r.sem6,
                      r.sem7),
        gate_kernel(plan, r.ctx, r.x1, r.valid, r.packed, r.x2, r.n3, r.gates, r.u, r.w_gate, r.w_o, r.w_pi,
                    r.g5, r.g6, r.mix, r.sem8),
        depth_kernel(plan, r.u, r.valid, r.packed, r.depth, r.sums, r.padded, r.taps, r.taps_b, r.part, r.line,
                     r.cross, r.sem9, r.sem10, r.sem11, r.sem12, r.sem13, r.sem14),
    ]
    run_all(ready, runs, 1)


def backward_kernel(plan, r):
    ready = everyone(plan)
    runs = [
        middle_kernel(plan, r.x2, r.depth, r.sums, r.cot, r.valid, r.packed, r.y, r.d3, r.dz, r.local, r.stats, r.e3,
                      r.r3, r.a4, r.h4, r.n4, r.dh4, r.vec_mid, r.w_po, r.w_in, r.w_second, r.w_mix, r.hid, r.g0,
                      r.g1, r.g2, r.g3, r.bias, r.acc, r.mix, r.sem0),
        depth_back_kernel(plan, r.dz, r.depth, r.stats, r.local, r.valid, r.padded, r.packed, r.du, r.tap, r.wide,
                          r.own, r.taps, r.taps_b, r.part, r.line, r.cross, r.sem1, r.sem2, r.sem3, r.sem4, r.sem5,
                          r.sem6),
        gate_back_kernel(plan, r.du, r.gates, r.x2, r.d3, r.valid, r.w_gate, r.packed, r.dg, r.d2, r.r2, r.dctx,
                         r.vec_gate, r.w_o, r.g4, r.sem7),
        attend_back_kernel(plan, r.dctx, r.q, r.k, r.v, r.lse, r.length, r.tables, r.packed, r.dn, r.dq, r.dk, r.dv,
                           r.dt, r.vec_att, r.w_q, r.w_k, r.w_v, r.d_in, r.dq_part, r.dk_sum, r.dv_sum, r.give, r.take,
                           r.final, r.sem8, r.sem9, r.sem10, r.sem11, r.sem12, r.sem13, r.sem14),
        ffn_first_back_kernel(plan, r.x, r.x1, r.d2, r.dn, r.w_first, r.packed, r.d0, r.a1, r.h1, r.n1, r.dh1,
                              r.vec_first, r.w_tall, r.g5, r.g6, r.g7, r.bias, r.acc, r.sem15),
    ]
    run_all(ready, runs, 1)


def stage(kernel, plan, operands, packed, outs, scratch, name, number):
    keys = list(operands) + ["packed"] + list(outs) + list(scratch)
    results = pl.pallas_call(
        lambda *refs: kernel(plan, types.SimpleNamespace(**dict(zip(keys, refs)))),
        out_shape=[jax.ShapeDtypeStruct(shape, dtype) for shape, dtype in outs.values()],
        in_specs=[VMEM_SPEC] * len(operands) + [ANY_SPEC],
        out_specs=[VMEM_SPEC] * len(outs),
        scratch_shapes=list(scratch.values()),
        compiler_params=pltpu.CompilerParams(
            vmem_limit_bytes=67043328, collective_id=number, has_side_effects=True
        ),
        name=name,
    )(*operands.values(), packed)
    return types.SimpleNamespace(**dict(zip(outs, results)))


F32, BF16 = jnp.float32, jnp.bfloat16
DMA = pltpu.SemaphoreType.DMA


def vm(shape, dtype=jnp.bfloat16):
    return pltpu.VMEM(shape, dtype)


def per_device(inputs, lengths, rel_bucket, params, moment_one, moment_two, cotangent):
    seq_count, block_len, model_width = inputs.shape
    rows = seq_count * block_len
    first_pos = lax.axis_index(SEQ) * block_len
    positions = first_pos + jnp.arange(block_len, dtype=jnp.int32)
    valid_own = positions[None, :] < lengths[:, None]
    valid = valid_own.astype(jnp.float32).reshape(-1, 1)
    onehot = bucket_windows(rel_bucket, block_len, lax.axis_size(SEQ))
    assert 2 * seq_count == lax.axis_size(SEQ)
    length = jnp.broadcast_to(jnp.pad(lengths, (0, 8 - seq_count))[:, None], (8, 128))
    plan = Plan(lax.axis_size(DP), lax.axis_size(SEQ), params.shape[0])
    packed = gather(plan, params).reshape(-1, LANES)
    full, wide, nseq = (rows, D), (rows, FF), plan.nseq
    square, tall, group = vm((D, D)), vm((FF, D)), vm((8, D))
    mix, taps, taps_b = vm((LANES // 128, 256, 128), F32), vm((40, D), F32), vm((40, D))
    half, sums = vm((D, D // 2)), ((4, D), F32)
    long, whole = nseq * block_len, (nseq * block_len, D)
    local3, split = (seq_count, block_len, D), (nseq, block_len, D // 2)
    padded = (seq_count, block_len + 2 * HALO, D)
    few = vm((nseq // 2, block_len, D))
    x = inputs.reshape(full)
    table_row = plan.places["rel"]
    rel = packed[table_row : table_row + 1, : NB * H].reshape(NB, H)
    tables = jnp.einsum("nh,bnw->bhw", rel, onehot.astype(BF16), preferred_element_type=F32)
    f = stage(
        forward_kernel, plan, dict(x=x, valid=valid, lengths=length, tables=tables), packed,
        dict(x1=(full, F32), w_first=((FF // D, D, D), BF16), ctx=(local3, BF16), owned=((nseq, block_len, D), BF16),
             q=((long, D // 2), BF16), k=((long, D // 2), BF16), v=((long, D // 2), BF16), lse=((long, 128), F32),
             length=((8, 128), jnp.int32), x2=(full, F32), n3=(full, BF16), gates=((rows, 2 * D), F32),
             w_gate=((2, D, D), BF16), depth=(full, F32), sums=sums, padded=(padded, F32)),
        dict(n2=vm(local3), w_in=tall, w_second=tall, g0=group, g1=group, g2=group, g3=group, g4=group, g5=group,
             g6=group, bias=vm((8, D), F32), acc=vm(full, F32), one=vm(full), mix=mix, w_q=half, w_k=half, w_v=half,
             held=vm(split), mine=vm((2, 8, D), F32), u=vm(full, F32), w_o=square, w_pi=vm((2 * D, D)), taps=taps,
             taps_b=taps_b, part=vm(*sums), line=vm((nseq, 4, D), F32), cross=vm((plan.ndp, 4, D), F32),
             sem0=DMA((5,)), sem1=DMA((5,)), sem2=DMA((seq_count,)), sem3=DMA((nseq,)), sem4=DMA((nseq,)),
             sem5=DMA((nseq,)), sem6=DMA((2 * seq_count,)), sem7=DMA((2,)), sem8=DMA((4,)), sem9=DMA((1,)),
             sem10=DMA((4,)), sem11=DMA((nseq,)), sem12=DMA((nseq,)), sem13=DMA((plan.ndp,)),
             sem14=DMA((plan.ndp,))), "forward", 2,
    )
    b = stage(
        backward_kernel, plan,
        dict(x=x, valid=valid, cot=cotangent.reshape(full), tables=tables, x1=f.x1, x2=f.x2, depth=f.depth,
             sums=f.sums, padded=f.padded, gates=f.gates, w_gate=f.w_gate, q=f.q, k=f.k, v=f.v, lse=f.lse,
             length=f.length, w_first=f.w_first), packed,
        dict(y=(full, F32), d0=(full, F32), e3=(full, BF16), r3=(full, BF16), a4=(wide, BF16), h4=(full, BF16),
             n4=(full, BF16), dh4=(wide, BF16), vec_mid=((16, D), F32), tap=((32, D), F32), dg=((rows, 2 * D), BF16),
             r2=(full, BF16), vec_gate=((8, D), F32), dq=(whole, BF16), dk=(whole, BF16), dv=(whole, BF16),
             dt=(tables.shape, F32), vec_att=((8, D), F32), a1=(wide, BF16), h1=(full, BF16), n1=(full, BF16),
             dh1=(wide, BF16), vec_first=((16, D), F32)),
        dict(d3=vm(full, F32), dz=vm(full, F32), local=vm(*sums), stats=vm(*sums), w_po=square, w_in=tall,
             w_second=tall, w_mix=vm((FF // D, D, D)), hid=vm((FF // D, rows, D), F32), g0=vm((40, D)), g1=group,
             g2=group, g3=group, g4=group, g5=group, g6=group, g7=group, bias=vm((8, D), F32), acc=vm(full, F32),
             mix=mix, du=vm(full, F32), wide=vm(padded, F32), own=vm((seq_count, block_len + 16, D), F32), taps=taps,
             taps_b=taps_b, part=vm(*sums), line=vm((nseq, 4, D), F32), cross=vm((plan.ndp, 4, D), F32),
             d2=vm(full, F32), dctx=vm(local3), w_o=square, dn=vm(local3), w_q=half, w_k=half, w_v=half,
             d_in=vm(split), dq_part=vm((long, D // 2)), dk_sum=vm((long, D // 2), F32),
             dv_sum=vm((long, D // 2), F32), give=few, take=few, final=few, w_tall=tall, sem0=DMA((7,)),
             sem1=DMA((1,)), sem2=DMA((4,)), sem3=DMA((nseq,)), sem4=DMA((nseq,)), sem5=DMA((plan.ndp,)),
             sem6=DMA((plan.ndp,)), sem7=DMA((2,)), sem8=DMA((3,)), sem9=DMA((2 * seq_count,)), sem10=DMA((nseq,)),
             sem11=DMA((nseq // 2,)), sem12=DMA((nseq // 2,)), sem13=DMA((nseq // 2,)), sem14=DMA((seq_count,)),
             sem15=DMA((4,))), "backward", 3,
    )
    rel_grad = jnp.einsum("bnw,bhw->nh", onehot, b.dt, precision=lax.Precision.HIGHEST).reshape(1, -1)
    owned = f.owned.reshape(whole)
    gradients = {
        "w_k": (owned, b.dk), "w_v": (owned, b.dv), "w_q": (owned, b.dq), "second_w_in": (b.n4, b.dh4),
        "second_w_out": (b.a4, b.h4), "w_pi": (f.n3, b.dg), "w_po": (b.e3, b.r3), "w_o": (f.ctx.reshape(full), b.r2),
        "first_w_in": (b.n1, b.dh1), "first_w_out": (b.a1, b.h1),
    }
    places = {
        "attn_ng": (0, 0), "attn_nb": (0, 1), "first_b_out": (0, 2), "first_ng": (0, 3), "first_nb": (0, 4),
        "first_b_in": (0, 5), "b_pi": (1, 0), "conv_ng": (1, 2), "conv_nb": (1, 3), "b_o": (1, 4),
        "fin_g": (2, 0), "fin_b": (2, 1), "second_b_out": (2, 2), "second_ng": (2, 3), "second_nb": (2, 4),
        "b_po": (2, 5), "bng": (2, 6), "bnb": (2, 7), "second_b_in": (2, 8), "w_depth": (3, 0),
        "b_q": (4, 0), "b_v": (4, 1), "rel": (5, 0),
    }
    vectors = [b.vec_first, b.vec_gate, b.vec_mid, b.tap, b.vec_att, rel_grad]
    window = scatter(plan, weight_grads(plan, gradients, vectors, places))
    grad_shard = own_shard(plan, window)
    new_params, new_first, new_second = adam_update(params, grad_shard, moment_one, moment_two)
    return (
        b.y.reshape(inputs.shape),
        b.d0.reshape(inputs.shape),
        grad_shard,
        new_params,
        new_first,
        new_second,
    )


def solution(mesh):
    return jax.shard_map(
        per_device,
        mesh=mesh,
        in_specs=(
            P(DP, SEQ, None),
            P(DP),
            P(),
            P((DP, SEQ)),
            P((DP, SEQ)),
            P((DP, SEQ)),
            P(DP, SEQ, None),
        ),
        out_specs=(
            P(DP, SEQ, None),
            P(DP, SEQ, None),
            P((DP, SEQ)),
            P((DP, SEQ)),
            P((DP, SEQ)),
            P((DP, SEQ)),
        ),
        check_vma=False,
    )
```

```python
import functools
import math
import types

import jax
import jax.numpy as jnp
from jax import lax
from jax.experimental import pallas as pl
from jax.experimental.pallas import tpu as pltpu
from jax.sharding import PartitionSpec as P

D = 512
H = 8
HD = 64
FF = 2048
K = 31
NB = 32
DP = "dp"
SEQ = "seq"
STEP = 4


NORM_EPS = 1e-05
BATCH_EPS = 1e-05
LEARN_RATE = 0.005
DECAY = 0.01
BETA_ONE = 0.9
BETA_TWO = 0.98
ADAM_EPS = 1e-08


def segments():

    def feed_block(prefix):
        return [
            (prefix + "_ng", (D,)),
            (prefix + "_nb", (D,)),
            (prefix + "_w_in", (D, FF)),
            (prefix + "_b_in", (FF,)),
            (prefix + "_w_out", (FF, D)),
            (prefix + "_b_out", (D,)),
        ]

    listing = feed_block("first")
    listing = listing + [
        ("attn_ng", (D,)),
        ("attn_nb", (D,)),
        ("w_q", (D, D)),
        ("b_q", (D,)),
        ("w_k", (D, D)),
        ("w_v", (D, D)),
        ("b_v", (D,)),
        ("w_o", (D, D)),
        ("b_o", (D,)),
        ("rel", (NB, H)),
    ]
    listing = listing + [
        ("conv_ng", (D,)),
        ("conv_nb", (D,)),
        ("w_pi", (D, 2 * D)),
        ("b_pi", (2 * D,)),
        ("w_depth", (K, D)),
        ("bng", (D,)),
        ("bnb", (D,)),
        ("w_po", (D, D)),
        ("b_po", (D,)),
    ]
    listing = listing + feed_block("second") + [("fin_g", (D,)), ("fin_b", (D,))]
    return listing


def arrange():
    places, gaps = {}, []
    linear = inner = 0
    for entry_name, entry_shape in segments():
        extent = math.prod(entry_shape)
        tail = 2 * D if entry_name == "conv_ng" else 0
        if extent >= D * D or tail:
            pad = -(inner + tail) % TILE
            if pad:
                gaps.append((linear, pad))
                inner = inner + pad
        places[entry_name] = inner // LANES
        linear, inner = linear + extent, inner + extent
    return places, gaps, -(-inner // TILE)


def device_index():
    return lax.axis_index(DP) * lax.axis_size(SEQ) + lax.axis_index(SEQ)


def own_shard(plan, window):
    table = jnp.asarray(plan.shard_table, jnp.int32)[device_index()]
    flat = window.reshape(-1)
    early = lax.dynamic_slice(flat, (table[0],), (plan.shard,))
    late = lax.dynamic_slice(flat, (table[0] + table[2],), (plan.shard,))
    return jnp.where(jnp.arange(plan.shard, dtype=jnp.int32) < table[1], early, late)


def swish_act(values):
    return values * jax.nn.sigmoid(values)


def swish_grad(values):
    sig_vals = jax.nn.sigmoid(values)
    return sig_vals * (1.0 + values * (1.0 - sig_vals))


def forward_dot(left_mat, weight):
    return jnp.dot(left_mat, weight, preferred_element_type=jnp.float32)


def back_dot(grad_in, weight):
    return lax.dot_general(
        grad_in, weight, (((1,), (1,)), ((), ())), preferred_element_type=jnp.float32
    )


MESH = pl.DeviceIdType.MESH
LANES=512
TILE=8*LANES

class Plan:
    def __init__(self, ndp, nseq, shard):
        self.ndp, self.nseq, self.shard = ndp, nseq, shard
        self.k = ndp.bit_length() - 1
        self.phases = self.k - 1
        self.n = n = ndp * nseq
        self.places, self.gaps, self.total = arrange()
        begins = [self.inner(d * shard) for d in range(n)]
        starts = [-(-b // TILE) for b in begins] + [self.total]
        sizes = [b - a for a, b in zip(starts, starts[1:])]
        self.lo, self.hi = min(sizes), max(sizes)
        self.slots = nseq * 2**self.phases
        floors = [b // TILE for b in begins]
        ends = [self.inner((d + 1) * shard - 1) // TILE + 1 for d in range(n)]
        self.win = max(e - f for e, f in zip(ends, floors))
        self.win += self.win % 2
        self.padded = max(self.total, max(floors) + self.win)
        self.block_table, self.shard_table = [], []
        for d in range(n):
            near = [g for g in self.gaps if d * shard < g[0] < (d + 1) * shard + TILE]
            assert len(near) <= 1
            cut, size = near[0] if near else (2**30, 0)
            lead = starts[d] * TILE - begins[d]
            self.block_table.append((lead, cut - d * shard - lead, size))
            self.shard_table.append((begins[d] - floors[d] * TILE, cut - d * shard, size))

    def inner(self, position):
        if isinstance(position, int):
            return position + sum(size for at, size in self.gaps if at <= position)
        result = position
        for at, size in self.gaps:
            result = result + jnp.where(position >= at, size, 0)
        return result

    def order(self):
        ev=[]
        for s in range(self.nseq):
            for sign in ((0,) if s==0 else (-1,1)):
                for t in range(2**self.phases):
                    ev.append((s+0.5*bin(t).count("1")+0.01*t, s, sign, t))
        ev.sort()
        return [e[1:] for e in ev]

def flip(di, mask_bits, bits, t, phases):
    out=di
    for p in range(phases):
        if (t>>p)&1:
            out = out + mask_bits[p]*(1-2*bits[p])
    return out

def phase_masks(di, c, phases):
    masks, bits=[],[]
    for p in range(phases):
        a, b = 1<<(p+1), 1<<(phases-p)
        masks.append(a+c*(b-a))
        ba, bb = (di//a)%2, (di//b)%2
        bits.append(ba+c*(bb-ba))
    return masks, bits

def block_of(plan, dpi, z):
    d = dpi*plan.nseq+z
    a = (plan.inner(d*plan.shard)+TILE-1)//TILE
    b = (plan.inner((d+1)*plan.shard)+TILE-1)//TILE
    b = jnp.where(d == plan.n-1, plan.total, b)
    return a, b-a

def floor_of(plan, dpi, z):
    return plan.inner((dpi*plan.nseq+z)*plan.shard)//TILE

FRONT, NEAR, BACK = 32, 40, 64


def shard_rows(plan):
    return -(-plan.shard // 1024) * 8


def place_rows(plan, rolled, block, first, rows, lead, cut, skip):
    shift, begin = lead % 128, FRONT + lead // 128
    lane = lax.broadcasted_iota(jnp.int32, (rows, 128), 1)
    at = (lax.broadcasted_iota(jnp.int32, (rows, 128), 0) + first) * LANES + lane
    for j in range(LANES // 128):

        def read(start):
            here = rolled[pl.ds(start, rows, stride=4), :]
            after = rolled[pl.ds(start + 1, rows, stride=4), :]
            return jnp.where(lane < 128 - shift, here, after)

        start = begin + j + 4 * first
        value = jnp.where(at + 128 * j < cut, read(start), read(start - skip)).astype(block.dtype)
        part = slice(first // 8, (first + rows) // 8)
        block[part, :, j * 128 : (j + 1) * 128] = value.reshape(rows // 8, 8, 128)


def gather_kernel(plan, x, out, src, line, rolled, give, take, near_sem, send_a, recv_a, loc_sem):
    di, z = lax.axis_index(DP), lax.axis_index(SEQ)
    ns, ph = plan.nseq, plan.phases
    c = di%2
    masks, bits = phase_masks(di, c, ph)
    other = di+1-2*c
    omasks, obits = phase_masks(other, 1-c, ph)
    up, down = lax.rem(z+1,ns), lax.rem(z+ns-1,ns)
    partners=[(di,up),(di,down),(other,z)]+[(flip(di,masks,bits,1<<p,ph),z) for p in range(ph)]
    barrier=pltpu.get_barrier_semaphore()
    for a,b in partners:
        pl.semaphore_signal(barrier,inc=1,device_id=(a,b),device_id_type=MESH)
    index = di * ns + z
    following, before = lax.rem(index + 1, plan.n), lax.rem(index + plan.n - 1, plan.n)
    pl.semaphore_signal(barrier, inc=1, device_id=(following // ns, lax.rem(following, ns)), device_id_type=MESH)
    lo, more = plan.lo-1, plan.hi-plan.lo+1
    start_own, size_own = block_of(plan, di, z)
    rows = x.shape[0]
    joint, shift = divmod(plan.shard, 128)
    lane = lax.broadcasted_iota(jnp.int32, (NEAR, 128), 1)
    moved = pltpu.roll(x[:NEAR], shift, 1)
    earlier = jnp.concatenate([jnp.zeros((1, 128), jnp.float32), moved[: NEAR - 1]], 0)
    give[...] = jnp.where(lane >= shift, moved, earlier)
    line[:FRONT] = jnp.zeros((FRONT, 128), jnp.float32)
    line[FRONT : FRONT + rows] = x[...]
    line[FRONT + rows :] = jnp.zeros((line.shape[0] - FRONT - rows, 128), jnp.float32)
    begin = index * plan.shard
    inner = plan.inner(begin)
    lead = (inner + TILE - 1) // TILE * TILE - inner
    cut, skip = 2**30, 0
    for position, size in plan.gaps:
        hit = jnp.logical_and(position > begin, position < begin + plan.shard + TILE)
        cut = jnp.where(hit, position - begin - lead, cut)
        skip = jnp.where(hit, size // 128, skip)
    turn = lax.rem(128 - lead % 128, 128)
    rolled[...] = pltpu.roll(line[...], turn, 1)
    place_rows(plan, rolled, src, 0, 8 * lo, lead, cut, skip)
    pl.semaphore_wait(barrier,len(partners)+1)
    near = pltpu.make_async_remote_copy(src_ref=give,dst_ref=take,send_sem=near_sem.at[0],recv_sem=near_sem.at[1],
        device_id=(before // ns, lax.rem(before, ns)),device_id_type=MESH)
    near.start()

    pieces = gather_pieces(plan)
    number = sum(len(p) for p in pieces)
    last = len(pieces) - 1
    used = [0]

    def pair(kind, ref, base, target, size, ridx, dev, fresh):
        copies = []
        for x, (at, tiles) in enumerate(pieces[kind]):
            copies.append(pltpu.make_async_remote_copy(
                src_ref=ref.at[pl.ds(base + at, tiles)], dst_ref=out.at[pl.ds(target + at, tiles)],
                send_sem=send_a.at[used[0] if fresh else 0], recv_sem=recv_a.at[ridx * number + kind + x],
                device_id=dev, device_id_type=MESH))
            used[0] += fresh
        return copies, size

    def each(p, act, part=None):
        for x, copy in enumerate(p[0]):
            if part is not None and (x == 0) != (part == 0):
                continue
            if x < 2:
                act(copy)
            else:
                pl.when(p[1] >= lo + x)(functools.partial(act, copy))

    def guard(conds, fn):
        if not conds:
            fn()
            return
        cond = conds[0]
        for x in conds[1:]:
            cond = jnp.logical_and(cond, x)
        pl.when(cond)(fn)

    own = []
    for at, tiles in sum(pieces, []):
        own.append(pltpu.make_async_copy(src.at[pl.ds(at, tiles)], out.at[pl.ds(start_own + at, tiles)],
                                         loc_sem.at[len(own)]))

    def mine_each(act, part):
        for x, copy in enumerate(own):
            if (x <= last) != (part == 0):
                continue
            if x <= last + 1:
                act(copy)
            else:
                pl.when(size_own >= lo + x - last)(functools.partial(act, copy))

    mine_each(lambda c: c.start(), 0)

    def finish_block():
        near.wait_recv()
        at = FRONT + joint
        line[at : at + 1] = line[at : at + 1] + take[0:1]
        line[at + 1 : at + NEAR] = take[1:]
        low = at // 8 * 8
        rolled[low:] = pltpu.roll(line[low:], turn, 1)
        place_rows(plan, rolled, src, 8 * lo, 8 * more, lead, cut, skip)
        mine_each(lambda c: c.start(), 1)

    nslot = plan.slots
    sends, tasks = [], []
    events = [(s + 0.5 * bin(t).count("1") + ROUTES[kind][2], kind, s, sign, t)
              for kind in range(len(pieces)) for s, sign, t in plan.order()]
    events.sort()
    blocks = {}
    for s, sign, t in plan.order():
        zz = z + sign * s
        blocks[s, sign, t] = (block_of(plan, flip(di, masks, bits, t, ph), zz),
                              block_of(plan, flip(other, omasks, obits, t, ph), zz))
    for _, kind, s, sign, t in events:
        zz = z + sign * s
        conds = [] if s == 0 else ([zz >= 0] if sign < 0 else [zz < ns])
        st, size = blocks[s, sign, t][0]
        mine = s == 0 and t == 0
        ref, base = (src, 0) if mine else (out, st)
        slot = t * ns + zz
        got = None if mine else pair(kind, out, st, st, size, slot, (di, z), 0)
        copies = []

        def forward(conds, ridx, dev):
            p = pair(kind, ref, base, st, size, ridx, dev, 1)
            sends.append((conds, p))
            copies.append((conds, p))

        plane = ROUTES[kind][1]
        if t == 0 or plane:
            if sign <= 0:
                forward(conds + [z < ns - 1], slot, (di, lax.rem(z + 1, ns)))
            if sign >= 0:
                forward(conds + [z > 0], slot, (di, lax.rem(z + ns - 1, ns)))
        if s == 0 or not plane:
            for pp in range(t.bit_length(), ph):
                forward(conds, slot + (1 << pp) * ns, (flip(di, masks, bits, 1 << pp, ph), z))
        forward(conds, nslot + slot, (other, z))
        tasks.append((kind, conds, got, copies))

    def run(task, part):
        kind, conds, got, copies = task
        if part and kind != last:
            return
        if got is None:
            if part:
                finish_block()
        else:
            guard(conds, lambda: each(got, lambda c: c.wait_recv(), part))
        for also, p in copies:
            guard(also, lambda: each(p, lambda c: c.start(), part))

    lag = 8
    for i in range(len(tasks) + lag):
        if i < len(tasks):
            run(tasks[i], 0)
        if i >= lag:
            run(tasks[i - lag], 1)
    for _, kind, s, sign, t in events:
        zz = z + sign * s
        conds = [] if s == 0 else ([zz >= 0] if sign < 0 else [zz < ns])
        st, size = blocks[s, sign, t][1]
        p = pair(kind, out, st, st, size, nslot + t * ns + zz, (di, z), 0)
        guard(conds, lambda: each(p, lambda c: c.wait_recv()))
    for conds, p in sends:
        guard(conds, lambda: each(p, lambda c: c.wait_send()))
    for part in range(2):
        mine_each(lambda c: c.wait(), part)
    near.wait_send()


ROUTES = ((0.39, 0, 0.0), (0.39, 0, 0.3), (0.22, 1, 0.6))


def gather_pieces(plan):
    lo, more = plan.lo - 1, plan.hi - plan.lo + 1
    pieces, at, share = [], 0, 0.0
    for part, _, _ in ROUTES:
        share += part
        until = lo if len(pieces) == len(ROUTES) - 1 else round(share * plan.lo)
        pieces.append([(at, until - at)])
        at = until
    pieces[-1] += [(lo + x, 1) for x in range(more)]
    return pieces


def count_sends(plan):
    pieces = gather_pieces(plan)
    total = 0
    for kind, (_, plane, _) in enumerate(ROUTES):
        for s, sign, t in plan.order():
            along = (2 if s == 0 else 1) if t == 0 or plane else 0
            across = plan.phases - t.bit_length() if s == 0 or not plane else 0
            total += (along + across + 1) * len(pieces[kind])
    return total


def gather(plan, params):
    ns, more = count_sends(plan), plan.hi - plan.lo + 1
    rows = shard_rows(plan)
    lines = FRONT + rows + NEAR + BACK
    lines += -lines % 8
    values = jnp.pad(params, (0, rows * 128 - plan.shard)).reshape(rows, 128)
    return pl.pallas_call(
        functools.partial(gather_kernel, plan),
        out_shape=jax.ShapeDtypeStruct((plan.total, 8, LANES), jnp.bfloat16),
        in_specs=[pl.BlockSpec(memory_space=pltpu.VMEM)],
        out_specs=pl.BlockSpec(memory_space=pl.ANY),
        scratch_shapes=[
            pltpu.VMEM((plan.hi, 8, LANES), jnp.bfloat16), pltpu.VMEM((lines, 128), jnp.float32),
            pltpu.VMEM((lines, 128), jnp.float32), pltpu.VMEM((NEAR, 128), jnp.float32),
            pltpu.VMEM((NEAR, 128), jnp.float32), pltpu.SemaphoreType.DMA((2,)),
            pltpu.SemaphoreType.DMA((ns,)), pltpu.SemaphoreType.DMA((2 * plan.slots * (len(ROUTES) + more),)),
            pltpu.SemaphoreType.DMA((len(ROUTES) + more,)),
        ],
        compiler_params=pltpu.CompilerParams(collective_id=0, has_side_effects=True),
        name="gather_params",
    )(values)


def scatter_pieces(plan):
    pieces, at, share = [], 0, 0.0
    for number, (part, _, _) in enumerate(ROUTES):
        share += part
        until = plan.win if number == len(ROUTES) - 1 else round(share * plan.win / 2) * 2
        pieces.append((at, until - at))
        at = until
    return pieces


def scatter_kernel(plan, g, out, acc, rc, *refs):
    kinds = len(ROUTES)
    pieces = scatter_pieces(plan)
    rps, rzs = refs[:kinds], refs[kinds : 2 * kinds]
    load_sem, send_sem, core_send, core_recv, ph_recv, z_recv = refs[2 * kinds :]
    di, z = lax.axis_index(DP), lax.axis_index(SEQ)
    ns, ph, nslot = plan.nseq, plan.phases, plan.slots
    c = di % 2
    masks, bits = phase_masks(di, c, ph)
    other = di + 1 - 2 * c
    omasks, obits = phase_masks(other, 1 - c, ph)
    up, down = lax.rem(z + 1, ns), lax.rem(z + ns - 1, ns)
    partners = [(di, up), (di, down), (other, z)] + [(flip(di, masks, bits, 1 << p, ph), z) for p in range(ph)]
    barrier = pltpu.get_barrier_semaphore()
    for partner in partners:
        pl.semaphore_signal(barrier, inc=1, device_id=partner, device_id_type=MESH)
    order = [(s + 0.5 * bin(t).count("1") + ROUTES[kind][2], kind, s, sign, t)
             for kind in range(kinds) for s, sign, t in plan.order()]
    order = [event[1:] for event in sorted(order, reverse=True)]

    def guard(conds, fn):
        if not conds:
            fn()
            return
        cond = conds[0]
        for x in conds[1:]:
            cond = jnp.logical_and(cond, x)
        pl.when(cond)(fn)

    def where(kind, s, sign, t):
        zz = z + sign * s
        conds = [] if s == 0 else ([zz >= 0] if sign < 0 else [zz < ns])
        return zz, conds, t * ns + zz

    begins = {}
    for s, sign, t in plan.order():
        zz = z + sign * s
        begins[s, sign, t] = (floor_of(plan, flip(di, masks, bits, t, ph), zz),
                              floor_of(plan, flip(other, omasks, obits, t, ph), zz))

    def load(kind, s, sign, t):
        zz, conds, slot = where(kind, s, sign, t)
        at, tiles = pieces[kind]
        first = begins[s, sign, t][0] + at
        return conds, pltpu.make_async_copy(
            g.at[pl.ds(first, tiles)], acc.at[slot, pl.ds(at, tiles)], load_sem.at[kind * nslot + slot])

    def core(kind, s, sign, t):
        zz, conds, slot = where(kind, s, sign, t)
        at, tiles = pieces[kind]
        first = begins[s, sign, t][1] + at
        return conds, pltpu.make_async_remote_copy(
            src_ref=g.at[pl.ds(first, tiles)], dst_ref=rc.at[slot, pl.ds(at, tiles)],
            send_sem=core_send.at[kind * nslot + slot], recv_sem=core_recv.at[kind * nslot + slot],
            device_id=(other, z), device_id_type=MESH)

    for event in order:
        conds, copy = load(*event)
        guard(conds, copy.start)
    pl.semaphore_wait(barrier, len(partners))
    for event in order:
        conds, copy = core(*event)
        guard(conds, copy.start)
    sends = []

    def send(conds, source, target, recv, device):
        copy = pltpu.make_async_remote_copy(
            src_ref=source, dst_ref=target, send_sem=send_sem.at[len(sends)], recv_sem=recv,
            device_id=device, device_id_type=MESH)
        sends.append((conds, copy))
        guard(conds, copy.start)

    def waiting(target, recv):
        pltpu.make_async_remote_copy(
            src_ref=target, dst_ref=target, send_sem=send_sem.at[0], recv_sem=recv,
            device_id=(di, z), device_id_type=MESH).wait_recv()

    for event in order:
        kind, s, sign, t = event
        zz, conds, slot = where(*event)
        at, tiles = pieces[kind]
        plane, rp, rz = ROUTES[kind][1], rps[kind], rzs[kind]
        final = s == 0 and t == 0
        high = t.bit_length()

        def combine():
            part = acc.at[slot, pl.ds(at, tiles)]
            pltpu.make_async_copy(g.at[pl.ds(0, tiles)], part, load_sem.at[kind * nslot + slot]).wait()
            waiting(rc.at[slot, pl.ds(at, tiles)], core_recv.at[kind * nslot + slot])
            sources = []
            if s == 0 or not plane:
                for pp in range(high, ph):
                    entry = ((1 << pp) - 1) * ns + slot
                    waiting(rp.at[entry], ph_recv.at[kind * nslot + entry])
                    sources.append(entry)

            @pl.loop(0, tiles // 2)
            def _(i):
                here, there = pl.ds(at + i * 2, 2), pl.ds(i * 2, 2)
                value = acc[slot, here].astype(jnp.float32) + rc[slot, here].astype(jnp.float32)
                for entry in sources:
                    value = value + rp[entry, there].astype(jnp.float32)
                if final:
                    out[here] = value
                else:
                    acc[slot, here] = value.astype(acc.dtype)

        guard(conds, combine)

        def along(stream, extra):
            entry = (t * 2 + stream) * ns + zz

            def merge():
                waiting(rz.at[entry], z_recv.at[kind * 2 * nslot + entry])

                @pl.loop(0, tiles // 2)
                def _(i):
                    here, there = pl.ds(at + i * 2, 2), pl.ds(i * 2, 2)
                    if final:
                        out[here] = out[here] + rz[entry, there].astype(jnp.float32)
                    else:
                        value = acc[slot, here].astype(jnp.float32) + rz[entry, there].astype(jnp.float32)
                        acc[slot, here] = value.astype(acc.dtype)

            guard(conds + extra, merge)

        chained = t == 0 or plane
        if chained:
            if sign >= 0:
                along(0, [z > 0])
            if sign <= 0:
                along(1, [z < ns - 1])
        source = acc.at[slot, pl.ds(at, tiles)]
        if chained and s:
            stream = 0 if sign > 0 else 1
            entry = (t * 2 + stream) * ns + zz
            send(conds, source, rz.at[entry], z_recv.at[kind * 2 * nslot + entry], (di, up if sign > 0 else down))
        elif t:
            pp = high - 1
            entry = ((1 << pp) - 1) * ns + slot - (1 << pp) * ns
            send(conds, source, rp.at[entry], ph_recv.at[kind * nslot + entry],
                 (flip(di, masks, bits, 1 << pp, ph), z))
    for event in order:
        conds, copy = core(*event)
        guard(conds, copy.wait_send)
    for conds, copy in sends:
        guard(conds, copy.wait_send)


def scatter(plan, g):
    win, nslot, kinds = plan.win, plan.slots, len(ROUTES)
    buffers = []
    for at, tiles in scatter_pieces(plan):
        buffers.append(pltpu.VMEM(((2**plan.phases - 1) * plan.nseq, tiles, 8, LANES), g.dtype))
    for (_, plane, _), (at, tiles) in zip(ROUTES, scatter_pieces(plan)):
        buffers.append(pltpu.VMEM((2 * nslot if plane else 2 * plan.nseq, tiles, 8, LANES), g.dtype))
    counts = (kinds * nslot, kinds * len(plan.order()), kinds * nslot, kinds * nslot, kinds * nslot, kinds * 2 * nslot)
    return pl.pallas_call(
        functools.partial(scatter_kernel, plan),
        out_shape=jax.ShapeDtypeStruct((win, 8, LANES), jnp.float32),
        in_specs=[pl.BlockSpec(memory_space=pl.ANY)],
        out_specs=pl.BlockSpec(memory_space=pltpu.VMEM),
        scratch_shapes=[pltpu.VMEM((nslot, win, 8, LANES), g.dtype), pltpu.VMEM((nslot, win, 8, LANES), g.dtype)]
        + buffers + [pltpu.SemaphoreType.DMA((count,)) for count in counts],
        compiler_params=pltpu.CompilerParams(
            collective_id=1, has_side_effects=True, vmem_limit_bytes=48 * 1024 * 1024
        ),
        name="scatter_grads",
    )(g)


def weight_kernel(plan, names, places, *refs):
    count = 2 * len(names)
    sources, refs = refs[:count], refs[count:]
    vectors, refs = refs[: len(refs) - count - 4], refs[len(refs) - count - 4 :]
    target, stores, (out, mix, sem) = refs[0], refs[1 : count + 1], refs[count + 1 :]
    loads = []
    for i in range(count):
        loads.append(pltpu.make_async_copy(sources[i], stores[i], sem.at[i]))
        loads[i].start()
    rows = (((0,), (0,)), ((), ()))
    sent = []

    def send(first, tiles):
        if tiles:
            part = pl.ds(first, tiles)
            copy = pltpu.make_async_copy(out.at[part], target.at[part], sem.at[count + len(sent)])
            copy.start()
            sent.append(copy)

    edge = 0
    for name, shape in segments():
        if math.prod(shape) < D * D:
            first = plan.places[name]
            array, begin = places[name]
            for r in range(-(-math.prod(shape) // LANES)):
                line = vectors[array][begin + r : begin + r + 1, :]
                tile, row = divmod(first + r, 8)
                out[tile, row : row + 1, : line.shape[1]] = line.astype(out.dtype)
    for name, shape in segments():
        if math.prod(shape) >= D * D:
            first = plan.places[name] // 8
            send(edge, first - edge)
            edge = first + math.prod(shape) // TILE
    send(edge, plan.total - edge)
    shapes = dict(segments())
    for number, name in enumerate(names):
        shape, first = shapes[name], plan.places[name]
        left, right = stores[2 * number], stores[2 * number + 1]
        wait_all(*loads[2 * number : 2 * number + 2])
        fold = shape[1] // LANES
        step = 256 if fold == 1 else 128

        @pl.loop(0, shape[0] // step)
        def _(i):
            part = left[:, pl.ds(pl.multiple_of(i * step, step), step)]
            value = lax.dot_general(part, right[...], rows, preferred_element_type=jnp.float32)
            if fold > 1:
                for j in range(fold):
                    for lane in range(LANES // 128):
                        at = j * LANES + lane * 128
                        mix[lane, pl.ds(j, step, stride=fold), :] = value[:, at : at + 128]
                value = jnp.concatenate([mix[lane, : step * fold] for lane in range(LANES // 128)], 1)
            tiles = step * fold // 8
            out[pl.ds(first // 8 + i * tiles, tiles)] = value.astype(out.dtype).reshape(tiles, 8, LANES)

        send(first // 8, math.prod(shape) // TILE)
    wait_all(*sent)


def weight_grads(plan, gradients, vectors, places):
    names = list(gradients)
    operands = [value for name in names for value in gradients[name]]
    return pl.pallas_call(
        functools.partial(weight_kernel, plan, names, places),
        out_shape=jax.ShapeDtypeStruct((plan.padded, 8, LANES), jnp.bfloat16),
        in_specs=[ANY_SPEC] * len(operands) + [VMEM_SPEC] * len(vectors),
        out_specs=ANY_SPEC,
        scratch_shapes=[vm(value.shape) for value in operands] + [
            vm((plan.padded, 8, LANES)), vm((LANES // 128, 512, 128), F32),
            DMA((len(operands) + len(segments()),)),
        ],
        compiler_params=pltpu.CompilerParams(vmem_limit_bytes=60 * 1024 * 1024),
        name="weight_grads",
    )(*operands, *vectors)


def bucket_windows(rel_bucket, block_len, count):
    width = -(-(block_len * (count + 1) - 1) // 128) * 128
    padded = jnp.concatenate([rel_bucket, jnp.full((width,), -1, jnp.int32)])
    windows = [padded[(count - 1 - b) * block_len :][:width] for b in range(count)]
    return (jnp.stack(windows)[:, None, :] == jnp.arange(NB, dtype=jnp.int32)[None, :, None]).astype(jnp.float32)


def adam_update(param_vec, grad_in, first_mom, second):
    new_first = BETA_ONE * first_mom + (1.0 - BETA_ONE) * grad_in
    new_second = BETA_TWO * second + (1.0 - BETA_TWO) * grad_in * grad_in
    corr_one = 1.0 - BETA_ONE**STEP
    corr_two = 1.0 - BETA_TWO**STEP
    step_size = new_first / corr_one / (jnp.sqrt(new_second / corr_two) + ADAM_EPS)
    return (param_vec - LEARN_RATE * (step_size + DECAY * param_vec), new_first, new_second)


def unit_rows(values):
    centre = values - jnp.mean(values, -1, keepdims=True)
    scale = lax.rsqrt(jnp.mean(centre * centre, -1, keepdims=True) + NORM_EPS)
    return centre * scale, scale


def unit_back(unit, scale, gain, grad):
    shifted = grad * gain
    first = jnp.mean(shifted, -1, keepdims=True)
    second = jnp.mean(shifted * unit, -1, keepdims=True)
    return scale * (shifted - first - unit * second), total_rows(grad * unit), total_rows(grad)


def total_rows(values):
    return jnp.sum(values, 0, keepdims=True)


def split_rows(source, mix, target, fold):
    block = mix.shape[1]
    lanes = LANES // 128

    @pl.loop(0, source.shape[0] // block)
    def _(i):
        part = source[pl.ds(pl.multiple_of(i * block, block), block), :].astype(jnp.float32)
        for lane in range(lanes):
            mix[lane] = part[:, lane * 128 : (lane + 1) * 128]
        for j in range(fold):
            rows = [mix[lane, pl.ds(j, block // fold, stride=fold), :] for lane in range(lanes)]
            at = pl.multiple_of(i * (block // fold), block // fold)
            target[j, pl.ds(at, block // fold), :] = jnp.concatenate(rows, 1).astype(target.dtype)


class Fetch:
    def __init__(self, plan, packed, sem):
        self.plan, self.packed, self.sem, self.count = plan, packed, sem, 0

    def __call__(self, name, target):
        row = self.plan.places[name] // 8 * 8
        copy = pltpu.make_async_copy(
            self.packed.at[pl.ds(row, target.shape[0])], target, self.sem.at[self.count]
        )
        self.count += 1
        copy.start()
        return copy


def column(j):
    return pl.ds(pl.multiple_of(j * LANES, LANES), LANES)


def wait_all(*copies):
    for copy in copies:
        copy.wait()


def ffn_first_kernel(plan, x, packed, x_out, n_out, w_out, w_in, w_second, v0, v1, v2, bias, acc, one, mix, sem):
    fetch = Fetch(plan, packed, sem)
    early = [fetch("first_ng", v0), fetch("first_b_in", v1), fetch("first_b_out", v2)]
    in_copy = fetch("first_w_in", w_in)
    late = [fetch("first_w_out", w_second)]
    yield
    wait_all(*early)
    gains, bias_in, tail = v0[...].astype(jnp.float32), v1[...].astype(jnp.float32), v2[...].astype(jnp.float32)
    stream = x[...]
    unit, _ = unit_rows(stream)
    normed = (unit * gains[0:1] + gains[1:2]).astype(jnp.bfloat16)
    in_copy.wait()
    split_rows(w_in, mix, w_out, FF // LANES)
    wait_all(*late)
    one[...] = normed
    bias[...] = bias_in
    acc[...] = jnp.zeros(acc.shape, jnp.float32)

    @pl.loop(0, FF // LANES)
    def _(j):
        hidden = forward_dot(one[...], w_out[j]) + bias[pl.ds(j, 1), :]
        active = swish_act(hidden).astype(jnp.bfloat16)
        acc[...] += forward_dot(active, w_second[column(j), :])

    stream = x[...] + 0.5 * (acc[...] + tail[0:1])
    x_out[...] = stream
    unit, _ = unit_rows(stream)
    normed = (unit * tail[1:2] + tail[2:3]).astype(jnp.bfloat16)
    n_out[...] = normed.reshape(n_out.shape)


def ffn_first_back_kernel(plan, x, x_one, d_two, d_norm_in, w_in, packed,
                          d_out, a_out, r_out, n_out, h_out, vec_out, w_second, v0, v1, v2, bias, acc, sem):
    fetch = Fetch(plan, packed, sem)
    early = [fetch("first_ng", v0), fetch("first_b_in", v1), fetch("first_b_out", v2)]
    late = fetch("first_w_out", w_second)
    yield
    wait_all(*early)
    gains, bias_in, tail = v0[...].astype(jnp.float32), v1[...].astype(jnp.float32), v2[...].astype(jnp.float32)
    unit, scale = unit_rows(x_one[...])
    d_normed = d_norm_in[...].astype(jnp.float32).reshape(-1, D)
    d_norm, gain_grad, shift_grad = unit_back(unit, scale, tail[1:2], d_normed)
    vec_out[0:1] = gain_grad
    vec_out[1:2] = shift_grad
    grad = d_two[...] + d_norm
    half = 0.5 * grad
    vec_out[2:3] = total_rows(half)
    half_b = half.astype(jnp.bfloat16)
    r_out[...] = half_b
    unit, scale = unit_rows(x[...])
    normed = (unit * gains[0:1] + gains[1:2]).astype(jnp.bfloat16)
    n_out[...] = normed
    late.wait()
    bias[...] = bias_in
    acc[...] = jnp.zeros(acc.shape, jnp.float32)
    d_out[...] = grad

    @pl.loop(0, FF // LANES)
    def _(j):
        cols = column(j)
        hidden = forward_dot(n_out[...], w_in[j]) + bias[pl.ds(j, 1), :]
        a_out[:, cols] = swish_act(hidden).astype(jnp.bfloat16)
        d_hidden = back_dot(r_out[...], w_second[cols, :]) * swish_grad(hidden)
        vec_out[pl.ds(5 + j, 1), :] = total_rows(d_hidden)
        d_hidden = d_hidden.astype(jnp.bfloat16)
        h_out[:, cols] = d_hidden
        acc[...] += back_dot(d_hidden, w_in[j])

    unit, scale = unit_rows(x[...])
    d_norm, gain_grad, shift_grad = unit_back(unit, scale, gains[0:1], acc[...])
    vec_out[3:4] = gain_grad
    vec_out[4:5] = shift_grad
    d_out[...] += d_norm


def gate_kernel(plan, ctx, x, valid, packed, x_out, n_out, g_out, u_out, w_out, w_o, w_pi, v0, v1, mix, sem):
    fetch = Fetch(plan, packed, sem)
    early = [fetch("w_o", w_o), fetch("b_o", v0), fetch("b_pi", v1)]
    late = fetch("w_pi", w_pi)
    yield
    wait_all(*early)
    rows, bias_in = v0[...].astype(jnp.float32), v1[...].astype(jnp.float32)
    stream = x[...] + forward_dot(ctx[...].reshape(-1, D), w_o[...]) + rows[0:1]
    x_out[...] = stream
    unit, _ = unit_rows(stream)
    normed = (unit * rows[6:7] + rows[7:8]).astype(jnp.bfloat16)
    n_out[...] = normed
    late.wait()
    split_rows(w_pi, mix, w_out, 2)
    linear = forward_dot(normed, w_out[0]) + bias_in[0:1]
    gate = forward_dot(normed, w_out[1]) + bias_in[1:2]
    g_out[:, :D] = linear
    g_out[:, D:] = gate
    u_out[...] = linear * jax.nn.sigmoid(gate) * valid[...]


def gate_back_kernel(plan, du, pre_gate, x, d_three, valid, w_pi, packed,
                     g_out, d_out, o_out, c_out, vec_out, w_o, v0, sem):
    fetch = Fetch(plan, packed, sem)
    copies = [fetch("b_o", v0), fetch("w_o", w_o)]
    yield
    d_gated = du[...] * valid[...]
    gate_sig = jax.nn.sigmoid(pre_gate[:, D:])
    d_linear = d_gated * gate_sig
    d_gate = d_gated * pre_gate[:, :D] * gate_sig * (1.0 - gate_sig)
    vec_out[0:1] = total_rows(d_linear)
    vec_out[1:2] = total_rows(d_gate)
    d_linear, d_gate = d_linear.astype(jnp.bfloat16), d_gate.astype(jnp.bfloat16)
    g_out[:, :D] = d_linear
    g_out[:, D:] = d_gate
    d_normed = back_dot(d_linear, w_pi[0]) + back_dot(d_gate, w_pi[1])
    unit, scale = unit_rows(x[...])
    wait_all(*copies)
    d_norm, gain_grad, shift_grad = unit_back(unit, scale, v0[...].astype(jnp.float32)[6:7], d_normed)
    vec_out[2:3] = gain_grad
    vec_out[3:4] = shift_grad
    grad = d_three[...] + d_norm
    d_out[...] = grad
    vec_out[4:5] = total_rows(grad)
    grad_b = grad.astype(jnp.bfloat16)
    o_out[...] = grad_b
    c_out[...] = back_dot(grad_b, w_o[...]).astype(jnp.bfloat16).reshape(c_out.shape)


def middle_kernel(plan, x, depth, sums, cot, valid, packed,
                  y_out, d_out, z_out, part_out, stat_out, e_out, rb_out, a_out, r_out, n_out, h_out, vec_out,
                  w_po, w_in, w_second, w_mix, held, v_bn, v0, v1, v2, bias, acc, mix, sem):
    fetch = Fetch(plan, packed, sem)
    early = [fetch("b_pi", v_bn), fetch("w_po", w_po), fetch("b_po", v0), fetch("second_b_in", v1)]
    early.append(fetch("second_b_out", v2))
    in_copy = fetch("second_w_in", w_in)
    late = fetch("second_w_out", w_second)
    yield
    wait_all(*early)
    base = plan.places["bng"] - plan.places["b_pi"]
    batch, head = v_bn[...].astype(jnp.float32), v0[...].astype(jnp.float32)
    bias_in, tail = v1[...].astype(jnp.float32), v2[...].astype(jnp.float32)
    gain, shift = batch[base : base + 1], batch[base + 1 : base + 2]
    count = sums[2:3]
    mean = sums[0:1] / count
    inv_std = lax.rsqrt(sums[1:2] / count - mean * mean + BATCH_EPS)
    stat_out[0:1] = mean
    stat_out[1:2] = inv_std
    stat_out[2:3] = count
    stat_out[3:4] = jnp.zeros((1, D), jnp.float32)
    standard = (depth[...] - mean) * inv_std
    e_out[...] = swish_act(standard * gain + shift).astype(jnp.bfloat16)
    three = x[...] + forward_dot(e_out[...], w_po[...]) + head[0:1]
    unit, scale = unit_rows(three)
    n_out[...] = (unit * head[1:2] + head[2:3]).astype(jnp.bfloat16)
    in_copy.wait()
    split_rows(w_in, mix, w_mix, FF // LANES)
    late.wait()
    bias[...] = bias_in
    acc[...] = jnp.zeros(acc.shape, jnp.float32)
    d_out[...] = three

    @pl.loop(0, FF // LANES)
    def _(j):
        cols = column(j)
        hidden = forward_dot(n_out[...], w_mix[j]) + bias[pl.ds(j, 1), :]
        held[j] = hidden
        active = swish_act(hidden).astype(jnp.bfloat16)
        a_out[:, cols] = active
        acc[...] += forward_dot(active, w_second[cols, :])

    three = d_out[...]
    four = three + 0.5 * (acc[...] + tail[0:1])
    last, last_scale = unit_rows(four)
    y_out[...] = last * tail[1:2] + tail[2:3]
    grad = cot[...] * valid[...]
    grad, gain_grad, shift_grad = unit_back(last, last_scale, tail[1:2], grad)
    vec_out[0:1] = gain_grad
    vec_out[1:2] = shift_grad
    half = 0.5 * grad
    vec_out[2:3] = total_rows(half)
    r_out[...] = half.astype(jnp.bfloat16)
    acc[...] = jnp.zeros(acc.shape, jnp.float32)
    z_out[...] = grad

    @pl.loop(0, FF // LANES)
    def _(j):
        cols = column(j)
        d_hidden = back_dot(r_out[...], w_second[cols, :]) * swish_grad(held[j])
        vec_out[pl.ds(8 + j, 1), :] = total_rows(d_hidden)
        d_hidden = d_hidden.astype(jnp.bfloat16)
        h_out[:, cols] = d_hidden
        acc[...] += back_dot(d_hidden, w_mix[j])

    unit, scale = unit_rows(d_out[...])
    d_norm, gain_grad, shift_grad = unit_back(unit, scale, head[1:2], acc[...])
    vec_out[3:4] = gain_grad
    vec_out[4:5] = shift_grad
    grad = z_out[...] + d_norm
    d_out[...] = grad
    vec_out[5:6] = total_rows(grad)
    rb_out[...] = grad.astype(jnp.bfloat16)
    standard = (depth[...] - mean) * inv_std
    d_active = back_dot(rb_out[...], w_po[...]) * swish_grad(standard * gain + shift)
    d_gain, d_shift = total_rows(d_active * standard), total_rows(d_active)
    vec_out[6:7] = d_gain
    vec_out[7:8] = d_shift
    vec_out[12:16] = jnp.zeros((4, D), jnp.float32)
    d_standard = d_active * gain * valid[...]
    z_out[...] = d_standard
    part_out[0:1] = total_rows(d_standard)
    part_out[1:2] = total_rows(d_standard * standard)
    part_out[2:4] = jnp.zeros((2, D), jnp.float32)


def everyone(plan):
    di, z = lax.axis_index(DP), lax.axis_index(SEQ)
    other = di + 1 - 2 * (di % 2)
    peers = [(lax.rem(di + i, plan.ndp), z) for i in range(1, plan.ndp)]
    for i in range(1, plan.nseq):
        to = lax.rem(z + i, plan.nseq)
        peers += [(di, to), (other, to)]
    barrier = pltpu.get_barrier_semaphore()
    for peer in peers:
        pl.semaphore_signal(barrier, inc=1, device_id=peer, device_id_type=MESH)
    return lambda: pl.semaphore_wait(barrier, len(peers))


def exchange_sum(ndp, nseq, part, line, cross, sems):
    di, z = lax.axis_index(DP), lax.axis_index(SEQ)

    def phase(count, me, target, slots, send, recv):
        copies = []
        for i in range(1, count):
            copy = pltpu.make_async_remote_copy(
                src_ref=part, dst_ref=slots.at[me], send_sem=send.at[i], recv_sem=recv.at[me],
                device_id=target(lax.rem(me + i, count)), device_id_type=MESH,
            )
            copy.start()
            copies.append(copy)
        slots[me] = part[...]
        for i in range(1, count):
            source = lax.rem(me + count - i, count)
            pltpu.make_async_remote_copy(
                src_ref=part, dst_ref=slots.at[source], send_sem=send.at[i], recv_sem=recv.at[source],
                device_id=(di, z), device_id_type=MESH,
            ).wait_recv()
        for copy in copies:
            copy.wait_send()
        total = slots[0]
        for i in range(1, count):
            total = total + slots[i]
        return total

    part[...] = phase(nseq, z, lambda i: (di, i), line, sems[0], sems[1])
    return phase(ndp, di, lambda i: (i, z), cross, sems[2], sems[3])


HALO = 16


class Halo:
    def __init__(self, nseq, buffer, sem):
        di, z = lax.axis_index(DP), lax.axis_index(SEQ)
        rows = buffer.shape[1]
        self.has = (z > 0, z < nseq - 1)

        def copy(source, target, number, to):
            return pltpu.make_async_remote_copy(
                src_ref=buffer.at[:, pl.ds(source, HALO)], dst_ref=buffer.at[:, pl.ds(target, HALO)],
                send_sem=sem.at[number], recv_sem=sem.at[2 + number], device_id=(di, to), device_id_type=MESH,
            )

        self.up = copy(rows - 2 * HALO, 0, 0, lax.rem(z + 1, nseq))
        self.down = copy(HALO, rows - HALO, 1, lax.rem(z + nseq - 1, nseq))
        self.buffer, self.rows = buffer, rows

    def start(self):
        @pl.when(self.has[1])
        def _():
            self.up.start()

        @pl.when(self.has[0])
        def _():
            self.down.start()

    def finish(self):
        empty = jnp.zeros((self.buffer.shape[0], HALO, self.buffer.shape[2]), jnp.float32)

        @pl.when(self.has[0])
        def _():
            self.up.wait_recv()
            self.down.wait_send()

        @pl.when(jnp.logical_not(self.has[0]))
        def _():
            self.buffer[:, :HALO] = empty

        @pl.when(self.has[1])
        def _():
            self.down.wait_recv()
            self.up.wait_send()

        @pl.when(jnp.logical_not(self.has[1]))
        def _():
            self.buffer[:, self.rows - HALO :] = empty


def slide(padded, taps, index, out, length):
    lanes = LANES // 128

    @pl.loop(0, padded.shape[0] * lanes)
    def _(i):
        s, lane = i // lanes, pl.ds(pl.multiple_of(i % lanes * 128, 128), 128)
        total = jnp.zeros((length, 128), jnp.float32)
        for b in range(8):
            part = None
            for a in range(4):
                if 0 < 8 * a + b < K + 1:
                    row = index(8 * a + b)
                    term = taps[row : row + 1, lane] * padded[s, 8 * a : 8 * a + length + 8, lane]
                    part = term if part is None else part + term
            total = total + part[b : b + length]
        out[pl.ds(pl.multiple_of(s * length, length), length), lane] = total


def depth_kernel(plan, u, valid, packed, c_out, sum_out, padded, taps, taps_b, part, line, cross, sem,
                 halo_sem, *sems):
    ndp, nseq = plan.ndp, plan.nseq
    length = padded.shape[1] - 2 * HALO
    copy = Fetch(plan, packed, sem)("b_pi", taps_b)
    yield
    padded[:, HALO : HALO + length] = u[...].reshape(-1, length, D)
    halo = Halo(nseq, padded, halo_sem)
    halo.start()
    copy.wait()
    taps[...] = taps_b[...].astype(jnp.float32)
    halo.finish()
    base = plan.places["w_depth"] - plan.places["b_pi"]
    slide(padded, taps, lambda i: base + i - 1, c_out, length)
    depth, mask = c_out[...], valid[...]
    value = depth * mask
    part[0:1] = total_rows(value)
    part[1:2] = total_rows(value * depth)
    part[2:3] = jnp.broadcast_to(total_rows(mask), (1, LANES))
    part[3:4] = jnp.zeros((1, LANES), jnp.float32)
    sum_out[...] = exchange_sum(ndp, nseq, part, line, cross, sems)


def depth_back_kernel(plan, dz, depth, stats, local, valid, u_pad, packed, u_out, tap_out,
                      padded, own, taps, taps_b, part, line, cross, sem, halo_sem, *sems):
    ndp, nseq = plan.ndp, plan.nseq
    seqs, length = padded.shape[0], padded.shape[1] - 2 * HALO
    copy = Fetch(plan, packed, sem)("b_pi", taps_b)
    yield
    part[...] = local[...]
    sums = exchange_sum(ndp, nseq, part, line, cross, sems)
    mean, inv_std, count = stats[0:1], stats[1:2], stats[2:3]
    standard = (depth[...] - mean) * inv_std
    d_depth = valid[...] * inv_std * (dz[...] - sums[0:1] / count - standard * (sums[1:2] / count))
    d_depth = d_depth.reshape(seqs, length, D)
    padded[:, HALO : HALO + length] = d_depth
    halo = Halo(nseq, padded, halo_sem)
    halo.start()
    own[:, :8] = jnp.zeros((seqs, 8, D), jnp.float32)
    own[:, 8 : 8 + length] = d_depth
    own[:, 8 + length :] = jnp.zeros((seqs, 8, D), jnp.float32)
    copy.wait()
    taps[...] = taps_b[...].astype(jnp.float32)
    base = plan.places["w_depth"] - plan.places["b_pi"]

    @pl.loop(0, LANES // 128)
    def _(i):
        lane = pl.ds(pl.multiple_of(i * 128, 128), 128)
        for b in range(8):
            sums_b = [None] * 4
            for s in range(seqs):
                moved = own[s, 8 - b : 8 - b + length + 8, lane]
                for a in range(4):
                    if 0 < 8 * a + b < K + 1:
                        term = total_rows(u_pad[s, 8 * a : 8 * a + length + 8, lane] * moved)
                        sums_b[a] = term if sums_b[a] is None else sums_b[a] + term
            for a in range(4):
                if sums_b[a] is not None:
                    tap_out[8 * a + b - 1 : 8 * a + b, lane] = sums_b[a]
        tap_out[K : K + 1, lane] = jnp.zeros((1, 128), jnp.float32)

    halo.finish()
    slide(padded, taps, lambda i: base + K - i, u_out, length)


def head_scores(q, k, line, valid):
    block, full, width = q.shape[0], k.shape[0], line.shape[1]
    scores = lax.dot_general(q, k, (((1,), (1,)), ((), ())), preferred_element_type=jnp.float32)
    spread = jnp.broadcast_to(line, (block, width))
    bias = pltpu.roll(spread, width - block + 1, 1, stride=1, stride_axis=0)[:, :full]
    return jnp.where(valid, scores + bias, -jnp.inf)


def remote(source, target, send, recv, device):
    return pltpu.make_async_remote_copy(
        src_ref=source, dst_ref=target, send_sem=send, recv_sem=recv, device_id=device, device_id_type=MESH
    )


class Team:
    def __init__(self, plan, seqs):
        self.di, self.z = lax.axis_index(DP), lax.axis_index(SEQ)
        self.count, self.seqs = plan.nseq, seqs
        self.c = self.di % 2
        self.base = self.di - self.c
        self.other = self.base + 1 - self.c
        self.owner = self.base + self.z // seqs
        self.main = self.z // seqs == self.c
        self.slot = self.z % seqs
        self.half = pl.ds(pl.multiple_of(self.c * (D // 2), D // 2), D // 2)

    def turn(self, i):
        return lax.rem(self.z + i, self.count)


def half_copy(packed, plan, name, team, target, sem):
    copy = pltpu.make_async_copy(packed.at[pl.ds(plan.places[name], D), team.half], target, sem)
    copy.start()
    return copy


def attend_kernel(plan, normed, lengths, tables, packed, ctx_out, all_out, q_out, k_out, v_out, lse_out, len_out,
                  w_q, w_k, w_v, b_q, b_v, held, mine, sem, in_send, relay_send, in_recv, ctx_send, ctx_recv, len_sem):
    seqs, block, _ = normed.shape
    count = plan.nseq
    team = Team(plan, seqs)
    fetch = Fetch(plan, packed, sem)
    copies = [fetch("b_q", b_q), fetch("b_v", b_v)]
    for i, (name, target) in enumerate((("w_q", w_q), ("w_k", w_k), ("w_v", w_v))):
        copies.append(half_copy(packed, plan, name, team, target, sem.at[2 + i]))
    yield
    c, z = team.c, team.z
    sends = []
    for s in range(seqs):
        to = c * seqs + s
        copy = remote(normed.at[s], all_out.at[z], in_send.at[s], in_recv.at[z], (team.di, to))
        sends.append((to != z, copy))
        pl.when(to != z)(copy.start)
    relays = []
    for i in range(count):
        b = team.turn(i)
        source = normed.at[team.slot] if i == 0 else all_out.at[b]
        relays.append(remote(source, all_out.at[b], relay_send.at[b], in_recv.at[b], (team.other, z)))
    pl.when(team.main)(relays[0].start)
    note = remote(lengths, len_out, len_sem.at[0], len_sem.at[1], (team.other, z))
    pl.when(team.main)(note.start)

    @pl.when(team.main)
    def _():
        all_out[z] = normed[team.slot]
        len_out[...] = lengths[...]

    wait_all(*copies)
    mine[0] = b_q[...].astype(jnp.float32)
    mine[1] = b_v[...].astype(jnp.float32)
    bias_q, bias_v = mine[0, 0:1, team.half], mine[1, 0:1, team.half]
    for i in range(count):
        b = team.turn(i)
        if i == 0:
            pl.when(jnp.logical_not(team.main))(relays[0].wait_recv)
        else:
            relays[i].wait_recv()
            pl.when(team.main)(relays[i].start)
        part = all_out[b]
        at = pl.ds(pl.multiple_of(b * block, block), block)
        query = (forward_dot(part, w_q[...]) + bias_q).astype(jnp.bfloat16).astype(jnp.float32)
        q_out[at, :] = (query * (1.0 / math.sqrt(HD))).astype(jnp.bfloat16)
        k_out[at, :] = forward_dot(part, w_k[...]).astype(jnp.bfloat16)
        v_out[at, :] = (forward_dot(part, w_v[...]) + bias_v).astype(jnp.bfloat16)
    full = count * block
    pl.when(jnp.logical_not(team.main))(note.wait_recv)
    valid = lax.broadcasted_iota(jnp.int32, (1, full), 1) < len_out[pl.ds(team.slot, 1), :][:, 0:1]
    lane = lax.broadcasted_iota(jnp.int32, (block, 128), 1)

    def back(b):
        return remote(held.at[b], ctx_out.at[team.slot, :, team.half], ctx_send.at[b],
                      ctx_recv.at[team.slot * 2 + c], (team.owner, b))

    @pl.loop(0, count)
    def _(i):
        b = lax.rem(z + 1 + i, count)
        at = pl.ds(pl.multiple_of(b * block, block), block)
        lse_out[at, :] = jnp.zeros((block, 128), jnp.float32)

        @pl.loop(0, H // 4)
        def _(pair):
            lanes = pl.ds(pl.multiple_of(pair * 128, 128), 128)
            both = []
            for part in range(2):
                h, cols = 2 * pair + part, slice(part * HD, (part + 1) * HD)
                line = tables[b, pl.ds(c * (H // 2) + h, 1), :]
                scores = head_scores(q_out[at, lanes][:, cols], k_out[:, lanes][:, cols], line, valid)
                top = jnp.max(scores, -1, keepdims=True)
                weights = jnp.exp(scores - top)
                total = jnp.sum(weights, -1, keepdims=True)
                probs = (weights * (1.0 / total)).astype(jnp.bfloat16)
                both.append(jnp.dot(probs, v_out[:, lanes][:, cols], preferred_element_type=jnp.float32))
                lse_out[at, :] = jnp.where(lane == h, top + jnp.log(total), lse_out[at, :])
            held[b, :, lanes] = jnp.concatenate(both, 1).astype(jnp.bfloat16)

        own = jnp.logical_and(b == z, team.main)

        @pl.when(own)
        def _():
            ctx_out[team.slot, :, team.half] = held[b]

        @pl.when(jnp.logical_not(own))
        def _():
            back(b).start()

    for s in range(seqs):
        for h in range(2):
            own = jnp.logical_and(c * seqs + s == z, c == h)
            here = ctx_out.at[s, :, pl.ds(h * (D // 2), D // 2)]
            copy = remote(held.at[0], here, ctx_send.at[0], ctx_recv.at[s * 2 + h], (team.di, z))
            pl.when(jnp.logical_not(own))(copy.wait_recv)
    pl.when(team.main)(note.wait_send)
    for flag, copy in sends:
        pl.when(flag)(copy.wait_send)
    for i in range(count):
        pl.when(team.main)(relays[i].wait_send)
        b = team.turn(i)
        own = jnp.logical_and(b == z, team.main)
        pl.when(jnp.logical_not(own))(back(b).wait_send)


def attend_back_kernel(plan, d_ctx, q_all, k_all, v_all, lse_all, length, tables, packed,
                       dn_out, dq_out, dk_out, dv_out, dt_out, vec_out,
                       w_q, w_k, w_v, d_in, dq_part, dk_sum, dv_sum, give, take, final, sem,
                       in_send, in_recv, swap_send, swap_recv, dn_send, dn_recv):
    seqs, block, _ = d_ctx.shape
    count = plan.nseq
    full = count * block
    team = Team(plan, seqs)
    copies = []
    for i, (name, target) in enumerate((("w_q", w_q), ("w_k", w_k), ("w_v", w_v))):
        copies.append(half_copy(packed, plan, name, team, target, sem.at[i]))
    yield
    c, z = team.c, team.z
    sends = []
    for s in range(seqs):
        for h in range(2):
            to = c * seqs + s
            own = jnp.logical_and(to == z, c == h)
            source = d_ctx.at[s, :, pl.ds(h * (D // 2), D // 2)]
            copy = remote(source, d_in.at[z], in_send.at[2 * s + h], in_recv.at[z], (team.base + h, to))
            sends.append((jnp.logical_not(own), copy))
            pl.when(jnp.logical_not(own))(copy.start)

    @pl.when(team.main)
    def _():
        d_in[z] = d_ctx[team.slot, :, team.half]

    dk_sum[...] = jnp.zeros(dk_sum.shape, jnp.float32)
    dv_sum[...] = jnp.zeros(dv_sum.shape, jnp.float32)
    dt_out[...] = jnp.zeros(dt_out.shape, jnp.float32)
    vec_out[...] = jnp.zeros(vec_out.shape, jnp.float32)
    away = pl.ds(pl.multiple_of((1 - c) * (D // 2), D // 2), D // 2)
    for out in (dq_out, dk_out, dv_out):
        out[:, away] = jnp.zeros((full, D // 2), jnp.bfloat16)
    valid = lax.broadcasted_iota(jnp.int32, (1, full), 1) < length[pl.ds(team.slot, 1), :][:, 0:1]
    rows = (((0,), (0,)), ((), ()))
    inv = 1.0 / math.sqrt(HD)
    lane = lax.broadcasted_iota(jnp.int32, (block, 128), 1)

    @pl.loop(0, count)
    def _(i):
        b = lax.rem(z + i, count)
        own = jnp.logical_and(b == z, team.main)
        copy = remote(d_in.at[b], d_in.at[b], in_send.at[0], in_recv.at[b], (team.di, z))
        pl.when(jnp.logical_not(own))(copy.wait_recv)
        at = pl.ds(pl.multiple_of(b * block, block), block)

        @pl.loop(0, H // 4)
        def _(pair):
            lanes = pl.ds(pl.multiple_of(pair * 128, 128), 128)
            parts = []
            for part in range(2):
                h, cols = 2 * pair + part, slice(part * HD, (part + 1) * HD)
                q, k, v = q_all[at, lanes][:, cols], k_all[:, lanes][:, cols], v_all[:, lanes][:, cols]
                dctx = d_in[b, :, lanes][:, cols]
                line = tables[b, pl.ds(c * (H // 2) + h, 1), :]
                width = line.shape[1]
                lse = jnp.sum(jnp.where(lane == h, lse_all[at, :], 0.0), -1, keepdims=True)
                probs = jnp.exp(head_scores(q, k, line, valid) - lse)
                d_probs = lax.dot_general(
                    dctx, v, (((1,), (1,)), ((), ())), preferred_element_type=jnp.float32
                )
                delta = jnp.sum(probs * d_probs, -1, keepdims=True)
                d_scores = probs * (d_probs - delta)
                d_scores_b = d_scores.astype(jnp.bfloat16)
                parts.append((
                    jnp.dot(d_scores_b, k, preferred_element_type=jnp.float32) * inv,
                    lax.dot_general(d_scores_b, q, rows, preferred_element_type=jnp.float32),
                    lax.dot_general(probs.astype(jnp.bfloat16), dctx, rows, preferred_element_type=jnp.float32),
                ))
                wide = jnp.concatenate([d_scores, jnp.zeros((block, width - full), jnp.float32)], 1)
                folded = pltpu.roll(wide[0:8], block - 1, 1)
                for g in range(1, block // 8):
                    folded = folded + pltpu.roll(wide[8 * g : 8 * g + 8], block - 1 - 8 * g, 1)
                line = folded[0:1]
                for r in range(1, 8):
                    line = line + pltpu.roll(folded[r : r + 1], width - r, 1)
                dt_out[b, pl.ds(c * (H // 2) + h, 1), :] = line
            dq, dk, dv = [jnp.concatenate(values, 1) for values in zip(*parts)]
            dq_part[at, lanes] = dq.astype(jnp.bfloat16)
            dk_sum[:, lanes] += dk
            dv_sum[:, lanes] += dv
            mine = pl.ds(pl.multiple_of(c * (D // 2) + pair * 128, 128), 128)
            vec_out[0:1, mine] += total_rows(dq)

    vec_out[1:2, team.half] = total_rows(dv_sum[...])
    dk_part = dk_sum[...].astype(jnp.bfloat16)
    dk_out[:, team.half] = dk_part
    dv_part = dv_sum[...].astype(jnp.bfloat16)
    dv_out[:, team.half] = dv_part
    dq_out[:, team.half] = dq_part[...]
    wait_all(*copies)

    def partial(b):
        at = pl.ds(pl.multiple_of(b * block, block), block)
        dk_rows, dv_rows = dk_out[at, team.half], dv_out[at, team.half]
        return back_dot(dq_part[at, :], w_q[...]) + back_dot(dk_rows, w_k[...]) + back_dot(dv_rows, w_v[...])

    share = count // 2
    swaps, ends = [], []
    for i in range(share):
        give[i] = partial((1 - c) * share + i).astype(jnp.bfloat16)
        copy = remote(give.at[i], take.at[i], swap_send.at[i], swap_recv.at[i], (team.other, z))
        copy.start()
        swaps.append(copy)
    for i in range(share):
        b = c * share + i
        value = partial(b)
        swaps[i].wait_recv()
        value = (value + take[i].astype(jnp.float32)).astype(jnp.bfloat16)
        final[i] = value
        own = jnp.logical_and(b == z, team.main)
        copy = remote(final.at[i], dn_out.at[team.slot], dn_send.at[i], dn_recv.at[team.slot], (team.owner, b))
        ends.append((jnp.logical_not(own), copy))
        pl.when(jnp.logical_not(own))(copy.start)

        @pl.when(own)
        def _():
            dn_out[team.slot] = final[i]

    for s in range(seqs):
        own = jnp.logical_and(c * seqs + s == z, z // share == c)
        copy = remote(final.at[0], dn_out.at[s], dn_send.at[0], dn_recv.at[s], (team.di, z))
        pl.when(jnp.logical_not(own))(copy.wait_recv)
    for copy in swaps:
        copy.wait_send()
    for flag, copy in sends + ends:
        pl.when(flag)(copy.wait_send)


VMEM_SPEC = pl.BlockSpec(memory_space=pltpu.VMEM)
ANY_SPEC = pl.BlockSpec(memory_space=pl.ANY)


def run_all(ready, runs, first):
    for run in runs:
        next(run)
    for number, run in enumerate(runs):
        if number == first:
            ready()
        for _ in run:
            pass


def forward_kernel(plan, r):
    ready = everyone(plan)
    runs = [
        ffn_first_kernel(plan, r.x, r.packed, r.x1, r.n2, r.w_first, r.w_in, r.w_second, r.g0, r.g1, r.g2, r.bias,
                         r.acc, r.one, r.mix, r.sem0),
        attend_kernel(plan, r.n2, r.lengths, r.tables, r.packed, r.ctx, r.owned, r.q, r.k, r.v, r.lse, r.length,
                      r.w_q, r.w_k, r.w_v, r.g3, r.g4, r.held, r.mine, r.sem1, r.sem2, r.sem3, r.sem4, r.sem5, r.sem6,
                      r.sem7),
        gate_kernel(plan, r.ctx, r.x1, r.valid, r.packed, r.x2, r.n3, r.gates, r.u, r.w_gate, r.w_o, r.w_pi,
                    r.g5, r.g6, r.mix, r.sem8),
        depth_kernel(plan, r.u, r.valid, r.packed, r.depth, r.sums, r.padded, r.taps, r.taps_b, r.part, r.line,
                     r.cross, r.sem9, r.sem10, r.sem11, r.sem12, r.sem13, r.sem14),
    ]
    run_all(ready, runs, 1)


def backward_kernel(plan, r):
    ready = everyone(plan)
    runs = [
        middle_kernel(plan, r.x2, r.depth, r.sums, r.cot, r.valid, r.packed, r.y, r.d3, r.dz, r.local, r.stats, r.e3,
                      r.r3, r.a4, r.h4, r.n4, r.dh4, r.vec_mid, r.w_po, r.w_in, r.w_second, r.w_mix, r.hid, r.g0,
                      r.g1, r.g2, r.g3, r.bias, r.acc, r.mix, r.sem0),
        depth_back_kernel(plan, r.dz, r.depth, r.stats, r.local, r.valid, r.padded, r.packed, r.du, r.tap, r.wide,
                          r.own, r.taps, r.taps_b, r.part, r.line, r.cross, r.sem1, r.sem2, r.sem3, r.sem4, r.sem5,
                          r.sem6),
        gate_back_kernel(plan, r.du, r.gates, r.x2, r.d3, r.valid, r.w_gate, r.packed, r.dg, r.d2, r.r2, r.dctx,
                         r.vec_gate, r.w_o, r.g4, r.sem7),
        attend_back_kernel(plan, r.dctx, r.q, r.k, r.v, r.lse, r.length, r.tables, r.packed, r.dn, r.dq, r.dk, r.dv,
                           r.dt, r.vec_att, r.w_q, r.w_k, r.w_v, r.d_in, r.dq_part, r.dk_sum, r.dv_sum, r.give, r.take,
                           r.final, r.sem8, r.sem9, r.sem10, r.sem11, r.sem12, r.sem13, r.sem14),
        ffn_first_back_kernel(plan, r.x, r.x1, r.d2, r.dn, r.w_first, r.packed, r.d0, r.a1, r.h1, r.n1, r.dh1,
                              r.vec_first, r.w_tall, r.g5, r.g6, r.g7, r.bias, r.acc, r.sem15),
    ]
    run_all(ready, runs, 1)


def stage(kernel, plan, operands, packed, outs, scratch, name, number):
    keys = list(operands) + ["packed"] + list(outs) + list(scratch)
    results = pl.pallas_call(
        lambda *refs: kernel(plan, types.SimpleNamespace(**dict(zip(keys, refs)))),
        out_shape=[jax.ShapeDtypeStruct(shape, dtype) for shape, dtype in outs.values()],
        in_specs=[VMEM_SPEC] * len(operands) + [ANY_SPEC],
        out_specs=[VMEM_SPEC] * len(outs),
        scratch_shapes=list(scratch.values()),
        compiler_params=pltpu.CompilerParams(
            vmem_limit_bytes=67043328, collective_id=number, has_side_effects=True
        ),
        name=name,
    )(*operands.values(), packed)
    return types.SimpleNamespace(**dict(zip(outs, results)))


F32, BF16 = jnp.float32, jnp.bfloat16
DMA = pltpu.SemaphoreType.DMA


def vm(shape, dtype=jnp.bfloat16):
    return pltpu.VMEM(shape, dtype)


def per_device(inputs, lengths, rel_bucket, params, moment_one, moment_two, cotangent):
    seq_count, block_len, model_width = inputs.shape
    rows = seq_count * block_len
    first_pos = lax.axis_index(SEQ) * block_len
    positions = first_pos + jnp.arange(block_len, dtype=jnp.int32)
    valid_own = positions[None, :] < lengths[:, None]
    valid = valid_own.astype(jnp.float32).reshape(-1, 1)
    onehot = bucket_windows(rel_bucket, block_len, lax.axis_size(SEQ))
    assert 2 * seq_count == lax.axis_size(SEQ)
    length = jnp.broadcast_to(jnp.pad(lengths, (0, 8 - seq_count))[:, None], (8, 128))
    plan = Plan(lax.axis_size(DP), lax.axis_size(SEQ), params.shape[0])
    packed = gather(plan, params).reshape(-1, LANES)
    full, wide, nseq = (rows, D), (rows, FF), plan.nseq
    square, tall, group = vm((D, D)), vm((FF, D)), vm((8, D))
    mix, taps, taps_b = vm((LANES // 128, 256, 128), F32), vm((40, D), F32), vm((40, D))
    half, sums = vm((D, D // 2)), ((4, D), F32)
    long, whole = nseq * block_len, (nseq * block_len, D)
    local3, split = (seq_count, block_len, D), (nseq, block_len, D // 2)
    padded = (seq_count, block_len + 2 * HALO, D)
    few = vm((nseq // 2, block_len, D))
    x = inputs.reshape(full)
    table_row = plan.places["rel"]
    rel = packed[table_row : table_row + 1, : NB * H].reshape(NB, H)
    tables = jnp.einsum("nh,bnw->bhw", rel, onehot.astype(BF16), preferred_element_type=F32)
    f = stage(
        forward_kernel, plan, dict(x=x, valid=valid, lengths=length, tables=tables), packed,
        dict(x1=(full, F32), w_first=((FF // D, D, D), BF16), ctx=(local3, BF16), owned=((nseq, block_len, D), BF16),
             q=((long, D // 2), BF16), k=((long, D // 2), BF16), v=((long, D // 2), BF16), lse=((long, 128), F32),
             length=((8, 128), jnp.int32), x2=(full, F32), n3=(full, BF16), gates=((rows, 2 * D), F32),
             w_gate=((2, D, D), BF16), depth=(full, F32), sums=sums, padded=(padded, F32)),
        dict(n2=vm(local3), w_in=tall, w_second=tall, g0=group, g1=group, g2=group, g3=group, g4=group, g5=group,
             g6=group, bias=vm((8, D), F32), acc=vm(full, F32), one=vm(full), mix=mix, w_q=half, w_k=half, w_v=half,
             held=vm(split), mine=vm((2, 8, D), F32), u=vm(full, F32), w_o=square, w_pi=vm((2 * D, D)), taps=taps,
             taps_b=taps_b, part=vm(*sums), line=vm((nseq, 4, D), F32), cross=vm((plan.ndp, 4, D), F32),
             sem0=DMA((5,)), sem1=DMA((5,)), sem2=DMA((seq_count,)), sem3=DMA((nseq,)), sem4=DMA((nseq,)),
             sem5=DMA((nseq,)), sem6=DMA((2 * seq_count,)), sem7=DMA((2,)), sem8=DMA((4,)), sem9=DMA((1,)),
             sem10=DMA((4,)), sem11=DMA((nseq,)), sem12=DMA((nseq,)), sem13=DMA((plan.ndp,)),
             sem14=DMA((plan.ndp,))), "forward", 2,
    )
    b = stage(
        backward_kernel, plan,
        dict(x=x, valid=valid, cot=cotangent.reshape(full), tables=tables, x1=f.x1, x2=f.x2, depth=f.depth,
             sums=f.sums, padded=f.padded, gates=f.gates, w_gate=f.w_gate, q=f.q, k=f.k, v=f.v, lse=f.lse,
             length=f.length, w_first=f.w_first), packed,
        dict(y=(full, F32), d0=(full, F32), e3=(full, BF16), r3=(full, BF16), a4=(wide, BF16), h4=(full, BF16),
             n4=(full, BF16), dh4=(wide, BF16), vec_mid=((16, D), F32), tap=((32, D), F32), dg=((rows, 2 * D), BF16),
             r2=(full, BF16), vec_gate=((8, D), F32), dq=(whole, BF16), dk=(whole, BF16), dv=(whole, BF16),
             dt=(tables.shape, F32), vec_att=((8, D), F32), a1=(wide, BF16), h1=(full, BF16), n1=(full, BF16),
             dh1=(wide, BF16), vec_first=((16, D), F32)),
        dict(d3=vm(full, F32), dz=vm(full, F32), local=vm(*sums), stats=vm(*sums), w_po=square, w_in=tall,
             w_second=tall, w_mix=vm((FF // D, D, D)), hid=vm((FF // D, rows, D), F32), g0=vm((40, D)), g1=group,
             g2=group, g3=group, g4=group, g5=group, g6=group, g7=group, bias=vm((8, D), F32), acc=vm(full, F32),
             mix=mix, du=vm(full, F32), wide=vm(padded, F32), own=vm((seq_count, block_len + 16, D), F32), taps=taps,
             taps_b=taps_b, part=vm(*sums), line=vm((nseq, 4, D), F32), cross=vm((plan.ndp, 4, D), F32),
             d2=vm(full, F32), dctx=vm(local3), w_o=square, dn=vm(local3), w_q=half, w_k=half, w_v=half,
             d_in=vm(split), dq_part=vm((long, D // 2)), dk_sum=vm((long, D // 2), F32),
             dv_sum=vm((long, D // 2), F32), give=few, take=few, final=few, w_tall=tall, sem0=DMA((7,)),
             sem1=DMA((1,)), sem2=DMA((4,)), sem3=DMA((nseq,)), sem4=DMA((nseq,)), sem5=DMA((plan.ndp,)),
             sem6=DMA((plan.ndp,)), sem7=DMA((2,)), sem8=DMA((3,)), sem9=DMA((2 * seq_count,)), sem10=DMA((nseq,)),
             sem11=DMA((nseq // 2,)), sem12=DMA((nseq // 2,)), sem13=DMA((nseq // 2,)), sem14=DMA((seq_count,)),
             sem15=DMA((4,))), "backward", 3,
    )
    rel_grad = jnp.einsum("bnw,bhw->nh", onehot, b.dt, precision=lax.Precision.HIGHEST).reshape(1, -1)
    owned = f.owned.reshape(whole)
    gradients = {
        "w_k": (owned, b.dk), "w_v": (owned, b.dv), "w_q": (owned, b.dq), "second_w_in": (b.n4, b.dh4),
        "second_w_out": (b.a4, b.h4), "w_pi": (f.n3, b.dg), "w_po": (b.e3, b.r3), "w_o": (f.ctx.reshape(full), b.r2),
        "first_w_in": (b.n1, b.dh1), "first_w_out": (b.a1, b.h1),
    }
    places = {
        "attn_ng": (0, 0), "attn_nb": (0, 1), "first_b_out": (0, 2), "first_ng": (0, 3), "first_nb": (0, 4),
        "first_b_in": (0, 5), "b_pi": (1, 0), "conv_ng": (1, 2), "conv_nb": (1, 3), "b_o": (1, 4),
        "fin_g": (2, 0), "fin_b": (2, 1), "second_b_out": (2, 2), "second_ng": (2, 3), "second_nb": (2, 4),
        "b_po": (2, 5), "bng": (2, 6), "bnb": (2, 7), "second_b_in": (2, 8), "w_depth": (3, 0),
        "b_q": (4, 0), "b_v": (4, 1), "rel": (5, 0),
    }
    vectors = [b.vec_first, b.vec_gate, b.vec_mid, b.tap, b.vec_att, rel_grad]
    window = scatter(plan, weight_grads(plan, gradients, vectors, places))
    grad_shard = own_shard(plan, window)
    new_params, new_first, new_second = adam_update(params, grad_shard, moment_one, moment_two)
    return (
        b.y.reshape(inputs.shape),
        b.d0.reshape(inputs.shape),
        grad_shard,
        new_params,
        new_first,
        new_second,
    )


def solution(mesh):
    return jax.shard_map(
        per_device,
        mesh=mesh,
        in_specs=(
            P(DP, SEQ, None),
            P(DP),
            P(),
            P((DP, SEQ)),
            P((DP, SEQ)),
            P((DP, SEQ)),
            P(DP, SEQ, None),
        ),
        out_specs=(
            P(DP, SEQ, None),
            P(DP, SEQ, None),
            P((DP, SEQ)),
            P((DP, SEQ)),
            P((DP, SEQ)),
            P((DP, SEQ)),
        ),
        check_vma=False,
    )
```
